32 devices in a mesh: dp: 8 (over z, x), mp: 4 (over y, core).
Axes of the slice: x: 2, y: 2, z: 4, core: 2. Of those that a mesh axis runs over, the one named last changes fastest.
Arguments:
- tokens: bfloat16 [16384, 1024], P(('dp', 'mp')), may hold values from -6 to 6
- lengths: int32 [8, 1], P('dp'), may hold values from 30 to 2048, as said below
- query_weight: bfloat16 [1024, 1024], P(None, 'mp'), may hold values from -0.25 to 0.25
- query_bias: bfloat16 [1024], P('mp'), may hold values from -3 to 3
- key_weight: bfloat16 [1024, 1024], P(None, 'mp'), may hold values from -0.25 to 0.25
- value_weight: bfloat16 [1024, 1024], P(None, 'mp'), may hold values from -0.1875 to 0.1875
- value_bias: bfloat16 [1024], P('mp'), may hold values from -3 to 3
- out_weight: bfloat16 [1024, 1024], P('mp'), may hold values from -0.75 to 0.75
- out_bias: bfloat16 [1024], replicated, may hold values from -3 to 3
- first_gain: bfloat16 [1024], replicated, may hold values from 0.25 to 1.75
- first_shift: bfloat16 [1024], replicated, may hold values from -3 to 3
- up_weight: bfloat16 [1024, 4096], P(None, 'mp'), may hold values from -0.1875 to 0.1875
- up_bias: bfloat16 [4096], P('mp'), may hold values from -3 to 3
- down_weight: bfloat16 [4096, 1024], P('mp'), may hold values from -0.09375 to 0.09375
- down_bias: bfloat16 [1024], replicated, may hold values from -3 to 3
- second_gain: bfloat16 [1024], replicated, may hold values from 0.25 to 1.75
- second_shift: bfloat16 [1024], replicated, may hold values from -3 to 3
- output_grad: bfloat16 [16384, 1024], P(('dp', 'mp')), may hold values from -6 to 6
Outputs:
- layer_out: bfloat16 [16384, 1024], P(('dp', 'mp'))
- tokens_grad: bfloat16 [16384, 1024], P(('dp', 'mp'))
- query_weight_grad: float32 [1024, 1024], P(None, 'mp')
- query_bias_grad: float32 [1024], P('mp')
- key_weight_grad: float32 [1024, 1024], P(None, 'mp')
- value_weight_grad: float32 [1024, 1024], P(None, 'mp')
- value_bias_grad: float32 [1024], P('mp')
- out_weight_grad: float32 [1024, 1024], P('mp')
- out_bias_grad: float32 [1024], replicated
- first_gain_grad: float32 [1024], replicated
- first_shift_grad: float32 [1024], replicated
- up_weight_grad: float32 [1024, 4096], P(None, 'mp')
- up_bias_grad: float32 [4096], P('mp')
- down_weight_grad: float32 [4096, 1024], P('mp')
- down_bias_grad: float32 [1024], replicated
- second_gain_grad: float32 [1024], replicated
- second_shift_grad: float32 [1024], replicated
The draws below stay inside these ranges and needn't reach their ends.
Inputs may be any that keep to these rules, and one draw needn't show every extreme that they name: Batch b holds 1 sequence of 2048 rows; sequence s counts its first lengths[b, s] rows as keys; in every draw some sequence has exactly 2048.
All inputs are finite; a program needn't handle non-finite values.
Results may differ from the reference program's by a relative error of at most 0.023.
Values may be sent and summed in bfloat16 or wider, within the bound.
A program may use at most 320 MiB of HBM per device.

```python
from functools import partial
import jax
import jax.numpy as jnp
from jax import lax

D = 1024
H = 16
FF = 4096
HD = 64
L = 2048
SEQS = 1
BATCHES = 8
TOKENS = 16384


def draw_lengths(key, part):
    first_key, second_key = jax.random.split(key, 2)
    drawn = jax.random.randint(first_key, (BATCHES * SEQS,), 30, L + 1)
    chosen = jax.random.randint(second_key, (), 0, BATCHES * SEQS)
    drawn = jnp.where(jnp.arange(BATCHES * SEQS) == chosen, L, drawn)
    return drawn.reshape(BATCHES, SEQS).astype(jnp.int32)


def level_of(own_key, dims, cuts, least, largest):
    loudness = 1.0
    for axis_at, shards_of in cuts:
        draws = jax.random.uniform(jax.random.fold_in(jax.random.fold_in(own_key, 6), axis_at), (shards_of,), jnp.float32, least / len(cuts), largest / len(cuts))
        loudness = loudness * jnp.repeat(jnp.exp(draws), dims[axis_at] // shards_of).reshape((-1,) + (1,) * (len(dims) - 1 - axis_at))
    return loudness


def noise(rng, shape, scale, reach, shards=(), held_as=jnp.bfloat16):
    loudness = level_of(rng, shape, shards, -0.22, 0.18) if shards else 1.0
    array = jax.random.normal(rng, shape, jnp.float32) * scale * loudness
    return jnp.minimum(jnp.maximum(array, -reach), reach).astype(held_as)


def setup_inputs(seed: int = 0) -> dict:
    keys = jax.random.split(jax.random.key(seed), 19)
    return {
        "tokens": noise(keys[0], (TOKENS, D), 1.0, 6.0, ((0, 32),)),
        "lengths": draw_lengths(jax.random.fold_in(keys[18], 71), 0),
        "query_weight": noise(keys[2], (D, D), (D // 2) ** -0.5, 0.25, ((1, 4),)),
        "query_bias": noise(keys[3], (D,), 0.5, 3.0, ((0, 4),)),
        "key_weight": noise(keys[4], (D, D), (D // 2) ** -0.5, 0.25, ((1, 4),)),
        "value_weight": noise(keys[5], (D, D), D ** -0.5, 0.1875, ((1, 4),)),
        "value_bias": noise(keys[6], (D,), 0.5, 3.0, ((0, 4),)),
        "out_weight": noise(keys[7], (D, D), HD ** -0.5, 0.75, ((0, 4),)),
        "out_bias": noise(keys[8], (D,), 0.5, 3.0),
        "first_gain": jnp.clip(1.0 + 0.15 * jax.random.normal(keys[9], (D,), jnp.float32), 0.25, 1.75).astype(jnp.bfloat16),
        "first_shift": noise(keys[10], (D,), 0.5, 3.0),
        "up_weight": noise(keys[11], (D, FF), D ** -0.5, 0.1875, ((1, 4),)),
        "up_bias": noise(keys[12], (FF,), 0.5, 3.0, ((0, 4),)),
        "down_weight": noise(keys[13], (FF, D), FF ** -0.5, 0.09375, ((0, 4),)),
        "down_bias": noise(keys[14], (D,), 0.5, 3.0),
        "second_gain": jnp.clip(1.0 + 0.15 * jax.random.normal(keys[15], (D,), jnp.float32), 0.25, 1.75).astype(jnp.bfloat16),
        "second_shift": noise(keys[16], (D,), 0.5, 3.0),
        "output_grad": noise(keys[17], (TOKENS, D), 1.0, 6.0, ((0, 32),)),
    }


HIGHEST = lax.Precision.HIGHEST
epsilon = 1e-12

@jax.custom_vjp
def low(v):
    return lax.optimization_barrier(v.astype(jnp.bfloat16)).astype(jnp.float32)

@jax.custom_vjp
def low_back(v):
    return v

def low_keep(v):
    return (low(v), None)

def low_pass(kept, grad):
    return (grad,)

def back_keep(v):
    return (v, None)

def back_low(kept, grad):
    return (low(grad),)
low.defvjp(low_keep, low_pass)
low_back.defvjp(back_keep, back_low)

def matmul(left, right):
    return jnp.dot(left, right, precision=HIGHEST, preferred_element_type=jnp.float32)

def layer_norm(resid, gain, shift):
    center = resid - lax.optimization_barrier(jnp.mean(resid, -1, keepdims=True))
    variance = lax.optimization_barrier(jnp.mean(center * center, -1, keepdims=True))
    return center * lax.rsqrt(variance + epsilon) * gain + shift

def attend(inputs):
    queries, key_rows, values, length = inputs
    scores = low_back(jnp.einsum('qhd,khd->hqk', queries, key_rows, precision=HIGHEST) * HD ** (-0.5))
    valid = jnp.arange(L) < length
    scores = jnp.where(valid[None, None, :], scores, -1000000000.0)
    row_max = lax.optimization_barrier(jnp.max(scores, -1, keepdims=True))
    expon = jnp.exp(scores - row_max)
    probs = low(expon / lax.optimization_barrier(jnp.sum(expon, -1, keepdims=True)))
    return jnp.einsum('hqk,khd->qhd', probs, values, precision=HIGHEST)

def layer(lens_flat, tokens, query_weight, query_bias, key_weight, value_weight, value_bias, out_weight, out_bias, first_gain, first_shift, up_weight, up_bias, down_weight, down_bias, second_gain, second_shift):
    queries = low_back(low(matmul(tokens, query_weight) + query_bias))
    key_rows = low_back(low(matmul(tokens, key_weight)))
    values = low_back(low(matmul(tokens, value_weight) + value_bias))
    shape4 = (BATCHES * SEQS, L, H, HD)
    attended = lax.map(jax.checkpoint(attend), (queries.reshape(shape4), key_rows.reshape(shape4), values.reshape(shape4), lens_flat))
    attended = low_back(low(attended.reshape(TOKENS, D)))
    branch_one = low_back(matmul(attended, out_weight))
    hidden = layer_norm(tokens + branch_one + out_bias, first_gain, first_shift)
    pre_act = low_back(matmul(low(hidden), up_weight) + up_bias)
    activated = low(jax.nn.gelu(pre_act, approximate=False))
    branch_two = low_back(matmul(activated, down_weight))
    return layer_norm(hidden + branch_two + down_bias, second_gain, second_shift)

def reference(tokens, lengths, query_weight, query_bias, key_weight, value_weight, value_bias, out_weight, out_bias, first_gain, first_shift, up_weight, up_bias, down_weight, down_bias, second_gain, second_shift, output_grad):
    lens_flat = lengths.reshape(BATCHES * SEQS).astype(jnp.int32)
    params = [tokens, query_weight, query_bias, key_weight, value_weight, value_bias, out_weight, out_bias, first_gain, first_shift, up_weight, up_bias, down_weight, down_bias, second_gain, second_shift]
    params = [p.astype(jnp.float32) for p in params]
    result, back_fn = jax.vjp(partial(layer, lens_flat), *params)
    grads = back_fn(output_grad.astype(jnp.float32))
    return (result.astype(jnp.bfloat16), grads[0].astype(jnp.bfloat16), grads[1], grads[2], grads[3], grads[4], grads[5], grads[6], grads[7], grads[8], grads[9], grads[10], grads[11], grads[12], grads[13], grads[14], grads[15])
```

```python
from functools import partial

import jax
import jax.numpy as jnp
from jax import lax
from jax.experimental import pallas as pl
from jax.experimental.pallas import tpu as pltpu
from jax.sharding import PartitionSpec as P

HD = 64


epsilon = 1e-12


def norm_forward(resid, gain, shift):
    center = resid - jnp.mean(resid, -1, keepdims=True)
    inv_std = lax.rsqrt(jnp.mean(center * center, -1, keepdims=True) + epsilon)
    normed = center * inv_std
    return (normed * gain + shift, normed, inv_std)


def norm_backward(grad, normed, inv_std, gain):
    scaled = grad * gain
    back = inv_std * (
        scaled
        - jnp.mean(scaled, -1, keepdims=True)
        - normed * jnp.mean(scaled * normed, -1, keepdims=True)
    )
    return (back, jnp.sum(grad * normed, 0), jnp.sum(grad, 0))


F32 = jnp.float32
BF = jnp.bfloat16
MASKED = -1000000000.0
WIDE = 2 * HD


def mm(a, b, ca, cb):
    return lax.dot_general(a, b, (((ca,), (cb,)), ((), ())), preferred_element_type=F32)


def forward_kernel(heads, len_ref, q_ref, k_ref, vt_ref, e_ref, o_ref, r_ref, v_aug, k_aug):
    seq, step = pl.program_id(0), pl.program_id(2)
    seq_len, block = k_ref.shape[0], q_ref.shape[0]

    @pl.when(step == 0)
    def _():
        rows = lax.broadcasted_iota(jnp.int32, (seq_len, WIDE), 0)
        lanes = lax.broadcasted_iota(jnp.int32, (seq_len, WIDE), 1)
        bias = jnp.where(rows < len_ref[seq], 0.0, MASKED)
        keys = k_ref[...].astype(F32)
        for h in range(heads):
            other = (1 - h) * HD
            k_aug[h] = jnp.where(
                lanes // HD == h, keys, jnp.where(lanes == other, bias, 0.0)
            ).astype(BF)
            v_aug[h, :HD] = vt_ref[h * HD : (h + 1) * HD, :]
            v_aug[h, HD:] = jnp.ones((16, seq_len), BF)

    query = q_ref[...].astype(F32) * HD**-0.5
    lanes = lax.broadcasted_iota(jnp.int32, (block, WIDE), 1)
    scores = []
    for h in range(heads):
        other = (1 - h) * HD
        q_aug = jnp.where(
            lanes // HD == h, query, jnp.where(lanes == other, 1.0, 0.0)
        ).astype(BF)
        scores.append(mm(k_aug[h], q_aug, 1, 1))
    outs = []
    for h in range(heads):
        top = jnp.max(scores[h], 0, keepdims=True)
        expon = jnp.exp(scores[h] - top).astype(BF)
        e_ref[h] = expon
        total = mm(v_aug[h], expon, 1, 0)
        inverse = 1.0 / total[HD : HD + 1]
        r_ref[h] = inverse
        outs.append(total[:HD] * inverse)
    if heads == 1:
        outs.append(jnp.zeros_like(outs[0]))
    o_ref[...] = jnp.concatenate(outs, 0).T.astype(BF)


def backward_kernel(
    heads, e_ref, r_ref, q_ref, k_ref, v_ref, o_ref, g_ref, dq_ref, dk_ref, dv_ref, v_aug, k_t, dks, dvs
):
    step, last = pl.program_id(2), pl.num_programs(2) - 1
    seq_len, block = k_ref.shape[0], q_ref.shape[0]

    @pl.when(step == 0)
    def _():
        lanes = lax.broadcasted_iota(jnp.int32, (seq_len, WIDE), 1)
        values = v_ref[...].astype(F32)
        for h in range(heads):
            other = (1 - h) * HD
            ones = jnp.where((lanes >= other) & (lanes < other + 2), 1.0, 0.0)
            v_aug[h] = jnp.where(lanes // HD == h, values, ones).astype(BF)
        k_t[...] = (k_ref[...].astype(F32) * HD**-0.5).T.astype(BF)
        dks[...] = jnp.zeros_like(dks)
        dvs[...] = jnp.zeros_like(dvs)

    lanes = lax.broadcasted_iota(jnp.int32, (block, WIDE), 1)
    inverse = jnp.concatenate(
        [jnp.broadcast_to(r_ref[h % heads], (HD, block)) for h in range(2)], 0
    ).T
    grad = (g_ref[...].astype(F32) * inverse).astype(BF)
    grad_wide = grad.astype(F32)
    scaled_query = (q_ref[...].astype(F32) * HD**-0.5).astype(BF)
    product = grad_wide * o_ref[...].astype(F32)
    centered = []
    for h in range(heads):
        other = (1 - h) * HD
        inside = lanes // HD == h
        row_dot = jnp.sum(jnp.where(inside, product, 0.0), -1, keepdims=True)
        high = row_dot.astype(BF).astype(F32)
        g_aug = jnp.where(
            inside,
            grad_wide,
            jnp.where(lanes == other, -high, jnp.where(lanes == other + 1, high - row_dot, 0.0)),
        ).astype(BF)
        centered.append(mm(v_aug[h], g_aug, 1, 1))
    query_grads = []
    for h in range(heads):
        cols = slice(h * HD, (h + 1) * HD)
        expon = e_ref[h]
        score_grad = (expon.astype(F32) * centered[h]).astype(BF)
        dvs[h] += mm(expon, grad[:, cols], 1, 0)
        dks[h] += mm(score_grad, scaled_query[:, cols], 1, 0)
        query_grads.append(mm(k_t[cols, :], score_grad, 1, 0))
    if heads == 1:
        query_grads.append(jnp.zeros_like(query_grads[0]))
    dq_ref[...] = jnp.concatenate(query_grads, 0).T.astype(BF)

    @pl.when(step == last)
    def _():
        for total, out in ((dks, dk_ref), (dvs, dv_ref)):
            halves = [total[h] for h in range(heads)]
            if heads == 1:
                halves.append(jnp.zeros_like(halves[0]))
            out[...] = jnp.concatenate(halves, 1).astype(BF)


def attention_shape(rows, cols, seqs):
    seq_len = rows // seqs
    block = min(512, seq_len)
    steps = seq_len // block
    pairs = max(1, cols // WIDE)
    heads = cols // HD // pairs
    row_spec = pl.BlockSpec((block, WIDE), lambda s, p, j, *_: (s * steps + j, p))
    key_spec = pl.BlockSpec((seq_len, WIDE), lambda s, p, j, *_: (s, p))
    e_spec = pl.BlockSpec((heads, seq_len, block), lambda s, p, j, *_: (p, s, j))
    r_spec = pl.BlockSpec((heads, 1, block), lambda s, p, j, *_: (p, 0, s * steps + j))
    return seq_len, heads, pairs, (seqs, pairs, steps), row_spec, key_spec, e_spec, r_spec


def widen(array):
    short = WIDE - array.shape[1]
    return array if short <= 0 else jnp.pad(array, ((0, 0), (0, short)))


def attention_forward(queries, keys, values, lengths):
    rows, cols = queries.shape
    seqs = lengths.shape[0]
    seq_len, heads, pairs, grid, row_spec, key_spec, e_spec, r_spec = attention_shape(rows, cols, seqs)
    wide_cols = pairs * WIDE
    expon, attended, inverse = pl.pallas_call(
        partial(forward_kernel, heads),
        grid_spec=pltpu.PrefetchScalarGridSpec(
            num_scalar_prefetch=1,
            grid=grid,
            in_specs=[
                row_spec,
                key_spec,
                pl.BlockSpec((WIDE, seq_len), lambda s, p, j, *_: (p, s)),
            ],
            out_specs=[e_spec, row_spec, r_spec],
            scratch_shapes=[
                pltpu.VMEM((heads, HD + 16, seq_len), BF),
                pltpu.VMEM((heads, seq_len, WIDE), BF),
            ],
        ),
        out_shape=[
            jax.ShapeDtypeStruct((heads * pairs, rows, seq_len), BF),
            jax.ShapeDtypeStruct((rows, wide_cols), BF),
            jax.ShapeDtypeStruct((heads * pairs, 1, rows), F32),
        ],
        name="attention_forward",
        compiler_params=pltpu.CompilerParams(vmem_limit_bytes=60 * 1024 * 1024),
    )(lengths, widen(queries), widen(keys), widen(values).T)
    return expon, attended[:, :cols], inverse


def attention_backward(expon, inverse, queries, keys, values, attended, grad, seqs):
    rows, cols = queries.shape
    seq_len, heads, pairs, grid, row_spec, key_spec, e_spec, r_spec = attention_shape(rows, cols, seqs)
    shape = jax.ShapeDtypeStruct((rows, pairs * WIDE), BF)
    outs = pl.pallas_call(
        partial(backward_kernel, heads),
        grid=grid,
        in_specs=[e_spec, r_spec, row_spec, key_spec, key_spec, row_spec, row_spec],
        out_specs=[row_spec, key_spec, key_spec],
        scratch_shapes=[
            pltpu.VMEM((heads, seq_len, WIDE), BF),
            pltpu.VMEM((WIDE, seq_len), BF),
            pltpu.VMEM((heads, seq_len, HD), F32),
            pltpu.VMEM((heads, seq_len, HD), F32),
        ],
        out_shape=[shape] * 3,
        name="attention_backward",
        compiler_params=pltpu.CompilerParams(vmem_limit_bytes=60 * 1024 * 1024),
    )(expon, inverse, *[widen(x) for x in (queries, keys, values, attended, grad)])
    return [x[:, :cols] for x in outs]


def contract_rows(left, right):
    return lax.dot_general(
        left, right, (((0,), (0,)), ((), ())), preferred_element_type=jnp.float32
    )


def contract_cols(left, right):
    return lax.dot_general(
        left, right, (((1,), (1,)), ((), ())), preferred_element_type=jnp.float32
    )


def split_projection(projected, width, q_bias, v_bias):
    query_part = (projected[:, :width] + q_bias).astype(jnp.bfloat16)
    key_part = projected[:, width : 2 * width].astype(jnp.bfloat16)
    value_part = (projected[:, 2 * width :] + v_bias).astype(jnp.bfloat16)
    return (query_part, key_part, value_part)


def per_device(
    tokens,
    lengths,
    query_weight,
    query_bias,
    key_weight,
    value_weight,
    value_bias,
    out_weight,
    out_bias,
    first_gain,
    first_shift,
    up_weight,
    up_bias,
    down_weight,
    down_bias,
    second_gain,
    second_shift,
    output_grad,
):
    local_rows = tokens.shape[0]
    head_cols = query_weight.shape[1]
    seq_count = lengths.shape[1]
    all_rows = local_rows * lax.axis_size("mp")
    gathered = lax.all_gather(tokens, "mp", axis=0, tiled=True)
    joint_weight = jnp.concatenate([query_weight, key_weight, value_weight], 1)
    projected = jnp.dot(gathered, joint_weight, preferred_element_type=jnp.float32)
    queries, key_rows, values = split_projection(projected, head_cols, query_bias, value_bias)
    expon, attended, inverse = attention_forward(queries, key_rows, values, lengths[0])
    branch_one = lax.psum_scatter(
        jnp.dot(
            lax.slice_in_dim(attended, 0, local_rows * lax.axis_size("mp"), axis=0),
            out_weight,
            preferred_element_type=jnp.float32,
        ).astype(jnp.bfloat16),
        "mp",
        scatter_dimension=0,
        tiled=True,
    ).astype(jnp.float32)
    hidden, normed_one, inv_one = norm_forward(
        tokens.astype(jnp.float32) + branch_one + out_bias, first_gain, first_shift
    )
    hidden_low = hidden.astype(jnp.bfloat16)
    hidden_all = lax.all_gather(hidden_low, "mp", axis=0, tiled=True)
    pre_act = jnp.dot(hidden_all, up_weight, preferred_element_type=jnp.float32) + up_bias
    act_low = jax.nn.gelu(pre_act, approximate=False).astype(jnp.bfloat16)
    branch_two = lax.psum_scatter(
        jnp.dot(
            lax.slice_in_dim(act_low, 0, local_rows * lax.axis_size("mp"), axis=0),
            down_weight,
            preferred_element_type=jnp.float32,
        ).astype(jnp.bfloat16),
        "mp",
        scatter_dimension=0,
        tiled=True,
    ).astype(jnp.float32)
    layer_out, normed_two, inv_two = norm_forward(
        hidden + branch_two + down_bias, second_gain, second_shift
    )
    resid_two_grad, second_gain_grad, second_shift_grad = norm_backward(
        output_grad.astype(jnp.float32), normed_two, inv_two, second_gain
    )
    down_bias_grad = jnp.sum(resid_two_grad, 0)
    branch_two_low = resid_two_grad.astype(jnp.bfloat16)
    row_piece = lax.all_gather(branch_two_low, "mp", axis=0, tiled=True)
    row_start = jnp.int32(0)
    weight_acc = jnp.zeros(down_weight.shape, jnp.float32)
    act_acc = jnp.zeros(act_low.shape, jnp.float32)
    act_rows = lax.dynamic_slice_in_dim(act_low, row_start, row_piece.shape[0], 0)
    weight_acc = weight_acc + contract_rows(act_rows, row_piece)
    act_acc = lax.dynamic_update_slice_in_dim(
        act_acc, contract_cols(row_piece, down_weight), row_start, 0
    )
    down_weight_grad = weight_acc
    unused_two, gelu_back = jax.vjp(partial(jax.nn.gelu, approximate=False), pre_act)
    pre_grad = gelu_back(act_acc)[0].astype(jnp.bfloat16)
    up_bias_grad = jnp.sum(pre_grad, 0, dtype=jnp.float32)
    up_weight_grad = contract_rows(hidden_all, pre_grad)
    hidden_back = lax.psum_scatter(
        contract_cols(
            lax.slice_in_dim(pre_grad, 0, local_rows * lax.axis_size("mp"), axis=0), up_weight
        ).astype(jnp.bfloat16),
        "mp",
        scatter_dimension=0,
        tiled=True,
    ).astype(jnp.float32)
    hidden_grad = resid_two_grad + hidden_back
    resid_one_grad, first_gain_grad, first_shift_grad = norm_backward(
        hidden_grad, normed_one, inv_one, first_gain
    )
    out_bias_grad = jnp.sum(resid_one_grad, 0)
    branch_one_low = resid_one_grad.astype(jnp.bfloat16)
    row_piece = lax.all_gather(branch_one_low, "mp", axis=0, tiled=True)
    row_start = jnp.int32(0)
    weight_acc = jnp.zeros(out_weight.shape, jnp.float32)
    attn_acc = jnp.zeros(attended.shape, jnp.float32)
    attn_rows = lax.dynamic_slice_in_dim(attended, row_start, row_piece.shape[0], 0)
    weight_acc = weight_acc + contract_rows(attn_rows, row_piece)
    attn_acc = lax.dynamic_update_slice_in_dim(
        attn_acc, contract_cols(row_piece, out_weight), row_start, 0
    )
    out_weight_grad = weight_acc
    attn_low = attn_acc.astype(jnp.bfloat16)
    query_flat, key_flat, value_flat = attention_backward(
        expon, inverse, queries, key_rows, values, attended, attn_low, seq_count
    )
    width_now = query_flat.shape[1]
    joint_grad = jnp.concatenate([query_flat, key_flat, value_flat], 1)
    query_bias_grad = jnp.sum(query_flat, 0, dtype=jnp.float32)
    value_bias_grad = jnp.sum(value_flat, 0, dtype=jnp.float32)
    joint_weight_grad = contract_rows(gathered, joint_grad)
    input_back = lax.psum_scatter(
        contract_cols(
            lax.slice_in_dim(joint_grad, 0, local_rows * lax.axis_size("mp"), axis=0), joint_weight
        ).astype(jnp.bfloat16),
        "mp",
        scatter_dimension=0,
        tiled=True,
    ).astype(jnp.float32)
    tokens_grad = (resid_one_grad + input_back).astype(jnp.bfloat16)
    query_weight_grad = joint_weight_grad[:, :width_now]
    key_weight_grad = joint_weight_grad[:, width_now : 2 * width_now]
    value_weight_grad = joint_weight_grad[:, 2 * width_now :]
    (
        query_weight_grad,
        query_bias_grad,
        key_weight_grad,
        value_weight_grad,
        value_bias_grad,
        out_weight_grad,
        up_weight_grad,
        up_bias_grad,
        down_weight_grad,
    ) = (
        lax.psum(query_weight_grad.astype(jnp.bfloat16), "dp").astype(jnp.float32),
        lax.psum(query_bias_grad.astype(jnp.bfloat16), "dp").astype(jnp.float32),
        lax.psum(key_weight_grad.astype(jnp.bfloat16), "dp").astype(jnp.float32),
        lax.psum(value_weight_grad.astype(jnp.bfloat16), "dp").astype(jnp.float32),
        lax.psum(value_bias_grad.astype(jnp.bfloat16), "dp").astype(jnp.float32),
        lax.psum(out_weight_grad.astype(jnp.bfloat16), "dp").astype(jnp.float32),
        lax.psum(up_weight_grad.astype(jnp.bfloat16), "dp").astype(jnp.float32),
        lax.psum(up_bias_grad.astype(jnp.bfloat16), "dp").astype(jnp.float32),
        lax.psum(down_weight_grad.astype(jnp.bfloat16), "dp").astype(jnp.float32),
    )
    (
        out_bias_grad,
        first_gain_grad,
        first_shift_grad,
        down_bias_grad,
        second_gain_grad,
        second_shift_grad,
    ) = lax.psum(
        (
            out_bias_grad,
            first_gain_grad,
            first_shift_grad,
            down_bias_grad,
            second_gain_grad,
            second_shift_grad,
        ),
        ("dp", "mp"),
    )
    return (
        layer_out.astype(jnp.bfloat16),
        tokens_grad,
        query_weight_grad,
        query_bias_grad,
        key_weight_grad,
        value_weight_grad,
        value_bias_grad,
        out_weight_grad,
        out_bias_grad,
        first_gain_grad,
        first_shift_grad,
        up_weight_grad,
        up_bias_grad,
        down_weight_grad,
        down_bias_grad,
        second_gain_grad,
        second_shift_grad,
    )


def solution(mesh):
    placed = (
        P(("dp", "mp"), None),
        P("dp", None),
        P(None, "mp"),
        P("mp"),
        P(None, "mp"),
        P(None, "mp"),
        P("mp"),
        P("mp", None),
        P(),
        P(),
        P(),
        P(None, "mp"),
        P("mp"),
        P("mp", None),
        P(),
        P(),
        P(),
        P(("dp", "mp"), None),
    )
    return jax.shard_map(
        per_device,
        mesh=mesh,
        in_specs=placed,
        out_specs=(
            P(("dp", "mp"), None),
            P(("dp", "mp"), None),
            P(None, "mp"),
            P("mp"),
            P(None, "mp"),
            P(None, "mp"),
            P("mp"),
            P("mp", None),
            P(),
            P(),
            P(),
            P(None, "mp"),
            P("mp"),
            P("mp", None),
            P(),
            P(),
            P(),
        ),
        check_vma=False,
    )
```

```python
from functools import partial

import jax
import jax.numpy as jnp
from jax import lax
from jax.experimental import pallas as pl
from jax.experimental.pallas import tpu as pltpu
from jax.sharding import PartitionSpec as P

HD = 64


epsilon = 1e-12


def norm_forward(resid, gain, shift):
    center = resid - jnp.mean(resid, -1, keepdims=True)
    inv_std = lax.rsqrt(jnp.mean(center * center, -1, keepdims=True) + epsilon)
    normed = center * inv_std
    return (normed * gain + shift, normed, inv_std)


def norm_backward(grad, normed, inv_std, gain):
    scaled = grad * gain
    back = inv_std * (
        scaled
        - jnp.mean(scaled, -1, keepdims=True)
        - normed * jnp.mean(scaled * normed, -1, keepdims=True)
    )
    return (back, jnp.sum(grad * normed, 0), jnp.sum(grad, 0))


F32 = jnp.float32
BF = jnp.bfloat16
MASKED = -1000000000.0
WIDE = 2 * HD


def mm(a, b, ca, cb):
    return lax.dot_general(a, b, (((ca,), (cb,)), ((), ())), preferred_element_type=F32)


def forward_kernel(heads, len_ref, q_ref, k_ref, vt_ref, e_ref, o_ref, r_ref, v_aug, k_aug):
    seq, step = pl.program_id(0), pl.program_id(2)
    seq_len, block = k_ref.shape[0], q_ref.shape[0]

    @pl.when(step == 0)
    def _():
        rows = lax.broadcasted_iota(jnp.int32, (seq_len, WIDE), 0)
        lanes = lax.broadcasted_iota(jnp.int32, (seq_len, WIDE), 1)
        bias = jnp.where(rows < len_ref[seq], 0.0, MASKED)
        keys = k_ref[...].astype(F32)
        for h in range(heads):
            other = (1 - h) * HD
            k_aug[h] = jnp.where(
                lanes // HD == h, keys, jnp.where(lanes == other, bias, 0.0)
            ).astype(BF)
            v_aug[h, :HD] = vt_ref[h * HD : (h + 1) * HD, :]
            v_aug[h, HD:] = jnp.ones((16, seq_len), BF)

    query = q_ref[...].astype(F32) * HD**-0.5
    lanes = lax.broadcasted_iota(jnp.int32, (block, WIDE), 1)
    scores = []
    for h in range(heads):
        other = (1 - h) * HD
        q_aug = jnp.where(
            lanes // HD == h, query, jnp.where(lanes == other, 1.0, 0.0)
        ).astype(BF)
        scores.append(mm(k_aug[h], q_aug, 1, 1))
    outs = []
    for h in range(heads):
        top = jnp.max(scores[h], 0, keepdims=True)
        expon = jnp.exp(scores[h] - top).astype(BF)
        e_ref[h] = expon
        total = mm(v_aug[h], expon, 1, 0)
        inverse = 1.0 / total[HD : HD + 1]
        r_ref[h] = inverse
        outs.append(total[:HD] * inverse)
    if heads == 1:
        outs.append(jnp.zeros_like(outs[0]))
    o_ref[...] = jnp.concatenate(outs, 0).T.astype(BF)


def backward_kernel(
    heads, e_ref, r_ref, q_ref, k_ref, v_ref, o_ref, g_ref, dq_ref, dk_ref, dv_ref, v_aug, k_t, dks, dvs
):
    step, last = pl.program_id(2), pl.num_programs(2) - 1
    seq_len, block = k_ref.shape[0], q_ref.shape[0]

    @pl.when(step == 0)
    def _():
        lanes = lax.broadcasted_iota(jnp.int32, (seq_len, WIDE), 1)
        values = v_ref[...].astype(F32)
        for h in range(heads):
            other = (1 - h) * HD
            ones = jnp.where((lanes >= other) & (lanes < other + 2), 1.0, 0.0)
            v_aug[h] = jnp.where(lanes // HD == h, values, ones).astype(BF)
        k_t[...] = (k_ref[...].astype(F32) * HD**-0.5).T.astype(BF)
        dks[...] = jnp.zeros_like(dks)
        dvs[...] = jnp.zeros_like(dvs)

    lanes = lax.broadcasted_iota(jnp.int32, (block, WIDE), 1)
    inverse = jnp.concatenate(
        [jnp.broadcast_to(r_ref[h % heads], (HD, block)) for h in range(2)], 0
    ).T
    grad = (g_ref[...].astype(F32) * inverse).astype(BF)
    grad_wide = grad.astype(F32)
    scaled_query = (q_ref[...].astype(F32) * HD**-0.5).astype(BF)
    product = grad_wide * o_ref[...].astype(F32)
    centered = []
    for h in range(heads):
        other = (1 - h) * HD
        inside = lanes // HD == h
        row_dot = jnp.sum(jnp.where(inside, product, 0.0), -1, keepdims=True)
        high = row_dot.astype(BF).astype(F32)
        g_aug = jnp.where(
            inside,
            grad_wide,
            jnp.where(lanes == other, -high, jnp.where(lanes == other + 1, high - row_dot, 0.0)),
        ).astype(BF)
        centered.append(mm(v_aug[h], g_aug, 1, 1))
    query_grads = []
    for h in range(heads):
        cols = slice(h * HD, (h + 1) * HD)
        expon = e_ref[h]
        score_grad = (expon.astype(F32) * centered[h]).astype(BF)
        dvs[h] += mm(expon, grad[:, cols], 1, 0)
        dks[h] += mm(score_grad, scaled_query[:, cols], 1, 0)
        query_grads.append(mm(k_t[cols, :], score_grad, 1, 0))
    if heads == 1:
        query_grads.append(jnp.zeros_like(query_grads[0]))
    dq_ref[...] = jnp.concatenate(query_grads, 0).T.astype(BF)

    @pl.when(step == last)
    def _():
        for total, out in ((dks, dk_ref), (dvs, dv_ref)):
            halves = [total[h] for h in range(heads)]
            if heads == 1:
                halves.append(jnp.zeros_like(halves[0]))
            out[...] = jnp.concatenate(halves, 1).astype(BF)


def attention_shape(rows, cols, seqs):
    seq_len = rows // seqs
    block = min(512, seq_len)
    steps = seq_len // block
    pairs = max(1, cols // WIDE)
    heads = cols // HD // pairs
    row_spec = pl.BlockSpec((block, WIDE), lambda s, p, j, *_: (s * steps + j, p))
    key_spec = pl.BlockSpec((seq_len, WIDE), lambda s, p, j, *_: (s, p))
    e_spec = pl.BlockSpec((heads, seq_len, block), lambda s, p, j, *_: (p, s, j))
    r_spec = pl.BlockSpec((heads, 1, block), lambda s, p, j, *_: (p, 0, s * steps + j))
    return seq_len, heads, pairs, (seqs, pairs, steps), row_spec, key_spec, e_spec, r_spec


def widen(array):
    short = WIDE - array.shape[1]
    return array if short <= 0 else jnp.pad(array, ((0, 0), (0, short)))


def attention_forward(queries, keys, values, lengths):
    rows, cols = queries.shape
    seqs = lengths.shape[0]
    seq_len, heads, pairs, grid, row_spec, key_spec, e_spec, r_spec = attention_shape(rows, cols, seqs)
    wide_cols = pairs * WIDE
    expon, attended, inverse = pl.pallas_call(
        partial(forward_kernel, heads),
        grid_spec=pltpu.PrefetchScalarGridSpec(
            num_scalar_prefetch=1,
            grid=grid,
            in_specs=[
                row_spec,
                key_spec,
                pl.BlockSpec((WIDE, seq_len), lambda s, p, j, *_: (p, s)),
            ],
            out_specs=[e_spec, row_spec, r_spec],
            scratch_shapes=[
                pltpu.VMEM((heads, HD + 16, seq_len), BF),
                pltpu.VMEM((heads, seq_len, WIDE), BF),
            ],
        ),
        out_shape=[
            jax.ShapeDtypeStruct((heads * pairs, rows, seq_len), BF),
            jax.ShapeDtypeStruct((rows, wide_cols), BF),
            jax.ShapeDtypeStruct((heads * pairs, 1, rows), F32),
        ],
        name="attention_forward",
        compiler_params=pltpu.CompilerParams(vmem_limit_bytes=60 * 1024 * 1024),
    )(lengths, widen(queries), widen(keys), widen(values).T)
    return expon, attended[:, :cols], inverse


def attention_backward(expon, inverse, queries, keys, values, attended, grad, seqs):
    rows, cols = queries.shape
    seq_len, heads, pairs, grid, row_spec, key_spec, e_spec, r_spec = attention_shape(rows, cols, seqs)
    shape = jax.ShapeDtypeStruct((rows, pairs * WIDE), BF)
    outs = pl.pallas_call(
        partial(backward_kernel, heads),
        grid=grid,
        in_specs=[e_spec, r_spec, row_spec, key_spec, key_spec, row_spec, row_spec],
        out_specs=[row_spec, key_spec, key_spec],
        scratch_shapes=[
            pltpu.VMEM((heads, seq_len, WIDE), BF),
            pltpu.VMEM((WIDE, seq_len), BF),
            pltpu.VMEM((heads, seq_len, HD), F32),
            pltpu.VMEM((heads, seq_len, HD), F32),
        ],
        out_shape=[shape] * 3,
        name="attention_backward",
        compiler_params=pltpu.CompilerParams(vmem_limit_bytes=60 * 1024 * 1024),
    )(expon, inverse, *[widen(x) for x in (queries, keys, values, attended, grad)])
    return [x[:, :cols] for x in outs]


def contract_rows(left, right):
    return lax.dot_general(
        left, right, (((0,), (0,)), ((), ())), preferred_element_type=jnp.float32
    )


def contract_cols(left, right):
    return lax.dot_general(
        left, right, (((1,), (1,)), ((), ())), preferred_element_type=jnp.float32
    )


def split_projection(projected, width, q_bias, v_bias):
    query_part = (projected[:, :width] + q_bias).astype(jnp.bfloat16)
    key_part = projected[:, width : 2 * width].astype(jnp.bfloat16)
    value_part = (projected[:, 2 * width :] + v_bias).astype(jnp.bfloat16)
    return (query_part, key_part, value_part)


def per_device_general(
    tokens,
    lengths,
    query_weight,
    query_bias,
    key_weight,
    value_weight,
    value_bias,
    out_weight,
    out_bias,
    first_gain,
    first_shift,
    up_weight,
    up_bias,
    down_weight,
    down_bias,
    second_gain,
    second_shift,
    output_grad,
):
    local_rows = tokens.shape[0]
    head_cols = query_weight.shape[1]
    seq_count = lengths.shape[1]
    all_rows = local_rows * lax.axis_size("mp")
    gathered = lax.all_gather(tokens, "mp", axis=0, tiled=True)
    joint_weight = jnp.concatenate([query_weight, key_weight, value_weight], 1)
    projected = jnp.dot(gathered, joint_weight, preferred_element_type=jnp.float32)
    queries, key_rows, values = split_projection(projected, head_cols, query_bias, value_bias)
    expon, attended, inverse = attention_forward(queries, key_rows, values, lengths[0])
    branch_one = lax.psum_scatter(
        jnp.dot(
            lax.slice_in_dim(attended, 0, local_rows * lax.axis_size("mp"), axis=0),
            out_weight,
            preferred_element_type=jnp.float32,
        ).astype(jnp.bfloat16),
        "mp",
        scatter_dimension=0,
        tiled=True,
    ).astype(jnp.float32)
    hidden, normed_one, inv_one = norm_forward(
        tokens.astype(jnp.float32) + branch_one + out_bias, first_gain, first_shift
    )
    hidden_low = hidden.astype(jnp.bfloat16)
    hidden_all = lax.all_gather(hidden_low, "mp", axis=0, tiled=True)
    pre_act = jnp.dot(hidden_all, up_weight, preferred_element_type=jnp.float32) + up_bias
    act_low = jax.nn.gelu(pre_act, approximate=False).astype(jnp.bfloat16)
    branch_two = lax.psum_scatter(
        jnp.dot(
            lax.slice_in_dim(act_low, 0, local_rows * lax.axis_size("mp"), axis=0),
            down_weight,
            preferred_element_type=jnp.float32,
        ).astype(jnp.bfloat16),
        "mp",
        scatter_dimension=0,
        tiled=True,
    ).astype(jnp.float32)
    layer_out, normed_two, inv_two = norm_forward(
        hidden + branch_two + down_bias, second_gain, second_shift
    )
    resid_two_grad, second_gain_grad, second_shift_grad = norm_backward(
        output_grad.astype(jnp.float32), normed_two, inv_two, second_gain
    )
    down_bias_grad = jnp.sum(resid_two_grad, 0)
    branch_two_low = resid_two_grad.astype(jnp.bfloat16)
    row_piece = lax.all_gather(branch_two_low, "mp", axis=0, tiled=True)
    row_start = jnp.int32(0)
    weight_acc = jnp.zeros(down_weight.shape, jnp.float32)
    act_acc = jnp.zeros(act_low.shape, jnp.float32)
    act_rows = lax.dynamic_slice_in_dim(act_low, row_start, row_piece.shape[0], 0)
    weight_acc = weight_acc + contract_rows(act_rows, row_piece)
    act_acc = lax.dynamic_update_slice_in_dim(
        act_acc, contract_cols(row_piece, down_weight), row_start, 0
    )
    down_weight_grad = weight_acc
    unused_two, gelu_back = jax.vjp(partial(jax.nn.gelu, approximate=False), pre_act)
    pre_grad = gelu_back(act_acc)[0].astype(jnp.bfloat16)
    up_bias_grad = jnp.sum(pre_grad, 0, dtype=jnp.float32)
    up_weight_grad = contract_rows(hidden_all, pre_grad)
    hidden_back = lax.psum_scatter(
        contract_cols(
            lax.slice_in_dim(pre_grad, 0, local_rows * lax.axis_size("mp"), axis=0), up_weight
        ).astype(jnp.bfloat16),
        "mp",
        scatter_dimension=0,
        tiled=True,
    ).astype(jnp.float32)
    hidden_grad = resid_two_grad + hidden_back
    resid_one_grad, first_gain_grad, first_shift_grad = norm_backward(
        hidden_grad, normed_one, inv_one, first_gain
    )
    out_bias_grad = jnp.sum(resid_one_grad, 0)
    branch_one_low = resid_one_grad.astype(jnp.bfloat16)
    row_piece = lax.all_gather(branch_one_low, "mp", axis=0, tiled=True)
    row_start = jnp.int32(0)
    weight_acc = jnp.zeros(out_weight.shape, jnp.float32)
    attn_acc = jnp.zeros(attended.shape, jnp.float32)
    attn_rows = lax.dynamic_slice_in_dim(attended, row_start, row_piece.shape[0], 0)
    weight_acc = weight_acc + contract_rows(attn_rows, row_piece)
    attn_acc = lax.dynamic_update_slice_in_dim(
        attn_acc, contract_cols(row_piece, out_weight), row_start, 0
    )
    out_weight_grad = weight_acc
    attn_low = attn_acc.astype(jnp.bfloat16)
    query_flat, key_flat, value_flat = attention_backward(
        expon, inverse, queries, key_rows, values, attended, attn_low, seq_count
    )
    width_now = query_flat.shape[1]
    joint_grad = jnp.concatenate([query_flat, key_flat, value_flat], 1)
    query_bias_grad = jnp.sum(query_flat, 0, dtype=jnp.float32)
    value_bias_grad = jnp.sum(value_flat, 0, dtype=jnp.float32)
    joint_weight_grad = contract_rows(gathered, joint_grad)
    input_back = lax.psum_scatter(
        contract_cols(
            lax.slice_in_dim(joint_grad, 0, local_rows * lax.axis_size("mp"), axis=0), joint_weight
        ).astype(jnp.bfloat16),
        "mp",
        scatter_dimension=0,
        tiled=True,
    ).astype(jnp.float32)
    tokens_grad = (resid_one_grad + input_back).astype(jnp.bfloat16)
    query_weight_grad = joint_weight_grad[:, :width_now]
    key_weight_grad = joint_weight_grad[:, width_now : 2 * width_now]
    value_weight_grad = joint_weight_grad[:, 2 * width_now :]
    (
        query_weight_grad,
        query_bias_grad,
        key_weight_grad,
        value_weight_grad,
        value_bias_grad,
        out_weight_grad,
        up_weight_grad,
        up_bias_grad,
        down_weight_grad,
    ) = (
        lax.psum(query_weight_grad.astype(jnp.bfloat16), "dp").astype(jnp.float32),
        lax.psum(query_bias_grad.astype(jnp.bfloat16), "dp").astype(jnp.float32),
        lax.psum(key_weight_grad.astype(jnp.bfloat16), "dp").astype(jnp.float32),
        lax.psum(value_weight_grad.astype(jnp.bfloat16), "dp").astype(jnp.float32),
        lax.psum(value_bias_grad.astype(jnp.bfloat16), "dp").astype(jnp.float32),
        lax.psum(out_weight_grad.astype(jnp.bfloat16), "dp").astype(jnp.float32),
        lax.psum(up_weight_grad.astype(jnp.bfloat16), "dp").astype(jnp.float32),
        lax.psum(up_bias_grad.astype(jnp.bfloat16), "dp").astype(jnp.float32),
        lax.psum(down_weight_grad.astype(jnp.bfloat16), "dp").astype(jnp.float32),
    )
    (
        out_bias_grad,
        first_gain_grad,
        first_shift_grad,
        down_bias_grad,
        second_gain_grad,
        second_shift_grad,
    ) = lax.psum(
        (
            out_bias_grad,
            first_gain_grad,
            first_shift_grad,
            down_bias_grad,
            second_gain_grad,
            second_shift_grad,
        ),
        ("dp", "mp"),
    )
    return (
        layer_out.astype(jnp.bfloat16),
        tokens_grad,
        query_weight_grad,
        query_bias_grad,
        key_weight_grad,
        value_weight_grad,
        value_bias_grad,
        out_weight_grad,
        out_bias_grad,
        first_gain_grad,
        first_shift_grad,
        up_weight_grad,
        up_bias_grad,
        down_weight_grad,
        down_bias_grad,
        second_gain_grad,
        second_shift_grad,
    )


MESH = pl.DeviceIdType.MESH
VMEM_BYTES = 63 * 1024 * 1024
CHUNKS = 4


def flip(index, bit):
    low = index // bit % 2
    return index + bit * (1 - 2 * low)


def mp_peer(relation):
    dp, mp = lax.axis_index("dp"), lax.axis_index("mp")
    for bit in (1, 2):
        if relation // bit % 2:
            mp = flip(mp, bit)
    return (dp, mp)


def dp_peer(bit):
    return (flip(lax.axis_index("dp"), bit), lax.axis_index("mp"))


def greet(peers):
    barrier = pltpu.get_barrier_semaphore()
    for device in peers:
        pl.semaphore_signal(barrier, inc=1, device_id=device, device_id_type=MESH)
    pl.semaphore_wait(barrier, len(peers))


def remote(src, dst, send, recv, device):
    return pltpu.make_async_remote_copy(
        src_ref=src, dst_ref=dst, send_sem=send, recv_sem=recv, device_id=device, device_id_type=MESH
    )


def repeat(count, body):
    def step(i, carry):
        body(i)
        return carry

    lax.fori_loop(0, count, step, 0)


class Gather:
    def __init__(self, own, land, send, recv, chunks=CHUNKS):
        self.own, self.land, self.send, self.recv, self.chunks = own, land, send, recv, chunks
        self.size = own.shape[0] // chunks

    def copy(self, relation, j):
        rows = pl.ds(j * self.size, self.size)
        src = self.land.at[1, rows] if relation == 3 else self.own.at[rows]
        return remote(
            src,
            self.land.at[relation - 1, rows],
            self.send.at[relation - 1, j],
            self.recv.at[relation - 1, j],
            mp_peer(2 if relation == 2 else 1),
        )

    def start(self, j):
        self.copy(2, j).start()
        self.copy(1, j).start()

    def arrive(self, relation, j):
        self.copy(relation, j).wait_recv()
        if relation == 2:
            self.copy(3, j).start()

    def drain(self):
        def body(j):
            for relation in (1, 2, 3):
                self.copy(relation, j).wait_send()

        repeat(self.chunks, body)


PAIR, FAR, NEAR = 0, 1, 2


class Reduce:
    def __init__(self, out, land, send, recv, chunks=CHUNKS):
        self.out, self.land, self.send, self.recv, self.chunks = out, land, send, recv, chunks
        self.size = out.shape[1] // chunks

    def copy(self, kind, j):
        rows = pl.ds(j * self.size, self.size)
        return remote(
            self.out.at[kind, rows],
            self.land.at[kind, rows],
            self.send.at[kind, j],
            self.recv.at[kind, j],
            mp_peer(2 if kind == FAR else 1),
        )

    def post(self, kind, j, value):
        self.out[kind, pl.ds(j * self.size, self.size)] = value.astype(BF)
        self.copy(kind, j).start()

    def forward_pair(self, j, mine):
        self.copy(PAIR, j).wait_recv()
        rows = pl.ds(j * self.size, self.size)
        self.post(FAR, j, mine + self.land[PAIR, rows].astype(F32))

    def total(self, j, mine):
        self.copy(NEAR, j).wait_recv()
        self.copy(FAR, j).wait_recv()
        rows = pl.ds(j * self.size, self.size)
        return mine + self.land[NEAR, rows].astype(F32) + self.land[FAR, rows].astype(F32)

    def drain(self):
        def body(j):
            for kind in (PAIR, FAR, NEAR):
                self.copy(kind, j).wait_send()

        repeat(self.chunks, body)


def transfer_sems(chunks=CHUNKS):
    return [pltpu.SemaphoreType.DMA((3, chunks)), pltpu.SemaphoreType.DMA((3, chunks))]


def comm_params(collective_id):
    return pltpu.CompilerParams(
        collective_id=collective_id, has_side_effects=True, vmem_limit_bytes=VMEM_BYTES
    )


WHOLE = pl.BlockSpec(memory_space=pltpu.VMEM)


def shaped(*shape, dtype=None):
    return jax.ShapeDtypeStruct(shape, dtype or BF)


def column_sum(value):
    return jnp.sum(value, 0, keepdims=True)


def row_mean(value):
    return jnp.mean(value, -1, keepdims=True)


def project_kernel(
    x_ref, wq_ref, wk_ref, wv_ref, qb_ref, vb_ref, q_ref, k_ref, v_ref, vt_ref, all_ref, land, send, recv, save
):
    rows_here = x_ref.shape[0]
    greet([mp_peer(1), mp_peer(2)])
    gather = Gather(x_ref, land, send, recv)
    repeat(CHUNKS, gather.start)
    size = gather.size

    def emit(x, at):
        rows = pl.ds(at, x.shape[0])
        q = (mm(x, wq_ref[...], 1, 0) + qb_ref[...]).astype(BF)
        q_ref[rows] = (q.astype(F32) * HD**-0.5).astype(BF)
        k_ref[rows] = mm(x, wk_ref[...], 1, 0).astype(BF)
        v = mm(x, wv_ref[...], 1, 0) + vb_ref[...]
        v_ref[rows] = v.astype(BF)
        vt_ref[:, rows] = v.T.astype(BF)

    stores = [pltpu.make_async_copy(x_ref, all_ref.at[0], save.at[0])]
    stores[0].start()
    for i in range(2):
        emit(x_ref[pl.ds(i * 2 * size, 2 * size)], i * 2 * size)
    for i in range(2):
        gather.arrive(1, 2 * i)
        gather.arrive(1, 2 * i + 1)
        emit(land[0, pl.ds(i * 2 * size, 2 * size)], rows_here + i * 2 * size)
    for j in range(CHUNKS):
        gather.arrive(2, j)
        gather.arrive(3, j)
        for s in (2, 3):
            emit(land[s - 1, pl.ds(j * size, size)], s * rows_here + j * size)
    for s in (1, 2, 3):
        stores.append(pltpu.make_async_copy(land.at[s - 1], all_ref.at[s], save.at[s]))
        stores[-1].start()
    gather.drain()
    for store in stores:
        store.wait()


def gather_project(tokens, wq, wk, wv, q_bias, v_bias):
    rows, width = tokens.shape
    cols = wq.shape[1]
    return pl.pallas_call(
        project_kernel,
        in_specs=[WHOLE] * 6,
        out_specs=[WHOLE] * 4 + [pl.BlockSpec(memory_space=pl.ANY)],
        out_shape=[shaped(4 * rows, cols)] * 3 + [shaped(cols, 4 * rows), shaped(4, rows, width)],
        scratch_shapes=[
            pltpu.VMEM((3, rows, width), BF),
            *transfer_sems(),
            pltpu.SemaphoreType.DMA((4,)),
        ],
        name="gather_project",
        compiler_params=comm_params(0),
    )(tokens, wq, wk, wv, q_bias, v_bias)


HALVES = 2


def forward_order(step):
    far = 2 * (3 - step % 2) + step // 2
    near = 2 * (1 - (step - 4) // 2) + step % 2
    return jnp.where(step < 4, far, near)


def attend_kernel(
    q_ref, k_ref, vt_ref, bias_ref, w_ref, x_ref, vec_ref,
    e_ref, o_ref, r_ref, n_ref, i_ref, h_ref,
    k_aug, v_aug, out, land, mine, pending, send, recv,
):
    step = pl.program_id(0)
    seq_len, block = k_ref.shape[0], q_ref.shape[0]
    pairs = k_ref.shape[1] // WIDE
    reduce = Reduce(out, land, send, recv, HALVES)

    @pl.when(step == 0)
    def _():
        greet([mp_peer(1), mp_peer(2)])
        lanes = lax.broadcasted_iota(jnp.int32, (seq_len, WIDE), 1)
        for p in range(pairs):
            keys = k_ref[:, p * WIDE : (p + 1) * WIDE].astype(F32)
            for h in range(2):
                other = (1 - h) * HD
                k_aug[2 * p + h] = jnp.where(
                    lanes // HD == h, keys, jnp.where(lanes == other, bias_ref[...], 0.0)
                ).astype(BF)
                at = (2 * p + h) * HD
                v_aug[2 * p + h, :HD] = vt_ref[at : at + HD, :]
                v_aug[2 * p + h, HD:] = jnp.ones((16, seq_len), BF)

    lanes = lax.broadcasted_iota(jnp.int32, (block, WIDE), 1)
    outs = []
    for p in range(pairs):
        query = q_ref[:, p * WIDE : (p + 1) * WIDE].astype(F32)
        scores = []
        for h in range(2):
            other = (1 - h) * HD
            q_aug = jnp.where(
                lanes // HD == h, query, jnp.where(lanes == other, 1.0, 0.0)
            ).astype(BF)
            scores.append(mm(k_aug[2 * p + h], q_aug, 1, 1))
        for h in range(2):
            top = jnp.max(scores[h], 0, keepdims=True)
            expon = jnp.exp(scores[h] - top).astype(BF)
            e_ref[0, 2 * p + h] = expon
            total = mm(v_aug[2 * p + h], expon, 1, 0)
            inverse = 1.0 / total[HD : HD + 1]
            r_ref[0, 2 * p + h] = inverse
            outs.append(total[:HD] * inverse)
    attended = jnp.concatenate(outs, 0).T.astype(BF)
    o_ref[...] = attended
    partial_rows = mm(attended, w_ref[...], 1, 0)

    for t in range(4 * HALVES):

        @pl.when(step == t)
        def _(t=t):
            if t < 4 and t % 2 == 0:
                reduce.post(PAIR, t // 2, partial_rows)
            elif t < 4:
                pending[...] = partial_rows
                reduce.forward_pair(t // 2, pending[...])
            elif t < 6:
                reduce.post(NEAR, t - 4, partial_rows)
            else:
                mine[pl.ds((t - 6) * block, block)] = partial_rows

    @pl.when(step == 4 * HALVES - 1)
    def _():
        for j in range(HALVES):
            rows = pl.ds(j * block, block)
            resid = x_ref[rows].astype(F32) + reduce.total(j, mine[rows]) + vec_ref[0:1]
            center = resid - row_mean(resid)
            inv_std = lax.rsqrt(row_mean(center * center) + epsilon)
            normed = center * inv_std
            n_ref[rows] = normed
            i_ref[rows] = inv_std
            h_ref[rows] = (normed * vec_ref[1:2] + vec_ref[2:3]).astype(BF)
        reduce.drain()


def attend(q, k, vt, bias, out_weight, tokens, vectors):
    all_rows, cols = q.shape
    rows, width = tokens.shape
    block = rows // HALVES
    heads = cols // HD
    steps = all_rows // block

    def fixed(*shape):
        return pl.BlockSpec(shape, lambda i: (0,) * len(shape))

    return pl.pallas_call(
        attend_kernel,
        grid=(steps,),
        in_specs=[
            pl.BlockSpec((block, cols), lambda i: (forward_order(i), 0)),
            fixed(all_rows, cols),
            fixed(cols, all_rows),
            fixed(all_rows, 1),
            fixed(cols, width),
            fixed(rows, width),
            fixed(*vectors.shape),
        ],
        out_specs=[
            pl.BlockSpec((1, heads, all_rows, block), lambda i: (forward_order(i), 0, 0, 0)),
            pl.BlockSpec((block, cols), lambda i: (forward_order(i), 0)),
            pl.BlockSpec((1, heads, 1, block), lambda i: (forward_order(i), 0, 0, 0)),
            fixed(rows, width),
            fixed(rows, 1),
            fixed(rows, width),
        ],
        out_shape=[
            shaped(steps, heads, all_rows, block),
            shaped(all_rows, cols),
            shaped(steps, heads, 1, block, dtype=F32),
            shaped(rows, width, dtype=F32),
            shaped(rows, 1, dtype=F32),
            shaped(rows, width),
        ],
        scratch_shapes=[
            pltpu.VMEM((heads, all_rows, WIDE), BF),
            pltpu.VMEM((heads, HD + 16, all_rows), BF),
            pltpu.VMEM((3, rows, width), BF),
            pltpu.VMEM((3, rows, width), BF),
            pltpu.VMEM((rows, width), F32),
            pltpu.VMEM((block, width), F32),
            *transfer_sems(HALVES),
        ],
        name="attend",
        compiler_params=comm_params(1),
    )(q, k, vt, bias, out_weight, tokens, vectors)


ROOT_HALF = 0.7071067811865476
ROOT_TAU = 0.3989422804014327


def feed_forward_kernel(
    h_ref, n_ref, i_ref, g_ref, up_ref, ub_ref, down_ref, vec_ref,
    out_ref, b1_ref, r1_ref, upg_ref, downg_ref, ubg_ref, small_ref,
    land_h, act, slope, branch, land_b, out1, land1, out2, land2, mine, pending, r2,
    gs1, gr1, gs2, gr2, rs1, rr1, rs2, rr2,
):
    rows_here, width = h_ref.shape
    size = rows_here // CHUNKS
    first_gain, first_shift, down_bias, second_gain, second_shift = (vec_ref[i : i + 1] for i in range(5))
    greet([mp_peer(1), mp_peer(2)])
    gather1, gather2 = Gather(h_ref, land_h, gs1, gr1), Gather(branch, land_b, gs2, gr2)
    reduce1, reduce2 = Reduce(out1, land1, rs1, rr1), Reduce(out2, land2, rs2, rr2)
    repeat(CHUNKS, gather1.start)
    small_ref[...] = jnp.zeros_like(small_ref)
    ubg_ref[...] = jnp.zeros_like(ubg_ref)

    def forward(x):
        pre = mm(x, up_ref[...], 1, 0) + ub_ref[...]
        cdf = 0.5 + 0.5 * lax.erf(pre * ROOT_HALF)
        active = (pre * cdf).astype(BF)
        steep = (cdf + pre * jnp.exp(-0.5 * pre * pre) * ROOT_TAU).astype(BF)
        return active, steep, mm(active, down_ref[...], 1, 0)

    def backward(grad, steep):
        pre_grad = (mm(grad, down_ref[...], 1, 1) * steep.astype(F32)).astype(BF)
        ubg_ref[...] += column_sum(pre_grad.astype(F32))
        return pre_grad, mm(pre_grad, up_ref[...], 1, 1)

    def chunk_rows(j):
        return pl.ds(pl.multiple_of(j * size, size), size)

    def double_rows(j):
        return pl.ds(pl.multiple_of(j * 2 * size, 2 * size), 2 * size)

    def halves(value):
        return value[:size], value[size:]

    def own_forward(i):
        rows = double_rows(i)
        act[0, rows], slope[0, rows], mine[rows] = forward(h_ref[rows])

    def near_forward(i):
        gather1.arrive(1, 2 * i)
        gather1.arrive(1, 2 * i + 1)
        rows = double_rows(i)
        act[1, rows], slope[1, rows], part = forward(land_h[0, rows])
        for k, half in enumerate(halves(part)):
            reduce1.post(NEAR, 2 * i + k, half)

    def far_forward(j):
        gather1.arrive(2, j)
        gather1.arrive(3, j)
        rows = chunk_rows(j)
        active, steep, part = forward(jnp.concatenate([land_h[1, rows], land_h[2, rows]], 0))
        for s in (2, 3):
            act[s, rows] = halves(active)[s - 2]
            slope[s, rows] = halves(steep)[s - 2]
        pending[rows] = part[:size]
        reduce1.post(PAIR, j, part[size:])

        @pl.when(j > 0)
        def _():
            reduce1.forward_pair(j - 1, pending[chunk_rows(j - 1)])

    repeat(2, own_forward)
    repeat(2, near_forward)
    repeat(CHUNKS, far_forward)
    reduce1.forward_pair(CHUNKS - 1, pending[chunk_rows(CHUNKS - 1)])

    def second_norm(j):
        rows = chunk_rows(j)
        hidden = n_ref[rows] * first_gain + first_shift
        resid = hidden + reduce1.total(j, mine[rows]) + down_bias
        center = resid - row_mean(resid)
        inv_std = lax.rsqrt(row_mean(center * center) + epsilon)
        normed = center * inv_std
        out_ref[rows] = (normed * second_gain + second_shift).astype(BF)
        grad = g_ref[rows].astype(F32)
        product = grad * normed
        small_ref[0:1] += column_sum(product)
        small_ref[1:2] += column_sum(grad)
        scaled = grad * second_gain
        back = inv_std * (scaled - row_mean(scaled) - normed * row_mean(scaled * normed))
        small_ref[2:3] += column_sum(back)
        r2[rows] = back
        branch[rows] = back.astype(BF)
        gather2.start(j)

    repeat(CHUNKS, second_norm)

    def own_backward(i):
        rows = double_rows(i)
        slope[0, rows], mine[rows] = backward(branch[rows], slope[0, rows])

    def near_backward(i):
        gather2.arrive(1, 2 * i)
        gather2.arrive(1, 2 * i + 1)
        rows = double_rows(i)
        slope[1, rows], part = backward(land_b[0, rows], slope[1, rows])
        for k, half in enumerate(halves(part)):
            reduce2.post(NEAR, 2 * i + k, half)

    def far_backward(j):
        gather2.arrive(2, j)
        gather2.arrive(3, j)
        rows = chunk_rows(j)
        pre_grad, part = backward(
            jnp.concatenate([land_b[1, rows], land_b[2, rows]], 0),
            jnp.concatenate([slope[2, rows], slope[3, rows]], 0),
        )
        for s in (2, 3):
            slope[s, rows] = halves(pre_grad)[s - 2]
        pending[rows] = part[:size]
        reduce2.post(PAIR, j, part[size:])

        @pl.when(j > 0)
        def _():
            reduce2.forward_pair(j - 1, pending[chunk_rows(j - 1)])

    repeat(2, own_backward)
    repeat(2, near_backward)
    repeat(CHUNKS, far_backward)
    reduce2.forward_pair(CHUNKS - 1, pending[chunk_rows(CHUNKS - 1)])

    tile = 256

    def down_grad(t):
        cols = pl.ds(pl.multiple_of(t * tile, tile), tile)
        total = mm(act[0, :, cols], branch[...], 0, 0)
        for s in (1, 2, 3):
            total += mm(act[s, :, cols], land_b[s - 1], 0, 0)
        downg_ref[cols] = total.astype(BF)

    def up_grad(t):
        cols = pl.ds(pl.multiple_of(t * tile, tile), tile)
        total = mm(h_ref[:, cols], slope[0], 0, 0)
        for s in (1, 2, 3):
            total += mm(land_h[s - 1, :, cols], slope[s], 0, 0)
        upg_ref[cols] = total.astype(BF)

    repeat(down_ref.shape[0] // tile, down_grad)
    repeat(width // tile, up_grad)

    def first_norm(j):
        rows = chunk_rows(j)
        normed = n_ref[rows]
        grad = r2[rows] + reduce2.total(j, mine[rows])
        small_ref[3:4] += column_sum(grad * normed)
        small_ref[4:5] += column_sum(grad)
        scaled = grad * first_gain
        back = i_ref[rows] * (scaled - row_mean(scaled) - normed * row_mean(scaled * normed))
        small_ref[5:6] += column_sum(back)
        r1_ref[rows] = back
        b1_ref[rows] = back.astype(BF)

    repeat(CHUNKS, first_norm)
    for transfer in (gather1, gather2, reduce1, reduce2):
        transfer.drain()


def feed_forward(hidden, normed, inv_std, output_grad, up, up_bias, down, vectors):
    rows, width = hidden.shape
    units = up.shape[1]
    tall = (4, rows, units)
    return pl.pallas_call(
        feed_forward_kernel,
        in_specs=[WHOLE] * 8,
        out_specs=[WHOLE] * 7,
        out_shape=[
            shaped(rows, width),
            shaped(rows, width),
            shaped(rows, width, dtype=F32),
            shaped(width, units),
            shaped(units, width),
            shaped(1, units, dtype=F32),
            shaped(8, width, dtype=F32),
        ],
        scratch_shapes=[
            pltpu.VMEM((3, rows, width), BF),
            pltpu.VMEM(tall, BF),
            pltpu.VMEM(tall, BF),
            pltpu.VMEM((rows, width), BF),
            *[pltpu.VMEM((3, rows, width), BF)] * 5,
            *[pltpu.VMEM((rows, width), F32)] * 3,
            *transfer_sems(),
            *transfer_sems(),
            *transfer_sems(),
            *transfer_sems(),
        ],
        name="feed_forward",
        compiler_params=comm_params(2),
    )(hidden, normed, inv_std, output_grad, up, up_bias, down, vectors)


def attend_back_kernel(
    b_ref, w_ref, e_ref, r_ref, q_ref, k_ref, v_ref, o_ref,
    dq_ref, dk_ref, dv_ref, wg_ref,
    land, v_aug, k_t, dks, dvs, w_total, rows_now, send, recv,
):
    step, last = pl.program_id(0), pl.num_programs(0) - 1
    seq_len, block = k_ref.shape[0], q_ref.shape[0]
    heads = k_ref.shape[1] // HD
    pairs = heads // 2
    gather = Gather(b_ref, land, send, recv, HALVES)

    @pl.when(step == 0)
    def _():
        greet([mp_peer(1), mp_peer(2)])
        repeat(HALVES, gather.start)
        lanes = lax.broadcasted_iota(jnp.int32, (seq_len, WIDE), 1)
        for p in range(pairs):
            values = v_ref[:, p * WIDE : (p + 1) * WIDE].astype(F32)
            for h in range(2):
                other = (1 - h) * HD
                ones = jnp.where((lanes >= other) & (lanes < other + 2), 1.0, 0.0)
                v_aug[2 * p + h] = jnp.where(lanes // HD == h, values, ones).astype(BF)
        k_t[...] = (k_ref[...].astype(F32) * HD**-0.5).T.astype(BF)
        for total in (dks, dvs, w_total):
            total[...] = jnp.zeros_like(total)

    for t in range(4 * HALVES):

        @pl.when(step == t)
        def _(t=t):
            s, j = t // HALVES, t % HALVES
            if t == 2 * HALVES:
                for each in range(HALVES):
                    gather.arrive(2, each)
            elif s in (1, 3):
                gather.arrive(s, j)
            rows = pl.ds(j * block, block)
            rows_now[...] = b_ref[rows] if s == 0 else land[s - 1, rows]

    branch = rows_now[...]
    w_total[...] += mm(o_ref[...], branch, 0, 0)
    attended_grad = mm(branch, w_ref[...], 1, 1).astype(BF).astype(F32)
    lanes = lax.broadcasted_iota(jnp.int32, (block, WIDE), 1)
    query_grads = []
    for p in range(pairs):
        wide = slice(p * WIDE, (p + 1) * WIDE)
        inverse = jnp.concatenate(
            [jnp.broadcast_to(r_ref[0, 2 * p + h], (HD, block)) for h in range(2)], 0
        ).T
        grad = (attended_grad[:, wide] * inverse).astype(BF)
        grad_wide = grad.astype(F32)
        product = grad_wide * o_ref[:, wide].astype(F32)
        centered = []
        for h in range(2):
            other = (1 - h) * HD
            inside = lanes // HD == h
            row_dot = jnp.sum(jnp.where(inside, product, 0.0), -1, keepdims=True)
            high = row_dot.astype(BF).astype(F32)
            g_aug = jnp.where(
                inside,
                grad_wide,
                jnp.where(
                    lanes == other, -high, jnp.where(lanes == other + 1, high - row_dot, 0.0)
                ),
            ).astype(BF)
            centered.append(mm(v_aug[2 * p + h], g_aug, 1, 1))
        for h in range(2):
            at = 2 * p + h
            cols = slice(at * HD, (at + 1) * HD)
            expon = e_ref[0, at]
            score_grad = (expon.astype(F32) * centered[h]).astype(BF)
            dvs[at] += mm(expon, grad[:, h * HD : (h + 1) * HD], 1, 0)
            dks[at] += mm(score_grad, q_ref[:, cols], 1, 0)
            query_grads.append(mm(k_t[cols, :], score_grad, 1, 0))
    dq_ref[...] = jnp.concatenate(query_grads, 0).T.astype(BF)

    @pl.when(step == last)
    def _():
        for total, out in ((dks, dk_ref), (dvs, dv_ref)):
            out[...] = jnp.concatenate([total[h] for h in range(heads)], 1).astype(BF)
        wg_ref[...] = w_total[...].astype(BF)
        gather.drain()


def attend_back(branch, out_weight, expon, inverse, q, k, v, attended):
    rows, width = branch.shape
    all_rows, cols = q.shape
    block = rows // HALVES
    heads = cols // HD
    steps = all_rows // block

    def fixed(*shape):
        return pl.BlockSpec(shape, lambda i: (0,) * len(shape))

    row_spec = pl.BlockSpec((block, cols), lambda i: (i, 0))
    return pl.pallas_call(
        attend_back_kernel,
        grid=(steps,),
        in_specs=[
            fixed(rows, width),
            fixed(cols, width),
            pl.BlockSpec((1, heads, all_rows, block), lambda i: (i, 0, 0, 0)),
            pl.BlockSpec((1, heads, 1, block), lambda i: (i, 0, 0, 0)),
            row_spec,
            fixed(all_rows, cols),
            fixed(all_rows, cols),
            row_spec,
        ],
        out_specs=[row_spec, fixed(all_rows, cols), fixed(all_rows, cols), fixed(cols, width)],
        out_shape=[shaped(all_rows, cols)] * 3 + [shaped(cols, width)],
        scratch_shapes=[
            pltpu.VMEM((3, rows, width), BF),
            pltpu.VMEM((heads, all_rows, WIDE), BF),
            pltpu.VMEM((cols, all_rows), BF),
            pltpu.VMEM((heads, all_rows, HD), F32),
            pltpu.VMEM((heads, all_rows, HD), F32),
            pltpu.VMEM((cols, width), F32),
            pltpu.VMEM((block, width), BF),
            *transfer_sems(HALVES),
        ],
        name="attend_back",
        compiler_params=comm_params(3),
    )(branch, out_weight, expon, inverse, q, k, v, attended)


def input_back_kernel(
    dq_ref, dk_ref, dv_ref, wq_ref, wk_ref, wv_ref, all_ref, r1_ref,
    x_ref, qg_ref, kg_ref, vg_ref, bias_ref,
    out, land, mine, pending, send, recv,
):
    rows_here = r1_ref.shape[0]
    size = rows_here // CHUNKS
    greet([mp_peer(1), mp_peer(2)])
    reduce = Reduce(out, land, send, recv)
    grads = ((dq_ref, wq_ref), (dk_ref, wk_ref), (dv_ref, wv_ref))

    def part_of(starts, count):
        total = None
        for grad, weight in grads:
            pieces = [grad[pl.ds(pl.multiple_of(at, size), count)] for at in starts]
            x = pieces[0] if len(pieces) == 1 else jnp.concatenate(pieces, 0)
            term = mm(x, weight[...], 1, 1)
            total = term if total is None else total + term
        return total

    def chunk_rows(j):
        return pl.ds(pl.multiple_of(j * size, size), size)

    def far(j):
        part = part_of((2 * rows_here + j * size, 3 * rows_here + j * size), size)
        pending[chunk_rows(j)] = part[:size]
        reduce.post(PAIR, j, part[size:])

        @pl.when(j > 0)
        def _():
            reduce.forward_pair(j - 1, pending[chunk_rows(j - 1)])

    repeat(CHUNKS, far)
    reduce.forward_pair(CHUNKS - 1, pending[chunk_rows(CHUNKS - 1)])

    def near(i):
        part = part_of((rows_here + i * 2 * size,), 2 * size)
        reduce.post(NEAR, 2 * i, part[:size])
        reduce.post(NEAR, 2 * i + 1, part[size:])

    repeat(2, near)

    def own(i):
        mine[pl.ds(pl.multiple_of(i * 2 * size, size), 2 * size)] = part_of((i * 2 * size,), 2 * size)

    repeat(2, own)
    tile = 256

    def weights(t):
        cols = pl.ds(pl.multiple_of(t * tile, tile), tile)
        for (grad, _), out_ref in zip(grads, (qg_ref, kg_ref, vg_ref)):
            total = None
            for s in range(4):
                term = mm(all_ref[s, :, cols], grad[pl.ds(s * rows_here, rows_here)], 0, 0)
                total = term if total is None else total + term
            out_ref[cols] = total.astype(BF)

    repeat(all_ref.shape[2] // tile, weights)
    bias_ref[...] = jnp.concatenate(
        [column_sum(dq_ref[...].astype(F32)), column_sum(dv_ref[...].astype(F32))], 0
    )

    def finish(j):
        rows = chunk_rows(j)
        x_ref[rows] = (r1_ref[rows] + reduce.total(j, mine[rows])).astype(BF)

    repeat(CHUNKS, finish)
    reduce.drain()


def input_back(dq, dk, dv, wq, wk, wv, gathered, resid_grad):
    rows, width = resid_grad.shape
    cols = dq.shape[1]
    return pl.pallas_call(
        input_back_kernel,
        in_specs=[WHOLE] * 8,
        out_specs=[WHOLE] * 5,
        out_shape=[shaped(rows, width)] + [shaped(width, cols)] * 3 + [shaped(2, cols, dtype=F32)],
        scratch_shapes=[
            pltpu.VMEM((3, rows, width), BF),
            pltpu.VMEM((3, rows, width), BF),
            pltpu.VMEM((rows, width), F32),
            pltpu.VMEM((rows, width), F32),
            *transfer_sems(),
        ],
        name="input_back",
        compiler_params=comm_params(4),
    )(dq, dk, dv, wq, wk, wv, gathered, resid_grad)


def per_device(
    tokens, lengths, query_weight, query_bias, key_weight, value_weight, value_bias, out_weight,
    out_bias, first_gain, first_shift, up_weight, up_bias, down_weight, down_bias, second_gain,
    second_shift, output_grad,
):
    if lax.axis_size("mp") != 4 or lengths.shape[1] != 1:
        return per_device_general(
            tokens, lengths, query_weight, query_bias, key_weight, value_weight, value_bias,
            out_weight, out_bias, first_gain, first_shift, up_weight, up_bias, down_weight,
            down_bias, second_gain, second_shift, output_grad,
        )
    rows = tokens.shape[0]

    def as_row(vector):
        return vector.astype(F32)[None]

    q, k, v, vt, gathered = gather_project(
        tokens, query_weight, key_weight, value_weight, as_row(query_bias), as_row(value_bias)
    )
    relation = lax.iota(jnp.int32, 4)
    place = jnp.bitwise_xor(relation, lax.axis_index("mp"))[:, None] * rows + lax.iota(jnp.int32, rows)
    bias = jnp.where(place.reshape(-1, 1) < lengths[0, 0], 0.0, MASKED)
    expon, attended, inverse, normed, inv_std, hidden = attend(
        q, k, vt, bias, out_weight, tokens,
        jnp.stack([out_bias, first_gain, first_shift]).astype(F32),
    )
    layer_out, branch, resid_grad, up_grad, down_grad, up_bias_grad, small = feed_forward(
        hidden, normed, inv_std, output_grad, up_weight, as_row(up_bias), down_weight,
        jnp.stack([first_gain, first_shift, down_bias, second_gain, second_shift]).astype(F32),
    )
    dq, dk, dv, out_grad = attend_back(branch, out_weight, expon, inverse, q, k, v, attended)
    tokens_grad, query_grad, key_grad, value_grad, bias_grads = input_back(
        dq, dk, dv, query_weight, key_weight, value_weight, gathered, resid_grad
    )

    def over_batches(array):
        return lax.psum(array.astype(BF), "dp").astype(F32)

    small = lax.psum(small, ("dp", "mp"))
    return (
        layer_out,
        tokens_grad,
        over_batches(query_grad),
        over_batches(bias_grads[0]),
        over_batches(key_grad),
        over_batches(value_grad),
        over_batches(bias_grads[1]),
        over_batches(out_grad),
        small[5],
        small[3],
        small[4],
        over_batches(up_grad),
        over_batches(up_bias_grad[0]),
        over_batches(down_grad),
        small[2],
        small[0],
        small[1],
    )


def solution(mesh):
    placed = (
        P(("dp", "mp"), None),
        P("dp", None),
        P(None, "mp"),
        P("mp"),
        P(None, "mp"),
        P(None, "mp"),
        P("mp"),
        P("mp", None),
        P(),
        P(),
        P(),
        P(None, "mp"),
        P("mp"),
        P("mp", None),
        P(),
        P(),
        P(),
        P(("dp", "mp"), None),
    )
    return jax.shard_map(
        per_device,
        mesh=mesh,
        in_specs=placed,
        out_specs=(
            P(("dp", "mp"), None),
            P(("dp", "mp"), None),
            P(None, "mp"),
            P("mp"),
            P(None, "mp"),
            P(None, "mp"),
            P("mp"),
            P("mp", None),
            P(),
            P(),
            P(),
            P(None, "mp"),
            P("mp"),
            P("mp", None),
            P(),
            P(),
            P(),
        ),
        check_vma=False,
    )
```

```python
from functools import partial

import jax
import jax.numpy as jnp
from jax import lax
from jax.experimental import pallas as pl
from jax.experimental.pallas import tpu as pltpu
from jax.sharding import PartitionSpec as P

HD = 64


epsilon = 1e-12


def norm_forward(resid, gain, shift):
    center = resid - jnp.mean(resid, -1, keepdims=True)
    inv_std = lax.rsqrt(jnp.mean(center * center, -1, keepdims=True) + epsilon)
    normed = center * inv_std
    return (normed * gain + shift, normed, inv_std)


def norm_backward(grad, normed, inv_std, gain):
    scaled = grad * gain
    back = inv_std * (
        scaled
        - jnp.mean(scaled, -1, keepdims=True)
        - normed * jnp.mean(scaled * normed, -1, keepdims=True)
    )
    return (back, jnp.sum(grad * normed, 0), jnp.sum(grad, 0))


F32 = jnp.float32
BF = jnp.bfloat16
MASKED = -1000000000.0
WIDE = 2 * HD


def mm(a, b, ca, cb):
    return lax.dot_general(a, b, (((ca,), (cb,)), ((), ())), preferred_element_type=F32)


def forward_kernel(heads, len_ref, q_ref, k_ref, vt_ref, e_ref, o_ref, r_ref, v_aug, k_aug):
    seq, step = pl.program_id(0), pl.program_id(2)
    seq_len, block = k_ref.shape[0], q_ref.shape[0]

    @pl.when(step == 0)
    def _():
        rows = lax.broadcasted_iota(jnp.int32, (seq_len, WIDE), 0)
        lanes = lax.broadcasted_iota(jnp.int32, (seq_len, WIDE), 1)
        bias = jnp.where(rows < len_ref[seq], 0.0, MASKED)
        keys = k_ref[...].astype(F32)
        for h in range(heads):
            other = (1 - h) * HD
            k_aug[h] = jnp.where(
                lanes // HD == h, keys, jnp.where(lanes == other, bias, 0.0)
            ).astype(BF)
            v_aug[h, :HD] = vt_ref[h * HD : (h + 1) * HD, :]
            v_aug[h, HD:] = jnp.ones((16, seq_len), BF)

    query = q_ref[...].astype(F32) * HD**-0.5
    lanes = lax.broadcasted_iota(jnp.int32, (block, WIDE), 1)
    scores = []
    for h in range(heads):
        other = (1 - h) * HD
        q_aug = jnp.where(
            lanes // HD == h, query, jnp.where(lanes == other, 1.0, 0.0)
        ).astype(BF)
        scores.append(mm(k_aug[h], q_aug, 1, 1))
    outs = []
    for h in range(heads):
        top = jnp.max(scores[h], 0, keepdims=True)
        expon = jnp.exp(scores[h] - top).astype(BF)
        e_ref[h] = expon
        total = mm(v_aug[h], expon, 1, 0)
        inverse = 1.0 / total[HD : HD + 1]
        r_ref[h] = inverse
        outs.append(total[:HD] * inverse)
    if heads == 1:
        outs.append(jnp.zeros_like(outs[0]))
    o_ref[...] = jnp.concatenate(outs, 0).T.astype(BF)


def backward_kernel(
    heads, e_ref, r_ref, q_ref, k_ref, v_ref, o_ref, g_ref, dq_ref, dk_ref, dv_ref, v_aug, k_t, dks, dvs
):
    step, last = pl.program_id(2), pl.num_programs(2) - 1
    seq_len, block = k_ref.shape[0], q_ref.shape[0]

    @pl.when(step == 0)
    def _():
        lanes = lax.broadcasted_iota(jnp.int32, (seq_len, WIDE), 1)
        values = v_ref[...].astype(F32)
        for h in range(heads):
            other = (1 - h) * HD
            ones = jnp.where((lanes >= other) & (lanes < other + 2), 1.0, 0.0)
            v_aug[h] = jnp.where(lanes // HD == h, values, ones).astype(BF)
        k_t[...] = (k_ref[...].astype(F32) * HD**-0.5).T.astype(BF)
        dks[...] = jnp.zeros_like(dks)
        dvs[...] = jnp.zeros_like(dvs)

    lanes = lax.broadcasted_iota(jnp.int32, (block, WIDE), 1)
    inverse = jnp.concatenate(
        [jnp.broadcast_to(r_ref[h % heads], (HD, block)) for h in range(2)], 0
    ).T
    grad = (g_ref[...].astype(F32) * inverse).astype(BF)
    grad_wide = grad.astype(F32)
    scaled_query = (q_ref[...].astype(F32) * HD**-0.5).astype(BF)
    product = grad_wide * o_ref[...].astype(F32)
    centered = []
    for h in range(heads):
        other = (1 - h) * HD
        inside = lanes // HD == h
        row_dot = jnp.sum(jnp.where(inside, product, 0.0), -1, keepdims=True)
        high = row_dot.astype(BF).astype(F32)
        g_aug = jnp.where(
            inside,
            grad_wide,
            jnp.where(lanes == other, -high, jnp.where(lanes == other + 1, high - row_dot, 0.0)),
        ).astype(BF)
        centered.append(mm(v_aug[h], g_aug, 1, 1))
    query_grads = []
    for h in range(heads):
        cols = slice(h * HD, (h + 1) * HD)
        expon = e_ref[h]
        score_grad = (expon.astype(F32) * centered[h]).astype(BF)
        dvs[h] += mm(expon, grad[:, cols], 1, 0)
        dks[h] += mm(score_grad, scaled_query[:, cols], 1, 0)
        query_grads.append(mm(k_t[cols, :], score_grad, 1, 0))
    if heads == 1:
        query_grads.append(jnp.zeros_like(query_grads[0]))
    dq_ref[...] = jnp.concatenate(query_grads, 0).T.astype(BF)

    @pl.when(step == last)
    def _():
        for total, out in ((dks, dk_ref), (dvs, dv_ref)):
            halves = [total[h] for h in range(heads)]
            if heads == 1:
                halves.append(jnp.zeros_like(halves[0]))
            out[...] = jnp.concatenate(halves, 1).astype(BF)


def attention_shape(rows, cols, seqs):
    seq_len = rows // seqs
    block = min(512, seq_len)
    steps = seq_len // block
    pairs = max(1, cols // WIDE)
    heads = cols // HD // pairs
    row_spec = pl.BlockSpec((block, WIDE), lambda s, p, j, *_: (s * steps + j, p))
    key_spec = pl.BlockSpec((seq_len, WIDE), lambda s, p, j, *_: (s, p))
    e_spec = pl.BlockSpec((heads, seq_len, block), lambda s, p, j, *_: (p, s, j))
    r_spec = pl.BlockSpec((heads, 1, block), lambda s, p, j, *_: (p, 0, s * steps + j))
    return seq_len, heads, pairs, (seqs, pairs, steps), row_spec, key_spec, e_spec, r_spec


def widen(array):
    short = WIDE - array.shape[1]
    return array if short <= 0 else jnp.pad(array, ((0, 0), (0, short)))


def attention_forward(queries, keys, values, lengths):
    rows, cols = queries.shape
    seqs = lengths.shape[0]
    seq_len, heads, pairs, grid, row_spec, key_spec, e_spec, r_spec = attention_shape(rows, cols, seqs)
    wide_cols = pairs * WIDE
    expon, attended, inverse = pl.pallas_call(
        partial(forward_kernel, heads),
        grid_spec=pltpu.PrefetchScalarGridSpec(
            num_scalar_prefetch=1,
            grid=grid,
            in_specs=[
                row_spec,
                key_spec,
                pl.BlockSpec((WIDE, seq_len), lambda s, p, j, *_: (p, s)),
            ],
            out_specs=[e_spec, row_spec, r_spec],
            scratch_shapes=[
                pltpu.VMEM((heads, HD + 16, seq_len), BF),
                pltpu.VMEM((heads, seq_len, WIDE), BF),
            ],
        ),
        out_shape=[
            jax.ShapeDtypeStruct((heads * pairs, rows, seq_len), BF),
            jax.ShapeDtypeStruct((rows, wide_cols), BF),
            jax.ShapeDtypeStruct((heads * pairs, 1, rows), F32),
        ],
        name="attention_forward",
        compiler_params=pltpu.CompilerParams(vmem_limit_bytes=60 * 1024 * 1024),
    )(lengths, widen(queries), widen(keys), widen(values).T)
    return expon, attended[:, :cols], inverse


def attention_backward(expon, inverse, queries, keys, values, attended, grad, seqs):
    rows, cols = queries.shape
    seq_len, heads, pairs, grid, row_spec, key_spec, e_spec, r_spec = attention_shape(rows, cols, seqs)
    shape = jax.ShapeDtypeStruct((rows, pairs * WIDE), BF)
    outs = pl.pallas_call(
        partial(backward_kernel, heads),
        grid=grid,
        in_specs=[e_spec, r_spec, row_spec, key_spec, key_spec, row_spec, row_spec],
        out_specs=[row_spec, key_spec, key_spec],
        scratch_shapes=[
            pltpu.VMEM((heads, seq_len, WIDE), BF),
            pltpu.VMEM((WIDE, seq_len), BF),
            pltpu.VMEM((heads, seq_len, HD), F32),
            pltpu.VMEM((heads, seq_len, HD), F32),
        ],
        out_shape=[shape] * 3,
        name="attention_backward",
        compiler_params=pltpu.CompilerParams(vmem_limit_bytes=60 * 1024 * 1024),
    )(expon, inverse, *[widen(x) for x in (queries, keys, values, attended, grad)])
    return [x[:, :cols] for x in outs]


def contract_rows(left, right):
    return lax.dot_general(
        left, right, (((0,), (0,)), ((), ())), preferred_element_type=jnp.float32
    )


def contract_cols(left, right):
    return lax.dot_general(
        left, right, (((1,), (1,)), ((), ())), preferred_element_type=jnp.float32
    )


def split_projection(projected, width, q_bias, v_bias):
    query_part = (projected[:, :width] + q_bias).astype(jnp.bfloat16)
    key_part = projected[:, width : 2 * width].astype(jnp.bfloat16)
    value_part = (projected[:, 2 * width :] + v_bias).astype(jnp.bfloat16)
    return (query_part, key_part, value_part)


def per_device_general(
    tokens,
    lengths,
    query_weight,
    query_bias,
    key_weight,
    value_weight,
    value_bias,
    out_weight,
    out_bias,
    first_gain,
    first_shift,
    up_weight,
    up_bias,
    down_weight,
    down_bias,
    second_gain,
    second_shift,
    output_grad,
):
    local_rows = tokens.shape[0]
    head_cols = query_weight.shape[1]
    seq_count = lengths.shape[1]
    all_rows = local_rows * lax.axis_size("mp")
    gathered = lax.all_gather(tokens, "mp", axis=0, tiled=True)
    joint_weight = jnp.concatenate([query_weight, key_weight, value_weight], 1)
    projected = jnp.dot(gathered, joint_weight, preferred_element_type=jnp.float32)
    queries, key_rows, values = split_projection(projected, head_cols, query_bias, value_bias)
    expon, attended, inverse = attention_forward(queries, key_rows, values, lengths[0])
    branch_one = lax.psum_scatter(
        jnp.dot(
            lax.slice_in_dim(attended, 0, local_rows * lax.axis_size("mp"), axis=0),
            out_weight,
            preferred_element_type=jnp.float32,
        ).astype(jnp.bfloat16),
        "mp",
        scatter_dimension=0,
        tiled=True,
    ).astype(jnp.float32)
    hidden, normed_one, inv_one = norm_forward(
        tokens.astype(jnp.float32) + branch_one + out_bias, first_gain, first_shift
    )
    hidden_low = hidden.astype(jnp.bfloat16)
    hidden_all = lax.all_gather(hidden_low, "mp", axis=0, tiled=True)
    pre_act = jnp.dot(hidden_all, up_weight, preferred_element_type=jnp.float32) + up_bias
    act_low = jax.nn.gelu(pre_act, approximate=False).astype(jnp.bfloat16)
    branch_two = lax.psum_scatter(
        jnp.dot(
            lax.slice_in_dim(act_low, 0, local_rows * lax.axis_size("mp"), axis=0),
            down_weight,
            preferred_element_type=jnp.float32,
        ).astype(jnp.bfloat16),
        "mp",
        scatter_dimension=0,
        tiled=True,
    ).astype(jnp.float32)
    layer_out, normed_two, inv_two = norm_forward(
        hidden + branch_two + down_bias, second_gain, second_shift
    )
    resid_two_grad, second_gain_grad, second_shift_grad = norm_backward(
        output_grad.astype(jnp.float32), normed_two, inv_two, second_gain
    )
    down_bias_grad = jnp.sum(resid_two_grad, 0)
    branch_two_low = resid_two_grad.astype(jnp.bfloat16)
    row_piece = lax.all_gather(branch_two_low, "mp", axis=0, tiled=True)
    row_start = jnp.int32(0)
    weight_acc = jnp.zeros(down_weight.shape, jnp.float32)
    act_acc = jnp.zeros(act_low.shape, jnp.float32)
    act_rows = lax.dynamic_slice_in_dim(act_low, row_start, row_piece.shape[0], 0)
    weight_acc = weight_acc + contract_rows(act_rows, row_piece)
    act_acc = lax.dynamic_update_slice_in_dim(
        act_acc, contract_cols(row_piece, down_weight), row_start, 0
    )
    down_weight_grad = weight_acc
    unused_two, gelu_back = jax.vjp(partial(jax.nn.gelu, approximate=False), pre_act)
    pre_grad = gelu_back(act_acc)[0].astype(jnp.bfloat16)
    up_bias_grad = jnp.sum(pre_grad, 0, dtype=jnp.float32)
    up_weight_grad = contract_rows(hidden_all, pre_grad)
    hidden_back = lax.psum_scatter(
        contract_cols(
            lax.slice_in_dim(pre_grad, 0, local_rows * lax.axis_size("mp"), axis=0), up_weight
        ).astype(jnp.bfloat16),
        "mp",
        scatter_dimension=0,
        tiled=True,
    ).astype(jnp.float32)
    hidden_grad = resid_two_grad + hidden_back
    resid_one_grad, first_gain_grad, first_shift_grad = norm_backward(
        hidden_grad, normed_one, inv_one, first_gain
    )
    out_bias_grad = jnp.sum(resid_one_grad, 0)
    branch_one_low = resid_one_grad.astype(jnp.bfloat16)
    row_piece = lax.all_gather(branch_one_low, "mp", axis=0, tiled=True)
    row_start = jnp.int32(0)
    weight_acc = jnp.zeros(out_weight.shape, jnp.float32)
    attn_acc = jnp.zeros(attended.shape, jnp.float32)
    attn_rows = lax.dynamic_slice_in_dim(attended, row_start, row_piece.shape[0], 0)
    weight_acc = weight_acc + contract_rows(attn_rows, row_piece)
    attn_acc = lax.dynamic_update_slice_in_dim(
        attn_acc, contract_cols(row_piece, out_weight), row_start, 0
    )
    out_weight_grad = weight_acc
    attn_low = attn_acc.astype(jnp.bfloat16)
    query_flat, key_flat, value_flat = attention_backward(
        expon, inverse, queries, key_rows, values, attended, attn_low, seq_count
    )
    width_now = query_flat.shape[1]
    joint_grad = jnp.concatenate([query_flat, key_flat, value_flat], 1)
    query_bias_grad = jnp.sum(query_flat, 0, dtype=jnp.float32)
    value_bias_grad = jnp.sum(value_flat, 0, dtype=jnp.float32)
    joint_weight_grad = contract_rows(gathered, joint_grad)
    input_back = lax.psum_scatter(
        contract_cols(
            lax.slice_in_dim(joint_grad, 0, local_rows * lax.axis_size("mp"), axis=0), joint_weight
        ).astype(jnp.bfloat16),
        "mp",
        scatter_dimension=0,
        tiled=True,
    ).astype(jnp.float32)
    tokens_grad = (resid_one_grad + input_back).astype(jnp.bfloat16)
    query_weight_grad = joint_weight_grad[:, :width_now]
    key_weight_grad = joint_weight_grad[:, width_now : 2 * width_now]
    value_weight_grad = joint_weight_grad[:, 2 * width_now :]
    (
        query_weight_grad,
        query_bias_grad,
        key_weight_grad,
        value_weight_grad,
        value_bias_grad,
        out_weight_grad,
        up_weight_grad,
        up_bias_grad,
        down_weight_grad,
    ) = (
        lax.psum(query_weight_grad.astype(jnp.bfloat16), "dp").astype(jnp.float32),
        lax.psum(query_bias_grad.astype(jnp.bfloat16), "dp").astype(jnp.float32),
        lax.psum(key_weight_grad.astype(jnp.bfloat16), "dp").astype(jnp.float32),
        lax.psum(value_weight_grad.astype(jnp.bfloat16), "dp").astype(jnp.float32),
        lax.psum(value_bias_grad.astype(jnp.bfloat16), "dp").astype(jnp.float32),
        lax.psum(out_weight_grad.astype(jnp.bfloat16), "dp").astype(jnp.float32),
        lax.psum(up_weight_grad.astype(jnp.bfloat16), "dp").astype(jnp.float32),
        lax.psum(up_bias_grad.astype(jnp.bfloat16), "dp").astype(jnp.float32),
        lax.psum(down_weight_grad.astype(jnp.bfloat16), "dp").astype(jnp.float32),
    )
    (
        out_bias_grad,
        first_gain_grad,
        first_shift_grad,
        down_bias_grad,
        second_gain_grad,
        second_shift_grad,
    ) = lax.psum(
        (
            out_bias_grad,
            first_gain_grad,
            first_shift_grad,
            down_bias_grad,
            second_gain_grad,
            second_shift_grad,
        ),
        ("dp", "mp"),
    )
    return (
        layer_out.astype(jnp.bfloat16),
        tokens_grad,
        query_weight_grad,
        query_bias_grad,
        key_weight_grad,
        value_weight_grad,
        value_bias_grad,
        out_weight_grad,
        out_bias_grad,
        first_gain_grad,
        first_shift_grad,
        up_weight_grad,
        up_bias_grad,
        down_weight_grad,
        down_bias_grad,
        second_gain_grad,
        second_shift_grad,
    )


MESH = pl.DeviceIdType.MESH
VMEM_BYTES = 63 * 1024 * 1024
CHUNKS = 4


def flip(index, bit):
    low = index // bit % 2
    return index + bit * (1 - 2 * low)


def mp_peer(relation):
    dp, mp = lax.axis_index("dp"), lax.axis_index("mp")
    for bit in (1, 2):
        if relation // bit % 2:
            mp = flip(mp, bit)
    return (dp, mp)


def dp_peer(bit):
    return (flip(lax.axis_index("dp"), bit), lax.axis_index("mp"))


def greet(peers):
    barrier = pltpu.get_barrier_semaphore()
    for device in peers:
        pl.semaphore_signal(barrier, inc=1, device_id=device, device_id_type=MESH)
    pl.semaphore_wait(barrier, len(peers))


def remote(src, dst, send, recv, device):
    return pltpu.make_async_remote_copy(
        src_ref=src, dst_ref=dst, send_sem=send, recv_sem=recv, device_id=device, device_id_type=MESH
    )


def repeat(count, body):
    def step(i, carry):
        body(i)
        return carry

    lax.fori_loop(0, count, step, 0)


class Gather:
    def __init__(self, own, land, send, recv, chunks=CHUNKS):
        self.own, self.land, self.send, self.recv, self.chunks = own, land, send, recv, chunks
        self.size = own.shape[0] // chunks

    def copy(self, relation, j):
        rows = pl.ds(j * self.size, self.size)
        src = self.land.at[1, rows] if relation == 3 else self.own.at[rows]
        return remote(
            src,
            self.land.at[relation - 1, rows],
            self.send.at[relation - 1, j],
            self.recv.at[relation - 1, j],
            mp_peer(2 if relation == 2 else 1),
        )

    def start(self, j):
        self.copy(2, j).start()
        self.copy(1, j).start()

    def arrive(self, relation, j):
        self.copy(relation, j).wait_recv()
        if relation == 2:
            self.copy(3, j).start()

    def drain(self):
        def body(j):
            for relation in (1, 2, 3):
                self.copy(relation, j).wait_send()

        repeat(self.chunks, body)


PAIR, FAR, NEAR = 0, 1, 2


class Reduce:
    def __init__(self, out, land, send, recv, chunks=CHUNKS):
        self.out, self.land, self.send, self.recv, self.chunks = out, land, send, recv, chunks
        self.size = out.shape[1] // chunks

    def copy(self, kind, j):
        rows = pl.ds(j * self.size, self.size)
        return remote(
            self.out.at[kind, rows],
            self.land.at[kind, rows],
            self.send.at[kind, j],
            self.recv.at[kind, j],
            mp_peer(2 if kind == FAR else 1),
        )

    def post(self, kind, j, value):
        self.out[kind, pl.ds(j * self.size, self.size)] = value.astype(BF)
        self.copy(kind, j).start()

    def forward_pair(self, j, mine):
        self.copy(PAIR, j).wait_recv()
        rows = pl.ds(j * self.size, self.size)
        self.post(FAR, j, mine + self.land[PAIR, rows].astype(F32))

    def total(self, j, mine):
        self.copy(NEAR, j).wait_recv()
        self.copy(FAR, j).wait_recv()
        rows = pl.ds(j * self.size, self.size)
        return mine + self.land[NEAR, rows].astype(F32) + self.land[FAR, rows].astype(F32)

    def drain(self):
        def body(j):
            for kind in (PAIR, FAR, NEAR):
                self.copy(kind, j).wait_send()

        repeat(self.chunks, body)


LINKS = ((1, 2, 4), (2, 1, 4))


class Spread:
    def __init__(self, data, full, land, send, recv, first=0):
        self.data, self.full, self.land, self.send, self.recv = data, full, land, send, recv
        self.first = first
        self.count = (full if data is None else data).shape[0] // 2

    def place(self, part, i):
        dp = lax.axis_index("dp")
        start, size = part * self.count, self.count
        for bit in LINKS[part][:i]:
            size //= 2
            start += dp // bit % 2 * size
        return start, size

    def rows(self, start, size):
        return pl.ds(pl.multiple_of(start, size), size)

    def reduce_copy(self, part, i):
        start, size = self.place(part, i)
        bit, half = LINKS[part][i], size // 2
        other = 1 - lax.axis_index("dp") // bit % 2
        at = sum(self.count >> (k + 1) for k in range(self.first, i))
        return remote(
            self.data.at[self.rows(start + other * half, half)],
            self.land.at[part, pl.ds(at, half)],
            self.send.at[part, i],
            self.recv.at[part, i],
            dp_peer(bit),
        )

    def gather_copy(self, part, i):
        start, size = self.place(part, i + 1)
        rows = self.rows(start, size)
        return remote(
            self.full.at[rows],
            self.full.at[rows],
            self.send.at[part, 3 + i],
            self.recv.at[part, 3 + i],
            dp_peer(LINKS[part][i]),
        )

    def reduce_start(self, i):
        for part in range(2):
            self.reduce_copy(part, i).start()

    def reduce_finish(self, i):
        for part in range(2):
            copy = self.reduce_copy(part, i)
            copy.wait_send()
            copy.wait_recv()
            start, size = self.place(part, i + 1)
            rows = self.rows(start, size)
            at = sum(self.count >> (k + 1) for k in range(self.first, i))
            target = self.full if i == 2 else self.data
            target[rows] = (
                self.data[rows].astype(F32) + self.land[part, pl.ds(at, size)].astype(F32)
            ).astype(BF)

    def gather_start(self, i):
        for part in range(2):
            self.gather_copy(part, i).start()

    def gather_finish(self, i):
        for part in range(2):
            copy = self.gather_copy(part, i)
            copy.wait_send()
            copy.wait_recv()


def spread_scratch(data, first=0, steps=3):
    rows = sum(data[0] // 2 >> (k + 1) for k in range(first, first + steps))
    land = [pltpu.VMEM((2, rows, data[1]), BF)] if steps else []
    return land + [pltpu.SemaphoreType.DMA((2, 6)), pltpu.SemaphoreType.DMA((2, 6))]


class Hops:
    def __init__(self, value, land, send, recv, peers):
        self.value, self.land, self.send, self.recv, self.peers = value, land, send, recv, peers

    def copy(self, i):
        return remote(
            self.value.at[i], self.land.at[i], self.send.at[i], self.recv.at[i], self.peers[i]
        )

    def start(self, i):
        self.copy(i).start()

    def finish(self, i):
        self.copy(i).wait_recv()
        self.value[i + 1] = self.value[i] + self.land[i]
        self.copy(i).wait_send()


def hop_scratch(count, *shape):
    return [
        pltpu.VMEM((count + 1, *shape), F32),
        pltpu.VMEM((count, *shape), F32),
        pltpu.SemaphoreType.DMA((count,)),
        pltpu.SemaphoreType.DMA((count,)),
    ]


def greet_all():
    greet([mp_peer(1), mp_peer(2), dp_peer(1), dp_peer(2), dp_peer(4)])


def transfer_sems(chunks=CHUNKS):
    return [pltpu.SemaphoreType.DMA((3, chunks)), pltpu.SemaphoreType.DMA((3, chunks))]


def comm_params(collective_id):
    return pltpu.CompilerParams(
        collective_id=collective_id, has_side_effects=True, vmem_limit_bytes=VMEM_BYTES
    )


WHOLE = pl.BlockSpec(memory_space=pltpu.VMEM)


def shaped(*shape, dtype=None):
    return jax.ShapeDtypeStruct(shape, dtype or BF)


def column_sum(value):
    return jnp.sum(value, 0, keepdims=True)


def row_mean(value):
    return jnp.mean(value, -1, keepdims=True)


def project_kernel(
    x_ref, wq_ref, wk_ref, wv_ref, qb_ref, vb_ref, q_ref, k_ref, v_ref, vt_ref, all_ref, land, send, recv, save
):
    rows_here = x_ref.shape[0]
    greet([mp_peer(1), mp_peer(2)])
    gather = Gather(x_ref, land, send, recv)
    repeat(CHUNKS, gather.start)
    size = gather.size

    def emit(x, at):
        rows = pl.ds(at, x.shape[0])
        q = (mm(x, wq_ref[...], 1, 0) + qb_ref[...]).astype(BF)
        q_ref[rows] = (q.astype(F32) * HD**-0.5).astype(BF)
        k_ref[rows] = mm(x, wk_ref[...], 1, 0).astype(BF)
        v = mm(x, wv_ref[...], 1, 0) + vb_ref[...]
        v_ref[rows] = v.astype(BF)
        vt_ref[:, rows] = v.T.astype(BF)

    stores = [pltpu.make_async_copy(x_ref, all_ref.at[0], save.at[0])]
    stores[0].start()
    for i in range(2):
        emit(x_ref[pl.ds(i * 2 * size, 2 * size)], i * 2 * size)
    for i in range(2):
        gather.arrive(1, 2 * i)
        gather.arrive(1, 2 * i + 1)
        emit(land[0, pl.ds(i * 2 * size, 2 * size)], rows_here + i * 2 * size)
    for j in range(CHUNKS):
        gather.arrive(2, j)
        gather.arrive(3, j)
        for s in (2, 3):
            emit(land[s - 1, pl.ds(j * size, size)], s * rows_here + j * size)
    for s in (1, 2, 3):
        stores.append(pltpu.make_async_copy(land.at[s - 1], all_ref.at[s], save.at[s]))
        stores[-1].start()
    gather.drain()
    for store in stores:
        store.wait()


def gather_project(tokens, wq, wk, wv, q_bias, v_bias):
    rows, width = tokens.shape
    cols = wq.shape[1]
    return pl.pallas_call(
        project_kernel,
        in_specs=[WHOLE] * 6,
        out_specs=[WHOLE] * 4 + [pl.BlockSpec(memory_space=pl.ANY)],
        out_shape=[shaped(4 * rows, cols)] * 3 + [shaped(cols, 4 * rows), shaped(4, rows, width)],
        scratch_shapes=[
            pltpu.VMEM((3, rows, width), BF),
            *transfer_sems(),
            pltpu.SemaphoreType.DMA((4,)),
        ],
        name="gather_project",
        compiler_params=comm_params(0),
    )(tokens, wq, wk, wv, q_bias, v_bias)


HALVES = 2


def forward_order(step):
    far = 2 * (3 - step % 2) + step // 2
    near = 2 * (1 - (step - 4) // 2) + step % 2
    return jnp.where(step < 4, far, near)


def attend_kernel(
    q_ref, k_ref, vt_ref, bias_ref, w_ref, x_ref, vec_ref,
    e_ref, o_ref, r_ref, n_ref, i_ref, h_ref,
    k_aug, v_aug, out, land, mine, pending, send, recv,
):
    step = pl.program_id(0)
    seq_len, block = k_ref.shape[0], q_ref.shape[0]
    pairs = k_ref.shape[1] // WIDE
    reduce = Reduce(out, land, send, recv, HALVES)

    @pl.when(step == 0)
    def _():
        greet([mp_peer(1), mp_peer(2)])
        lanes = lax.broadcasted_iota(jnp.int32, (seq_len, WIDE), 1)
        for p in range(pairs):
            keys = k_ref[:, p * WIDE : (p + 1) * WIDE].astype(F32)
            for h in range(2):
                other = (1 - h) * HD
                k_aug[2 * p + h] = jnp.where(
                    lanes // HD == h, keys, jnp.where(lanes == other, bias_ref[...], 0.0)
                ).astype(BF)
                at = (2 * p + h) * HD
                v_aug[2 * p + h, :HD] = vt_ref[at : at + HD, :]
                v_aug[2 * p + h, HD:] = jnp.ones((16, seq_len), BF)

    lanes = lax.broadcasted_iota(jnp.int32, (block, WIDE), 1)
    outs = []
    for p in range(pairs):
        query = q_ref[:, p * WIDE : (p + 1) * WIDE].astype(F32)
        scores = []
        for h in range(2):
            other = (1 - h) * HD
            q_aug = jnp.where(
                lanes // HD == h, query, jnp.where(lanes == other, 1.0, 0.0)
            ).astype(BF)
            scores.append(mm(k_aug[2 * p + h], q_aug, 1, 1))
        for h in range(2):
            top = jnp.max(scores[h], 0, keepdims=True)
            expon = jnp.exp(scores[h] - top).astype(BF)
            e_ref[0, 2 * p + h] = expon
            total = mm(v_aug[2 * p + h], expon, 1, 0)
            inverse = 1.0 / total[HD : HD + 1]
            r_ref[0, 2 * p + h] = inverse
            outs.append(total[:HD] * inverse)
    attended = jnp.concatenate(outs, 0).T.astype(BF)
    o_ref[...] = attended
    partial_rows = mm(attended, w_ref[...], 1, 0)

    for t in range(4 * HALVES):

        @pl.when(step == t)
        def _(t=t):
            if t < 4 and t % 2 == 0:
                reduce.post(PAIR, t // 2, partial_rows)
            elif t < 4:
                pending[...] = partial_rows
                reduce.forward_pair(t // 2, pending[...])
            elif t < 6:
                reduce.post(NEAR, t - 4, partial_rows)
            else:
                mine[pl.ds((t - 6) * block, block)] = partial_rows

    @pl.when(step == 4 * HALVES - 1)
    def _():
        for j in range(HALVES):
            rows = pl.ds(j * block, block)
            resid = x_ref[rows].astype(F32) + reduce.total(j, mine[rows]) + vec_ref[0:1]
            center = resid - row_mean(resid)
            inv_std = lax.rsqrt(row_mean(center * center) + epsilon)
            normed = center * inv_std
            n_ref[rows] = normed
            i_ref[rows] = inv_std
            h_ref[rows] = (normed * vec_ref[1:2] + vec_ref[2:3]).astype(BF)
        reduce.drain()


def attend(q, k, vt, bias, out_weight, tokens, vectors):
    all_rows, cols = q.shape
    rows, width = tokens.shape
    block = rows // HALVES
    heads = cols // HD
    steps = all_rows // block

    def fixed(*shape):
        return pl.BlockSpec(shape, lambda i: (0,) * len(shape))

    return pl.pallas_call(
        attend_kernel,
        grid=(steps,),
        in_specs=[
            pl.BlockSpec((block, cols), lambda i: (forward_order(i), 0)),
            fixed(all_rows, cols),
            fixed(cols, all_rows),
            fixed(all_rows, 1),
            fixed(cols, width),
            fixed(rows, width),
            fixed(*vectors.shape),
        ],
        out_specs=[
            pl.BlockSpec((1, heads, all_rows, block), lambda i: (forward_order(i), 0, 0, 0)),
            pl.BlockSpec((block, cols), lambda i: (forward_order(i), 0)),
            pl.BlockSpec((1, heads, 1, block), lambda i: (forward_order(i), 0, 0, 0)),
            fixed(rows, width),
            fixed(rows, 1),
            fixed(rows, width),
        ],
        out_shape=[
            shaped(steps, heads, all_rows, block),
            shaped(all_rows, cols),
            shaped(steps, heads, 1, block, dtype=F32),
            shaped(rows, width, dtype=F32),
            shaped(rows, 1, dtype=F32),
            shaped(rows, width),
        ],
        scratch_shapes=[
            pltpu.VMEM((heads, all_rows, WIDE), BF),
            pltpu.VMEM((heads, HD + 16, all_rows), BF),
            pltpu.VMEM((3, rows, width), BF),
            pltpu.VMEM((3, rows, width), BF),
            pltpu.VMEM((rows, width), F32),
            pltpu.VMEM((block, width), F32),
            *transfer_sems(HALVES),
        ],
        name="attend",
        compiler_params=comm_params(1),
    )(q, k, vt, bias, out_weight, tokens, vectors)


ROOT_HALF = 0.7071067811865476
ROOT_TAU = 0.3989422804014327


def feed_forward_kernel(
    h_ref, n_ref, i_ref, g_ref, up_ref, ub_ref, down_ref, vec_ref,
    out_ref, b1_ref, r1_ref, upg_ref, downg_ref, small_ref,
    land_h, act, slope, branch, land_b, out1, land1, out2, land2, mine, pending, r2,
    gs1, gr1, gs2, gr2, rs1, rr1, rs2, rr2,
    down_land, down_send, down_recv, up_land, up_send, up_recv,
):
    rows_here, width = h_ref.shape
    size = rows_here // CHUNKS
    first_gain, first_shift, down_bias, second_gain, second_shift = (vec_ref[i : i + 1] for i in range(5))
    greet_all()
    down_sum = Spread(downg_ref, None, down_land, down_send, down_recv)
    up_sum = Spread(upg_ref, None, up_land, up_send, up_recv)
    gather1, gather2 = Gather(h_ref, land_h, gs1, gr1), Gather(branch, land_b, gs2, gr2)
    reduce1, reduce2 = Reduce(out1, land1, rs1, rr1), Reduce(out2, land2, rs2, rr2)
    repeat(CHUNKS, gather1.start)
    small_ref[...] = jnp.zeros_like(small_ref)

    def forward(x):
        pre = mm(x, up_ref[...], 1, 0) + ub_ref[...]
        cdf = 0.5 + 0.5 * lax.erf(pre * ROOT_HALF)
        active = (pre * cdf).astype(BF)
        steep = (cdf + pre * jnp.exp(-0.5 * pre * pre) * ROOT_TAU).astype(BF)
        return active, steep, mm(active, down_ref[...], 1, 0)

    def backward(grad, steep):
        pre_grad = (mm(grad, down_ref[...], 1, 1) * steep.astype(F32)).astype(BF)
        small_ref[6:7] += column_sum(pre_grad.astype(F32))
        return pre_grad, mm(pre_grad, up_ref[...], 1, 1)

    def chunk_rows(j):
        return pl.ds(pl.multiple_of(j * size, size), size)

    def double_rows(j):
        return pl.ds(pl.multiple_of(j * 2 * size, 2 * size), 2 * size)

    def halves(value):
        return value[:size], value[size:]

    def own_forward(i):
        rows = double_rows(i)
        act[0, rows], slope[0, rows], mine[rows] = forward(h_ref[rows])

    def near_forward(i):
        gather1.arrive(1, 2 * i)
        gather1.arrive(1, 2 * i + 1)
        rows = double_rows(i)
        act[1, rows], slope[1, rows], part = forward(land_h[0, rows])
        for k, half in enumerate(halves(part)):
            reduce1.post(NEAR, 2 * i + k, half)

    def far_forward(j):
        gather1.arrive(2, j)
        gather1.arrive(3, j)
        rows = chunk_rows(j)
        active, steep, part = forward(jnp.concatenate([land_h[1, rows], land_h[2, rows]], 0))
        for s in (2, 3):
            act[s, rows] = halves(active)[s - 2]
            slope[s, rows] = halves(steep)[s - 2]
        pending[rows] = part[:size]
        reduce1.post(PAIR, j, part[size:])

        @pl.when(j > 0)
        def _():
            reduce1.forward_pair(j - 1, pending[chunk_rows(j - 1)])

    repeat(2, own_forward)
    repeat(2, near_forward)
    repeat(CHUNKS, far_forward)
    reduce1.forward_pair(CHUNKS - 1, pending[chunk_rows(CHUNKS - 1)])

    def second_norm(j):
        rows = chunk_rows(j)
        hidden = n_ref[rows] * first_gain + first_shift
        resid = hidden + reduce1.total(j, mine[rows]) + down_bias
        center = resid - row_mean(resid)
        inv_std = lax.rsqrt(row_mean(center * center) + epsilon)
        normed = center * inv_std
        out_ref[rows] = (normed * second_gain + second_shift).astype(BF)
        grad = g_ref[rows].astype(F32)
        product = grad * normed
        small_ref[0:1] += column_sum(product)
        small_ref[1:2] += column_sum(grad)
        scaled = grad * second_gain
        back = inv_std * (scaled - row_mean(scaled) - normed * row_mean(scaled * normed))
        small_ref[2:3] += column_sum(back)
        r2[rows] = back
        branch[rows] = back.astype(BF)
        gather2.start(j)

    repeat(CHUNKS, second_norm)

    def own_backward(i):
        rows = double_rows(i)
        slope[0, rows], mine[rows] = backward(branch[rows], slope[0, rows])

    def near_backward(i):
        gather2.arrive(1, 2 * i)
        gather2.arrive(1, 2 * i + 1)
        rows = double_rows(i)
        slope[1, rows], part = backward(land_b[0, rows], slope[1, rows])
        for k, half in enumerate(halves(part)):
            reduce2.post(NEAR, 2 * i + k, half)

    def far_backward(j):
        gather2.arrive(2, j)
        gather2.arrive(3, j)
        rows = chunk_rows(j)
        pre_grad, part = backward(
            jnp.concatenate([land_b[1, rows], land_b[2, rows]], 0),
            jnp.concatenate([slope[2, rows], slope[3, rows]], 0),
        )
        for s in (2, 3):
            slope[s, rows] = halves(pre_grad)[s - 2]
        pending[rows] = part[:size]
        reduce2.post(PAIR, j, part[size:])

        @pl.when(j > 0)
        def _():
            reduce2.forward_pair(j - 1, pending[chunk_rows(j - 1)])

    repeat(2, own_backward)
    repeat(2, near_backward)
    repeat(CHUNKS, far_backward)
    reduce2.forward_pair(CHUNKS - 1, pending[chunk_rows(CHUNKS - 1)])

    tile = 256

    def down_grad(t):
        cols = pl.ds(pl.multiple_of(t * tile, tile), tile)
        total = mm(act[0, :, cols], branch[...], 0, 0)
        for s in (1, 2, 3):
            total += mm(act[s, :, cols], land_b[s - 1], 0, 0)
        downg_ref[cols] = total.astype(BF)

    def up_grad(t):
        cols = pl.ds(pl.multiple_of(t * tile, tile), tile)
        total = mm(h_ref[:, cols], slope[0], 0, 0)
        for s in (1, 2, 3):
            total += mm(land_h[s - 1, :, cols], slope[s], 0, 0)
        upg_ref[cols] = total.astype(BF)

    repeat(down_ref.shape[0] // tile, down_grad)
    down_sum.reduce_start(0)
    repeat(width // tile, up_grad)
    up_sum.reduce_start(0)

    def first_norm(j):
        rows = chunk_rows(j)
        normed = n_ref[rows]
        grad = r2[rows] + reduce2.total(j, mine[rows])
        small_ref[3:4] += column_sum(grad * normed)
        small_ref[4:5] += column_sum(grad)
        scaled = grad * first_gain
        back = i_ref[rows] * (scaled - row_mean(scaled) - normed * row_mean(scaled * normed))
        small_ref[5:6] += column_sum(back)
        r1_ref[rows] = back
        b1_ref[rows] = back.astype(BF)

    repeat(2, first_norm)
    down_sum.reduce_finish(0)
    down_sum.reduce_start(1)
    repeat(CHUNKS - 2, lambda j: first_norm(j + 2))
    up_sum.reduce_finish(0)
    down_sum.reduce_finish(1)
    for transfer in (gather1, gather2, reduce1, reduce2):
        transfer.drain()


def feed_forward(hidden, normed, inv_std, output_grad, up, up_bias, down, vectors):
    rows, width = hidden.shape
    units = up.shape[1]
    tall = (4, rows, units)
    return pl.pallas_call(
        feed_forward_kernel,
        in_specs=[WHOLE] * 8,
        out_specs=[WHOLE] * 6,
        out_shape=[
            shaped(rows, width),
            shaped(rows, width),
            shaped(rows, width, dtype=F32),
            shaped(width, units),
            shaped(units, width),
            shaped(8, width, dtype=F32),
        ],
        scratch_shapes=[
            pltpu.VMEM((3, rows, width), BF),
            pltpu.VMEM(tall, BF),
            pltpu.VMEM(tall, BF),
            pltpu.VMEM((rows, width), BF),
            *[pltpu.VMEM((3, rows, width), BF)] * 5,
            *[pltpu.VMEM((rows, width), F32)] * 3,
            *transfer_sems(),
            *transfer_sems(),
            *transfer_sems(),
            *transfer_sems(),
            *spread_scratch((units, width), 0, 2),
            *spread_scratch((width, units), 0, 1),
        ],
        name="feed_forward",
        compiler_params=comm_params(2),
    )(hidden, normed, inv_std, output_grad, up, up_bias, down, vectors)


def attend_back_kernel(
    b_ref, w_ref, e_ref, r_ref, q_ref, k_ref, v_ref, o_ref, small_in, up_in, down_in, all_in,
    dq_ref, dk_ref, dv_ref, wg_ref, pg_ref, small_ref, up_out, down_out,
    land, v_aug, k_t, dks, dvs, dqs, w_total, w_low, w_full, p_low, p_full, grads, up, up_full, down, down_full, tokens, loads, send, recv,
    up_land, up_send, up_recv, down_send, down_recv, down_land, out_land, out_send, out_recv,
    pair_land, pair_send, pair_recv, value, small_land, small_send, small_recv,
):
    pair, s_now = pl.program_id(0), pl.program_id(1)
    step = pair * 4 + s_now
    seq_len, block = k_ref.shape[0], q_ref.shape[0]
    pieces = e_ref.shape[0]
    cols = w_ref.shape[0]
    width = w_ref.shape[1]
    half = block // 2
    gather = Gather(b_ref, land, send, recv, HALVES)
    up_sum = Spread(up, up_full, up_land, up_send, up_recv, 1)
    down_sum = Spread(down, down_full, down_land, down_send, down_recv, 2)
    out_sum = Spread(w_low, w_full, out_land, out_send, out_recv)
    pair_sum = Spread(p_low, p_full, pair_land, pair_send, pair_recv)
    small = Hops(
        value, small_land, small_send, small_recv,
        [dp_peer(1), dp_peer(2), dp_peer(4), mp_peer(1), mp_peer(2)],
    )
    load_up = pltpu.make_async_copy(up_in, up, loads.at[0])
    load_down = pltpu.make_async_copy(down_in, down, loads.at[1])
    load_tokens = pltpu.make_async_copy(all_in, tokens, loads.at[2])
    save_up = pltpu.make_async_copy(up_full, up_out, loads.at[3])
    save_down = pltpu.make_async_copy(down_full, down_out, loads.at[4])

    def branch_rows(s):
        branch = b_ref[...] if s == 0 else land[s - 1]
        at = pl.ds(s * block, block)
        if s == 0:
            w_total[...] = mm(o_ref[...], branch, 0, 0)
        else:
            w_total[...] += mm(o_ref[...], branch, 0, 0)
        grads[at] = mm(branch, w_ref[...], 1, 1).astype(BF)

    @pl.when(step == 0)
    def _():
        load_down.start()
        load_up.start()
        load_tokens.start()
        load_down.wait()
        load_up.wait()
        greet_all()
        repeat(HALVES, gather.start)
        down_sum.reduce_start(2)
        up_sum.reduce_start(1)
        value[0] = small_in[...]
        small.start(0)
        branch_rows(0)

    @pl.when(step == 1)
    def _():
        repeat(HALVES, lambda j: gather.arrive(1, j))
        up_sum.reduce_finish(1)
        up_sum.reduce_start(2)
        small.finish(0)
        small.start(1)
        branch_rows(1)

    @pl.when(step == 2)
    def _():
        down_sum.reduce_finish(2)
        down_sum.gather_start(2)
        small.finish(1)
        small.start(2)
        repeat(HALVES, lambda j: gather.arrive(2, j))
        branch_rows(2)

    @pl.when(step == 3)
    def _():
        up_sum.reduce_finish(2)
        up_sum.gather_start(2)
        small.finish(2)
        small.start(3)
        repeat(HALVES, lambda j: gather.arrive(3, j))
        branch_rows(3)

    @pl.when(step == 4)
    def _():
        down_sum.gather_finish(2)
        down_sum.gather_start(1)
        w_low[...] = w_total[...].astype(BF)
        out_sum.reduce_start(0)
        small.finish(3)
        small.start(4)

    @pl.when(step == 5)
    def _():
        up_sum.gather_finish(2)
        up_sum.gather_start(1)
        down_sum.gather_finish(1)
        down_sum.gather_start(0)
        out_sum.reduce_finish(0)
        out_sum.reduce_start(1)
        small.finish(4)
        small_ref[...] = value[5]
        small_ref[6:7] = value[3, 6:7]

    @pl.when(step == 6)
    def _():
        pair_sum.reduce_finish(0)
        pair_sum.reduce_start(1)
        out_sum.reduce_finish(1)
        out_sum.reduce_start(2)
        up_sum.gather_finish(1)
        up_sum.gather_start(0)

    @pl.when(step == 7)
    def _():
        pair_sum.reduce_finish(1)
        pair_sum.reduce_start(2)
        out_sum.reduce_finish(2)
        out_sum.gather_start(2)
        down_sum.gather_finish(0)
        save_down.start()

    @pl.when(s_now == 0)
    def _():
        lanes = lax.broadcasted_iota(jnp.int32, (seq_len, WIDE), 1)
        values = v_ref[...].astype(F32)
        for h in range(2):
            other = (1 - h) * HD
            ones = jnp.where((lanes >= other) & (lanes < other + 2), 1.0, 0.0)
            v_aug[h] = jnp.where(lanes // HD == h, values, ones).astype(BF)
        k_t[...] = (k_ref[...].astype(F32) * HD**-0.5).T.astype(BF)
        dks[...] = jnp.zeros_like(dks)
        dvs[...] = jnp.zeros_like(dvs)

    lanes = lax.broadcasted_iota(jnp.int32, (block, WIDE), 1)
    row_start = pl.multiple_of(s_now * block, block)
    inverse = jnp.concatenate(
        [
            jnp.concatenate(
                [jnp.broadcast_to(r_ref[i, h], (HD, block // pieces)) for h in range(2)], 0
            )
            for i in range(pieces)
        ],
        1,
    ).T
    wide = pl.ds(pl.multiple_of(pair * WIDE, WIDE), WIDE)
    grad = (grads[pl.ds(row_start, block), wide].astype(F32) * inverse).astype(BF)
    grad_wide = grad.astype(F32)
    product = grad_wide * o_ref[:, wide].astype(F32)
    centered = []
    for h in range(2):
        other = (1 - h) * HD
        inside = lanes // HD == h
        row_dot = jnp.sum(jnp.where(inside, product, 0.0), -1, keepdims=True)
        high = row_dot.astype(BF).astype(F32)
        g_aug = jnp.where(
            inside,
            grad_wide,
            jnp.where(lanes == other, -high, jnp.where(lanes == other + 1, high - row_dot, 0.0)),
        ).astype(BF)
        centered.append(mm(v_aug[h], g_aug, 1, 1))
    query_grads = []
    for h in range(2):
        cols_h = slice(h * HD, (h + 1) * HD)
        expon = jnp.concatenate([e_ref[i, h] for i in range(pieces)], 1)
        score_grad = (expon.astype(F32) * centered[h]).astype(BF)
        dvs[h] += mm(expon, grad[:, cols_h], 1, 0)
        dks[h] += mm(score_grad, q_ref[:, cols_h], 1, 0)
        query_grads.append(mm(k_t[cols_h, :], score_grad, 1, 0))
    query_grad = jnp.concatenate(query_grads, 0).T.astype(BF)
    dq_ref[...] = query_grad
    dqs[pl.ds(row_start, block)] = query_grad

    @pl.when(s_now == 3)
    def _():
        for total, out in ((dks, dk_ref), (dvs, dv_ref)):
            out[...] = jnp.concatenate([total[h] for h in range(2)], 1).astype(BF)

    @pl.when(step == 3)
    def _():
        load_tokens.wait()
        projection_grads(tokens, (dqs, dk_ref, dv_ref), p_low)
        pair_sum.reduce_start(0)

    @pl.when(step == 7)
    def _():
        pair_sum.reduce_finish(2)
        out_sum.gather_finish(2)
        wg_ref[...] = w_full[...]
        pg_ref[...] = p_full[...]
        up_sum.gather_finish(0)
        save_up.start()
        gather.drain()
        save_down.wait()
        save_up.wait()


def projection_grads(tokens, parts, out_ref):
    tile = 256
    rows = tokens.shape[1]

    def body(t):
        cols = pl.ds(pl.multiple_of(t * tile, tile), tile)
        for at, part in enumerate(parts):
            total = None
            for s in range(4):
                term = mm(tokens[s, :, cols], part[pl.ds(s * rows, rows)], 0, 0)
                total = term if total is None else total + term
            out_ref[cols, at * WIDE : (at + 1) * WIDE] = total.astype(BF)

    repeat(tokens.shape[2] // tile, body)


def attend_back(branch, out_weight, expon, inverse, q, k, v, attended, small, up, down, gathered):
    rows, width = branch.shape
    all_rows, cols = q.shape
    pairs = cols // WIDE
    pieces = HALVES

    def fixed(*shape):
        return pl.BlockSpec(shape, lambda p, s: (0,) * len(shape))

    anywhere = pl.BlockSpec(memory_space=pl.ANY)
    pair_rows = pl.BlockSpec((rows, WIDE), lambda p, s: (s, p))
    pair_keys = pl.BlockSpec((all_rows, WIDE), lambda p, s: (0, p))
    return pl.pallas_call(
        attend_back_kernel,
        grid=(pairs, 4),
        in_specs=[
            fixed(rows, width),
            fixed(cols, width),
            pl.BlockSpec((pieces, 2, all_rows, rows // pieces), lambda p, s: (s, p, 0, 0)),
            pl.BlockSpec((pieces, 2, 1, rows // pieces), lambda p, s: (s, p, 0, 0)),
            pair_rows,
            pair_keys,
            pair_keys,
            pl.BlockSpec((rows, cols), lambda p, s: (s, 0)),
            fixed(*small.shape),
            anywhere,
            anywhere,
            anywhere,
        ],
        out_specs=[
            pair_rows,
            pair_keys,
            pair_keys,
            fixed(cols, width),
            fixed(width, 3 * WIDE),
            fixed(*small.shape),
            anywhere,
            anywhere,
        ],
        out_shape=[shaped(all_rows, cols)] * 3
        + [
            shaped(cols, width),
            shaped(width, 3 * WIDE),
            shaped(*small.shape, dtype=F32),
            shaped(*up.shape),
            shaped(*down.shape),
        ],
        scratch_shapes=[
            pltpu.VMEM((3, rows, width), BF),
            pltpu.VMEM((2, all_rows, WIDE), BF),
            pltpu.VMEM((WIDE, all_rows), BF),
            pltpu.VMEM((2, all_rows, HD), F32),
            pltpu.VMEM((2, all_rows, HD), F32),
            pltpu.VMEM((all_rows, WIDE), BF),
            pltpu.VMEM((cols, width), F32),
            *[pltpu.VMEM((cols, width), BF)] * 2,
            *[pltpu.VMEM((width, 3 * WIDE), BF)] * 2,
            pltpu.VMEM((all_rows, cols), BF),
            *[pltpu.VMEM(up.shape, BF)] * 2,
            *[pltpu.VMEM(down.shape, BF)] * 2,
            pltpu.VMEM(gathered.shape, BF),
            pltpu.SemaphoreType.DMA((5,)),
            *transfer_sems(HALVES),
            *spread_scratch(up.shape, 1, 2),
            *spread_scratch(down.shape, 2, 0),
            *spread_scratch(down.shape, 2, 1)[:1],
            *spread_scratch((cols, width)),
            *spread_scratch((width, 3 * WIDE)),
            *hop_scratch(5, *small.shape),
        ],
        name="attend_back",
        compiler_params=comm_params(3),
    )(branch, out_weight, expon, inverse, q, k, v, attended, small, up, down, gathered)


def input_back_kernel(
    dq_ref, dk_ref, dv_ref, wq_ref, wk_ref, wv_ref, all_ref, r1_ref, wg_in, pg_in,
    x_ref, wg_ref, pg_ref, last_ref, bias_ref,
    out, land, mine, pending, send, recv, out_send, out_recv, pair_send, pair_recv,
    w_full, p_full, last_full, last_low, last_land, last_send, last_recv, value, bias_land, bias_send, bias_recv,
):
    rows_here = r1_ref.shape[0]
    size = rows_here // CHUNKS
    last = dq_ref.shape[1] - WIDE
    w_full[...] = wg_in[...]
    p_full[...] = pg_in[...]
    greet_all()
    reduce = Reduce(out, land, send, recv)
    out_sum = Spread(None, w_full, None, out_send, out_recv)
    pair_sum = Spread(None, p_full, None, pair_send, pair_recv)
    last_sum = Spread(last_low, last_full, last_land, last_send, last_recv)
    bias = Hops(value, bias_land, bias_send, bias_recv, [dp_peer(1), dp_peer(2), dp_peer(4)])
    pair_sum.gather_start(2)
    out_sum.gather_start(1)
    tail = pl.ds(last, WIDE)
    projection_grads(all_ref, (dq_ref.at[:, tail], dk_ref.at[:, tail], dv_ref.at[:, tail]), last_low)
    last_sum.reduce_start(0)
    grads = ((dq_ref, wq_ref), (dk_ref, wk_ref), (dv_ref, wv_ref))

    def part_of(starts, count):
        total = None
        for grad, weight in grads:
            pieces = [grad[pl.ds(pl.multiple_of(at, size), count)] for at in starts]
            x = pieces[0] if len(pieces) == 1 else jnp.concatenate(pieces, 0)
            term = mm(x, weight[...], 1, 1)
            total = term if total is None else total + term
        return total

    def chunk_rows(j):
        return pl.ds(pl.multiple_of(j * size, size), size)

    def far(j):
        part = part_of((2 * rows_here + j * size, 3 * rows_here + j * size), size)
        pending[chunk_rows(j)] = part[:size]
        reduce.post(PAIR, j, part[size:])

        @pl.when(j > 0)
        def _():
            reduce.forward_pair(j - 1, pending[chunk_rows(j - 1)])

    repeat(CHUNKS, far)
    reduce.forward_pair(CHUNKS - 1, pending[chunk_rows(CHUNKS - 1)])
    value[0, 0:1] = column_sum(dq_ref[...].astype(F32))
    value[0, 1:8] = jnp.broadcast_to(column_sum(dv_ref[...].astype(F32)), (7, dv_ref.shape[1]))
    bias.start(0)
    last_sum.reduce_finish(0)
    last_sum.reduce_start(1)

    def near(i):
        part = part_of((rows_here + i * 2 * size,), 2 * size)
        reduce.post(NEAR, 2 * i, part[:size])
        reduce.post(NEAR, 2 * i + 1, part[size:])

    repeat(2, near)

    def own(i):
        mine[pl.ds(pl.multiple_of(i * 2 * size, 2 * size), 2 * size)] = part_of((i * 2 * size,), 2 * size)

    repeat(2, own)

    def finish(j):
        rows = chunk_rows(j)
        x_ref[rows] = (r1_ref[rows] + reduce.total(j, mine[rows])).astype(BF)

    last_sum.reduce_finish(1)
    last_sum.reduce_start(2)
    pair_sum.gather_finish(2)
    pair_sum.gather_start(1)
    out_sum.gather_finish(1)
    out_sum.gather_start(0)
    bias.finish(0)
    bias.start(1)
    last_sum.reduce_finish(2)
    last_sum.gather_start(2)
    pair_sum.gather_finish(1)
    pair_sum.gather_start(0)
    bias.finish(1)
    bias.start(2)
    repeat(2, finish)
    last_sum.gather_finish(2)
    last_sum.gather_start(1)
    repeat(CHUNKS - 2, lambda j: finish(j + 2))
    last_sum.gather_finish(1)
    last_sum.gather_start(0)
    bias.finish(2)
    bias_ref[...] = value[3]
    out_sum.gather_finish(0)
    pair_sum.gather_finish(0)
    wg_ref[...] = w_full[...]
    pg_ref[...] = p_full[...]
    last_sum.gather_finish(0)
    last_ref[...] = last_full[...]
    reduce.drain()


def input_back(dq, dk, dv, wq, wk, wv, gathered, resid_grad, out_grad, pair_grad):
    rows, width = resid_grad.shape
    cols = dq.shape[1]
    return pl.pallas_call(
        input_back_kernel,
        in_specs=[WHOLE] * 10,
        out_specs=[WHOLE] * 5,
        out_shape=[
            shaped(rows, width),
            shaped(*out_grad.shape),
            shaped(*pair_grad.shape),
            shaped(*pair_grad.shape),
            shaped(8, cols, dtype=F32),
        ],
        scratch_shapes=[
            pltpu.VMEM((3, rows, width), BF),
            pltpu.VMEM((3, rows, width), BF),
            pltpu.VMEM((rows, width), F32),
            pltpu.VMEM((rows, width), F32),
            *transfer_sems(),
            *spread_scratch(out_grad.shape, 2, 0),
            *spread_scratch(pair_grad.shape, 2, 0),
            pltpu.VMEM(out_grad.shape, BF),
            *[pltpu.VMEM(pair_grad.shape, BF)] * 3,
            *spread_scratch(pair_grad.shape),
            *hop_scratch(3, 8, cols),
        ],
        name="input_back",
        compiler_params=comm_params(4),
    )(dq, dk, dv, wq, wk, wv, gathered, resid_grad, out_grad, pair_grad)


def per_device(
    tokens, lengths, query_weight, query_bias, key_weight, value_weight, value_bias, out_weight,
    out_bias, first_gain, first_shift, up_weight, up_bias, down_weight, down_bias, second_gain,
    second_shift, output_grad,
):
    pairs = query_weight.shape[1] // WIDE
    if (lax.axis_size("dp"), lax.axis_size("mp"), lengths.shape[1], pairs) != (8, 4, 1, 2):
        return per_device_general(
            tokens, lengths, query_weight, query_bias, key_weight, value_weight, value_bias,
            out_weight, out_bias, first_gain, first_shift, up_weight, up_bias, down_weight,
            down_bias, second_gain, second_shift, output_grad,
        )
    rows = tokens.shape[0]

    def as_row(vector):
        return vector.astype(F32)[None]

    q, k, v, vt, gathered = gather_project(
        tokens, query_weight, key_weight, value_weight, as_row(query_bias), as_row(value_bias)
    )
    relation = lax.iota(jnp.int32, 4)
    place = jnp.bitwise_xor(relation, lax.axis_index("mp"))[:, None] * rows + lax.iota(jnp.int32, rows)
    bias = jnp.where(place.reshape(-1, 1) < lengths[0, 0], 0.0, MASKED)
    expon, attended, inverse, normed, inv_std, hidden = attend(
        q, k, vt, bias, out_weight, tokens,
        jnp.stack([out_bias, first_gain, first_shift]).astype(F32),
    )
    layer_out, branch, resid_grad, up_grad, down_grad, small = feed_forward(
        hidden, normed, inv_std, output_grad, up_weight, as_row(up_bias), down_weight,
        jnp.stack([first_gain, first_shift, down_bias, second_gain, second_shift]).astype(F32),
    )
    dq, dk, dv, out_grad, pair_grad, small, up_grad, down_grad = attend_back(
        branch, out_weight, expon, inverse, q, k, v, attended, small, up_grad, down_grad, gathered
    )
    tokens_grad, out_grad, pair_grad, last_grad, bias_grads = input_back(
        dq, dk, dv, query_weight, key_weight, value_weight, gathered, resid_grad, out_grad, pair_grad
    )

    def joined(at):
        cols = slice(at * WIDE, (at + 1) * WIDE)
        return jnp.concatenate([pair_grad[:, cols], last_grad[:, cols]], 1).astype(F32)

    return (
        layer_out,
        tokens_grad,
        joined(0),
        bias_grads[0],
        joined(1),
        joined(2),
        bias_grads[1],
        out_grad.astype(F32),
        small[5],
        small[3],
        small[4],
        up_grad.astype(F32),
        small[6],
        down_grad.astype(F32),
        small[2],
        small[0],
        small[1],
    )


def solution(mesh):
    placed = (
        P(("dp", "mp"), None),
        P("dp", None),
        P(None, "mp"),
        P("mp"),
        P(None, "mp"),
        P(None, "mp"),
        P("mp"),
        P("mp", None),
        P(),
        P(),
        P(),
        P(None, "mp"),
        P("mp"),
        P("mp", None),
        P(),
        P(),
        P(),
        P(("dp", "mp"), None),
    )
    return jax.shard_map(
        per_device,
        mesh=mesh,
        in_specs=placed,
        out_specs=(
            P(("dp", "mp"), None),
            P(("dp", "mp"), None),
            P(None, "mp"),
            P("mp"),
            P(None, "mp"),
            P(None, "mp"),
            P("mp"),
            P("mp", None),
            P(),
            P(),
            P(),
            P(None, "mp"),
            P("mp"),
            P("mp", None),
            P(),
            P(),
            P(),
        ),
        check_vma=False,
    )
```

```python
from functools import partial

import jax
import jax.numpy as jnp
from jax import lax
from jax.experimental import pallas as pl
from jax.experimental.pallas import tpu as pltpu
from jax.sharding import PartitionSpec as P

HD = 64


epsilon = 1e-12


def norm_forward(resid, gain, shift):
    center = resid - jnp.mean(resid, -1, keepdims=True)
    inv_std = lax.rsqrt(jnp.mean(center * center, -1, keepdims=True) + epsilon)
    normed = center * inv_std
    return (normed * gain + shift, normed, inv_std)


def norm_backward(grad, normed, inv_std, gain):
    scaled = grad * gain
    back = inv_std * (
        scaled
        - jnp.mean(scaled, -1, keepdims=True)
        - normed * jnp.mean(scaled * normed, -1, keepdims=True)
    )
    return (back, jnp.sum(grad * normed, 0), jnp.sum(grad, 0))


F32 = jnp.float32
BF = jnp.bfloat16
MASKED = -1000000000.0
WIDE = 2 * HD


def mm(a, b, ca, cb):
    return lax.dot_general(a, b, (((ca,), (cb,)), ((), ())), preferred_element_type=F32)


def forward_kernel(heads, len_ref, q_ref, k_ref, vt_ref, e_ref, o_ref, r_ref, v_aug, k_aug):
    seq, step = pl.program_id(0), pl.program_id(2)
    seq_len, block = k_ref.shape[0], q_ref.shape[0]

    @pl.when(step == 0)
    def _():
        rows = lax.broadcasted_iota(jnp.int32, (seq_len, WIDE), 0)
        lanes = lax.broadcasted_iota(jnp.int32, (seq_len, WIDE), 1)
        bias = jnp.where(rows < len_ref[seq], 0.0, MASKED)
        keys = k_ref[...].astype(F32)
        for h in range(heads):
            other = (1 - h) * HD
            k_aug[h] = jnp.where(
                lanes // HD == h, keys, jnp.where(lanes == other, bias, 0.0)
            ).astype(BF)
            v_aug[h, :HD] = vt_ref[h * HD : (h + 1) * HD, :]
            v_aug[h, HD:] = jnp.ones((16, seq_len), BF)

    query = q_ref[...].astype(F32) * HD**-0.5
    lanes = lax.broadcasted_iota(jnp.int32, (block, WIDE), 1)
    scores = []
    for h in range(heads):
        other = (1 - h) * HD
        q_aug = jnp.where(
            lanes // HD == h, query, jnp.where(lanes == other, 1.0, 0.0)
        ).astype(BF)
        scores.append(mm(k_aug[h], q_aug, 1, 1))
    outs = []
    for h in range(heads):
        top = jnp.max(scores[h], 0, keepdims=True)
        expon = jnp.exp(scores[h] - top).astype(BF)
        e_ref[h] = expon
        total = mm(v_aug[h], expon, 1, 0)
        inverse = 1.0 / total[HD : HD + 1]
        r_ref[h] = inverse
        outs.append(total[:HD] * inverse)
    if heads == 1:
        outs.append(jnp.zeros_like(outs[0]))
    o_ref[...] = jnp.concatenate(outs, 0).T.astype(BF)


def backward_kernel(
    heads, e_ref, r_ref, q_ref, k_ref, v_ref, o_ref, g_ref, dq_ref, dk_ref, dv_ref, v_aug, k_t, dks, dvs
):
    step, last = pl.program_id(2), pl.num_programs(2) - 1
    seq_len, block = k_ref.shape[0], q_ref.shape[0]

    @pl.when(step == 0)
    def _():
        lanes = lax.broadcasted_iota(jnp.int32, (seq_len, WIDE), 1)
        values = v_ref[...].astype(F32)
        for h in range(heads):
            other = (1 - h) * HD
            ones = jnp.where((lanes >= other) & (lanes < other + 2), 1.0, 0.0)
            v_aug[h] = jnp.where(lanes // HD == h, values, ones).astype(BF)
        k_t[...] = (k_ref[...].astype(F32) * HD**-0.5).T.astype(BF)
        dks[...] = jnp.zeros_like(dks)
        dvs[...] = jnp.zeros_like(dvs)

    lanes = lax.broadcasted_iota(jnp.int32, (block, WIDE), 1)
    inverse = jnp.concatenate(
        [jnp.broadcast_to(r_ref[h % heads], (HD, block)) for h in range(2)], 0
    ).T
    grad = (g_ref[...].astype(F32) * inverse).astype(BF)
    grad_wide = grad.astype(F32)
    scaled_query = (q_ref[...].astype(F32) * HD**-0.5).astype(BF)
    product = grad_wide * o_ref[...].astype(F32)
    centered = []
    for h in range(heads):
        other = (1 - h) * HD
        inside = lanes // HD == h
        row_dot = jnp.sum(jnp.where(inside, product, 0.0), -1, keepdims=True)
        high = row_dot.astype(BF).astype(F32)
        g_aug = jnp.where(
            inside,
            grad_wide,
            jnp.where(lanes == other, -high, jnp.where(lanes == other + 1, high - row_dot, 0.0)),
        ).astype(BF)
        centered.append(mm(v_aug[h], g_aug, 1, 1))
    query_grads = []
    for h in range(heads):
        cols = slice(h * HD, (h + 1) * HD)
        expon = e_ref[h]
        score_grad = (expon.astype(F32) * centered[h]).astype(BF)
        dvs[h] += mm(expon, grad[:, cols], 1, 0)
        dks[h] += mm(score_grad, scaled_query[:, cols], 1, 0)
        query_grads.append(mm(k_t[cols, :], score_grad, 1, 0))
    if heads == 1:
        query_grads.append(jnp.zeros_like(query_grads[0]))
    dq_ref[...] = jnp.concatenate(query_grads, 0).T.astype(BF)

    @pl.when(step == last)
    def _():
        for total, out in ((dks, dk_ref), (dvs, dv_ref)):
            halves = [total[h] for h in range(heads)]
            if heads == 1:
                halves.append(jnp.zeros_like(halves[0]))
            out[...] = jnp.concatenate(halves, 1).astype(BF)


def attention_shape(rows, cols, seqs):
    seq_len = rows // seqs
    block = min(512, seq_len)
    steps = seq_len // block
    pairs = max(1, cols // WIDE)
    heads = cols // HD // pairs
    row_spec = pl.BlockSpec((block, WIDE), lambda s, p, j, *_: (s * steps + j, p))
    key_spec = pl.BlockSpec((seq_len, WIDE), lambda s, p, j, *_: (s, p))
    e_spec = pl.BlockSpec((heads, seq_len, block), lambda s, p, j, *_: (p, s, j))
    r_spec = pl.BlockSpec((heads, 1, block), lambda s, p, j, *_: (p, 0, s * steps + j))
    return seq_len, heads, pairs, (seqs, pairs, steps), row_spec, key_spec, e_spec, r_spec


def widen(array):
    short = WIDE - array.shape[1]
    return array if short <= 0 else jnp.pad(array, ((0, 0), (0, short)))


def attention_forward(queries, keys, values, lengths):
    rows, cols = queries.shape
    seqs = lengths.shape[0]
    seq_len, heads, pairs, grid, row_spec, key_spec, e_spec, r_spec = attention_shape(rows, cols, seqs)
    wide_cols = pairs * WIDE
    expon, attended, inverse = pl.pallas_call(
        partial(forward_kernel, heads),
        grid_spec=pltpu.PrefetchScalarGridSpec(
            num_scalar_prefetch=1,
            grid=grid,
            in_specs=[
                row_spec,
                key_spec,
                pl.BlockSpec((WIDE, seq_len), lambda s, p, j, *_: (p, s)),
            ],
            out_specs=[e_spec, row_spec, r_spec],
            scratch_shapes=[
                pltpu.VMEM((heads, HD + 16, seq_len), BF),
                pltpu.VMEM((heads, seq_len, WIDE), BF),
            ],
        ),
        out_shape=[
            jax.ShapeDtypeStruct((heads * pairs, rows, seq_len), BF),
            jax.ShapeDtypeStruct((rows, wide_cols), BF),
            jax.ShapeDtypeStruct((heads * pairs, 1, rows), F32),
        ],
        name="attention_forward",
        compiler_params=pltpu.CompilerParams(vmem_limit_bytes=60 * 1024 * 1024),
    )(lengths, widen(queries), widen(keys), widen(values).T)
    return expon, attended[:, :cols], inverse


def attention_backward(expon, inverse, queries, keys, values, attended, grad, seqs):
    rows, cols = queries.shape
    seq_len, heads, pairs, grid, row_spec, key_spec, e_spec, r_spec = attention_shape(rows, cols, seqs)
    shape = jax.ShapeDtypeStruct((rows, pairs * WIDE), BF)
    outs = pl.pallas_call(
        partial(backward_kernel, heads),
        grid=grid,
        in_specs=[e_spec, r_spec, row_spec, key_spec, key_spec, row_spec, row_spec],
        out_specs=[row_spec, key_spec, key_spec],
        scratch_shapes=[
            pltpu.VMEM((heads, seq_len, WIDE), BF),
            pltpu.VMEM((WIDE, seq_len), BF),
            pltpu.VMEM((heads, seq_len, HD), F32),
            pltpu.VMEM((heads, seq_len, HD), F32),
        ],
        out_shape=[shape] * 3,
        name="attention_backward",
        compiler_params=pltpu.CompilerParams(vmem_limit_bytes=60 * 1024 * 1024),
    )(expon, inverse, *[widen(x) for x in (queries, keys, values, attended, grad)])
    return [x[:, :cols] for x in outs]


def contract_rows(left, right):
    return lax.dot_general(
        left, right, (((0,), (0,)), ((), ())), preferred_element_type=jnp.float32
    )


def contract_cols(left, right):
    return lax.dot_general(
        left, right, (((1,), (1,)), ((), ())), preferred_element_type=jnp.float32
    )


def split_projection(projected, width, q_bias, v_bias):
    query_part = (projected[:, :width] + q_bias).astype(jnp.bfloat16)
    key_part = projected[:, width : 2 * width].astype(jnp.bfloat16)
    value_part = (projected[:, 2 * width :] + v_bias).astype(jnp.bfloat16)
    return (query_part, key_part, value_part)


def per_device_general(
    tokens,
    lengths,
    query_weight,
    query_bias,
    key_weight,
    value_weight,
    value_bias,
    out_weight,
    out_bias,
    first_gain,
    first_shift,
    up_weight,
    up_bias,
    down_weight,
    down_bias,
    second_gain,
    second_shift,
    output_grad,
):
    local_rows = tokens.shape[0]
    head_cols = query_weight.shape[1]
    seq_count = lengths.shape[1]
    all_rows = local_rows * lax.axis_size("mp")
    gathered = lax.all_gather(tokens, "mp", axis=0, tiled=True)
    joint_weight = jnp.concatenate([query_weight, key_weight, value_weight], 1)
    projected = jnp.dot(gathered, joint_weight, preferred_element_type=jnp.float32)
    queries, key_rows, values = split_projection(projected, head_cols, query_bias, value_bias)
    expon, attended, inverse = attention_forward(queries, key_rows, values, lengths[0])
    branch_one = lax.psum_scatter(
        jnp.dot(
            lax.slice_in_dim(attended, 0, local_rows * lax.axis_size("mp"), axis=0),
            out_weight,
            preferred_element_type=jnp.float32,
        ).astype(jnp.bfloat16),
        "mp",
        scatter_dimension=0,
        tiled=True,
    ).astype(jnp.float32)
    hidden, normed_one, inv_one = norm_forward(
        tokens.astype(jnp.float32) + branch_one + out_bias, first_gain, first_shift
    )
    hidden_low = hidden.astype(jnp.bfloat16)
    hidden_all = lax.all_gather(hidden_low, "mp", axis=0, tiled=True)
    pre_act = jnp.dot(hidden_all, up_weight, preferred_element_type=jnp.float32) + up_bias
    act_low = jax.nn.gelu(pre_act, approximate=False).astype(jnp.bfloat16)
    branch_two = lax.psum_scatter(
        jnp.dot(
            lax.slice_in_dim(act_low, 0, local_rows * lax.axis_size("mp"), axis=0),
            down_weight,
            preferred_element_type=jnp.float32,
        ).astype(jnp.bfloat16),
        "mp",
        scatter_dimension=0,
        tiled=True,
    ).astype(jnp.float32)
    layer_out, normed_two, inv_two = norm_forward(
        hidden + branch_two + down_bias, second_gain, second_shift
    )
    resid_two_grad, second_gain_grad, second_shift_grad = norm_backward(
        output_grad.astype(jnp.float32), normed_two, inv_two, second_gain
    )
    down_bias_grad = jnp.sum(resid_two_grad, 0)
    branch_two_low = resid_two_grad.astype(jnp.bfloat16)
    row_piece = lax.all_gather(branch_two_low, "mp", axis=0, tiled=True)
    row_start = jnp.int32(0)
    weight_acc = jnp.zeros(down_weight.shape, jnp.float32)
    act_acc = jnp.zeros(act_low.shape, jnp.float32)
    act_rows = lax.dynamic_slice_in_dim(act_low, row_start, row_piece.shape[0], 0)
    weight_acc = weight_acc + contract_rows(act_rows, row_piece)
    act_acc = lax.dynamic_update_slice_in_dim(
        act_acc, contract_cols(row_piece, down_weight), row_start, 0
    )
    down_weight_grad = weight_acc
    unused_two, gelu_back = jax.vjp(partial(jax.nn.gelu, approximate=False), pre_act)
    pre_grad = gelu_back(act_acc)[0].astype(jnp.bfloat16)
    up_bias_grad = jnp.sum(pre_grad, 0, dtype=jnp.float32)
    up_weight_grad = contract_rows(hidden_all, pre_grad)
    hidden_back = lax.psum_scatter(
        contract_cols(
            lax.slice_in_dim(pre_grad, 0, local_rows * lax.axis_size("mp"), axis=0), up_weight
        ).astype(jnp.bfloat16),
        "mp",
        scatter_dimension=0,
        tiled=True,
    ).astype(jnp.float32)
    hidden_grad = resid_two_grad + hidden_back
    resid_one_grad, first_gain_grad, first_shift_grad = norm_backward(
        hidden_grad, normed_one, inv_one, first_gain
    )
    out_bias_grad = jnp.sum(resid_one_grad, 0)
    branch_one_low = resid_one_grad.astype(jnp.bfloat16)
    row_piece = lax.all_gather(branch_one_low, "mp", axis=0, tiled=True)
    row_start = jnp.int32(0)
    weight_acc = jnp.zeros(out_weight.shape, jnp.float32)
    attn_acc = jnp.zeros(attended.shape, jnp.float32)
    attn_rows = lax.dynamic_slice_in_dim(attended, row_start, row_piece.shape[0], 0)
    weight_acc = weight_acc + contract_rows(attn_rows, row_piece)
    attn_acc = lax.dynamic_update_slice_in_dim(
        attn_acc, contract_cols(row_piece, out_weight), row_start, 0
    )
    out_weight_grad = weight_acc
    attn_low = attn_acc.astype(jnp.bfloat16)
    query_flat, key_flat, value_flat = attention_backward(
        expon, inverse, queries, key_rows, values, attended, attn_low, seq_count
    )
    width_now = query_flat.shape[1]
    joint_grad = jnp.concatenate([query_flat, key_flat, value_flat], 1)
    query_bias_grad = jnp.sum(query_flat, 0, dtype=jnp.float32)
    value_bias_grad = jnp.sum(value_flat, 0, dtype=jnp.float32)
    joint_weight_grad = contract_rows(gathered, joint_grad)
    input_back = lax.psum_scatter(
        contract_cols(
            lax.slice_in_dim(joint_grad, 0, local_rows * lax.axis_size("mp"), axis=0), joint_weight
        ).astype(jnp.bfloat16),
        "mp",
        scatter_dimension=0,
        tiled=True,
    ).astype(jnp.float32)
    tokens_grad = (resid_one_grad + input_back).astype(jnp.bfloat16)
    query_weight_grad = joint_weight_grad[:, :width_now]
    key_weight_grad = joint_weight_grad[:, width_now : 2 * width_now]
    value_weight_grad = joint_weight_grad[:, 2 * width_now :]
    (
        query_weight_grad,
        query_bias_grad,
        key_weight_grad,
        value_weight_grad,
        value_bias_grad,
        out_weight_grad,
        up_weight_grad,
        up_bias_grad,
        down_weight_grad,
    ) = (
        lax.psum(query_weight_grad.astype(jnp.bfloat16), "dp").astype(jnp.float32),
        lax.psum(query_bias_grad.astype(jnp.bfloat16), "dp").astype(jnp.float32),
        lax.psum(key_weight_grad.astype(jnp.bfloat16), "dp").astype(jnp.float32),
        lax.psum(value_weight_grad.astype(jnp.bfloat16), "dp").astype(jnp.float32),
        lax.psum(value_bias_grad.astype(jnp.bfloat16), "dp").astype(jnp.float32),
        lax.psum(out_weight_grad.astype(jnp.bfloat16), "dp").astype(jnp.float32),
        lax.psum(up_weight_grad.astype(jnp.bfloat16), "dp").astype(jnp.float32),
        lax.psum(up_bias_grad.astype(jnp.bfloat16), "dp").astype(jnp.float32),
        lax.psum(down_weight_grad.astype(jnp.bfloat16), "dp").astype(jnp.float32),
    )
    (
        out_bias_grad,
        first_gain_grad,
        first_shift_grad,
        down_bias_grad,
        second_gain_grad,
        second_shift_grad,
    ) = lax.psum(
        (
            out_bias_grad,
            first_gain_grad,
            first_shift_grad,
            down_bias_grad,
            second_gain_grad,
            second_shift_grad,
        ),
        ("dp", "mp"),
    )
    return (
        layer_out.astype(jnp.bfloat16),
        tokens_grad,
        query_weight_grad,
        query_bias_grad,
        key_weight_grad,
        value_weight_grad,
        value_bias_grad,
        out_weight_grad,
        out_bias_grad,
        first_gain_grad,
        first_shift_grad,
        up_weight_grad,
        up_bias_grad,
        down_weight_grad,
        down_bias_grad,
        second_gain_grad,
        second_shift_grad,
    )


MESH = pl.DeviceIdType.MESH
VMEM_BYTES = 63 * 1024 * 1024
CHUNKS = 4
KINDS = "HBHB"
JOBS = len(KINDS)


def flip(index, bit):
    low = index // bit % 2
    return index + bit * (1 - 2 * low)


def mp_peer(relation):
    dp, mp = lax.axis_index("dp"), lax.axis_index("mp")
    for bit in (1, 2):
        if relation // bit % 2:
            mp = flip(mp, bit)
    return (dp, mp)


def dp_peer(bit):
    return (flip(lax.axis_index("dp"), bit), lax.axis_index("mp"))


def greet(peers):
    barrier = pltpu.get_barrier_semaphore()
    for device in peers:
        pl.semaphore_signal(barrier, inc=1, device_id=device, device_id_type=MESH)
    pl.semaphore_wait(barrier, len(peers))


def remote(src, dst, send, recv, device):
    return pltpu.make_async_remote_copy(
        src_ref=src, dst_ref=dst, send_sem=send, recv_sem=recv, device_id=device, device_id_type=MESH
    )


def repeat(count, body):
    def step(i, carry):
        body(i)
        return carry

    lax.fori_loop(0, count, step, 0)


class Gather:
    def __init__(self, own, land, send, recv, chunks=CHUNKS):
        self.own, self.land, self.send, self.recv, self.chunks = own, land, send, recv, chunks
        self.size = own.shape[0] // chunks

    def copy(self, relation, j):
        rows = pl.ds(j * self.size, self.size)
        src = self.land.at[1, rows] if relation == 3 else self.own.at[rows]
        return remote(
            src,
            self.land.at[relation - 1, rows],
            self.send.at[relation - 1, j],
            self.recv.at[relation - 1, j],
            mp_peer(2 if relation == 2 else 1),
        )

    def start(self, j):
        self.copy(2, j).start()
        self.copy(1, j).start()

    def arrive(self, relation, j):
        self.copy(relation, j).wait_recv()
        if relation == 2:
            self.copy(3, j).start()

    def drain(self):
        def body(j):
            for relation in (1, 2, 3):
                self.copy(relation, j).wait_send()

        repeat(self.chunks, body)


PAIR, FAR, NEAR = 0, 1, 2


class Reduce:
    def __init__(self, out, land, send, recv, chunks=CHUNKS):
        self.out, self.land, self.send, self.recv, self.chunks = out, land, send, recv, chunks
        self.size = out.shape[1] // chunks

    def copy(self, kind, j):
        rows = pl.ds(j * self.size, self.size)
        return remote(
            self.out.at[kind, rows],
            self.land.at[kind, rows],
            self.send.at[kind, j],
            self.recv.at[kind, j],
            mp_peer(2 if kind == FAR else 1),
        )

    def post(self, kind, j, value):
        self.out[kind, pl.ds(j * self.size, self.size)] = value.astype(BF)
        self.copy(kind, j).start()

    def forward_pair(self, j, mine):
        self.copy(PAIR, j).wait_recv()
        rows = pl.ds(j * self.size, self.size)
        self.post(FAR, j, mine + self.land[PAIR, rows].astype(F32))

    def total(self, j, mine):
        self.copy(NEAR, j).wait_recv()
        self.copy(FAR, j).wait_recv()
        rows = pl.ds(j * self.size, self.size)
        return mine + self.land[NEAR, rows].astype(F32) + self.land[FAR, rows].astype(F32)

    def drain(self):
        def body(j):
            for kind in (PAIR, FAR, NEAR):
                self.copy(kind, j).wait_send()

        repeat(self.chunks, body)


ROUTES = {"H": "xlh", "B": "lxh"}


class Spread:
    def __init__(self, data, full, land, send, recv, kinds, first=0, last=3):
        self.data, self.full, self.land, self.send, self.recv = data, full, land, send, recv
        self.sums, self.hands = first < 2, last > 1
        self.kinds, self.jobs = kinds, len(kinds)
        self.count = (full if data is None else data).shape[0] // self.jobs

    def route(self, job):
        return ROUTES[self.kinds[job if isinstance(job, int) else 0]]

    def side(self, axis):
        dp = lax.axis_index("dp")
        return {"x": dp % 2, "z": dp // 2, "l": dp // 2 % 2, "h": dp // 4}[axis]

    def range_of(self, start, size):
        return pl.ds(pl.multiple_of(start, size), size)

    def place(self, job, level):
        start, size = job * self.count, self.count
        for axis in self.route(job)[:level]:
            size //= 4 if axis == "z" else 2
            start += self.side(axis) * size
        return start, size

    def landing(self, job, stage, k=1):
        at, size = 0, self.count
        for level in range(stage + 1):
            ways = 4 if self.route(job)[level] == "z" else 2
            size //= ways
            if level < stage:
                at += size * (ways - 1)
        return self.land.at[job, pl.ds(at + (k - 1) * size, size)]

    def copies(self, job, stage):
        dp, mp = lax.axis_index("dp"), lax.axis_index("mp")
        levels = len(self.route(job))
        back = stage >= levels
        level = 2 * levels - 1 - stage if back else stage
        start, size = self.place(job, level)
        axis = self.route(job)[level]
        here = self.side(axis)
        ways, step = (4, 2) if axis == "z" else (2, {"x": 1, "l": 2, "h": 4}[axis])
        found = []
        for k in range(1, ways):
            there = (here + k) % ways
            if back:
                src = dst = self.full.at[self.range_of(*self.place(job, level + 1))]
            else:
                src = self.data.at[self.range_of(start + there * (size // ways), size // ways)]
                dst = self.landing(job, level, k)
            at = (job, stage * 3 + k - 1)
            device = (dp + (there - here) * step, mp)
            found.append(remote(src, dst, self.send.at[at], self.recv.at[at], device))
        return found

    def own(self, job):
        return self.range_of(*self.place(job, len(self.route(job))))

    def stages(self, job):
        levels = len(self.route(job))
        return (0 if self.sums else levels), (2 * levels if self.hands else levels)

    def step(self, job, stage):
        first, end = self.stages(job)
        levels = len(self.route(job))
        if stage > first:
            arrived = self.copies(job, stage - 1)
            for done in arrived:
                done.wait_send()
                done.wait_recv()
            if stage <= levels:
                rows = self.range_of(*self.place(job, stage))
                total = self.data[rows].astype(F32)
                for k in range(len(arrived)):
                    total += self.landing(job, stage - 1, k + 1)[...].astype(F32)
                target = self.full if stage == levels and self.full is not None else self.data
                target[rows] = total.astype(BF)
        if stage < end:
            for copy in self.copies(job, stage):
                copy.start()


def advance(*moves):
    for total, jobs, stage in moves:
        for job in jobs if isinstance(jobs, tuple) else (jobs,):
            total.step(job, stage)


def spread_land(data, kinds):
    count = data[0] // len(kinds)
    return pltpu.VMEM((len(kinds), count - count // 8, data[1]), BF)


def spread_sems(kinds):
    return [pltpu.SemaphoreType.DMA((len(kinds), 18)), pltpu.SemaphoreType.DMA((len(kinds), 18))]


class Hops:
    def __init__(self, value, land, send, recv, peers):
        self.value, self.land, self.send, self.recv, self.peers = value, land, send, recv, peers

    def copy(self, i):
        return remote(
            self.value.at[i], self.land.at[i], self.send.at[i], self.recv.at[i], self.peers[i]
        )

    def start(self, i):
        self.copy(i).start()

    def finish(self, i):
        self.copy(i).wait_recv()
        self.value[i + 1] = self.value[i] + self.land[i]
        self.copy(i).wait_send()


def hop_scratch(count, *shape):
    return [
        pltpu.VMEM((count + 1, *shape), F32),
        pltpu.VMEM((count, *shape), F32),
        pltpu.SemaphoreType.DMA((count,)),
        pltpu.SemaphoreType.DMA((count,)),
    ]


def greet_all():
    dp, mp = lax.axis_index("dp"), lax.axis_index("mp")
    across = [((dp // 2 + k) % 4 * 2 + dp % 2, mp) for k in (1, 2, 3)]
    greet([mp_peer(1), mp_peer(2), dp_peer(1), *across])


def transfer_sems(chunks=CHUNKS):
    return [pltpu.SemaphoreType.DMA((3, chunks)), pltpu.SemaphoreType.DMA((3, chunks))]


def comm_params(collective_id):
    return pltpu.CompilerParams(
        collective_id=collective_id, has_side_effects=True, vmem_limit_bytes=VMEM_BYTES
    )


WHOLE = pl.BlockSpec(memory_space=pltpu.VMEM)


def shaped(*shape, dtype=None):
    return jax.ShapeDtypeStruct(shape, dtype or BF)


def as_row(ref):
    return ref[...].astype(F32)[None]


def column_sum(value):
    return jnp.sum(value, 0, keepdims=True)


def row_mean(value):
    return jnp.mean(value, -1, keepdims=True)


def project_kernel(
    x_ref, wq_ref, wk_ref, wv_ref, qb_ref, vb_ref, q_ref, k_ref, v_ref, vt_ref, all_ref, land, send, recv, save
):
    rows_here = x_ref.shape[0]
    greet([mp_peer(1), mp_peer(2)])
    gather = Gather(x_ref, land, send, recv)
    repeat(CHUNKS, gather.start)
    size = gather.size

    def emit(x, at):
        rows = pl.ds(at, x.shape[0])
        q = (mm(x, wq_ref[...], 1, 0) + as_row(qb_ref)).astype(BF)
        q_ref[rows] = (q.astype(F32) * HD**-0.5).astype(BF)
        k_ref[rows] = mm(x, wk_ref[...], 1, 0).astype(BF)
        v = mm(x, wv_ref[...], 1, 0) + as_row(vb_ref)
        v_ref[rows] = v.astype(BF)
        vt_ref[:, rows] = v.T.astype(BF)

    stores = [pltpu.make_async_copy(x_ref, all_ref.at[0], save.at[0])]
    stores[0].start()
    for i in range(2):
        emit(x_ref[pl.ds(i * 2 * size, 2 * size)], i * 2 * size)
    for i in range(2):
        gather.arrive(1, 2 * i)
        gather.arrive(1, 2 * i + 1)
        emit(land[0, pl.ds(i * 2 * size, 2 * size)], rows_here + i * 2 * size)
    stores.append(pltpu.make_async_copy(land.at[0], all_ref.at[1], save.at[1]))
    stores[-1].start()
    for j in range(CHUNKS):
        gather.arrive(2, j)
        gather.arrive(3, j)
        rows = pl.ds(j * size, size)
        for s in (2, 3):
            stores.append(
                pltpu.make_async_copy(
                    land.at[s - 1, rows], all_ref.at[s, rows], save.at[2 * j + s]
                )
            )
            stores[-1].start()
            emit(land[s - 1, rows], s * rows_here + j * size)
    gather.drain()
    for store in stores:
        store.wait()


def gather_project(tokens, wq, wk, wv, q_bias, v_bias):
    rows, width = tokens.shape
    cols = wq.shape[1]
    return pl.pallas_call(
        project_kernel,
        in_specs=[WHOLE] * 6,
        out_specs=[WHOLE] * 4 + [pl.BlockSpec(memory_space=pl.ANY)],
        out_shape=[shaped(4 * rows, cols)] * 3 + [shaped(cols, 4 * rows), shaped(4, rows, width)],
        scratch_shapes=[
            pltpu.VMEM((3, rows, width), BF),
            *transfer_sems(),
            pltpu.SemaphoreType.DMA((2 * CHUNKS + 2,)),
        ],
        name="gather_project",
        compiler_params=comm_params(0),
    )(tokens, wq, wk, wv, q_bias, v_bias)


HALVES = 2


def forward_order(step):
    far = 2 * (3 - step % 2) + step // 2
    near = 2 * (1 - (step - 4) // 2) + step % 2
    return jnp.where(step < 4, far, near)


def attend_kernel(
    len_ref, q_ref, k_ref, vt_ref, w_ref, x_ref, ob_ref, gain_ref, shift_ref,
    e_ref, o_ref, r_ref, n_ref, i_ref, h_ref,
    k_aug, v_aug, out, land, mine, pending, send, recv,
):
    step = pl.program_id(0)
    seq_len, block = k_ref.shape[0], q_ref.shape[0]
    pairs = k_ref.shape[1] // WIDE
    reduce = Reduce(out, land, send, recv, HALVES)

    @pl.when(step == 0)
    def _():
        greet([mp_peer(1), mp_peer(2)])
        lanes = lax.broadcasted_iota(jnp.int32, (seq_len, WIDE), 1)
        rows = lax.broadcasted_iota(jnp.int32, (x_ref.shape[0], WIDE), 0)
        bias = jnp.concatenate(
            [
                jnp.where(rows + mp_peer(s)[1] * x_ref.shape[0] < len_ref[0, 0], 0.0, MASKED)
                for s in range(4)
            ],
            0,
        )
        for p in range(pairs):
            keys = k_ref[:, p * WIDE : (p + 1) * WIDE].astype(F32)
            for h in range(2):
                other = (1 - h) * HD
                k_aug[2 * p + h] = jnp.where(
                    lanes // HD == h, keys, jnp.where(lanes == other, bias, 0.0)
                ).astype(BF)
                at = (2 * p + h) * HD
                v_aug[2 * p + h, :HD] = vt_ref[at : at + HD, :]
                v_aug[2 * p + h, HD:] = jnp.ones((16, seq_len), BF)

    lanes = lax.broadcasted_iota(jnp.int32, (block, WIDE), 1)
    outs = []
    for p in range(pairs):
        query = q_ref[:, p * WIDE : (p + 1) * WIDE].astype(F32)
        scores = []
        for h in range(2):
            other = (1 - h) * HD
            q_aug = jnp.where(
                lanes // HD == h, query, jnp.where(lanes == other, 1.0, 0.0)
            ).astype(BF)
            scores.append(mm(k_aug[2 * p + h], q_aug, 1, 1))
        for h in range(2):
            top = jnp.max(scores[h], 0, keepdims=True)
            expon = jnp.exp(scores[h] - top).astype(BF)
            e_ref[0, 2 * p + h] = expon
            total = mm(v_aug[2 * p + h], expon, 1, 0)
            inverse = 1.0 / total[HD : HD + 1]
            r_ref[0, 2 * p + h] = inverse
            outs.append(total[:HD] * inverse)
    attended = jnp.concatenate(outs, 0).T.astype(BF)
    o_ref[...] = attended
    partial_rows = mm(attended, w_ref[...], 1, 0)

    for t in range(4 * HALVES):

        @pl.when(step == t)
        def _(t=t):
            if t < 4 and t % 2 == 0:
                reduce.post(PAIR, t // 2, partial_rows)
            elif t < 4:
                pending[...] = partial_rows
                reduce.forward_pair(t // 2, pending[...])
            elif t < 6:
                reduce.post(NEAR, t - 4, partial_rows)
            else:
                mine[pl.ds((t - 6) * block, block)] = partial_rows

    @pl.when(step == 4 * HALVES - 1)
    def _():
        for j in range(HALVES):
            rows = pl.ds(j * block, block)
            resid = x_ref[rows].astype(F32) + reduce.total(j, mine[rows]) + as_row(ob_ref)
            center = resid - row_mean(resid)
            inv_std = lax.rsqrt(row_mean(center * center) + epsilon)
            normed = center * inv_std
            n_ref[rows] = normed
            i_ref[rows] = inv_std
            h_ref[rows] = (normed * as_row(gain_ref) + as_row(shift_ref)).astype(BF)
        reduce.drain()


def attend(lengths, q, k, vt, out_weight, tokens, *vectors):
    all_rows, cols = q.shape
    rows, width = tokens.shape
    block = rows // HALVES
    heads = cols // HD
    steps = all_rows // block

    def fixed(*shape):
        return pl.BlockSpec(shape, lambda i: (0,) * len(shape))

    return pl.pallas_call(
        attend_kernel,
        grid=(steps,),
        in_specs=[
            pl.BlockSpec(memory_space=pltpu.SMEM),
            pl.BlockSpec((block, cols), lambda i: (forward_order(i), 0)),
            fixed(all_rows, cols),
            fixed(cols, all_rows),
            fixed(cols, width),
            fixed(rows, width),
            *[fixed(width)] * 3,
        ],
        out_specs=[
            pl.BlockSpec((1, heads, all_rows, block), lambda i: (forward_order(i), 0, 0, 0)),
            pl.BlockSpec((block, cols), lambda i: (forward_order(i), 0)),
            pl.BlockSpec((1, heads, 1, block), lambda i: (forward_order(i), 0, 0, 0)),
            fixed(rows, width),
            fixed(rows, 1),
            fixed(rows, width),
        ],
        out_shape=[
            shaped(steps, heads, all_rows, block),
            shaped(all_rows, cols),
            shaped(steps, heads, 1, block, dtype=F32),
            shaped(rows, width, dtype=F32),
            shaped(rows, 1, dtype=F32),
            shaped(rows, width),
        ],
        scratch_shapes=[
            pltpu.VMEM((heads, all_rows, WIDE), BF),
            pltpu.VMEM((heads, HD + 16, all_rows), BF),
            pltpu.VMEM((3, rows, width), BF),
            pltpu.VMEM((3, rows, width), BF),
            pltpu.VMEM((rows, width), F32),
            pltpu.VMEM((block, width), F32),
            *transfer_sems(HALVES),
        ],
        name="attend",
        compiler_params=comm_params(1),
    )(lengths, q, k, vt, out_weight, tokens, *vectors)


ROOT_HALF = 0.7071067811865476
ROOT_TAU = 0.3989422804014327


def feed_forward_kernel(
    h_ref, n_ref, i_ref, g_ref, up_ref, ub_ref, down_ref, *refs
):
    vectors, refs = refs[:5], refs[5:]
    (
        out_ref, b1_ref, r1_ref, upg_ref, downg_ref, small_ref,
        land_h, act, slope, branch, land_b, out1, land1, out2, land2, mine, pending, r2,
        gs1, gr1, gs2, gr2, rs1, rr1, rs2, rr2,
        down_land, down_send, down_recv,
    ) = refs
    rows_here, width = h_ref.shape
    size = rows_here // CHUNKS
    first_gain, first_shift, down_bias, second_gain, second_shift = map(as_row, vectors)
    greet_all()
    down_sum = Spread(downg_ref, None, down_land, down_send, down_recv, KINDS, 0, 1)
    gather1, gather2 = Gather(h_ref, land_h, gs1, gr1), Gather(branch, land_b, gs2, gr2)
    reduce1, reduce2 = Reduce(out1, land1, rs1, rr1), Reduce(out2, land2, rs2, rr2)
    repeat(CHUNKS, gather1.start)
    small_ref[...] = jnp.zeros_like(small_ref)

    def forward(x):
        pre = mm(x, up_ref[...], 1, 0) + as_row(ub_ref)
        cdf = 0.5 + 0.5 * lax.erf(pre * ROOT_HALF)
        active = (pre * cdf).astype(BF)
        steep = (cdf + pre * jnp.exp(-0.5 * pre * pre) * ROOT_TAU).astype(BF)
        return active, steep, mm(active, down_ref[...], 1, 0)

    def backward(grad, steep):
        pre_grad = (mm(grad, down_ref[...], 1, 1) * steep.astype(F32)).astype(BF)
        small_ref[6:7] += column_sum(pre_grad.astype(F32))
        return pre_grad, mm(pre_grad, up_ref[...], 1, 1)

    def chunk_rows(j):
        return pl.ds(pl.multiple_of(j * size, size), size)

    def double_rows(j):
        return pl.ds(pl.multiple_of(j * 2 * size, 2 * size), 2 * size)

    def halves(value):
        return value[:size], value[size:]

    def own_forward(i):
        rows = double_rows(i)
        act[0, rows], slope[0, rows], mine[rows] = forward(h_ref[rows])

    def near_forward(i):
        gather1.arrive(1, 2 * i)
        gather1.arrive(1, 2 * i + 1)
        rows = double_rows(i)
        act[1, rows], slope[1, rows], part = forward(land_h[0, rows])
        for k, half in enumerate(halves(part)):
            reduce1.post(NEAR, 2 * i + k, half)

    def far_forward(j):
        gather1.arrive(2, j)
        gather1.arrive(3, j)
        rows = chunk_rows(j)
        active, steep, part = forward(jnp.concatenate([land_h[1, rows], land_h[2, rows]], 0))
        for s in (2, 3):
            act[s, rows] = halves(active)[s - 2]
            slope[s, rows] = halves(steep)[s - 2]
        pending[rows] = part[:size]
        reduce1.post(PAIR, j, part[size:])

        @pl.when(j > 0)
        def _():
            reduce1.forward_pair(j - 1, pending[chunk_rows(j - 1)])

    repeat(2, own_forward)
    repeat(2, near_forward)
    repeat(CHUNKS, far_forward)
    reduce1.forward_pair(CHUNKS - 1, pending[chunk_rows(CHUNKS - 1)])

    def second_norm(j):
        rows = chunk_rows(j)
        hidden = n_ref[rows] * first_gain + first_shift
        resid = hidden + reduce1.total(j, mine[rows]) + down_bias
        center = resid - row_mean(resid)
        inv_std = lax.rsqrt(row_mean(center * center) + epsilon)
        normed = center * inv_std
        out_ref[rows] = (normed * second_gain + second_shift).astype(BF)
        grad = g_ref[rows].astype(F32)
        product = grad * normed
        small_ref[0:1] += column_sum(product)
        small_ref[1:2] += column_sum(grad)
        scaled = grad * second_gain
        back = inv_std * (scaled - row_mean(scaled) - normed * row_mean(scaled * normed))
        small_ref[2:3] += column_sum(back)
        r2[rows] = back
        branch[rows] = back.astype(BF)
        gather2.start(j)

    repeat(CHUNKS, second_norm)

    def own_backward(i):
        rows = double_rows(i)
        slope[0, rows], mine[rows] = backward(branch[rows], slope[0, rows])

    def near_backward(i):
        gather2.arrive(1, 2 * i)
        gather2.arrive(1, 2 * i + 1)
        rows = double_rows(i)
        slope[1, rows], part = backward(land_b[0, rows], slope[1, rows])
        for k, half in enumerate(halves(part)):
            reduce2.post(NEAR, 2 * i + k, half)

    def far_backward(j):
        gather2.arrive(2, j)
        gather2.arrive(3, j)
        rows = chunk_rows(j)
        pre_grad, part = backward(
            jnp.concatenate([land_b[1, rows], land_b[2, rows]], 0),
            jnp.concatenate([slope[2, rows], slope[3, rows]], 0),
        )
        for s in (2, 3):
            slope[s, rows] = halves(pre_grad)[s - 2]
        pending[rows] = part[:size]
        reduce2.post(PAIR, j, part[size:])

        @pl.when(j > 0)
        def _():
            reduce2.forward_pair(j - 1, pending[chunk_rows(j - 1)])

    repeat(2, own_backward)
    repeat(2, near_backward)
    repeat(CHUNKS, far_backward)
    reduce2.forward_pair(CHUNKS - 1, pending[chunk_rows(CHUNKS - 1)])

    tile = 256

    def down_grad(t):
        cols = pl.ds(pl.multiple_of(t * tile, tile), tile)
        total = mm(act[0, :, cols], branch[...], 0, 0)
        for s in (1, 2, 3):
            total += mm(act[s, :, cols], land_b[s - 1], 0, 0)
        downg_ref[cols] = total.astype(BF)

    def up_grad(t):
        cols = pl.ds(pl.multiple_of(t * tile, tile), tile)
        total = mm(h_ref[:, cols], slope[0], 0, 0)
        for s in (1, 2, 3):
            total += mm(land_h[s - 1, :, cols], slope[s], 0, 0)
        upg_ref[cols] = total.astype(BF)

    for job in range(JOBS):
        down_grad(job)
        down_sum.step(job, 0)
    repeat(width // tile, up_grad)

    def first_norm(j):
        rows = chunk_rows(j)
        normed = n_ref[rows]
        grad = r2[rows] + reduce2.total(j, mine[rows])
        small_ref[3:4] += column_sum(grad * normed)
        small_ref[4:5] += column_sum(grad)
        scaled = grad * first_gain
        back = i_ref[rows] * (scaled - row_mean(scaled) - normed * row_mean(scaled * normed))
        small_ref[5:6] += column_sum(back)
        r1_ref[rows] = back
        b1_ref[rows] = back.astype(BF)

    advance((down_sum, (0, 1), 1))
    first_norm(0)
    advance((down_sum, (2, 3), 1))
    first_norm(1)
    advance((down_sum, (0, 1), 2))
    first_norm(2)
    advance((down_sum, (2, 3), 2))
    first_norm(3)
    advance((down_sum, (0, 1, 2, 3), 3))
    for transfer in (gather1, gather2, reduce1, reduce2):
        transfer.drain()


def feed_forward(hidden, normed, inv_std, output_grad, up, up_bias, down, *vectors):
    rows, width = hidden.shape
    units = up.shape[1]
    tall = (4, rows, units)
    return pl.pallas_call(
        feed_forward_kernel,
        in_specs=[WHOLE] * 12,
        out_specs=[WHOLE] * 6,
        out_shape=[
            shaped(rows, width),
            shaped(rows, width),
            shaped(rows, width, dtype=F32),
            shaped(width, units),
            shaped(units, width),
            shaped(8, width, dtype=F32),
        ],
        scratch_shapes=[
            pltpu.VMEM((3, rows, width), BF),
            pltpu.VMEM(tall, BF),
            pltpu.VMEM(tall, BF),
            pltpu.VMEM((rows, width), BF),
            *[pltpu.VMEM((3, rows, width), BF)] * 5,
            *[pltpu.VMEM((rows, width), F32)] * 3,
            *transfer_sems(),
            *transfer_sems(),
            *transfer_sems(),
            *transfer_sems(),
            spread_land((units, width), KINDS),
            *spread_sems(KINDS),
        ],
        name="feed_forward",
        compiler_params=comm_params(2),
    )(hidden, normed, inv_std, output_grad, up, up_bias, down, *vectors)


def attend_back_kernel(
    b_ref, w_ref, e_ref, r_ref, q_ref, k_ref, v_ref, o_ref, small_in, up_in, down_in, all_in,
    dq_ref, dk_ref, dv_ref, wg_ref, pg_ref, small_ref, up_out, down_out,
    land, v_aug, k_t, dks, dvs, dqs, w_total, w_low, p_low, grads, up, down, tokens, loads, send, recv,
    up_land, up_send, up_recv, down_send, down_recv, out_land, out_send, out_recv,
    pair_land, pair_send, pair_recv, value, small_land, small_send, small_recv,
):
    step = pl.program_id(0)
    pair, s_now = step // 2 % 2, step // 4 * 2 + step % 2
    seq_len, block = k_ref.shape[0], q_ref.shape[0]
    pieces = e_ref.shape[0]
    cols = w_ref.shape[0]
    width = w_ref.shape[1]
    half = block // 2
    gather = Gather(b_ref, land, send, recv, HALVES)
    up_sum = Spread(up, None, up_land, up_send, up_recv, KINDS, 0, 1)
    down_sum = Spread(None, down, None, down_send, down_recv, KINDS, 2, 3)
    out_sum = Spread(w_low, None, out_land, out_send, out_recv, "H", 0, 1)
    pair_sum = Spread(p_low, None, pair_land, pair_send, pair_recv, KINDS, 0, 1)
    small = Hops(
        value, small_land, small_send, small_recv,
        [dp_peer(1), dp_peer(2), dp_peer(4), mp_peer(1), mp_peer(2)],
    )
    load_up = pltpu.make_async_copy(up_in, up, loads.at[0])
    load_down = [
        pltpu.make_async_copy(
            down_in.at[down_sum.own(job)], down.at[down_sum.own(job)], loads.at[5 + job]
        )
        for job in range(JOBS)
    ]
    load_tokens = pltpu.make_async_copy(all_in, tokens, loads.at[2])
    save_up = pltpu.make_async_copy(up, up_out, loads.at[3])
    save_down = pltpu.make_async_copy(down, down_out, loads.at[4])

    def branch_rows(s):
        branch = b_ref[...] if s == 0 else land[s - 1]
        at = pl.ds(s * block, block)
        if s == 0:
            w_total[...] = mm(o_ref[...], branch, 0, 0)
        else:
            w_total[...] += mm(o_ref[...], branch, 0, 0)
        grads[at] = mm(branch, w_ref[...], 1, 1).astype(BF)

    @pl.when(step == 0)
    def _():
        for load in load_down:
            load.start()
        load_up.start()
        load_tokens.start()
        value[0] = small_in[...]
        greet_all()
        repeat(HALVES, gather.start)
        for load in load_down:
            load.wait()
        advance((down_sum, (0, 1, 2, 3), 3))
        load_up.wait()
        advance((up_sum, (0, 1, 2, 3), 0))
        small.start(0)
        branch_rows(0)

    @pl.when(step == 1)
    def _():
        small.finish(0)
        small.start(1)
        repeat(HALVES, lambda j: gather.arrive(1, j))
        branch_rows(1)

    @pl.when(step == 2)
    def _():
        advance((down_sum, (0, 1, 2, 3), 4), (up_sum, (0, 1), 1))
        small.finish(1)
        small.start(2)

    @pl.when(step == 3)
    def _():
        advance((up_sum, (2, 3), 1), (down_sum, (0, 1), 5))
        small.finish(2)
        small.start(3)

    @pl.when(step == 4)
    def _():
        advance((up_sum, (0, 1), 2), (down_sum, (2, 3), 5))
        small.finish(3)
        small.start(4)
        repeat(HALVES, lambda j: gather.arrive(2, j))
        branch_rows(2)

    @pl.when(step == 5)
    def _():
        small.finish(4)
        small_ref[...] = value[5]
        small_ref[6:7] = value[3, 6:7]
        repeat(HALVES, lambda j: gather.arrive(3, j))
        branch_rows(3)
        w_low[...] = w_total[...].astype(BF)
        advance((out_sum, 0, 0), (up_sum, (2, 3), 2))

    @pl.when(step == 6)
    def _():
        advance((out_sum, 0, 1), (up_sum, (0, 1), 3), (down_sum, (0, 1), 6))

    @pl.when(step == 7)
    def _():
        advance(
            (pair_sum, (0, 1, 2, 3), 1), (out_sum, 0, 2), (up_sum, (2, 3), 3), (down_sum, (2, 3), 6)
        )
        save_up.start()
        save_down.start()

    @pl.when(s_now == 0)
    def _():
        lanes = lax.broadcasted_iota(jnp.int32, (seq_len, WIDE), 1)
        values = v_ref[...].astype(F32)
        for h in range(2):
            other = (1 - h) * HD
            ones = jnp.where((lanes >= other) & (lanes < other + 2), 1.0, 0.0)
            v_aug[pair, h] = jnp.where(lanes // HD == h, values, ones).astype(BF)
        k_t[pair] = (k_ref[...].astype(F32) * HD**-0.5).T.astype(BF)
        dks[pair] = jnp.zeros(dks.shape[1:], F32)
        dvs[pair] = jnp.zeros(dvs.shape[1:], F32)

    lanes = lax.broadcasted_iota(jnp.int32, (block, WIDE), 1)
    row_start = pl.multiple_of(s_now * block, block)
    inverse = jnp.concatenate(
        [
            jnp.concatenate(
                [jnp.broadcast_to(r_ref[i, h], (HD, block // pieces)) for h in range(2)], 0
            )
            for i in range(pieces)
        ],
        1,
    ).T
    wide = pl.ds(pl.multiple_of(pair * WIDE, WIDE), WIDE)
    grad = (grads[pl.ds(row_start, block), wide].astype(F32) * inverse).astype(BF)
    grad_wide = grad.astype(F32)
    product = grad_wide * o_ref[:, wide].astype(F32)
    centered = []
    for h in range(2):
        other = (1 - h) * HD
        inside = lanes // HD == h
        row_dot = jnp.sum(jnp.where(inside, product, 0.0), -1, keepdims=True)
        high = row_dot.astype(BF).astype(F32)
        g_aug = jnp.where(
            inside,
            grad_wide,
            jnp.where(lanes == other, -high, jnp.where(lanes == other + 1, high - row_dot, 0.0)),
        ).astype(BF)
        centered.append(mm(v_aug[pair, h], g_aug, 1, 1))
    query_grads = []
    for h in range(2):
        cols_h = slice(h * HD, (h + 1) * HD)
        expon = jnp.concatenate([e_ref[i, h] for i in range(pieces)], 1)
        score_grad = (expon.astype(F32) * centered[h]).astype(BF)
        dvs[pair, h] += mm(expon, grad[:, cols_h], 1, 0)
        dks[pair, h] += mm(score_grad, q_ref[:, cols_h], 1, 0)
        query_grads.append(mm(k_t[pair, cols_h, :], score_grad, 1, 0))
    query_grad = jnp.concatenate(query_grads, 0).T.astype(BF)
    dq_ref[...] = query_grad
    dqs[pair, pl.ds(row_start, block), :WIDE] = query_grad

    @pl.when(s_now == 3)
    def _():
        for total, out, at in ((dks, dk_ref, WIDE), (dvs, dv_ref, 2 * WIDE)):
            joined = jnp.concatenate([total[pair, h] for h in range(2)], 1).astype(BF)
            out[:, wide] = joined
            dqs[pair, :, at : at + WIDE] = joined

    @pl.when(step == 5)
    def _():
        load_tokens.wait()
        projection_grads(tokens, dqs.at[0], p_low)
        advance((pair_sum, (0, 1, 2, 3), 0))

    @pl.when(step == 7)
    def _():
        advance((pair_sum, (0, 1, 2, 3), 2), (out_sum, 0, 3), (pair_sum, (0, 1, 2, 3), 3))
        wg_ref[...] = w_low[...]
        pg_ref[...] = p_low[...]
        gather.drain()
        save_down.wait()
        save_up.wait()


def projection_grads(tokens, joint, out_ref):
    tile = 256
    rows = tokens.shape[1]

    def body(t):
        cols = pl.ds(pl.multiple_of(t * tile, tile), tile)
        total = mm(tokens[0, :, cols], joint[pl.ds(0, rows)], 0, 0)
        for s in (1, 2, 3):
            total += mm(tokens[s, :, cols], joint[pl.ds(s * rows, rows)], 0, 0)
        out_ref[cols] = total.astype(BF)

    repeat(tokens.shape[2] // tile, body)


def attend_back(branch, out_weight, expon, inverse, q, k, v, attended, small, up, down, gathered):
    rows, width = branch.shape
    all_rows, cols = q.shape
    pairs = cols // WIDE
    pieces = HALVES

    def fixed(*shape):
        return pl.BlockSpec(shape, lambda i: (0,) * len(shape))

    def pair_at(i):
        return i // 2 % 2

    def rows_at(i):
        return i // 4 * 2 + i % 2

    anywhere = pl.BlockSpec(memory_space=pl.ANY)
    pair_rows = pl.BlockSpec((rows, WIDE), lambda i: (rows_at(i), pair_at(i)))
    pair_keys = pl.BlockSpec((all_rows, WIDE), lambda i: (0, pair_at(i)))
    return pl.pallas_call(
        attend_back_kernel,
        grid=(4 * pairs,),
        in_specs=[
            fixed(rows, width),
            fixed(cols, width),
            pl.BlockSpec((pieces, 2, all_rows, rows // pieces), lambda i: (rows_at(i), pair_at(i), 0, 0)),
            pl.BlockSpec((pieces, 2, 1, rows // pieces), lambda i: (rows_at(i), pair_at(i), 0, 0)),
            pair_rows,
            pair_keys,
            pair_keys,
            pl.BlockSpec((rows, cols), lambda i: (rows_at(i), 0)),
            fixed(*small.shape),
            anywhere,
            anywhere,
            anywhere,
        ],
        out_specs=[
            pair_rows,
            fixed(all_rows, cols),
            fixed(all_rows, cols),
            fixed(cols, width),
            fixed(width, 3 * WIDE),
            fixed(*small.shape),
            anywhere,
            anywhere,
        ],
        out_shape=[shaped(all_rows, cols)] * 3
        + [
            shaped(cols, width),
            shaped(width, 3 * WIDE),
            shaped(*small.shape, dtype=F32),
            shaped(*up.shape),
            shaped(*down.shape),
        ],
        scratch_shapes=[
            pltpu.VMEM((3, rows, width), BF),
            pltpu.VMEM((pairs, 2, all_rows, WIDE), BF),
            pltpu.VMEM((pairs, WIDE, all_rows), BF),
            pltpu.VMEM((pairs, 2, all_rows, HD), F32),
            pltpu.VMEM((pairs, 2, all_rows, HD), F32),
            pltpu.VMEM((pairs, all_rows, 3 * WIDE), BF),
            pltpu.VMEM((cols, width), F32),
            pltpu.VMEM((cols, width), BF),
            pltpu.VMEM((width, 3 * WIDE), BF),
            pltpu.VMEM((all_rows, cols), BF),
            pltpu.VMEM(up.shape, BF),
            pltpu.VMEM(down.shape, BF),
            pltpu.VMEM(gathered.shape, BF),
            pltpu.SemaphoreType.DMA((5 + JOBS,)),
            *transfer_sems(HALVES),
            spread_land(up.shape, KINDS),
            *spread_sems(KINDS),
            *spread_sems(KINDS),
            spread_land((cols, width), "H"),
            *spread_sems("H"),
            spread_land((width, 3 * WIDE), KINDS),
            *spread_sems(KINDS),
            *hop_scratch(5, *small.shape),
        ],
        name="attend_back",
        compiler_params=comm_params(3),
    )(branch, out_weight, expon, inverse, q, k, v, attended, small, up, down, gathered)


def input_back_kernel(
    dq_ref, dk_ref, dv_ref, wq_ref, wk_ref, wv_ref, all_ref, r1_ref, wg_in, pg_in, up_in,
    x_ref, wg_ref, pg_ref, last_ref, bias_ref, up_out,
    out, land, mine, pending, send, recv, up, loads, up_send, up_recv, out_send, out_recv,
    pair_send, pair_recv, joint, w_full, p_full, last_full, last_low, last_land, last_send, last_recv,
    value, bias_land, bias_send, bias_recv,
):
    rows_here = r1_ref.shape[0]
    size = rows_here // CHUNKS
    last = dq_ref.shape[1] - WIDE
    up_sum = Spread(None, up, None, up_send, up_recv, KINDS, 2, 3)
    out_sum = Spread(None, w_full, None, out_send, out_recv, "H", 2, 3)
    pair_sum = Spread(None, p_full, None, pair_send, pair_recv, KINDS, 2, 3)
    last_sum = Spread(last_low, last_full, last_land, last_send, last_recv, KINDS)
    bias = Hops(value, bias_land, bias_send, bias_recv, [dp_peer(1), dp_peer(2), dp_peer(4)])
    reduce = Reduce(out, land, send, recv)
    save_up = pltpu.make_async_copy(up, up_out, loads.at[JOBS])
    load_up = [
        pltpu.make_async_copy(up_in.at[up_sum.own(job)], up.at[up_sum.own(job)], loads.at[job])
        for job in range(JOBS)
    ]
    for load in load_up:
        load.start()
    w_full[out_sum.own(0)] = wg_in[out_sum.own(0)]
    for job in range(JOBS):
        p_full[pair_sum.own(job)] = pg_in[pair_sum.own(job)]
    greet_all()
    for load in load_up:
        load.wait()
    advance((pair_sum, (0, 1, 2, 3), 3), (out_sum, 0, 3), (up_sum, (0, 1, 2, 3), 3))
    tail = pl.ds(last, WIDE)
    for at, grad in enumerate((dq_ref, dk_ref, dv_ref)):
        joint[:, at * WIDE : (at + 1) * WIDE] = grad[:, tail]
    projection_grads(all_ref, joint, last_low)
    advance((last_sum, (0, 1, 2, 3), 0))
    grads = ((dq_ref, wq_ref), (dk_ref, wk_ref), (dv_ref, wv_ref))

    def part_of(starts, count):
        total = None
        for grad, weight in grads:
            pieces = [grad[pl.ds(pl.multiple_of(at, size), count)] for at in starts]
            x = pieces[0] if len(pieces) == 1 else jnp.concatenate(pieces, 0)
            term = mm(x, weight[...], 1, 1)
            total = term if total is None else total + term
        return total

    def chunk_rows(j):
        return pl.ds(pl.multiple_of(j * size, size), size)

    def far(j):
        part = part_of((2 * rows_here + j * size, 3 * rows_here + j * size), size)
        pending[chunk_rows(j)] = part[:size]
        reduce.post(PAIR, j, part[size:])

        @pl.when(j > 0)
        def _():
            reduce.forward_pair(j - 1, pending[chunk_rows(j - 1)])

    repeat(CHUNKS, far)
    reduce.forward_pair(CHUNKS - 1, pending[chunk_rows(CHUNKS - 1)])
    value[0, 0:1] = column_sum(dq_ref[...].astype(F32))
    value[0, 1:8] = jnp.broadcast_to(column_sum(dv_ref[...].astype(F32)), (7, dv_ref.shape[1]))
    bias.start(0)
    advance((pair_sum, (0, 1, 2, 3), 4), (last_sum, (0, 1, 2, 3), 1), (up_sum, (0, 1), 4))

    def near(i):
        part = part_of((rows_here + i * 2 * size,), 2 * size)
        reduce.post(NEAR, 2 * i, part[:size])
        reduce.post(NEAR, 2 * i + 1, part[size:])

    repeat(2, near)

    def own(i):
        mine[pl.ds(pl.multiple_of(i * 2 * size, 2 * size), 2 * size)] = part_of((i * 2 * size,), 2 * size)

    repeat(2, own)

    def finish(j):
        rows = chunk_rows(j)
        x_ref[rows] = (r1_ref[rows] + reduce.total(j, mine[rows])).astype(BF)

    bias.finish(0)
    bias.start(1)
    advance((pair_sum, (0, 1, 2, 3), 5), (up_sum, (2, 3), 4))
    finish(0)
    advance((last_sum, (0, 1, 2, 3), 2), (up_sum, (0, 1), 5), (out_sum, 0, 4))
    bias.finish(1)
    bias.start(2)
    finish(1)
    advance((last_sum, (0, 1, 2, 3), 3), (up_sum, (2, 3), 5), (out_sum, 0, 5))
    finish(2)
    advance((last_sum, (0, 1, 2, 3), 4))
    finish(3)
    bias.finish(2)
    bias_ref[...] = value[3]
    advance((last_sum, (0, 1, 2, 3), 5), (up_sum, (0, 1, 2, 3), 6))
    save_up.start()
    advance((pair_sum, (0, 1, 2, 3), 6), (out_sum, 0, 6))
    wg_ref[...] = w_full[...]
    pg_ref[...] = p_full[...]
    advance((last_sum, (0, 1, 2, 3), 6))
    last_ref[...] = last_full[...]
    reduce.drain()
    save_up.wait()


def input_back(dq, dk, dv, wq, wk, wv, gathered, resid_grad, out_grad, pair_grad, up):
    rows, width = resid_grad.shape
    cols = dq.shape[1]
    return pl.pallas_call(
        input_back_kernel,
        in_specs=[WHOLE] * 10 + [pl.BlockSpec(memory_space=pl.ANY)],
        out_specs=[WHOLE] * 5 + [pl.BlockSpec(memory_space=pl.ANY)],
        out_shape=[
            shaped(rows, width),
            shaped(*out_grad.shape),
            shaped(*pair_grad.shape),
            shaped(*pair_grad.shape),
            shaped(8, cols, dtype=F32),
            shaped(*up.shape),
        ],
        scratch_shapes=[
            pltpu.VMEM((3, rows, width), BF),
            pltpu.VMEM((3, rows, width), BF),
            pltpu.VMEM((rows, width), F32),
            pltpu.VMEM((rows, width), F32),
            *transfer_sems(),
            pltpu.VMEM(up.shape, BF),
            pltpu.SemaphoreType.DMA((JOBS + 1,)),
            *spread_sems(KINDS),
            *spread_sems("H"),
            *spread_sems(KINDS),
            pltpu.VMEM((dq.shape[0], 3 * WIDE), BF),
            pltpu.VMEM(out_grad.shape, BF),
            *[pltpu.VMEM(pair_grad.shape, BF)] * 3,
            spread_land(pair_grad.shape, KINDS),
            *spread_sems(KINDS),
            *hop_scratch(3, 8, cols),
        ],
        name="input_back",
        compiler_params=comm_params(4),
    )(dq, dk, dv, wq, wk, wv, gathered, resid_grad, out_grad, pair_grad, up)


def widen_kernel(up_ref, down_ref, out_ref, pair_ref, last_ref, upw, downw, outw, qw, kw, vw):
    upw[...] = up_ref[...].astype(F32)
    downw[...] = down_ref[...].astype(F32)
    outw[...] = out_ref[...].astype(F32)
    for at, wide in enumerate((qw, kw, vw)):
        cols = slice(at * WIDE, (at + 1) * WIDE)
        wide[:, :WIDE] = pair_ref[:, cols].astype(F32)
        wide[:, WIDE:] = last_ref[:, cols].astype(F32)


def widen_grads(*grads):
    steps = 8
    shapes = [g.shape for g in grads[:3]] + [(grads[3].shape[0], 2 * WIDE)] * 3

    def tiles(shape):
        return pl.BlockSpec((shape[0] // steps, shape[1]), lambda i: (i, 0))

    return pl.pallas_call(
        widen_kernel,
        grid=(steps,),
        in_specs=[tiles(g.shape) for g in grads],
        out_specs=[tiles(shape) for shape in shapes],
        out_shape=[shaped(*shape, dtype=F32) for shape in shapes],
        name="widen_grads",
    )(*grads)


def per_device(
    tokens, lengths, query_weight, query_bias, key_weight, value_weight, value_bias, out_weight,
    out_bias, first_gain, first_shift, up_weight, up_bias, down_weight, down_bias, second_gain,
    second_shift, output_grad,
):
    pairs = query_weight.shape[1] // WIDE
    if (lax.axis_size("dp"), lax.axis_size("mp"), lengths.shape[1], pairs) != (8, 4, 1, 2):
        return per_device_general(
            tokens, lengths, query_weight, query_bias, key_weight, value_weight, value_bias,
            out_weight, out_bias, first_gain, first_shift, up_weight, up_bias, down_weight,
            down_bias, second_gain, second_shift, output_grad,
        )
    q, k, v, vt, gathered = gather_project(
        tokens, query_weight, key_weight, value_weight, query_bias, value_bias
    )
    expon, attended, inverse, normed, inv_std, hidden = attend(
        lengths, q, k, vt, out_weight, tokens, out_bias, first_gain, first_shift
    )
    layer_out, branch, resid_grad, up_grad, down_grad, small = feed_forward(
        hidden, normed, inv_std, output_grad, up_weight, up_bias, down_weight,
        first_gain, first_shift, down_bias, second_gain, second_shift,
    )
    dq, dk, dv, out_grad, pair_grad, small, up_grad, down_grad = attend_back(
        branch, out_weight, expon, inverse, q, k, v, attended, small, up_grad, down_grad, gathered
    )
    tokens_grad, out_grad, pair_grad, last_grad, bias_grads, up_grad = input_back(
        dq, dk, dv, query_weight, key_weight, value_weight, gathered, resid_grad, out_grad, pair_grad,
        up_grad,
    )

    up_grad, down_grad, out_grad, query_grad, key_grad, value_grad = widen_grads(
        up_grad, down_grad, out_grad, pair_grad, last_grad
    )
    return (
        layer_out,
        tokens_grad,
        query_grad,
        bias_grads[0],
        key_grad,
        value_grad,
        bias_grads[1],
        out_grad,
        small[5],
        small[3],
        small[4],
        up_grad,
        small[6],
        down_grad,
        small[2],
        small[0],
        small[1],
    )


def solution(mesh):
    placed = (
        P(("dp", "mp"), None),
        P("dp", None),
        P(None, "mp"),
        P("mp"),
        P(None, "mp"),
        P(None, "mp"),
        P("mp"),
        P("mp", None),
        P(),
        P(),
        P(),
        P(None, "mp"),
        P("mp"),
        P("mp", None),
        P(),
        P(),
        P(),
        P(("dp", "mp"), None),
    )
    return jax.shard_map(
        per_device,
        mesh=mesh,
        in_specs=placed,
        out_specs=(
            P(("dp", "mp"), None),
            P(("dp", "mp"), None),
            P(None, "mp"),
            P("mp"),
            P(None, "mp"),
            P(None, "mp"),
            P("mp"),
            P("mp", None),
            P(),
            P(),
            P(),
            P(None, "mp"),
            P("mp"),
            P("mp", None),
            P(),
            P(),
            P(),
        ),
        check_vma=False,
    )
```

```python
from functools import partial

import jax
import jax.numpy as jnp
from jax import lax
from jax.experimental import pallas as pl
from jax.experimental.pallas import tpu as pltpu
from jax.sharding import PartitionSpec as P

HD = 64


epsilon = 1e-12


def norm_forward(resid, gain, shift):
    center = resid - jnp.mean(resid, -1, keepdims=True)
    inv_std = lax.rsqrt(jnp.mean(center * center, -1, keepdims=True) + epsilon)
    normed = center * inv_std
    return (normed * gain + shift, normed, inv_std)


def norm_backward(grad, normed, inv_std, gain):
    scaled = grad * gain
    back = inv_std * (
        scaled
        - jnp.mean(scaled, -1, keepdims=True)
        - normed * jnp.mean(scaled * normed, -1, keepdims=True)
    )
    return (back, jnp.sum(grad * normed, 0), jnp.sum(grad, 0))


F32 = jnp.float32
BF = jnp.bfloat16
MASKED = -1000000000.0
WIDE = 2 * HD


def mm(a, b, ca, cb):
    return lax.dot_general(a, b, (((ca,), (cb,)), ((), ())), preferred_element_type=F32)


def forward_kernel(heads, len_ref, q_ref, k_ref, vt_ref, e_ref, o_ref, r_ref, v_aug, k_aug):
    seq, step = pl.program_id(0), pl.program_id(2)
    seq_len, block = k_ref.shape[0], q_ref.shape[0]

    @pl.when(step == 0)
    def _():
        rows = lax.broadcasted_iota(jnp.int32, (seq_len, WIDE), 0)
        lanes = lax.broadcasted_iota(jnp.int32, (seq_len, WIDE), 1)
        bias = jnp.where(rows < len_ref[seq], 0.0, MASKED)
        keys = k_ref[...].astype(F32)
        for h in range(heads):
            other = (1 - h) * HD
            k_aug[h] = jnp.where(
                lanes // HD == h, keys, jnp.where(lanes == other, bias, 0.0)
            ).astype(BF)
            v_aug[h, :HD] = vt_ref[h * HD : (h + 1) * HD, :]
            v_aug[h, HD:] = jnp.ones((16, seq_len), BF)

    query = q_ref[...].astype(F32) * HD**-0.5
    lanes = lax.broadcasted_iota(jnp.int32, (block, WIDE), 1)
    scores = []
    for h in range(heads):
        other = (1 - h) * HD
        q_aug = jnp.where(
            lanes // HD == h, query, jnp.where(lanes == other, 1.0, 0.0)
        ).astype(BF)
        scores.append(mm(k_aug[h], q_aug, 1, 1))
    outs = []
    for h in range(heads):
        top = jnp.max(scores[h], 0, keepdims=True)
        expon = jnp.exp(scores[h] - top).astype(BF)
        e_ref[h] = expon
        total = mm(v_aug[h], expon, 1, 0)
        inverse = 1.0 / total[HD : HD + 1]
        r_ref[h] = inverse
        outs.append(total[:HD] * inverse)
    if heads == 1:
        outs.append(jnp.zeros_like(outs[0]))
    o_ref[...] = jnp.concatenate(outs, 0).T.astype(BF)


def backward_kernel(
    heads, e_ref, r_ref, q_ref, k_ref, v_ref, o_ref, g_ref, dq_ref, dk_ref, dv_ref, v_aug, k_t, dks, dvs
):
    step, last = pl.program_id(2), pl.num_programs(2) - 1
    seq_len, block = k_ref.shape[0], q_ref.shape[0]

    @pl.when(step == 0)
    def _():
        lanes = lax.broadcasted_iota(jnp.int32, (seq_len, WIDE), 1)
        values = v_ref[...].astype(F32)
        for h in range(heads):
            other = (1 - h) * HD
            ones = jnp.where((lanes >= other) & (lanes < other + 2), 1.0, 0.0)
            v_aug[h] = jnp.where(lanes // HD == h, values, ones).astype(BF)
        k_t[...] = (k_ref[...].astype(F32) * HD**-0.5).T.astype(BF)
        dks[...] = jnp.zeros_like(dks)
        dvs[...] = jnp.zeros_like(dvs)

    lanes = lax.broadcasted_iota(jnp.int32, (block, WIDE), 1)
    inverse = jnp.concatenate(
        [jnp.broadcast_to(r_ref[h % heads], (HD, block)) for h in range(2)], 0
    ).T
    grad = (g_ref[...].astype(F32) * inverse).astype(BF)
    grad_wide = grad.astype(F32)
    scaled_query = (q_ref[...].astype(F32) * HD**-0.5).astype(BF)
    product = grad_wide * o_ref[...].astype(F32)
    centered = []
    for h in range(heads):
        other = (1 - h) * HD
        inside = lanes // HD == h
        row_dot = jnp.sum(jnp.where(inside, product, 0.0), -1, keepdims=True)
        high = row_dot.astype(BF).astype(F32)
        g_aug = jnp.where(
            inside,
            grad_wide,
            jnp.where(lanes == other, -high, jnp.where(lanes == other + 1, high - row_dot, 0.0)),
        ).astype(BF)
        centered.append(mm(v_aug[h], g_aug, 1, 1))
    query_grads = []
    for h in range(heads):
        cols = slice(h * HD, (h + 1) * HD)
        expon = e_ref[h]
        score_grad = (expon.astype(F32) * centered[h]).astype(BF)
        dvs[h] += mm(expon, grad[:, cols], 1, 0)
        dks[h] += mm(score_grad, scaled_query[:, cols], 1, 0)
        query_grads.append(mm(k_t[cols, :], score_grad, 1, 0))
    if heads == 1:
        query_grads.append(jnp.zeros_like(query_grads[0]))
    dq_ref[...] = jnp.concatenate(query_grads, 0).T.astype(BF)

    @pl.when(step == last)
    def _():
        for total, out in ((dks, dk_ref), (dvs, dv_ref)):
            halves = [total[h] for h in range(heads)]
            if heads == 1:
                halves.append(jnp.zeros_like(halves[0]))
            out[...] = jnp.concatenate(halves, 1).astype(BF)


def attention_shape(rows, cols, seqs):
    seq_len = rows // seqs
    block = min(512, seq_len)
    steps = seq_len // block
    pairs = max(1, cols // WIDE)
    heads = cols // HD // pairs
    row_spec = pl.BlockSpec((block, WIDE), lambda s, p, j, *_: (s * steps + j, p))
    key_spec = pl.BlockSpec((seq_len, WIDE), lambda s, p, j, *_: (s, p))
    e_spec = pl.BlockSpec((heads, seq_len, block), lambda s, p, j, *_: (p, s, j))
    r_spec = pl.BlockSpec((heads, 1, block), lambda s, p, j, *_: (p, 0, s * steps + j))
    return seq_len, heads, pairs, (seqs, pairs, steps), row_spec, key_spec, e_spec, r_spec


def widen(array):
    short = WIDE - array.shape[1]
    return array if short <= 0 else jnp.pad(array, ((0, 0), (0, short)))


def attention_forward(queries, keys, values, lengths):
    rows, cols = queries.shape
    seqs = lengths.shape[0]
    seq_len, heads, pairs, grid, row_spec, key_spec, e_spec, r_spec = attention_shape(rows, cols, seqs)
    wide_cols = pairs * WIDE
    expon, attended, inverse = pl.pallas_call(
        partial(forward_kernel, heads),
        grid_spec=pltpu.PrefetchScalarGridSpec(
            num_scalar_prefetch=1,
            grid=grid,
            in_specs=[
                row_spec,
                key_spec,
                pl.BlockSpec((WIDE, seq_len), lambda s, p, j, *_: (p, s)),
            ],
            out_specs=[e_spec, row_spec, r_spec],
            scratch_shapes=[
                pltpu.VMEM((heads, HD + 16, seq_len), BF),
                pltpu.VMEM((heads, seq_len, WIDE), BF),
            ],
        ),
        out_shape=[
            jax.ShapeDtypeStruct((heads * pairs, rows, seq_len), BF),
            jax.ShapeDtypeStruct((rows, wide_cols), BF),
            jax.ShapeDtypeStruct((heads * pairs, 1, rows), F32),
        ],
        name="attention_forward",
        compiler_params=pltpu.CompilerParams(vmem_limit_bytes=60 * 1024 * 1024),
    )(lengths, widen(queries), widen(keys), widen(values).T)
    return expon, attended[:, :cols], inverse


def attention_backward(expon, inverse, queries, keys, values, attended, grad, seqs):
    rows, cols = queries.shape
    seq_len, heads, pairs, grid, row_spec, key_spec, e_spec, r_spec = attention_shape(rows, cols, seqs)
    shape = jax.ShapeDtypeStruct((rows, pairs * WIDE), BF)
    outs = pl.pallas_call(
        partial(backward_kernel, heads),
        grid=grid,
        in_specs=[e_spec, r_spec, row_spec, key_spec, key_spec, row_spec, row_spec],
        out_specs=[row_spec, key_spec, key_spec],
        scratch_shapes=[
            pltpu.VMEM((heads, seq_len, WIDE), BF),
            pltpu.VMEM((WIDE, seq_len), BF),
            pltpu.VMEM((heads, seq_len, HD), F32),
            pltpu.VMEM((heads, seq_len, HD), F32),
        ],
        out_shape=[shape] * 3,
        name="attention_backward",
        compiler_params=pltpu.CompilerParams(vmem_limit_bytes=60 * 1024 * 1024),
    )(expon, inverse, *[widen(x) for x in (queries, keys, values, attended, grad)])
    return [x[:, :cols] for x in outs]


def contract_rows(left, right):
    return lax.dot_general(
        left, right, (((0,), (0,)), ((), ())), preferred_element_type=jnp.float32
    )


def contract_cols(left, right):
    return lax.dot_general(
        left, right, (((1,), (1,)), ((), ())), preferred_element_type=jnp.float32
    )


def split_projection(projected, width, q_bias, v_bias):
    query_part = (projected[:, :width] + q_bias).astype(jnp.bfloat16)
    key_part = projected[:, width : 2 * width].astype(jnp.bfloat16)
    value_part = (projected[:, 2 * width :] + v_bias).astype(jnp.bfloat16)
    return (query_part, key_part, value_part)


def per_device_general(
    tokens,
    lengths,
    query_weight,
    query_bias,
    key_weight,
    value_weight,
    value_bias,
    out_weight,
    out_bias,
    first_gain,
    first_shift,
    up_weight,
    up_bias,
    down_weight,
    down_bias,
    second_gain,
    second_shift,
    output_grad,
):
    local_rows = tokens.shape[0]
    head_cols = query_weight.shape[1]
    seq_count = lengths.shape[1]
    all_rows = local_rows * lax.axis_size("mp")
    gathered = lax.all_gather(tokens, "mp", axis=0, tiled=True)
    joint_weight = jnp.concatenate([query_weight, key_weight, value_weight], 1)
    projected = jnp.dot(gathered, joint_weight, preferred_element_type=jnp.float32)
    queries, key_rows, values = split_projection(projected, head_cols, query_bias, value_bias)
    expon, attended, inverse = attention_forward(queries, key_rows, values, lengths[0])
    branch_one = lax.psum_scatter(
        jnp.dot(
            lax.slice_in_dim(attended, 0, local_rows * lax.axis_size("mp"), axis=0),
            out_weight,
            preferred_element_type=jnp.float32,
        ).astype(jnp.bfloat16),
        "mp",
        scatter_dimension=0,
        tiled=True,
    ).astype(jnp.float32)
    hidden, normed_one, inv_one = norm_forward(
        tokens.astype(jnp.float32) + branch_one + out_bias, first_gain, first_shift
    )
    hidden_low = hidden.astype(jnp.bfloat16)
    hidden_all = lax.all_gather(hidden_low, "mp", axis=0, tiled=True)
    pre_act = jnp.dot(hidden_all, up_weight, preferred_element_type=jnp.float32) + up_bias
    act_low = jax.nn.gelu(pre_act, approximate=False).astype(jnp.bfloat16)
    branch_two = lax.psum_scatter(
        jnp.dot(
            lax.slice_in_dim(act_low, 0, local_rows * lax.axis_size("mp"), axis=0),
            down_weight,
            preferred_element_type=jnp.float32,
        ).astype(jnp.bfloat16),
        "mp",
        scatter_dimension=0,
        tiled=True,
    ).astype(jnp.float32)
    layer_out, normed_two, inv_two = norm_forward(
        hidden + branch_two + down_bias, second_gain, second_shift
    )
    resid_two_grad, second_gain_grad, second_shift_grad = norm_backward(
        output_grad.astype(jnp.float32), normed_two, inv_two, second_gain
    )
    down_bias_grad = jnp.sum(resid_two_grad, 0)
    branch_two_low = resid_two_grad.astype(jnp.bfloat16)
    row_piece = lax.all_gather(branch_two_low, "mp", axis=0, tiled=True)
    row_start = jnp.int32(0)
    weight_acc = jnp.zeros(down_weight.shape, jnp.float32)
    act_acc = jnp.zeros(act_low.shape, jnp.float32)
    act_rows = lax.dynamic_slice_in_dim(act_low, row_start, row_piece.shape[0], 0)
    weight_acc = weight_acc + contract_rows(act_rows, row_piece)
    act_acc = lax.dynamic_update_slice_in_dim(
        act_acc, contract_cols(row_piece, down_weight), row_start, 0
    )
    down_weight_grad = weight_acc
    unused_two, gelu_back = jax.vjp(partial(jax.nn.gelu, approximate=False), pre_act)
    pre_grad = gelu_back(act_acc)[0].astype(jnp.bfloat16)
    up_bias_grad = jnp.sum(pre_grad, 0, dtype=jnp.float32)
    up_weight_grad = contract_rows(hidden_all, pre_grad)
    hidden_back = lax.psum_scatter(
        contract_cols(
            lax.slice_in_dim(pre_grad, 0, local_rows * lax.axis_size("mp"), axis=0), up_weight
        ).astype(jnp.bfloat16),
        "mp",
        scatter_dimension=0,
        tiled=True,
    ).astype(jnp.float32)
    hidden_grad = resid_two_grad + hidden_back
    resid_one_grad, first_gain_grad, first_shift_grad = norm_backward(
        hidden_grad, normed_one, inv_one, first_gain
    )
    out_bias_grad = jnp.sum(resid_one_grad, 0)
    branch_one_low = resid_one_grad.astype(jnp.bfloat16)
    row_piece = lax.all_gather(branch_one_low, "mp", axis=0, tiled=True)
    row_start = jnp.int32(0)
    weight_acc = jnp.zeros(out_weight.shape, jnp.float32)
    attn_acc = jnp.zeros(attended.shape, jnp.float32)
    attn_rows = lax.dynamic_slice_in_dim(attended, row_start, row_piece.shape[0], 0)
    weight_acc = weight_acc + contract_rows(attn_rows, row_piece)
    attn_acc = lax.dynamic_update_slice_in_dim(
        attn_acc, contract_cols(row_piece, out_weight), row_start, 0
    )
    out_weight_grad = weight_acc
    attn_low = attn_acc.astype(jnp.bfloat16)
    query_flat, key_flat, value_flat = attention_backward(
        expon, inverse, queries, key_rows, values, attended, attn_low, seq_count
    )
    width_now = query_flat.shape[1]
    joint_grad = jnp.concatenate([query_flat, key_flat, value_flat], 1)
    query_bias_grad = jnp.sum(query_flat, 0, dtype=jnp.float32)
    value_bias_grad = jnp.sum(value_flat, 0, dtype=jnp.float32)
    joint_weight_grad = contract_rows(gathered, joint_grad)
    input_back = lax.psum_scatter(
        contract_cols(
            lax.slice_in_dim(joint_grad, 0, local_rows * lax.axis_size("mp"), axis=0), joint_weight
        ).astype(jnp.bfloat16),
        "mp",
        scatter_dimension=0,
        tiled=True,
    ).astype(jnp.float32)
    tokens_grad = (resid_one_grad + input_back).astype(jnp.bfloat16)
    query_weight_grad = joint_weight_grad[:, :width_now]
    key_weight_grad = joint_weight_grad[:, width_now : 2 * width_now]
    value_weight_grad = joint_weight_grad[:, 2 * width_now :]
    (
        query_weight_grad,
        query_bias_grad,
        key_weight_grad,
        value_weight_grad,
        value_bias_grad,
        out_weight_grad,
        up_weight_grad,
        up_bias_grad,
        down_weight_grad,
    ) = (
        lax.psum(query_weight_grad.astype(jnp.bfloat16), "dp").astype(jnp.float32),
        lax.psum(query_bias_grad.astype(jnp.bfloat16), "dp").astype(jnp.float32),
        lax.psum(key_weight_grad.astype(jnp.bfloat16), "dp").astype(jnp.float32),
        lax.psum(value_weight_grad.astype(jnp.bfloat16), "dp").astype(jnp.float32),
        lax.psum(value_bias_grad.astype(jnp.bfloat16), "dp").astype(jnp.float32),
        lax.psum(out_weight_grad.astype(jnp.bfloat16), "dp").astype(jnp.float32),
        lax.psum(up_weight_grad.astype(jnp.bfloat16), "dp").astype(jnp.float32),
        lax.psum(up_bias_grad.astype(jnp.bfloat16), "dp").astype(jnp.float32),
        lax.psum(down_weight_grad.astype(jnp.bfloat16), "dp").astype(jnp.float32),
    )
    (
        out_bias_grad,
        first_gain_grad,
        first_shift_grad,
        down_bias_grad,
        second_gain_grad,
        second_shift_grad,
    ) = lax.psum(
        (
            out_bias_grad,
            first_gain_grad,
            first_shift_grad,
            down_bias_grad,
            second_gain_grad,
            second_shift_grad,
        ),
        ("dp", "mp"),
    )
    return (
        layer_out.astype(jnp.bfloat16),
        tokens_grad,
        query_weight_grad,
        query_bias_grad,
        key_weight_grad,
        value_weight_grad,
        value_bias_grad,
        out_weight_grad,
        out_bias_grad,
        first_gain_grad,
        first_shift_grad,
        up_weight_grad,
        up_bias_grad,
        down_weight_grad,
        down_bias_grad,
        second_gain_grad,
        second_shift_grad,
    )


MESH = pl.DeviceIdType.MESH
VMEM_BYTES = 63 * 1024 * 1024
CHUNKS = 4
KINDS = "HBHB"
MORE_X = "HHHB"
JOBS = len(KINDS)


def flip(index, bit):
    low = index // bit % 2
    return index + bit * (1 - 2 * low)


def mp_peer(relation):
    dp, mp = lax.axis_index("dp"), lax.axis_index("mp")
    for bit in (1, 2):
        if relation // bit % 2:
            mp = flip(mp, bit)
    return (dp, mp)


def dp_peer(bit):
    return (flip(lax.axis_index("dp"), bit), lax.axis_index("mp"))


def greet(peers):
    barrier = pltpu.get_barrier_semaphore()
    for device in peers:
        pl.semaphore_signal(barrier, inc=1, device_id=device, device_id_type=MESH)
    pl.semaphore_wait(barrier, len(peers))


def remote(src, dst, send, recv, device):
    return pltpu.make_async_remote_copy(
        src_ref=src, dst_ref=dst, send_sem=send, recv_sem=recv, device_id=device, device_id_type=MESH
    )


def repeat(count, body):
    def step(i, carry):
        body(i)
        return carry

    lax.fori_loop(0, count, step, 0)


class Gather:
    def __init__(self, land, send, recv, chunks=CHUNKS):
        self.land, self.send, self.recv, self.chunks = land, send, recv, chunks
        self.size = land.shape[1] // chunks

    def copy(self, relation, j):
        rows = pl.ds(pl.multiple_of(j * self.size, self.size), self.size)
        return remote(
            self.land.at[2 if relation == 3 else 0, rows],
            self.land.at[relation, rows],
            self.send.at[relation - 1, j],
            self.recv.at[relation - 1, j],
            mp_peer(2 if relation == 2 else 1),
        )

    def start(self, j):
        self.copy(2, j).start()
        self.copy(1, j).start()

    def arrive(self, relation, j):
        self.copy(relation, j).wait_recv()
        if relation == 2:
            self.copy(3, j).start()

    def drain(self):
        def body(j):
            for relation in (1, 2, 3):
                self.copy(relation, j).wait_send()

        repeat(self.chunks, body)


PAIR, FAR, NEAR = 0, 1, 2


class Reduce:
    def __init__(self, out, land, send, recv, chunks=CHUNKS):
        self.out, self.land, self.send, self.recv, self.chunks = out, land, send, recv, chunks
        self.size = out.shape[1] // chunks

    def copy(self, kind, j):
        rows = pl.ds(j * self.size, self.size)
        return remote(
            self.out.at[kind, rows],
            self.land.at[kind, rows],
            self.send.at[kind, j],
            self.recv.at[kind, j],
            mp_peer(2 if kind == FAR else 1),
        )

    def post(self, kind, j, value):
        self.out[kind, pl.ds(j * self.size, self.size)] = value.astype(BF)
        self.copy(kind, j).start()

    def forward_pair(self, j, mine):
        self.copy(PAIR, j).wait_recv()
        rows = pl.ds(j * self.size, self.size)
        self.post(FAR, j, mine + self.land[PAIR, rows].astype(F32))

    def total(self, j, mine):
        self.copy(NEAR, j).wait_recv()
        self.copy(FAR, j).wait_recv()
        rows = pl.ds(j * self.size, self.size)
        return mine + self.land[NEAR, rows].astype(F32) + self.land[FAR, rows].astype(F32)

    def drain(self):
        def body(j):
            for kind in (PAIR, FAR, NEAR):
                self.copy(kind, j).wait_send()

        repeat(self.chunks, body)


ROUTES = {"H": "xlh", "B": "lxh"}


class Spread:
    def __init__(self, data, full, land, send, recv, kinds, first=0, last=3):
        self.data, self.full, self.land, self.send, self.recv = data, full, land, send, recv
        self.sums, self.hands = first < 2, last > 1
        self.kinds, self.jobs = kinds, len(kinds)
        self.count = (full if data is None else data).shape[0] // self.jobs

    def route(self, job):
        return ROUTES[self.kinds[job if isinstance(job, int) else 0]]

    def side(self, axis):
        dp = lax.axis_index("dp")
        return {"x": dp % 2, "z": dp // 2, "l": dp // 2 % 2, "h": dp // 4}[axis]

    def range_of(self, start, size):
        return pl.ds(pl.multiple_of(start, size), size)

    def place(self, job, level):
        start, size = job * self.count, self.count
        for axis in self.route(job)[:level]:
            size //= 4 if axis == "z" else 2
            start += self.side(axis) * size
        return start, size

    def landing(self, job, stage, k=1):
        at, size = 0, self.count
        for level in range(stage + 1):
            ways = 4 if self.route(job)[level] == "z" else 2
            size //= ways
            if level < stage:
                at += size * (ways - 1)
        return self.land.at[job, pl.ds(at + (k - 1) * size, size)]

    def copies(self, job, stage):
        dp, mp = lax.axis_index("dp"), lax.axis_index("mp")
        levels = len(self.route(job))
        back = stage >= levels
        level = 2 * levels - 1 - stage if back else stage
        start, size = self.place(job, level)
        axis = self.route(job)[level]
        here = self.side(axis)
        ways, step = (4, 2) if axis == "z" else (2, {"x": 1, "l": 2, "h": 4}[axis])
        found = []
        for k in range(1, ways):
            there = (here + k) % ways
            if back:
                src = dst = self.full.at[self.range_of(*self.place(job, level + 1))]
            else:
                src = self.data.at[self.range_of(start + there * (size // ways), size // ways)]
                dst = self.landing(job, level, k)
            at = (job, stage * 3 + k - 1)
            device = (dp + (there - here) * step, mp)
            found.append(remote(src, dst, self.send.at[at], self.recv.at[at], device))
        return found

    def own(self, job):
        return self.range_of(*self.place(job, len(self.route(job))))

    def stages(self, job):
        levels = len(self.route(job))
        return (0 if self.sums else levels), (2 * levels if self.hands else levels)

    def step(self, job, stage):
        first, end = self.stages(job)
        levels = len(self.route(job))
        if stage > first:
            arrived = self.copies(job, stage - 1)
            for done in arrived:
                done.wait_send()
                done.wait_recv()
            if stage <= levels:
                rows = self.range_of(*self.place(job, stage))
                total = self.data[rows].astype(F32)
                for k in range(len(arrived)):
                    total += self.landing(job, stage - 1, k + 1)[...].astype(F32)
                target = self.full if stage == levels and self.full is not None else self.data
                target[rows] = total.astype(BF)
        if stage < end:
            for copy in self.copies(job, stage):
                copy.start()


def advance(*moves):
    for total, jobs, stage in moves:
        for job in jobs if isinstance(jobs, tuple) else (jobs,):
            total.step(job, stage)


def spread_land(data, kinds):
    count = data[0] // len(kinds)
    return pltpu.VMEM((len(kinds), count - count // 8, data[1]), BF)


def spread_sems(kinds):
    return [pltpu.SemaphoreType.DMA((len(kinds), 18)), pltpu.SemaphoreType.DMA((len(kinds), 18))]


class Hops:
    def __init__(self, value, land, send, recv, peers):
        self.value, self.land, self.send, self.recv, self.peers = value, land, send, recv, peers

    def copy(self, i):
        return remote(
            self.value.at[i], self.land.at[i], self.send.at[i], self.recv.at[i], self.peers[i]
        )

    def start(self, i):
        self.copy(i).start()

    def finish(self, i):
        self.copy(i).wait_recv()
        self.value[i + 1] = self.value[i] + self.land[i]
        self.copy(i).wait_send()


def hop_scratch(count, *shape):
    return [
        pltpu.VMEM((count + 1, *shape), F32),
        pltpu.VMEM((count, *shape), F32),
        pltpu.SemaphoreType.DMA((count,)),
        pltpu.SemaphoreType.DMA((count,)),
    ]


def greet_all():
    dp, mp = lax.axis_index("dp"), lax.axis_index("mp")
    across = [((dp // 2 + k) % 4 * 2 + dp % 2, mp) for k in (1, 2, 3)]
    greet([mp_peer(1), mp_peer(2), dp_peer(1), *across])


def transfer_sems(chunks=CHUNKS):
    return [pltpu.SemaphoreType.DMA((3, chunks)), pltpu.SemaphoreType.DMA((3, chunks))]


def comm_params(collective_id):
    return pltpu.CompilerParams(
        collective_id=collective_id, has_side_effects=True, vmem_limit_bytes=VMEM_BYTES
    )


WHOLE = pl.BlockSpec(memory_space=pltpu.VMEM)


def shaped(*shape, dtype=None):
    return jax.ShapeDtypeStruct(shape, dtype or BF)


def as_row(ref):
    return ref[...].astype(F32)[None]


def column_sum(value):
    return jnp.sum(value, 0, keepdims=True)


def row_mean(value):
    return jnp.mean(value, -1, keepdims=True)


def project_kernel(
    x_ref, wq_ref, wk_ref, wv_ref, qb_ref, vb_ref, q_ref, k_ref, v_ref, vt_ref, all_ref, land, send, recv, save
):
    rows_here = land.shape[1]
    load = pltpu.make_async_copy(x_ref, land.at[0], save.at[0])
    load.start()
    load.wait()
    greet([mp_peer(1), mp_peer(2)])
    gather = Gather(land, send, recv)
    repeat(CHUNKS, gather.start)
    size = gather.size

    def store(s, j):
        rows = pl.ds(pl.multiple_of(j * size, size), size)
        return pltpu.make_async_copy(land.at[s, rows], all_ref.at[s, rows], save.at[1 + s * CHUNKS + j])

    def emit(x, at):
        rows = pl.ds(pl.multiple_of(at, x.shape[0]), x.shape[0])
        q = (mm(x, wq_ref[...], 1, 0) + as_row(qb_ref)).astype(BF)
        q_ref[rows] = (q.astype(F32) * HD**-0.5).astype(BF)
        k_ref[rows] = mm(x, wk_ref[...], 1, 0).astype(BF)
        v = mm(x, wv_ref[...], 1, 0) + as_row(vb_ref)
        v_ref[rows] = v.astype(BF)
        vt_ref[:, rows] = v.T.astype(BF)

    def close(i):
        s, j = i // 2, i % 2 * 2

        @pl.when(i >= 2)
        def _():
            gather.arrive(1, j)
            gather.arrive(1, j + 1)

        emit(land[s, pl.ds(pl.multiple_of(j * size, 2 * size), 2 * size)], i * 2 * size)
        store(s, j).start()
        store(s, j + 1).start()

    repeat(4, close)

    def far(j):
        gather.arrive(2, j)
        gather.arrive(3, j)

        def one(k):
            emit(land[2 + k, pl.ds(pl.multiple_of(j * size, size), size)], (2 + k) * rows_here + j * size)
            store(2 + k, j).start()

        repeat(2, one)

    repeat(CHUNKS, far)
    gather.drain()
    repeat(4, lambda s: repeat(CHUNKS, lambda j: store(s, j).wait()))


def gather_project(tokens, wq, wk, wv, q_bias, v_bias):
    rows, width = tokens.shape
    cols = wq.shape[1]
    return pl.pallas_call(
        project_kernel,
        in_specs=[pl.BlockSpec(memory_space=pl.ANY)] + [WHOLE] * 5,
        out_specs=[WHOLE] * 4 + [pl.BlockSpec(memory_space=pl.ANY)],
        out_shape=[shaped(4 * rows, cols)] * 3 + [shaped(cols, 4 * rows), shaped(4, rows, width)],
        scratch_shapes=[
            pltpu.VMEM((4, rows, width), BF),
            *transfer_sems(),
            pltpu.SemaphoreType.DMA((4 * CHUNKS + 1,)),
        ],
        name="gather_project",
        compiler_params=comm_params(0),
    )(tokens, wq, wk, wv, q_bias, v_bias)


HALVES = 2


def forward_order(step):
    far = 2 * (3 - step % 2) + step // 2
    near = 2 * (1 - (step - 4) // 2) + step % 2
    return jnp.where(step < 4, far, near)


def attend_kernel(
    len_ref, q_ref, k_ref, vt_ref, w_ref, x_ref, ob_ref, gain_ref, shift_ref,
    e_ref, o_ref, r_ref, n_ref, i_ref, h_ref,
    k_aug, v_aug, out, land, mine, pending, send, recv,
):
    step = pl.program_id(0)
    seq_len, block = k_ref.shape[0], q_ref.shape[0]
    pairs = k_ref.shape[1] // WIDE
    reduce = Reduce(out, land, send, recv, HALVES)

    @pl.when(step == 0)
    def _():
        greet([mp_peer(1), mp_peer(2)])
        lanes = lax.broadcasted_iota(jnp.int32, (seq_len, WIDE), 1)
        rows = lax.broadcasted_iota(jnp.int32, (x_ref.shape[0], WIDE), 0)
        bias = jnp.concatenate(
            [
                jnp.where(rows + mp_peer(s)[1] * x_ref.shape[0] < len_ref[0, 0], 0.0, MASKED)
                for s in range(4)
            ],
            0,
        )
        for p in range(pairs):
            keys = k_ref[:, p * WIDE : (p + 1) * WIDE].astype(F32)
            for h in range(2):
                other = (1 - h) * HD
                k_aug[2 * p + h] = jnp.where(
                    lanes // HD == h, keys, jnp.where(lanes == other, bias, 0.0)
                ).astype(BF)
                at = (2 * p + h) * HD
                v_aug[2 * p + h, :HD] = vt_ref[at : at + HD, :]
                v_aug[2 * p + h, HD:] = jnp.ones((16, seq_len), BF)

    lanes = lax.broadcasted_iota(jnp.int32, (block, WIDE), 1)
    outs = []
    for p in range(pairs):
        query = q_ref[:, p * WIDE : (p + 1) * WIDE].astype(F32)
        scores = []
        for h in range(2):
            other = (1 - h) * HD
            q_aug = jnp.where(
                lanes // HD == h, query, jnp.where(lanes == other, 1.0, 0.0)
            ).astype(BF)
            scores.append(mm(k_aug[2 * p + h], q_aug, 1, 1))
        for h in range(2):
            top = jnp.max(scores[h], 0, keepdims=True)
            expon = jnp.exp(scores[h] - top).astype(BF)
            e_ref[0, 2 * p + h] = expon
            total = mm(v_aug[2 * p + h], expon, 1, 0)
            inverse = 1.0 / total[HD : HD + 1]
            r_ref[0, 2 * p + h] = inverse
            outs.append(total[:HD] * inverse)
    attended = jnp.concatenate(outs, 0).T.astype(BF)
    o_ref[...] = attended
    partial_rows = mm(attended, w_ref[...], 1, 0)

    for t in range(4 * HALVES):

        @pl.when(step == t)
        def _(t=t):
            if t < 4 and t % 2 == 0:
                reduce.post(PAIR, t // 2, partial_rows)
            elif t < 4:
                pending[...] = partial_rows
                reduce.forward_pair(t // 2, pending[...])
            elif t < 6:
                reduce.post(NEAR, t - 4, partial_rows)
            else:
                mine[pl.ds((t - 6) * block, block)] = partial_rows

    @pl.when(step == 4 * HALVES - 1)
    def _():
        for j in range(HALVES):
            rows = pl.ds(j * block, block)
            resid = x_ref[rows].astype(F32) + reduce.total(j, mine[rows]) + as_row(ob_ref)
            center = resid - row_mean(resid)
            inv_std = lax.rsqrt(row_mean(center * center) + epsilon)
            normed = center * inv_std
            n_ref[rows] = normed
            i_ref[rows] = inv_std
            h_ref[rows] = (normed * as_row(gain_ref) + as_row(shift_ref)).astype(BF)
        reduce.drain()


def attend(lengths, q, k, vt, out_weight, tokens, *vectors):
    all_rows, cols = q.shape
    rows, width = tokens.shape
    block = rows // HALVES
    heads = cols // HD
    steps = all_rows // block

    def fixed(*shape):
        return pl.BlockSpec(shape, lambda i: (0,) * len(shape))

    return pl.pallas_call(
        attend_kernel,
        grid=(steps,),
        in_specs=[
            pl.BlockSpec(memory_space=pltpu.SMEM),
            pl.BlockSpec((block, cols), lambda i: (forward_order(i), 0)),
            fixed(all_rows, cols),
            fixed(cols, all_rows),
            fixed(cols, width),
            fixed(rows, width),
            *[fixed(width)] * 3,
        ],
        out_specs=[
            pl.BlockSpec((1, heads, all_rows, block), lambda i: (forward_order(i), 0, 0, 0)),
            pl.BlockSpec((block, cols), lambda i: (forward_order(i), 0)),
            pl.BlockSpec((1, heads, 1, block), lambda i: (forward_order(i), 0, 0, 0)),
            fixed(rows, width),
            fixed(rows, 1),
            fixed(rows, width),
        ],
        out_shape=[
            shaped(steps, heads, all_rows, block),
            shaped(all_rows, cols),
            shaped(steps, heads, 1, block, dtype=F32),
            shaped(rows, width, dtype=F32),
            shaped(rows, 1, dtype=F32),
            shaped(rows, width),
        ],
        scratch_shapes=[
            pltpu.VMEM((heads, all_rows, WIDE), BF),
            pltpu.VMEM((heads, HD + 16, all_rows), BF),
            pltpu.VMEM((3, rows, width), BF),
            pltpu.VMEM((3, rows, width), BF),
            pltpu.VMEM((rows, width), F32),
            pltpu.VMEM((block, width), F32),
            *transfer_sems(HALVES),
        ],
        name="attend",
        compiler_params=comm_params(1),
    )(lengths, q, k, vt, out_weight, tokens, *vectors)


ROOT_HALF = 0.7071067811865476
ROOT_TAU = 0.3989422804014327


def feed_forward_kernel(
    h_ref, n_ref, i_ref, g_ref, up_ref, ub_ref, down_ref, *refs
):
    vectors, refs = refs[:5], refs[5:]
    (
        out_ref, b1_ref, r1_ref, upg_ref, downg_ref, small_ref,
        hidden, act, slope, branch, out1, land1, out2, land2, mine, pending, r2,
        gs1, gr1, gs2, gr2, rs1, rr1, rs2, rr2,
        down_land, down_send, down_recv, load,
    ) = refs
    rows_here, width = h_ref.shape
    fetch = pltpu.make_async_copy(h_ref, hidden.at[0], load.at[0])
    fetch.start()
    size = rows_here // CHUNKS
    first_gain, first_shift, down_bias, second_gain, second_shift = map(as_row, vectors)
    greet_all()
    down_sum = Spread(downg_ref, None, down_land, down_send, down_recv, KINDS, 0, 1)
    gather1, gather2 = Gather(hidden, gs1, gr1), Gather(branch, gs2, gr2)
    reduce1, reduce2 = Reduce(out1, land1, rs1, rr1), Reduce(out2, land2, rs2, rr2)
    fetch.wait()
    repeat(CHUNKS, gather1.start)
    small_ref[...] = jnp.zeros_like(small_ref)

    def forward(x):
        pre = mm(x, up_ref[...], 1, 0) + as_row(ub_ref)
        cdf = 0.5 + 0.5 * lax.erf(pre * ROOT_HALF)
        active = (pre * cdf).astype(BF)
        steep = (cdf + pre * jnp.exp(-0.5 * pre * pre) * ROOT_TAU).astype(BF)
        return active, steep, mm(active, down_ref[...], 1, 0)

    def backward(grad, steep):
        pre_grad = (mm(grad, down_ref[...], 1, 1) * steep.astype(F32)).astype(BF)
        small_ref[6:7] += column_sum(pre_grad.astype(F32))
        return pre_grad, mm(pre_grad, up_ref[...], 1, 1)

    def chunk_rows(j):
        return pl.ds(pl.multiple_of(j * size, size), size)

    def double_rows(j):
        return pl.ds(pl.multiple_of(j * 2 * size, 2 * size), 2 * size)

    def halves(value):
        return value[:size], value[size:]

    def close_forward(i):
        s, half = i // 2, i % 2
        rows = double_rows(half)

        @pl.when(i >= 2)
        def _():
            gather1.arrive(1, 2 * half)
            gather1.arrive(1, 2 * half + 1)

        act[s, rows], slope[s, rows], part = forward(hidden[s, rows])

        @pl.when(i < 2)
        def _():
            mine[rows] = part

        @pl.when(i >= 2)
        def _():
            for k, piece in enumerate(halves(part)):
                reduce1.post(NEAR, 2 * half + k, piece)

    def far_forward(j):
        gather1.arrive(2, j)
        gather1.arrive(3, j)
        rows = chunk_rows(j)
        active, steep, part = forward(jnp.concatenate([hidden[2, rows], hidden[3, rows]], 0))
        for s in (2, 3):
            act[s, rows] = halves(active)[s - 2]
            slope[s, rows] = halves(steep)[s - 2]
        pending[rows] = part[:size]
        reduce1.post(PAIR, j, part[size:])

        @pl.when(j > 0)
        def _():
            reduce1.forward_pair(j - 1, pending[chunk_rows(j - 1)])

    repeat(4, close_forward)
    repeat(CHUNKS, far_forward)
    reduce1.forward_pair(CHUNKS - 1, pending[chunk_rows(CHUNKS - 1)])

    def second_norm(j):
        rows = chunk_rows(j)
        hidden = n_ref[rows] * first_gain + first_shift
        resid = hidden + reduce1.total(j, mine[rows]) + down_bias
        center = resid - row_mean(resid)
        inv_std = lax.rsqrt(row_mean(center * center) + epsilon)
        normed = center * inv_std
        out_ref[rows] = (normed * second_gain + second_shift).astype(BF)
        grad = g_ref[rows].astype(F32)
        product = grad * normed
        small_ref[0:1] += column_sum(product)
        small_ref[1:2] += column_sum(grad)
        scaled = grad * second_gain
        back = inv_std * (scaled - row_mean(scaled) - normed * row_mean(scaled * normed))
        small_ref[2:3] += column_sum(back)
        r2[rows] = back
        branch[0, rows] = back.astype(BF)
        gather2.start(j)

    repeat(CHUNKS, second_norm)

    def close_backward(i):
        s, half = i // 2, i % 2
        rows = double_rows(half)

        @pl.when(i >= 2)
        def _():
            gather2.arrive(1, 2 * half)
            gather2.arrive(1, 2 * half + 1)

        slope[s, rows], part = backward(branch[s, rows], slope[s, rows])

        @pl.when(i < 2)
        def _():
            mine[rows] = part

        @pl.when(i >= 2)
        def _():
            for k, piece in enumerate(halves(part)):
                reduce2.post(NEAR, 2 * half + k, piece)

    def far_backward(j):
        gather2.arrive(2, j)
        gather2.arrive(3, j)
        rows = chunk_rows(j)
        pre_grad, part = backward(
            jnp.concatenate([branch[2, rows], branch[3, rows]], 0),
            jnp.concatenate([slope[2, rows], slope[3, rows]], 0),
        )
        for s in (2, 3):
            slope[s, rows] = halves(pre_grad)[s - 2]
        pending[rows] = part[:size]
        reduce2.post(PAIR, j, part[size:])

        @pl.when(j > 0)
        def _():
            reduce2.forward_pair(j - 1, pending[chunk_rows(j - 1)])

    repeat(4, close_backward)
    repeat(CHUNKS, far_backward)
    reduce2.forward_pair(CHUNKS - 1, pending[chunk_rows(CHUNKS - 1)])

    tile = 256

    def down_grad(t):
        cols = pl.ds(pl.multiple_of(t * tile, tile), tile)
        total = mm(act[0, :, cols], branch[0], 0, 0)
        for s in (1, 2, 3):
            total += mm(act[s, :, cols], branch[s], 0, 0)
        downg_ref[cols] = total.astype(BF)

    def up_grad(t):
        cols = pl.ds(pl.multiple_of(t * tile, tile), tile)
        total = mm(hidden[0, :, cols], slope[0], 0, 0)
        for s in (1, 2, 3):
            total += mm(hidden[s, :, cols], slope[s], 0, 0)
        upg_ref[cols] = total.astype(BF)

    repeat(2, down_grad)
    advance((down_sum, (0, 1), 0))
    repeat(2, lambda t: down_grad(t + 2))
    advance((down_sum, (2, 3), 0))
    repeat(width // tile, up_grad)

    def first_norm(j):
        rows = chunk_rows(j)
        normed = n_ref[rows]
        grad = r2[rows] + reduce2.total(j, mine[rows])
        small_ref[3:4] += column_sum(grad * normed)
        small_ref[4:5] += column_sum(grad)
        scaled = grad * first_gain
        back = i_ref[rows] * (scaled - row_mean(scaled) - normed * row_mean(scaled * normed))
        small_ref[5:6] += column_sum(back)
        r1_ref[rows] = back
        b1_ref[rows] = back.astype(BF)

    advance((down_sum, (0, 1), 1))
    first_norm(0)
    advance((down_sum, (2, 3), 1))
    first_norm(1)
    advance((down_sum, (0, 1), 2))
    first_norm(2)
    advance((down_sum, (2, 3), 2))
    first_norm(3)
    advance((down_sum, (0, 1, 2, 3), 3))
    for transfer in (gather1, gather2, reduce1, reduce2):
        transfer.drain()


def feed_forward(hidden, normed, inv_std, output_grad, up, up_bias, down, *vectors):
    rows, width = hidden.shape
    units = up.shape[1]
    tall = (4, rows, units)
    return pl.pallas_call(
        feed_forward_kernel,
        in_specs=[pl.BlockSpec(memory_space=pl.ANY)] + [WHOLE] * 11,
        out_specs=[WHOLE] * 6,
        out_shape=[
            shaped(rows, width),
            shaped(rows, width),
            shaped(rows, width, dtype=F32),
            shaped(width, units),
            shaped(units, width),
            shaped(8, width, dtype=F32),
        ],
        scratch_shapes=[
            pltpu.VMEM((4, rows, width), BF),
            pltpu.VMEM(tall, BF),
            pltpu.VMEM(tall, BF),
            pltpu.VMEM((4, rows, width), BF),
            *[pltpu.VMEM((3, rows, width), BF)] * 4,
            *[pltpu.VMEM((rows, width), F32)] * 3,
            *transfer_sems(),
            *transfer_sems(),
            *transfer_sems(),
            *transfer_sems(),
            spread_land((units, width), KINDS),
            *spread_sems(KINDS),
            pltpu.SemaphoreType.DMA((1,)),
        ],
        name="feed_forward",
        compiler_params=comm_params(2),
    )(hidden, normed, inv_std, output_grad, up, up_bias, down, *vectors)


def attend_back_kernel(
    b_ref, w_ref, e_ref, r_ref, q_ref, k_ref, v_ref, o_ref, small_in, up_in, down_in, all_in,
    dq_ref, dk_ref, dv_ref, wg_ref, pg_ref, small_ref, up_out, down_out,
    land, v_aug, k_t, dks, dvs, dqs, w_total, w_low, p_low, grads, up, down, tokens, loads, send, recv,
    up_land, up_send, up_recv, down_send, down_recv, out_land, out_send, out_recv,
    pair_land, pair_send, pair_recv, value, small_land, small_send, small_recv,
):
    step = pl.program_id(0)
    pair, s_now = step // 2 % 2, step // 4 * 2 + step % 2
    seq_len, block = k_ref.shape[0], q_ref.shape[0]
    pieces = e_ref.shape[0]
    cols = w_ref.shape[0]
    width = w_ref.shape[1]
    half = block // 2
    gather = Gather(land, send, recv, HALVES)
    up_sum = Spread(up, None, up_land, up_send, up_recv, MORE_X, 0, 1)
    down_sum = Spread(None, down, None, down_send, down_recv, KINDS, 2, 3)
    out_sum = Spread(w_low, None, out_land, out_send, out_recv, "H", 0, 1)
    pair_sum = Spread(p_low, None, pair_land, pair_send, pair_recv, MORE_X, 0, 1)
    small = Hops(
        value, small_land, small_send, small_recv,
        [dp_peer(1), dp_peer(2), dp_peer(4), mp_peer(1), mp_peer(2)],
    )
    load_up = pltpu.make_async_copy(up_in, up, loads.at[0])
    load_down = [
        pltpu.make_async_copy(
            down_in.at[down_sum.own(job)], down.at[down_sum.own(job)], loads.at[5 + job]
        )
        for job in range(JOBS)
    ]
    load_tokens = pltpu.make_async_copy(all_in, tokens, loads.at[2])
    save_up = pltpu.make_async_copy(up, up_out, loads.at[3])
    save_down = pltpu.make_async_copy(down, down_out, loads.at[4])

    load_branch = pltpu.make_async_copy(b_ref, land.at[0], loads.at[5 + JOBS])

    @pl.when(step == 0)
    def _():
        load_branch.start()
        for load in load_down:
            load.start()
        load_up.start()
        load_tokens.start()
        value[0] = small_in[...]
        w_total[...] = jnp.zeros_like(w_total)
        greet_all()
        small.start(0)
        load_branch.wait()
        repeat(HALVES, gather.start)
        for load in load_down:
            load.wait()
        advance((down_sum, (0, 1, 2, 3), 3))
        load_up.wait()
        advance((up_sum, (3, 0, 1, 2), 0))

    @pl.when(step == 1)
    def _():
        repeat(HALVES, lambda j: gather.arrive(1, j))

    @pl.when(step == 2)
    def _():
        small.finish(0)
        small.start(1)
        advance((down_sum, (0, 1, 2, 3), 4), (up_sum, (3, 0), 1))

    @pl.when(step == 3)
    def _():
        advance((up_sum, (1, 2), 1), (down_sum, (0, 1), 5))

    @pl.when(step == 4)
    def _():
        small.finish(1)
        small.start(2)
        advance((up_sum, (3, 0), 2), (down_sum, (2, 3), 5))
        repeat(HALVES, lambda j: gather.arrive(2, j))

    @pl.when(step == 5)
    def _():
        repeat(HALVES, lambda j: gather.arrive(3, j))

    @pl.when(pair == 0)
    def _():
        branch = land[s_now]
        w_total[...] += mm(o_ref[...], branch, 0, 0)
        grads[pl.ds(pl.multiple_of(s_now * block, block), block)] = mm(
            branch, w_ref[...], 1, 1
        ).astype(BF)

    @pl.when(step == 5)
    def _():
        w_low[...] = w_total[...].astype(BF)
        advance((out_sum, 0, 0), (up_sum, (1, 2), 2))

    @pl.when(step == 6)
    def _():
        small.finish(2)
        small.start(3)
        advance((out_sum, 0, 1), (up_sum, (3, 0), 3), (down_sum, (0, 1), 6))

    @pl.when(step == 7)
    def _():
        small.finish(3)
        small.start(4)
        advance(
            (pair_sum, (3, 0, 1, 2), 1), (out_sum, 0, 2), (up_sum, (1, 2), 3), (down_sum, (2, 3), 6)
        )
        save_up.start()
        save_down.start()

    @pl.when(s_now == 0)
    def _():
        lanes = lax.broadcasted_iota(jnp.int32, (seq_len, WIDE), 1)
        values = v_ref[...].astype(F32)
        for h in range(2):
            other = (1 - h) * HD
            ones = jnp.where((lanes >= other) & (lanes < other + 2), 1.0, 0.0)
            v_aug[pair, h] = jnp.where(lanes // HD == h, values, ones).astype(BF)
        k_t[pair] = (k_ref[...].astype(F32) * HD**-0.5).T.astype(BF)
        dks[pair] = jnp.zeros(dks.shape[1:], F32)
        dvs[pair] = jnp.zeros(dvs.shape[1:], F32)

    lanes = lax.broadcasted_iota(jnp.int32, (block, WIDE), 1)
    row_start = pl.multiple_of(s_now * block, block)
    inverse = jnp.concatenate(
        [
            jnp.concatenate(
                [jnp.broadcast_to(r_ref[i, h], (HD, block // pieces)) for h in range(2)], 0
            )
            for i in range(pieces)
        ],
        1,
    ).T
    wide = pl.ds(pl.multiple_of(pair * WIDE, WIDE), WIDE)
    grad = (grads[pl.ds(row_start, block), wide].astype(F32) * inverse).astype(BF)
    grad_wide = grad.astype(F32)
    product = grad_wide * o_ref[:, wide].astype(F32)
    centered = []
    for h in range(2):
        other = (1 - h) * HD
        inside = lanes // HD == h
        row_dot = jnp.sum(jnp.where(inside, product, 0.0), -1, keepdims=True)
        high = row_dot.astype(BF).astype(F32)
        g_aug = jnp.where(
            inside,
            grad_wide,
            jnp.where(lanes == other, -high, jnp.where(lanes == other + 1, high - row_dot, 0.0)),
        ).astype(BF)
        centered.append(mm(v_aug[pair, h], g_aug, 1, 1))
    query_grads = []
    for h in range(2):
        cols_h = slice(h * HD, (h + 1) * HD)
        expon = jnp.concatenate([e_ref[i, h] for i in range(pieces)], 1)
        score_grad = (expon.astype(F32) * centered[h]).astype(BF)
        dvs[pair, h] += mm(expon, grad[:, cols_h], 1, 0)
        dks[pair, h] += mm(score_grad, q_ref[:, cols_h], 1, 0)
        query_grads.append(mm(k_t[pair, cols_h, :], score_grad, 1, 0))
    query_grad = jnp.concatenate(query_grads, 0).T.astype(BF)
    dq_ref[...] = query_grad
    dqs[pair, pl.ds(row_start, block), :WIDE] = query_grad

    @pl.when(s_now == 3)
    def _():
        for total, out, at in ((dks, dk_ref, WIDE), (dvs, dv_ref, 2 * WIDE)):
            joined = jnp.concatenate([total[pair, h] for h in range(2)], 1).astype(BF)
            out[:, wide] = joined
            dqs[pair, :, at : at + WIDE] = joined

    @pl.when(step == 5)
    def _():
        load_tokens.wait()
        projection_grads(tokens, dqs.at[0], p_low)
        advance((pair_sum, (3, 0, 1, 2), 0))

    @pl.when(step == 7)
    def _():
        advance((pair_sum, (3, 0, 1, 2), 2), (out_sum, 0, 3), (pair_sum, (3, 0, 1, 2), 3))
        small.finish(4)
        small_ref[...] = value[5]
        small_ref[6:7] = value[3, 6:7]
        wg_ref[...] = w_low[...]
        pg_ref[...] = p_low[...]
        gather.drain()
        save_down.wait()
        save_up.wait()


def projection_grads(tokens, joint, out_ref):
    tile = 256
    rows = tokens.shape[1]

    def body(t):
        cols = pl.ds(pl.multiple_of(t * tile, tile), tile)
        total = mm(tokens[0, :, cols], joint[pl.ds(0, rows)], 0, 0)
        for s in (1, 2, 3):
            total += mm(tokens[s, :, cols], joint[pl.ds(s * rows, rows)], 0, 0)
        out_ref[cols] = total.astype(BF)

    repeat(tokens.shape[2] // tile, body)


def attend_back(branch, out_weight, expon, inverse, q, k, v, attended, small, up, down, gathered):
    rows, width = branch.shape
    all_rows, cols = q.shape
    pairs = cols // WIDE
    pieces = HALVES

    def fixed(*shape):
        return pl.BlockSpec(shape, lambda i: (0,) * len(shape))

    def pair_at(i):
        return i // 2 % 2

    def rows_at(i):
        return i // 4 * 2 + i % 2

    anywhere = pl.BlockSpec(memory_space=pl.ANY)
    pair_rows = pl.BlockSpec((rows, WIDE), lambda i: (rows_at(i), pair_at(i)))
    pair_keys = pl.BlockSpec((all_rows, WIDE), lambda i: (0, pair_at(i)))
    return pl.pallas_call(
        attend_back_kernel,
        grid=(4 * pairs,),
        in_specs=[
            anywhere,
            fixed(cols, width),
            pl.BlockSpec((pieces, 2, all_rows, rows // pieces), lambda i: (rows_at(i), pair_at(i), 0, 0)),
            pl.BlockSpec((pieces, 2, 1, rows // pieces), lambda i: (rows_at(i), pair_at(i), 0, 0)),
            pair_rows,
            pair_keys,
            pair_keys,
            pl.BlockSpec((rows, cols), lambda i: (rows_at(i), 0)),
            fixed(*small.shape),
            anywhere,
            anywhere,
            anywhere,
        ],
        out_specs=[
            pair_rows,
            fixed(all_rows, cols),
            fixed(all_rows, cols),
            fixed(cols, width),
            fixed(width, 3 * WIDE),
            fixed(*small.shape),
            anywhere,
            anywhere,
        ],
        out_shape=[shaped(all_rows, cols)] * 3
        + [
            shaped(cols, width),
            shaped(width, 3 * WIDE),
            shaped(*small.shape, dtype=F32),
            shaped(*up.shape),
            shaped(*down.shape),
        ],
        scratch_shapes=[
            pltpu.VMEM((4, rows, width), BF),
            pltpu.VMEM((pairs, 2, all_rows, WIDE), BF),
            pltpu.VMEM((pairs, WIDE, all_rows), BF),
            pltpu.VMEM((pairs, 2, all_rows, HD), F32),
            pltpu.VMEM((pairs, 2, all_rows, HD), F32),
            pltpu.VMEM((pairs, all_rows, 3 * WIDE), BF),
            pltpu.VMEM((cols, width), F32),
            pltpu.VMEM((cols, width), BF),
            pltpu.VMEM((width, 3 * WIDE), BF),
            pltpu.VMEM((all_rows, cols), BF),
            pltpu.VMEM(up.shape, BF),
            pltpu.VMEM(down.shape, BF),
            pltpu.VMEM(gathered.shape, BF),
            pltpu.SemaphoreType.DMA((6 + JOBS,)),
            *transfer_sems(HALVES),
            spread_land(up.shape, MORE_X),
            *spread_sems(KINDS),
            *spread_sems(KINDS),
            spread_land((cols, width), "H"),
            *spread_sems("H"),
            spread_land((width, 3 * WIDE), KINDS),
            *spread_sems(KINDS),
            *hop_scratch(5, *small.shape),
        ],
        name="attend_back",
        compiler_params=comm_params(3),
    )(branch, out_weight, expon, inverse, q, k, v, attended, small, up, down, gathered)


def input_back_kernel(
    dq_ref, dk_ref, dv_ref, wq_ref, wk_ref, wv_ref, all_ref, r1_ref, wg_in, pg_in, up_in,
    x_ref, wg_ref, pg_ref, last_ref, bias_ref, up_out,
    out, land, mine, pending, send, recv, up, loads, up_send, up_recv, out_send, out_recv,
    pair_send, pair_recv, joint, w_full, p_full, last_full, last_low, last_land, last_send, last_recv,
    value, bias_land, bias_send, bias_recv,
):
    rows_here = r1_ref.shape[0]
    size = rows_here // CHUNKS
    last = dq_ref.shape[1] - WIDE
    up_sum = Spread(None, up, None, up_send, up_recv, MORE_X, 2, 3)
    out_sum = Spread(None, w_full, None, out_send, out_recv, "H", 2, 3)
    pair_sum = Spread(None, p_full, None, pair_send, pair_recv, MORE_X, 2, 3)
    last_sum = Spread(last_low, last_full, last_land, last_send, last_recv, KINDS)
    bias = Hops(value, bias_land, bias_send, bias_recv, [dp_peer(1), dp_peer(2), dp_peer(4)])
    reduce = Reduce(out, land, send, recv)
    save_up = pltpu.make_async_copy(up, up_out, loads.at[JOBS])
    load_up = [
        pltpu.make_async_copy(up_in.at[up_sum.own(job)], up.at[up_sum.own(job)], loads.at[job])
        for job in range(JOBS)
    ]
    for load in load_up:
        load.start()
    w_full[out_sum.own(0)] = wg_in[out_sum.own(0)]
    for job in range(JOBS):
        p_full[pair_sum.own(job)] = pg_in[pair_sum.own(job)]
    value[0, 0:1] = column_sum(dq_ref[...].astype(F32))
    value[0, 1:8] = jnp.broadcast_to(column_sum(dv_ref[...].astype(F32)), (7, dv_ref.shape[1]))
    greet_all()
    bias.start(0)
    for load in load_up:
        load.wait()
    advance((pair_sum, (3, 0, 1, 2), 3), (out_sum, 0, 3), (up_sum, (0, 1, 2, 3), 3))
    tail = pl.ds(last, WIDE)
    for at, grad in enumerate((dq_ref, dk_ref, dv_ref)):
        joint[:, at * WIDE : (at + 1) * WIDE] = grad[:, tail]
    projection_grads(all_ref, joint, last_low)
    advance((last_sum, (0, 1, 2, 3), 0))
    grads = ((dq_ref, wq_ref), (dk_ref, wk_ref), (dv_ref, wv_ref))

    def part_of(starts, count):
        total = None
        for grad, weight in grads:
            pieces = [grad[pl.ds(pl.multiple_of(at, size), count)] for at in starts]
            x = pieces[0] if len(pieces) == 1 else jnp.concatenate(pieces, 0)
            term = mm(x, weight[...], 1, 1)
            total = term if total is None else total + term
        return total

    def chunk_rows(j):
        return pl.ds(pl.multiple_of(j * size, size), size)

    def far(j):
        part = part_of((2 * rows_here + j * size, 3 * rows_here + j * size), size)
        pending[chunk_rows(j)] = part[:size]
        reduce.post(PAIR, j, part[size:])

        @pl.when(j > 0)
        def _():
            reduce.forward_pair(j - 1, pending[chunk_rows(j - 1)])

    repeat(CHUNKS, far)
    reduce.forward_pair(CHUNKS - 1, pending[chunk_rows(CHUNKS - 1)])
    bias.finish(0)
    bias.start(1)
    advance((pair_sum, (3, 0, 1, 2), 4), (last_sum, (0, 1, 2, 3), 1), (up_sum, (3, 0), 4))

    def near(i):
        part = part_of((rows_here + i * 2 * size,), 2 * size)
        reduce.post(NEAR, 2 * i, part[:size])
        reduce.post(NEAR, 2 * i + 1, part[size:])

    repeat(2, near)

    def own(i):
        mine[pl.ds(pl.multiple_of(i * 2 * size, 2 * size), 2 * size)] = part_of((i * 2 * size,), 2 * size)

    repeat(2, own)

    def finish(j):
        rows = chunk_rows(j)
        x_ref[rows] = (r1_ref[rows] + reduce.total(j, mine[rows])).astype(BF)

    advance((pair_sum, (3, 0, 1, 2), 5), (up_sum, (1, 2), 4))
    finish(0)
    bias.finish(1)
    bias.start(2)
    advance((last_sum, (0, 1, 2, 3), 2), (up_sum, (3, 0), 5), (out_sum, 0, 4))
    finish(1)
    advance((last_sum, (0, 1, 2, 3), 3), (up_sum, (1, 2), 5), (out_sum, 0, 5))
    finish(2)
    advance((last_sum, (0, 1, 2, 3), 4))
    finish(3)
    bias.finish(2)
    bias_ref[...] = value[3]
    advance((last_sum, (0, 1, 2, 3), 5), (up_sum, (0, 1, 2, 3), 6))
    save_up.start()
    advance((pair_sum, (3, 0, 1, 2), 6), (out_sum, 0, 6))
    wg_ref[...] = w_full[...]
    pg_ref[...] = p_full[...]
    advance((last_sum, (0, 1, 2, 3), 6))
    last_ref[...] = last_full[...]
    reduce.drain()
    save_up.wait()


def input_back(dq, dk, dv, wq, wk, wv, gathered, resid_grad, out_grad, pair_grad, up):
    rows, width = resid_grad.shape
    cols = dq.shape[1]
    return pl.pallas_call(
        input_back_kernel,
        in_specs=[WHOLE] * 10 + [pl.BlockSpec(memory_space=pl.ANY)],
        out_specs=[WHOLE] * 5 + [pl.BlockSpec(memory_space=pl.ANY)],
        out_shape=[
            shaped(rows, width),
            shaped(*out_grad.shape),
            shaped(*pair_grad.shape),
            shaped(*pair_grad.shape),
            shaped(8, cols, dtype=F32),
            shaped(*up.shape),
        ],
        scratch_shapes=[
            pltpu.VMEM((3, rows, width), BF),
            pltpu.VMEM((3, rows, width), BF),
            pltpu.VMEM((rows, width), F32),
            pltpu.VMEM((rows, width), F32),
            *transfer_sems(),
            pltpu.VMEM(up.shape, BF),
            pltpu.SemaphoreType.DMA((JOBS + 1,)),
            *spread_sems(KINDS),
            *spread_sems("H"),
            *spread_sems(KINDS),
            pltpu.VMEM((dq.shape[0], 3 * WIDE), BF),
            pltpu.VMEM(out_grad.shape, BF),
            *[pltpu.VMEM(pair_grad.shape, BF)] * 3,
            spread_land(pair_grad.shape, KINDS),
            *spread_sems(KINDS),
            *hop_scratch(3, 8, cols),
        ],
        name="input_back",
        compiler_params=comm_params(4),
    )(dq, dk, dv, wq, wk, wv, gathered, resid_grad, out_grad, pair_grad, up)


def widen_kernel(up_ref, down_ref, out_ref, pair_ref, last_ref, upw, downw, outw, qw, kw, vw):
    upw[...] = up_ref[...].astype(F32)
    downw[...] = down_ref[...].astype(F32)
    outw[...] = out_ref[...].astype(F32)
    for at, wide in enumerate((qw, kw, vw)):
        cols = slice(at * WIDE, (at + 1) * WIDE)
        wide[:, :WIDE] = pair_ref[:, cols].astype(F32)
        wide[:, WIDE:] = last_ref[:, cols].astype(F32)


def widen_grads(*grads):
    steps = 8
    shapes = [g.shape for g in grads[:3]] + [(grads[3].shape[0], 2 * WIDE)] * 3

    def tiles(shape):
        return pl.BlockSpec((shape[0] // steps, shape[1]), lambda i: (i, 0))

    return pl.pallas_call(
        widen_kernel,
        grid=(steps,),
        in_specs=[tiles(g.shape) for g in grads],
        out_specs=[tiles(shape) for shape in shapes],
        out_shape=[shaped(*shape, dtype=F32) for shape in shapes],
        name="widen_grads",
    )(*grads)


def per_device(
    tokens, lengths, query_weight, query_bias, key_weight, value_weight, value_bias, out_weight,
    out_bias, first_gain, first_shift, up_weight, up_bias, down_weight, down_bias, second_gain,
    second_shift, output_grad,
):
    pairs = query_weight.shape[1] // WIDE
    if (lax.axis_size("dp"), lax.axis_size("mp"), lengths.shape[1], pairs) != (8, 4, 1, 2):
        return per_device_general(
            tokens, lengths, query_weight, query_bias, key_weight, value_weight, value_bias,
            out_weight, out_bias, first_gain, first_shift, up_weight, up_bias, down_weight,
            down_bias, second_gain, second_shift, output_grad,
        )
    q, k, v, vt, gathered = gather_project(
        tokens, query_weight, key_weight, value_weight, query_bias, value_bias
    )
    expon, attended, inverse, normed, inv_std, hidden = attend(
        lengths, q, k, vt, out_weight, tokens, out_bias, first_gain, first_shift
    )
    layer_out, branch, resid_grad, up_grad, down_grad, small = feed_forward(
        hidden, normed, inv_std, output_grad, up_weight, up_bias, down_weight,
        first_gain, first_shift, down_bias, second_gain, second_shift,
    )
    dq, dk, dv, out_grad, pair_grad, small, up_grad, down_grad = attend_back(
        branch, out_weight, expon, inverse, q, k, v, attended, small, up_grad, down_grad, gathered
    )
    tokens_grad, out_grad, pair_grad, last_grad, bias_grads, up_grad = input_back(
        dq, dk, dv, query_weight, key_weight, value_weight, gathered, resid_grad, out_grad, pair_grad,
        up_grad,
    )

    up_grad, down_grad, out_grad, query_grad, key_grad, value_grad = widen_grads(
        up_grad, down_grad, out_grad, pair_grad, last_grad
    )
    return (
        layer_out,
        tokens_grad,
        query_grad,
        bias_grads[0],
        key_grad,
        value_grad,
        bias_grads[1],
        out_grad,
        small[5],
        small[3],
        small[4],
        up_grad,
        small[6],
        down_grad,
        small[2],
        small[0],
        small[1],
    )


def solution(mesh):
    placed = (
        P(("dp", "mp"), None),
        P("dp", None),
        P(None, "mp"),
        P("mp"),
        P(None, "mp"),
        P(None, "mp"),
        P("mp"),
        P("mp", None),
        P(),
        P(),
        P(),
        P(None, "mp"),
        P("mp"),
        P("mp", None),
        P(),
        P(),
        P(),
        P(("dp", "mp"), None),
    )
    return jax.shard_map(
        per_device,
        mesh=mesh,
        in_specs=placed,
        out_specs=(
            P(("dp", "mp"), None),
            P(("dp", "mp"), None),
            P(None, "mp"),
            P("mp"),
            P(None, "mp"),
            P(None, "mp"),
            P("mp"),
            P("mp", None),
            P(),
            P(),
            P(),
            P(None, "mp"),
            P("mp"),
            P("mp", None),
            P(),
            P(),
            P(),
        ),
        check_vma=False,
    )
```

```python
from functools import partial

import jax
import jax.numpy as jnp
from jax import lax
from jax.experimental import pallas as pl
from jax.experimental.pallas import tpu as pltpu
from jax.sharding import PartitionSpec as P

HD = 64


epsilon = 1e-12


def norm_forward(resid, gain, shift):
    center = resid - jnp.mean(resid, -1, keepdims=True)
    inv_std = lax.rsqrt(jnp.mean(center * center, -1, keepdims=True) + epsilon)
    normed = center * inv_std
    return (normed * gain + shift, normed, inv_std)


def norm_backward(grad, normed, inv_std, gain):
    scaled = grad * gain
    back = inv_std * (
        scaled
        - jnp.mean(scaled, -1, keepdims=True)
        - normed * jnp.mean(scaled * normed, -1, keepdims=True)
    )
    return (back, jnp.sum(grad * normed, 0), jnp.sum(grad, 0))


F32 = jnp.float32
BF = jnp.bfloat16
MASKED = -1000000000.0
WIDE = 2 * HD


def mm(a, b, ca, cb):
    return lax.dot_general(a, b, (((ca,), (cb,)), ((), ())), preferred_element_type=F32)


def forward_kernel(heads, len_ref, q_ref, k_ref, vt_ref, e_ref, o_ref, r_ref, v_aug, k_aug):
    seq, step = pl.program_id(0), pl.program_id(2)
    seq_len, block = k_ref.shape[0], q_ref.shape[0]

    @pl.when(step == 0)
    def _():
        rows = lax.broadcasted_iota(jnp.int32, (seq_len, WIDE), 0)
        lanes = lax.broadcasted_iota(jnp.int32, (seq_len, WIDE), 1)
        bias = jnp.where(rows < len_ref[seq], 0.0, MASKED)
        keys = k_ref[...].astype(F32)
        for h in range(heads):
            other = (1 - h) * HD
            k_aug[h] = jnp.where(
                lanes // HD == h, keys, jnp.where(lanes == other, bias, 0.0)
            ).astype(BF)
            v_aug[h, :HD] = vt_ref[h * HD : (h + 1) * HD, :]
            v_aug[h, HD:] = jnp.ones((16, seq_len), BF)

    query = q_ref[...].astype(F32) * HD**-0.5
    lanes = lax.broadcasted_iota(jnp.int32, (block, WIDE), 1)
    scores = []
    for h in range(heads):
        other = (1 - h) * HD
        q_aug = jnp.where(
            lanes // HD == h, query, jnp.where(lanes == other, 1.0, 0.0)
        ).astype(BF)
        scores.append(mm(k_aug[h], q_aug, 1, 1))
    outs = []
    for h in range(heads):
        top = jnp.max(scores[h], 0, keepdims=True)
        expon = jnp.exp(scores[h] - top).astype(BF)
        e_ref[h] = expon
        total = mm(v_aug[h], expon, 1, 0)
        inverse = 1.0 / total[HD : HD + 1]
        r_ref[h] = inverse
        outs.append(total[:HD] * inverse)
    if heads == 1:
        outs.append(jnp.zeros_like(outs[0]))
    o_ref[...] = jnp.concatenate(outs, 0).T.astype(BF)


def backward_kernel(
    heads, e_ref, r_ref, q_ref, k_ref, v_ref, o_ref, g_ref, dq_ref, dk_ref, dv_ref, v_aug, k_t, dks, dvs
):
    step, last = pl.program_id(2), pl.num_programs(2) - 1
    seq_len, block = k_ref.shape[0], q_ref.shape[0]

    @pl.when(step == 0)
    def _():
        lanes = lax.broadcasted_iota(jnp.int32, (seq_len, WIDE), 1)
        values = v_ref[...].astype(F32)
        for h in range(heads):
            other = (1 - h) * HD
            ones = jnp.where((lanes >= other) & (lanes < other + 2), 1.0, 0.0)
            v_aug[h] = jnp.where(lanes // HD == h, values, ones).astype(BF)
        k_t[...] = (k_ref[...].astype(F32) * HD**-0.5).T.astype(BF)
        dks[...] = jnp.zeros_like(dks)
        dvs[...] = jnp.zeros_like(dvs)

    lanes = lax.broadcasted_iota(jnp.int32, (block, WIDE), 1)
    inverse = jnp.concatenate(
        [jnp.broadcast_to(r_ref[h % heads], (HD, block)) for h in range(2)], 0
    ).T
    grad = (g_ref[...].astype(F32) * inverse).astype(BF)
    grad_wide = grad.astype(F32)
    scaled_query = (q_ref[...].astype(F32) * HD**-0.5).astype(BF)
    product = grad_wide * o_ref[...].astype(F32)
    centered = []
    for h in range(heads):
        other = (1 - h) * HD
        inside = lanes // HD == h
        row_dot = jnp.sum(jnp.where(inside, product, 0.0), -1, keepdims=True)
        high = row_dot.astype(BF).astype(F32)
        g_aug = jnp.where(
            inside,
            grad_wide,
            jnp.where(lanes == other, -high, jnp.where(lanes == other + 1, high - row_dot, 0.0)),
        ).astype(BF)
        centered.append(mm(v_aug[h], g_aug, 1, 1))
    query_grads = []
    for h in range(heads):
        cols = slice(h * HD, (h + 1) * HD)
        expon = e_ref[h]
        score_grad = (expon.astype(F32) * centered[h]).astype(BF)
        dvs[h] += mm(expon, grad[:, cols], 1, 0)
        dks[h] += mm(score_grad, scaled_query[:, cols], 1, 0)
        query_grads.append(mm(k_t[cols, :], score_grad, 1, 0))
    if heads == 1:
        query_grads.append(jnp.zeros_like(query_grads[0]))
    dq_ref[...] = jnp.concatenate(query_grads, 0).T.astype(BF)

    @pl.when(step == last)
    def _():
        for total, out in ((dks, dk_ref), (dvs, dv_ref)):
            halves = [total[h] for h in range(heads)]
            if heads == 1:
                halves.append(jnp.zeros_like(halves[0]))
            out[...] = jnp.concatenate(halves, 1).astype(BF)


def attention_shape(rows, cols, seqs):
    seq_len = rows // seqs
    block = min(512, seq_len)
    steps = seq_len // block
    pairs = max(1, cols // WIDE)
    heads = cols // HD // pairs
    row_spec = pl.BlockSpec((block, WIDE), lambda s, p, j, *_: (s * steps + j, p))
    key_spec = pl.BlockSpec((seq_len, WIDE), lambda s, p, j, *_: (s, p))
    e_spec = pl.BlockSpec((heads, seq_len, block), lambda s, p, j, *_: (p, s, j))
    r_spec = pl.BlockSpec((heads, 1, block), lambda s, p, j, *_: (p, 0, s * steps + j))
    return seq_len, heads, pairs, (seqs, pairs, steps), row_spec, key_spec, e_spec, r_spec


def widen(array):
    short = WIDE - array.shape[1]
    return array if short <= 0 else jnp.pad(array, ((0, 0), (0, short)))


def attention_forward(queries, keys, values, lengths):
    rows, cols = queries.shape
    seqs = lengths.shape[0]
    seq_len, heads, pairs, grid, row_spec, key_spec, e_spec, r_spec = attention_shape(rows, cols, seqs)
    wide_cols = pairs * WIDE
    expon, attended, inverse = pl.pallas_call(
        partial(forward_kernel, heads),
        grid_spec=pltpu.PrefetchScalarGridSpec(
            num_scalar_prefetch=1,
            grid=grid,
            in_specs=[
                row_spec,
                key_spec,
                pl.BlockSpec((WIDE, seq_len), lambda s, p, j, *_: (p, s)),
            ],
            out_specs=[e_spec, row_spec, r_spec],
            scratch_shapes=[
                pltpu.VMEM((heads, HD + 16, seq_len), BF),
                pltpu.VMEM((heads, seq_len, WIDE), BF),
            ],
        ),
        out_shape=[
            jax.ShapeDtypeStruct((heads * pairs, rows, seq_len), BF),
            jax.ShapeDtypeStruct((rows, wide_cols), BF),
            jax.ShapeDtypeStruct((heads * pairs, 1, rows), F32),
        ],
        name="attention_forward",
        compiler_params=pltpu.CompilerParams(vmem_limit_bytes=60 * 1024 * 1024),
    )(lengths, widen(queries), widen(keys), widen(values).T)
    return expon, attended[:, :cols], inverse


def attention_backward(expon, inverse, queries, keys, values, attended, grad, seqs):
    rows, cols = queries.shape
    seq_len, heads, pairs, grid, row_spec, key_spec, e_spec, r_spec = attention_shape(rows, cols, seqs)
    shape = jax.ShapeDtypeStruct((rows, pairs * WIDE), BF)
    outs = pl.pallas_call(
        partial(backward_kernel, heads),
        grid=grid,
        in_specs=[e_spec, r_spec, row_spec, key_spec, key_spec, row_spec, row_spec],
        out_specs=[row_spec, key_spec, key_spec],
        scratch_shapes=[
            pltpu.VMEM((heads, seq_len, WIDE), BF),
            pltpu.VMEM((WIDE, seq_len), BF),
            pltpu.VMEM((heads, seq_len, HD), F32),
            pltpu.VMEM((heads, seq_len, HD), F32),
        ],
        out_shape=[shape] * 3,
        name="attention_backward",
        compiler_params=pltpu.CompilerParams(vmem_limit_bytes=60 * 1024 * 1024),
    )(expon, inverse, *[widen(x) for x in (queries, keys, values, attended, grad)])
    return [x[:, :cols] for x in outs]


def contract_rows(left, right):
    return lax.dot_general(
        left, right, (((0,), (0,)), ((), ())), preferred_element_type=jnp.float32
    )


def contract_cols(left, right):
    return lax.dot_general(
        left, right, (((1,), (1,)), ((), ())), preferred_element_type=jnp.float32
    )


def split_projection(projected, width, q_bias, v_bias):
    query_part = (projected[:, :width] + q_bias).astype(jnp.bfloat16)
    key_part = projected[:, width : 2 * width].astype(jnp.bfloat16)
    value_part = (projected[:, 2 * width :] + v_bias).astype(jnp.bfloat16)
    return (query_part, key_part, value_part)


def per_device_general(
    tokens,
    lengths,
    query_weight,
    query_bias,
    key_weight,
    value_weight,
    value_bias,
    out_weight,
    out_bias,
    first_gain,
    first_shift,
    up_weight,
    up_bias,
    down_weight,
    down_bias,
    second_gain,
    second_shift,
    output_grad,
):
    local_rows = tokens.shape[0]
    head_cols = query_weight.shape[1]
    seq_count = lengths.shape[1]
    all_rows = local_rows * lax.axis_size("mp")
    gathered = lax.all_gather(tokens, "mp", axis=0, tiled=True)
    joint_weight = jnp.concatenate([query_weight, key_weight, value_weight], 1)
    projected = jnp.dot(gathered, joint_weight, preferred_element_type=jnp.float32)
    queries, key_rows, values = split_projection(projected, head_cols, query_bias, value_bias)
    expon, attended, inverse = attention_forward(queries, key_rows, values, lengths[0])
    branch_one = lax.psum_scatter(
        jnp.dot(
            lax.slice_in_dim(attended, 0, local_rows * lax.axis_size("mp"), axis=0),
            out_weight,
            preferred_element_type=jnp.float32,
        ).astype(jnp.bfloat16),
        "mp",
        scatter_dimension=0,
        tiled=True,
    ).astype(jnp.float32)
    hidden, normed_one, inv_one = norm_forward(
        tokens.astype(jnp.float32) + branch_one + out_bias, first_gain, first_shift
    )
    hidden_low = hidden.astype(jnp.bfloat16)
    hidden_all = lax.all_gather(hidden_low, "mp", axis=0, tiled=True)
    pre_act = jnp.dot(hidden_all, up_weight, preferred_element_type=jnp.float32) + up_bias
    act_low = jax.nn.gelu(pre_act, approximate=False).astype(jnp.bfloat16)
    branch_two = lax.psum_scatter(
        jnp.dot(
            lax.slice_in_dim(act_low, 0, local_rows * lax.axis_size("mp"), axis=0),
            down_weight,
            preferred_element_type=jnp.float32,
        ).astype(jnp.bfloat16),
        "mp",
        scatter_dimension=0,
        tiled=True,
    ).astype(jnp.float32)
    layer_out, normed_two, inv_two = norm_forward(
        hidden + branch_two + down_bias, second_gain, second_shift
    )
    resid_two_grad, second_gain_grad, second_shift_grad = norm_backward(
        output_grad.astype(jnp.float32), normed_two, inv_two, second_gain
    )
    down_bias_grad = jnp.sum(resid_two_grad, 0)
    branch_two_low = resid_two_grad.astype(jnp.bfloat16)
    row_piece = lax.all_gather(branch_two_low, "mp", axis=0, tiled=True)
    row_start = jnp.int32(0)
    weight_acc = jnp.zeros(down_weight.shape, jnp.float32)
    act_acc = jnp.zeros(act_low.shape, jnp.float32)
    act_rows = lax.dynamic_slice_in_dim(act_low, row_start, row_piece.shape[0], 0)
    weight_acc = weight_acc + contract_rows(act_rows, row_piece)
    act_acc = lax.dynamic_update_slice_in_dim(
        act_acc, contract_cols(row_piece, down_weight), row_start, 0
    )
    down_weight_grad = weight_acc
    unused_two, gelu_back = jax.vjp(partial(jax.nn.gelu, approximate=False), pre_act)
    pre_grad = gelu_back(act_acc)[0].astype(jnp.bfloat16)
    up_bias_grad = jnp.sum(pre_grad, 0, dtype=jnp.float32)
    up_weight_grad = contract_rows(hidden_all, pre_grad)
    hidden_back = lax.psum_scatter(
        contract_cols(
            lax.slice_in_dim(pre_grad, 0, local_rows * lax.axis_size("mp"), axis=0), up_weight
        ).astype(jnp.bfloat16),
        "mp",
        scatter_dimension=0,
        tiled=True,
    ).astype(jnp.float32)
    hidden_grad = resid_two_grad + hidden_back
    resid_one_grad, first_gain_grad, first_shift_grad = norm_backward(
        hidden_grad, normed_one, inv_one, first_gain
    )
    out_bias_grad = jnp.sum(resid_one_grad, 0)
    branch_one_low = resid_one_grad.astype(jnp.bfloat16)
    row_piece = lax.all_gather(branch_one_low, "mp", axis=0, tiled=True)
    row_start = jnp.int32(0)
    weight_acc = jnp.zeros(out_weight.shape, jnp.float32)
    attn_acc = jnp.zeros(attended.shape, jnp.float32)
    attn_rows = lax.dynamic_slice_in_dim(attended, row_start, row_piece.shape[0], 0)
    weight_acc = weight_acc + contract_rows(attn_rows, row_piece)
    attn_acc = lax.dynamic_update_slice_in_dim(
        attn_acc, contract_cols(row_piece, out_weight), row_start, 0
    )
    out_weight_grad = weight_acc
    attn_low = attn_acc.astype(jnp.bfloat16)
    query_flat, key_flat, value_flat = attention_backward(
        expon, inverse, queries, key_rows, values, attended, attn_low, seq_count
    )
    width_now = query_flat.shape[1]
    joint_grad = jnp.concatenate([query_flat, key_flat, value_flat], 1)
    query_bias_grad = jnp.sum(query_flat, 0, dtype=jnp.float32)
    value_bias_grad = jnp.sum(value_flat, 0, dtype=jnp.float32)
    joint_weight_grad = contract_rows(gathered, joint_grad)
    input_back = lax.psum_scatter(
        contract_cols(
            lax.slice_in_dim(joint_grad, 0, local_rows * lax.axis_size("mp"), axis=0), joint_weight
        ).astype(jnp.bfloat16),
        "mp",
        scatter_dimension=0,
        tiled=True,
    ).astype(jnp.float32)
    tokens_grad = (resid_one_grad + input_back).astype(jnp.bfloat16)
    query_weight_grad = joint_weight_grad[:, :width_now]
    key_weight_grad = joint_weight_grad[:, width_now : 2 * width_now]
    value_weight_grad = joint_weight_grad[:, 2 * width_now :]
    (
        query_weight_grad,
        query_bias_grad,
        key_weight_grad,
        value_weight_grad,
        value_bias_grad,
        out_weight_grad,
        up_weight_grad,
        up_bias_grad,
        down_weight_grad,
    ) = (
        lax.psum(query_weight_grad.astype(jnp.bfloat16), "dp").astype(jnp.float32),
        lax.psum(query_bias_grad.astype(jnp.bfloat16), "dp").astype(jnp.float32),
        lax.psum(key_weight_grad.astype(jnp.bfloat16), "dp").astype(jnp.float32),
        lax.psum(value_weight_grad.astype(jnp.bfloat16), "dp").astype(jnp.float32),
        lax.psum(value_bias_grad.astype(jnp.bfloat16), "dp").astype(jnp.float32),
        lax.psum(out_weight_grad.astype(jnp.bfloat16), "dp").astype(jnp.float32),
        lax.psum(up_weight_grad.astype(jnp.bfloat16), "dp").astype(jnp.float32),
        lax.psum(up_bias_grad.astype(jnp.bfloat16), "dp").astype(jnp.float32),
        lax.psum(down_weight_grad.astype(jnp.bfloat16), "dp").astype(jnp.float32),
    )
    (
        out_bias_grad,
        first_gain_grad,
        first_shift_grad,
        down_bias_grad,
        second_gain_grad,
        second_shift_grad,
    ) = lax.psum(
        (
            out_bias_grad,
            first_gain_grad,
            first_shift_grad,
            down_bias_grad,
            second_gain_grad,
            second_shift_grad,
        ),
        ("dp", "mp"),
    )
    return (
        layer_out.astype(jnp.bfloat16),
        tokens_grad,
        query_weight_grad,
        query_bias_grad,
        key_weight_grad,
        value_weight_grad,
        value_bias_grad,
        out_weight_grad,
        out_bias_grad,
        first_gain_grad,
        first_shift_grad,
        up_weight_grad,
        up_bias_grad,
        down_weight_grad,
        down_bias_grad,
        second_gain_grad,
        second_shift_grad,
    )


MESH = pl.DeviceIdType.MESH
VMEM_BYTES = 63 * 1024 * 1024
CHUNKS = 4
KINDS = "HBHB"
MORE_X = "HHHB"
JOBS = len(KINDS)


def flip(index, bit):
    low = index // bit % 2
    return index + bit * (1 - 2 * low)


def mp_peer(relation):
    dp, mp = lax.axis_index("dp"), lax.axis_index("mp")
    for bit in (1, 2):
        if relation // bit % 2:
            mp = flip(mp, bit)
    return (dp, mp)


def dp_peer(bit):
    return (flip(lax.axis_index("dp"), bit), lax.axis_index("mp"))


def greet(peers):
    barrier = pltpu.get_barrier_semaphore()
    for device in peers:
        pl.semaphore_signal(barrier, inc=1, device_id=device, device_id_type=MESH)
    pl.semaphore_wait(barrier, len(peers))


def remote(src, dst, send, recv, device):
    return pltpu.make_async_remote_copy(
        src_ref=src, dst_ref=dst, send_sem=send, recv_sem=recv, device_id=device, device_id_type=MESH
    )


def repeat(count, body):
    def step(i, carry):
        body(i)
        return carry

    lax.fori_loop(0, count, step, 0)


class Gather:
    def __init__(self, land, send, recv, chunks=CHUNKS):
        self.land, self.send, self.recv, self.chunks = land, send, recv, chunks
        self.size = land.shape[1] // chunks

    def copy(self, relation, j):
        rows = pl.ds(pl.multiple_of(j * self.size, self.size), self.size)
        return remote(
            self.land.at[2 if relation == 3 else 0, rows],
            self.land.at[relation, rows],
            self.send.at[relation - 1, j],
            self.recv.at[relation - 1, j],
            mp_peer(2 if relation == 2 else 1),
        )

    def start(self, j):
        self.copy(2, j).start()
        self.copy(1, j).start()

    def arrive(self, relation, j):
        self.copy(relation, j).wait_recv()
        if relation == 2:
            self.copy(3, j).start()

    def drain(self):
        def body(j):
            for relation in (1, 2, 3):
                self.copy(relation, j).wait_send()

        repeat(self.chunks, body)


PAIR, FAR, NEAR = 0, 1, 2


class Reduce:
    def __init__(self, out, land, send, recv, chunks=CHUNKS):
        self.out, self.land, self.send, self.recv, self.chunks = out, land, send, recv, chunks
        self.size = out.shape[1] // chunks

    def copy(self, kind, j):
        rows = pl.ds(j * self.size, self.size)
        return remote(
            self.out.at[kind, rows],
            self.land.at[kind, rows],
            self.send.at[kind, j],
            self.recv.at[kind, j],
            mp_peer(2 if kind == FAR else 1),
        )

    def post(self, kind, j, value):
        self.out[kind, pl.ds(j * self.size, self.size)] = value.astype(BF)
        self.copy(kind, j).start()

    def forward_pair(self, j, mine):
        self.copy(PAIR, j).wait_recv()
        rows = pl.ds(j * self.size, self.size)
        self.post(FAR, j, mine + self.land[PAIR, rows].astype(F32))

    def total(self, j, mine):
        self.copy(NEAR, j).wait_recv()
        self.copy(FAR, j).wait_recv()
        rows = pl.ds(j * self.size, self.size)
        return mine + self.land[NEAR, rows].astype(F32) + self.land[FAR, rows].astype(F32)

    def drain(self):
        def body(j):
            for kind in (PAIR, FAR, NEAR):
                self.copy(kind, j).wait_send()

        repeat(self.chunks, body)


ROUTES = {"H": "xlh", "B": "lxh"}


class Spread:
    def __init__(self, data, full, land, send, recv, kinds, first=0, last=3):
        self.data, self.full, self.land, self.send, self.recv = data, full, land, send, recv
        self.sums, self.hands = first < 2, last > 1
        self.kinds, self.jobs = kinds, len(kinds)
        self.count = (full if data is None else data).shape[0] // self.jobs

    def route(self, job):
        return ROUTES[self.kinds[job if isinstance(job, int) else 0]]

    def side(self, axis):
        dp = lax.axis_index("dp")
        return {"x": dp % 2, "z": dp // 2, "l": dp // 2 % 2, "h": dp // 4}[axis]

    def range_of(self, start, size):
        return pl.ds(pl.multiple_of(start, size), size)

    def place(self, job, level):
        start, size = job * self.count, self.count
        for axis in self.route(job)[:level]:
            size //= 4 if axis == "z" else 2
            start += self.side(axis) * size
        return start, size

    def landing(self, job, stage, k=1):
        at, size = 0, self.count
        for level in range(stage + 1):
            ways = 4 if self.route(job)[level] == "z" else 2
            size //= ways
            if level < stage:
                at += size * (ways - 1)
        return self.land.at[job, pl.ds(at + (k - 1) * size, size)]

    def copies(self, job, stage):
        dp, mp = lax.axis_index("dp"), lax.axis_index("mp")
        levels = len(self.route(job))
        back = stage >= levels
        level = 2 * levels - 1 - stage if back else stage
        start, size = self.place(job, level)
        axis = self.route(job)[level]
        here = self.side(axis)
        ways, step = (4, 2) if axis == "z" else (2, {"x": 1, "l": 2, "h": 4}[axis])
        found = []
        for k in range(1, ways):
            there = (here + k) % ways
            if back:
                src = dst = self.full.at[self.range_of(*self.place(job, level + 1))]
            else:
                src = self.data.at[self.range_of(start + there * (size // ways), size // ways)]
                dst = self.landing(job, level, k)
            at = (job, stage * 3 + k - 1)
            device = (dp + (there - here) * step, mp)
            found.append(remote(src, dst, self.send.at[at], self.recv.at[at], device))
        return found

    def own(self, job):
        return self.range_of(*self.place(job, len(self.route(job))))

    def stages(self, job):
        levels = len(self.route(job))
        return (0 if self.sums else levels), (2 * levels if self.hands else levels)

    def step(self, job, stage):
        first, end = self.stages(job)
        levels = len(self.route(job))
        if stage > first:
            arrived = self.copies(job, stage - 1)
            for done in arrived:
                done.wait_send()
                done.wait_recv()
            if stage <= levels:
                rows = self.range_of(*self.place(job, stage))
                total = self.data[rows].astype(F32)
                for k in range(len(arrived)):
                    total += self.landing(job, stage - 1, k + 1)[...].astype(F32)
                target = self.full if stage == levels and self.full is not None else self.data
                target[rows] = total.astype(BF)
        if stage < end:
            for copy in self.copies(job, stage):
                copy.start()


def advance(*moves):
    for total, jobs, stage in moves:
        for job in jobs if isinstance(jobs, tuple) else (jobs,):
            total.step(job, stage)


def spread_land(data, kinds):
    count = data[0] // len(kinds)
    return pltpu.VMEM((len(kinds), count - count // 8, data[1]), BF)


def spread_sems(kinds):
    return [pltpu.SemaphoreType.DMA((len(kinds), 18)), pltpu.SemaphoreType.DMA((len(kinds), 18))]


class Hops:
    def __init__(self, value, land, send, recv, peers):
        self.value, self.land, self.send, self.recv, self.peers = value, land, send, recv, peers

    def copy(self, i):
        return remote(
            self.value.at[i], self.land.at[i], self.send.at[i], self.recv.at[i], self.peers[i]
        )

    def start(self, i):
        self.copy(i).start()

    def finish(self, i):
        self.copy(i).wait_recv()
        self.value[i + 1] = self.value[i] + self.land[i]
        self.copy(i).wait_send()


def hop_scratch(count, *shape):
    return [
        pltpu.VMEM((count + 1, *shape), F32),
        pltpu.VMEM((count, *shape), F32),
        pltpu.SemaphoreType.DMA((count,)),
        pltpu.SemaphoreType.DMA((count,)),
    ]


def greet_all():
    dp, mp = lax.axis_index("dp"), lax.axis_index("mp")
    across = [((dp // 2 + k) % 4 * 2 + dp % 2, mp) for k in (1, 2, 3)]
    greet([mp_peer(1), mp_peer(2), dp_peer(1), *across])


def transfer_sems(chunks=CHUNKS):
    return [pltpu.SemaphoreType.DMA((3, chunks)), pltpu.SemaphoreType.DMA((3, chunks))]


def comm_params(collective_id):
    return pltpu.CompilerParams(
        collective_id=collective_id, has_side_effects=True, vmem_limit_bytes=VMEM_BYTES
    )


WHOLE = pl.BlockSpec(memory_space=pltpu.VMEM)


def shaped(*shape, dtype=None):
    return jax.ShapeDtypeStruct(shape, dtype or BF)


def as_row(ref):
    return ref[...].astype(F32)[None]


def column_sum(value):
    return jnp.sum(value, 0, keepdims=True)


def row_mean(value):
    return jnp.mean(value, -1, keepdims=True)


def project(x_ref, wq_ref, wk_ref, wv_ref, qb_ref, vb_ref, q_ref, k_ref, v_ref, vt_ref, land, send, recv, save):
    rows_here = land.shape[1]
    load = pltpu.make_async_copy(x_ref, land.at[0], save.at[0])
    load.start()
    load.wait()
    greet([mp_peer(1), mp_peer(2)])
    gather = Gather(land, send, recv)
    repeat(CHUNKS, gather.start)
    size = gather.size

    def emit(x, at):
        rows = pl.ds(pl.multiple_of(at, x.shape[0]), x.shape[0])
        q = (mm(x, wq_ref[...], 1, 0) + as_row(qb_ref)).astype(BF)
        q_ref[rows] = (q.astype(F32) * HD**-0.5).astype(BF)
        k_ref[rows] = mm(x, wk_ref[...], 1, 0).astype(BF)
        v = mm(x, wv_ref[...], 1, 0) + as_row(vb_ref)
        v_ref[rows] = v.astype(BF)
        vt_ref[:, rows] = v.T.astype(BF)

    def close(i):
        s, j = i // 2, i % 2 * 2

        @pl.when(i >= 2)
        def _():
            gather.arrive(1, j)
            gather.arrive(1, j + 1)

        emit(land[s, pl.ds(pl.multiple_of(j * size, 2 * size), 2 * size)], i * 2 * size)

    repeat(4, close)

    def far(j):
        gather.arrive(2, j)
        gather.arrive(3, j)

        def one(k):
            emit(land[2 + k, pl.ds(pl.multiple_of(j * size, size), size)], (2 + k) * rows_here + j * size)

        repeat(2, one)

    repeat(CHUNKS, far)
    gather.drain()


HALVES = 2


def forward_order(step):
    far = 2 * (3 - step % 2) + step // 2
    near = 2 * (1 - (step - 4) // 2) + step % 2
    return jnp.where(step < 4, far, near)


def attend_kernel(
    len_ref, x_ref, wq_ref, wk_ref, wv_ref, qb_ref, vb_ref, w_ref, ob_ref, gain_ref, shift_ref,
    q_out, k_out, v_out, all_out, e_ref, o_ref, r_ref, n_ref, i_ref, h_ref,
    tokens, q_ref, k_ref, v_ref, vt_ref, gather_send, gather_recv, save,
    k_aug, v_aug, out, land, mine, pending, send, recv,
):
    step = pl.program_id(0)
    seq_len, block = k_ref.shape[0], pending.shape[0]
    rows_here = tokens.shape[1]
    saves = [
        pltpu.make_async_copy(src, dst, save.at[1 + i])
        for i, (src, dst) in enumerate(
            ((q_ref, q_out), (k_ref, k_out), (v_ref, v_out), (tokens, all_out))
        )
    ]
    pairs = k_ref.shape[1] // WIDE
    reduce = Reduce(out, land, send, recv, HALVES)

    @pl.when(step == 0)
    def _():
        project(
            x_ref, wq_ref, wk_ref, wv_ref, qb_ref, vb_ref, q_ref, k_ref, v_ref, vt_ref,
            tokens, gather_send, gather_recv, save,
        )
        for each in saves:
            each.start()
        lanes = lax.broadcasted_iota(jnp.int32, (seq_len, WIDE), 1)
        rows = lax.broadcasted_iota(jnp.int32, (rows_here, WIDE), 0)
        bias = jnp.concatenate(
            [
                jnp.where(rows + mp_peer(s)[1] * rows_here < len_ref[0, 0], 0.0, MASKED)
                for s in range(4)
            ],
            0,
        )
        for p in range(pairs):
            keys = k_ref[:, p * WIDE : (p + 1) * WIDE].astype(F32)
            for h in range(2):
                other = (1 - h) * HD
                k_aug[2 * p + h] = jnp.where(
                    lanes // HD == h, keys, jnp.where(lanes == other, bias, 0.0)
                ).astype(BF)
                at = (2 * p + h) * HD
                v_aug[2 * p + h, :HD] = vt_ref[at : at + HD, :]
                v_aug[2 * p + h, HD:] = jnp.ones((16, seq_len), BF)

    lanes = lax.broadcasted_iota(jnp.int32, (block, WIDE), 1)
    q_rows = pl.ds(pl.multiple_of(forward_order(step) * block, block), block)
    outs = []
    for p in range(pairs):
        query = q_ref[q_rows, p * WIDE : (p + 1) * WIDE].astype(F32)
        scores = []
        for h in range(2):
            other = (1 - h) * HD
            q_aug = jnp.where(
                lanes // HD == h, query, jnp.where(lanes == other, 1.0, 0.0)
            ).astype(BF)
            scores.append(mm(k_aug[2 * p + h], q_aug, 1, 1))
        for h in range(2):
            top = jnp.max(scores[h], 0, keepdims=True)
            expon = jnp.exp(scores[h] - top).astype(BF)
            e_ref[0, 2 * p + h] = expon
            total = mm(v_aug[2 * p + h], expon, 1, 0)
            inverse = 1.0 / total[HD : HD + 1]
            r_ref[0, 2 * p + h] = inverse
            outs.append(total[:HD] * inverse)
    attended = jnp.concatenate(outs, 0).T.astype(BF)
    o_ref[...] = attended
    partial_rows = mm(attended, w_ref[...], 1, 0)

    for t in range(4 * HALVES):

        @pl.when(step == t)
        def _(t=t):
            if t < 4 and t % 2 == 0:
                reduce.post(PAIR, t // 2, partial_rows)
            elif t < 4:
                pending[...] = partial_rows
                reduce.forward_pair(t // 2, pending[...])
            elif t < 6:
                reduce.post(NEAR, t - 4, partial_rows)
            else:
                mine[pl.ds((t - 6) * block, block)] = partial_rows

    @pl.when(step == 4 * HALVES - 1)
    def _():
        for j in range(HALVES):
            rows = pl.ds(j * block, block)
            resid = tokens[0, rows].astype(F32) + reduce.total(j, mine[rows]) + as_row(ob_ref)
            center = resid - row_mean(resid)
            inv_std = lax.rsqrt(row_mean(center * center) + epsilon)
            normed = center * inv_std
            n_ref[rows] = normed
            i_ref[rows] = inv_std
            h_ref[rows] = (normed * as_row(gain_ref) + as_row(shift_ref)).astype(BF)
        reduce.drain()
        for each in saves:
            each.wait()


def attend(lengths, tokens, wq, wk, wv, q_bias, v_bias, out_weight, *vectors):
    rows, width = tokens.shape
    all_rows, cols = 4 * rows, wq.shape[1]
    block = rows // HALVES
    heads = cols // HD
    steps = all_rows // block

    def fixed(*shape):
        return pl.BlockSpec(shape, lambda i: (0,) * len(shape))

    anywhere = pl.BlockSpec(memory_space=pl.ANY)
    return pl.pallas_call(
        attend_kernel,
        grid=(steps,),
        in_specs=[
            pl.BlockSpec(memory_space=pltpu.SMEM),
            anywhere,
            *[fixed(width, cols)] * 3,
            *[fixed(cols)] * 2,
            fixed(cols, width),
            *[fixed(width)] * 3,
        ],
        out_specs=[
            *[anywhere] * 4,
            pl.BlockSpec((1, heads, all_rows, block), lambda i: (forward_order(i), 0, 0, 0)),
            pl.BlockSpec((block, cols), lambda i: (forward_order(i), 0)),
            pl.BlockSpec((1, heads, 1, block), lambda i: (forward_order(i), 0, 0, 0)),
            fixed(rows, width),
            fixed(rows, 1),
            fixed(rows, width),
        ],
        out_shape=[
            *[shaped(all_rows, cols)] * 3,
            shaped(4, rows, width),
            shaped(steps, heads, all_rows, block),
            shaped(all_rows, cols),
            shaped(steps, heads, 1, block, dtype=F32),
            shaped(rows, width, dtype=F32),
            shaped(rows, 1, dtype=F32),
            shaped(rows, width),
        ],
        scratch_shapes=[
            pltpu.VMEM((4, rows, width), BF),
            *[pltpu.VMEM((all_rows, cols), BF)] * 3,
            pltpu.VMEM((cols, all_rows), BF),
            *transfer_sems(),
            pltpu.SemaphoreType.DMA((5,)),
            pltpu.VMEM((heads, all_rows, WIDE), BF),
            pltpu.VMEM((heads, HD + 16, all_rows), BF),
            pltpu.VMEM((3, rows, width), BF),
            pltpu.VMEM((3, rows, width), BF),
            pltpu.VMEM((rows, width), F32),
            pltpu.VMEM((block, width), F32),
            *transfer_sems(HALVES),
        ],
        name="attend",
        compiler_params=comm_params(1),
    )(lengths, tokens, wq, wk, wv, q_bias, v_bias, out_weight, *vectors)


ROOT_HALF = 0.7071067811865476
ROOT_TAU = 0.3989422804014327


def feed_forward_kernel(
    h_ref, n_in, i_ref, g_in, up_in, ub_ref, down_in, *refs
):
    vectors, refs = refs[:5], refs[5:]
    (
        out_hbm, b1_ref, r1_ref, upg_hbm, downg_ref, small_ref,
        hidden, act, slope, branch, out1, land1, out2, land2, mine, pending, r2,
        gs1, gr1, gs2, gr2, rs1, rr1, rs2, rr2,
        down_land, down_send, down_recv, load, n_ref, g_ref, up_ref, down_ref, out_ref, upg_ref,
    ) = refs
    rows_here, width = h_ref.shape
    fetch = pltpu.make_async_copy(h_ref, hidden.at[0], load.at[0])
    fetch.start()
    fetches = [
        pltpu.make_async_copy(src, dst, load.at[1 + i])
        for i, (src, dst) in enumerate(
            ((up_in, up_ref), (down_in, down_ref), (n_in, n_ref), (g_in, g_ref))
        )
    ]
    save_out = pltpu.make_async_copy(out_ref, out_hbm, load.at[5])
    save_upg = pltpu.make_async_copy(upg_ref, upg_hbm, load.at[6])
    size = rows_here // CHUNKS
    first_gain, first_shift, down_bias, second_gain, second_shift = map(as_row, vectors)
    greet_all()
    down_sum = Spread(downg_ref, None, down_land, down_send, down_recv, KINDS, 0, 1)
    gather1, gather2 = Gather(hidden, gs1, gr1), Gather(branch, gs2, gr2)
    reduce1, reduce2 = Reduce(out1, land1, rs1, rr1), Reduce(out2, land2, rs2, rr2)
    fetch.wait()
    repeat(CHUNKS, gather1.start)
    for each in fetches:
        each.start()
    for each in fetches[:2]:
        each.wait()
    small_ref[...] = jnp.zeros_like(small_ref)

    def forward(x):
        pre = mm(x, up_ref[...], 1, 0) + as_row(ub_ref)
        cdf = 0.5 + 0.5 * lax.erf(pre * ROOT_HALF)
        active = (pre * cdf).astype(BF)
        steep = (cdf + pre * jnp.exp(-0.5 * pre * pre) * ROOT_TAU).astype(BF)
        return active, steep, mm(active, down_ref[...], 1, 0)

    def backward(grad, steep):
        pre_grad = (mm(grad, down_ref[...], 1, 1) * steep.astype(F32)).astype(BF)
        small_ref[6:7] += column_sum(pre_grad.astype(F32))
        return pre_grad, mm(pre_grad, up_ref[...], 1, 1)

    def chunk_rows(j):
        return pl.ds(pl.multiple_of(j * size, size), size)

    def double_rows(j):
        return pl.ds(pl.multiple_of(j * 2 * size, 2 * size), 2 * size)

    def halves(value):
        return value[:size], value[size:]

    def close_forward(i):
        s, half = i // 2, i % 2
        rows = double_rows(half)

        @pl.when(i >= 2)
        def _():
            gather1.arrive(1, 2 * half)
            gather1.arrive(1, 2 * half + 1)

        act[s, rows], slope[s, rows], part = forward(hidden[s, rows])

        @pl.when(i < 2)
        def _():
            mine[rows] = part

        @pl.when(i >= 2)
        def _():
            for k, piece in enumerate(halves(part)):
                reduce1.post(NEAR, 2 * half + k, piece)

    def far_forward(j):
        gather1.arrive(2, j)
        gather1.arrive(3, j)
        rows = chunk_rows(j)
        active, steep, part = forward(jnp.concatenate([hidden[2, rows], hidden[3, rows]], 0))
        for s in (2, 3):
            act[s, rows] = halves(active)[s - 2]
            slope[s, rows] = halves(steep)[s - 2]
        pending[rows] = part[:size]
        reduce1.post(PAIR, j, part[size:])

        @pl.when(j > 0)
        def _():
            reduce1.forward_pair(j - 1, pending[chunk_rows(j - 1)])

    repeat(4, close_forward)
    repeat(CHUNKS, far_forward)
    reduce1.forward_pair(CHUNKS - 1, pending[chunk_rows(CHUNKS - 1)])

    def second_norm(j):
        rows = chunk_rows(j)
        hidden = n_ref[rows] * first_gain + first_shift
        resid = hidden + reduce1.total(j, mine[rows]) + down_bias
        center = resid - row_mean(resid)
        inv_std = lax.rsqrt(row_mean(center * center) + epsilon)
        normed = center * inv_std
        out_ref[rows] = (normed * second_gain + second_shift).astype(BF)
        grad = g_ref[rows].astype(F32)
        product = grad * normed
        small_ref[0:1] += column_sum(product)
        small_ref[1:2] += column_sum(grad)
        scaled = grad * second_gain
        back = inv_std * (scaled - row_mean(scaled) - normed * row_mean(scaled * normed))
        small_ref[2:3] += column_sum(back)
        r2[rows] = back
        branch[0, rows] = back.astype(BF)
        gather2.start(j)

    for each in fetches[2:]:
        each.wait()
    repeat(CHUNKS, second_norm)
    save_out.start()

    def close_backward(i):
        s, half = i // 2, i % 2
        rows = double_rows(half)

        @pl.when(i >= 2)
        def _():
            gather2.arrive(1, 2 * half)
            gather2.arrive(1, 2 * half + 1)

        slope[s, rows], part = backward(branch[s, rows], slope[s, rows])

        @pl.when(i < 2)
        def _():
            mine[rows] = part

        @pl.when(i >= 2)
        def _():
            for k, piece in enumerate(halves(part)):
                reduce2.post(NEAR, 2 * half + k, piece)

    def far_backward(j):
        gather2.arrive(2, j)
        gather2.arrive(3, j)
        rows = chunk_rows(j)
        pre_grad, part = backward(
            jnp.concatenate([branch[2, rows], branch[3, rows]], 0),
            jnp.concatenate([slope[2, rows], slope[3, rows]], 0),
        )
        for s in (2, 3):
            slope[s, rows] = halves(pre_grad)[s - 2]
        pending[rows] = part[:size]
        reduce2.post(PAIR, j, part[size:])

        @pl.when(j > 0)
        def _():
            reduce2.forward_pair(j - 1, pending[chunk_rows(j - 1)])

    repeat(4, close_backward)
    repeat(CHUNKS, far_backward)
    reduce2.forward_pair(CHUNKS - 1, pending[chunk_rows(CHUNKS - 1)])

    tile = 256

    def down_grad(t):
        cols = pl.ds(pl.multiple_of(t * tile, tile), tile)
        total = mm(act[0, :, cols], branch[0], 0, 0)
        for s in (1, 2, 3):
            total += mm(act[s, :, cols], branch[s], 0, 0)
        downg_ref[cols] = total.astype(BF)

    def up_grad(t):
        cols = pl.ds(pl.multiple_of(t * tile, tile), tile)
        total = mm(hidden[0, :, cols], slope[0], 0, 0)
        for s in (1, 2, 3):
            total += mm(hidden[s, :, cols], slope[s], 0, 0)
        upg_ref[cols] = total.astype(BF)

    repeat(2, down_grad)
    advance((down_sum, (0, 1), 0))
    repeat(2, lambda t: down_grad(t + 2))
    advance((down_sum, (2, 3), 0))
    repeat(width // tile, up_grad)
    save_upg.start()

    def first_norm(j):
        rows = chunk_rows(j)
        normed = n_ref[rows]
        grad = r2[rows] + reduce2.total(j, mine[rows])
        small_ref[3:4] += column_sum(grad * normed)
        small_ref[4:5] += column_sum(grad)
        scaled = grad * first_gain
        back = i_ref[rows] * (scaled - row_mean(scaled) - normed * row_mean(scaled * normed))
        small_ref[5:6] += column_sum(back)
        r1_ref[rows] = back
        b1_ref[rows] = back.astype(BF)

    advance((down_sum, (0, 1), 1))
    first_norm(0)
    advance((down_sum, (2, 3), 1))
    first_norm(1)
    advance((down_sum, (0, 1), 2))
    first_norm(2)
    advance((down_sum, (2, 3), 2))
    first_norm(3)
    advance((down_sum, (0, 1, 2, 3), 3))
    for transfer in (gather1, gather2, reduce1, reduce2):
        transfer.drain()
    save_out.wait()
    save_upg.wait()


def feed_forward(hidden, normed, inv_std, output_grad, up, up_bias, down, *vectors):
    rows, width = hidden.shape
    units = up.shape[1]
    tall = (4, rows, units)
    anywhere = pl.BlockSpec(memory_space=pl.ANY)
    return pl.pallas_call(
        feed_forward_kernel,
        in_specs=[anywhere, anywhere, WHOLE, anywhere, anywhere, WHOLE, anywhere] + [WHOLE] * 5,
        out_specs=[anywhere, WHOLE, WHOLE, anywhere, WHOLE, WHOLE],
        out_shape=[
            shaped(rows, width),
            shaped(rows, width),
            shaped(rows, width, dtype=F32),
            shaped(width, units),
            shaped(units, width),
            shaped(8, width, dtype=F32),
        ],
        scratch_shapes=[
            pltpu.VMEM((4, rows, width), BF),
            pltpu.VMEM(tall, BF),
            pltpu.VMEM(tall, BF),
            pltpu.VMEM((4, rows, width), BF),
            *[pltpu.VMEM((3, rows, width), BF)] * 4,
            *[pltpu.VMEM((rows, width), F32)] * 3,
            *transfer_sems(),
            *transfer_sems(),
            *transfer_sems(),
            *transfer_sems(),
            spread_land((units, width), KINDS),
            *spread_sems(KINDS),
            pltpu.SemaphoreType.DMA((7,)),
            pltpu.VMEM((rows, width), F32),
            pltpu.VMEM((rows, width), BF),
            pltpu.VMEM((width, units), BF),
            pltpu.VMEM((units, width), BF),
            pltpu.VMEM((rows, width), BF),
            pltpu.VMEM((width, units), BF),
        ],
        name="feed_forward",
        compiler_params=comm_params(2),
    )(hidden, normed, inv_std, output_grad, up, up_bias, down, *vectors)


def attend_back_kernel(
    b_ref, w_ref, e_ref, r_ref, q_ref, k_ref, v_ref, o_ref, small_in, up_in, down_in, all_in,
    dq_ref, dk_ref, dv_ref, wg_ref, pg_ref, small_ref, up_out, down_out,
    land, v_aug, k_t, dks, dvs, dqs, w_total, w_low, p_low, grads, up, down, tokens, loads, send, recv,
    up_land, up_send, up_recv, down_send, down_recv, out_land, out_send, out_recv,
    pair_land, pair_send, pair_recv, value, small_land, small_send, small_recv,
):
    step = pl.program_id(0)
    pair, s_now = step // 2 % 2, step // 4 * 2 + step % 2
    seq_len, block = k_ref.shape[0], q_ref.shape[0]
    pieces = e_ref.shape[0]
    cols = w_ref.shape[0]
    width = w_ref.shape[1]
    half = block // 2
    gather = Gather(land, send, recv, HALVES)
    up_sum = Spread(up, None, up_land, up_send, up_recv, MORE_X, 0, 1)
    down_sum = Spread(None, down, None, down_send, down_recv, KINDS, 2, 3)
    out_sum = Spread(w_low, None, out_land, out_send, out_recv, "H", 0, 1)
    pair_sum = Spread(p_low, None, pair_land, pair_send, pair_recv, MORE_X, 0, 1)
    small = Hops(
        value, small_land, small_send, small_recv,
        [dp_peer(1), dp_peer(2), dp_peer(4), mp_peer(1), mp_peer(2)],
    )
    load_up = pltpu.make_async_copy(up_in, up, loads.at[0])
    load_down = [
        pltpu.make_async_copy(
            down_in.at[down_sum.own(job)], down.at[down_sum.own(job)], loads.at[5 + job]
        )
        for job in range(JOBS)
    ]
    load_tokens = pltpu.make_async_copy(all_in, tokens, loads.at[2])
    save_up = pltpu.make_async_copy(up, up_out, loads.at[3])
    save_down = pltpu.make_async_copy(down, down_out, loads.at[4])

    load_branch = pltpu.make_async_copy(b_ref, land.at[0], loads.at[5 + JOBS])

    @pl.when(step == 0)
    def _():
        load_branch.start()
        for load in load_down:
            load.start()
        load_up.start()
        load_tokens.start()
        value[0] = small_in[...]
        w_total[...] = jnp.zeros_like(w_total)
        greet_all()
        small.start(0)
        load_branch.wait()
        repeat(HALVES, gather.start)
        for load in load_down:
            load.wait()
        advance((down_sum, (0, 1, 2, 3), 3))
        load_up.wait()
        advance((up_sum, (3, 0, 1, 2), 0))

    @pl.when(step == 1)
    def _():
        repeat(HALVES, lambda j: gather.arrive(1, j))

    @pl.when(step == 2)
    def _():
        small.finish(0)
        small.start(1)
        advance((down_sum, (0, 1, 2, 3), 4), (up_sum, (3, 0), 1))

    @pl.when(step == 3)
    def _():
        advance((up_sum, (1, 2), 1), (down_sum, (0, 1), 5))

    @pl.when(step == 4)
    def _():
        small.finish(1)
        small.start(2)
        advance((up_sum, (3, 0), 2), (down_sum, (2, 3), 5))
        repeat(HALVES, lambda j: gather.arrive(2, j))

    @pl.when(step == 5)
    def _():
        repeat(HALVES, lambda j: gather.arrive(3, j))

    @pl.when(pair == 0)
    def _():
        branch = land[s_now]
        w_total[...] += mm(o_ref[...], branch, 0, 0)
        grads[pl.ds(pl.multiple_of(s_now * block, block), block)] = mm(
            branch, w_ref[...], 1, 1
        ).astype(BF)

    @pl.when(step == 5)
    def _():
        w_low[...] = w_total[...].astype(BF)
        advance((out_sum, 0, 0), (up_sum, (1, 2), 2))

    @pl.when(step == 6)
    def _():
        small.finish(2)
        small.start(3)
        advance((out_sum, 0, 1), (up_sum, (3, 0), 3), (down_sum, (0, 1), 6))

    @pl.when(step == 7)
    def _():
        small.finish(3)
        small.start(4)
        advance(
            (pair_sum, (3, 0, 1, 2), 1), (out_sum, 0, 2), (up_sum, (1, 2), 3), (down_sum, (2, 3), 6)
        )
        save_up.start()
        save_down.start()

    @pl.when(s_now == 0)
    def _():
        lanes = lax.broadcasted_iota(jnp.int32, (seq_len, WIDE), 1)
        values = v_ref[...].astype(F32)
        for h in range(2):
            other = (1 - h) * HD
            ones = jnp.where((lanes >= other) & (lanes < other + 2), 1.0, 0.0)
            v_aug[pair, h] = jnp.where(lanes // HD == h, values, ones).astype(BF)
        k_t[pair] = (k_ref[...].astype(F32) * HD**-0.5).T.astype(BF)
        dks[pair] = jnp.zeros(dks.shape[1:], F32)
        dvs[pair] = jnp.zeros(dvs.shape[1:], F32)

    lanes = lax.broadcasted_iota(jnp.int32, (block, WIDE), 1)
    row_start = pl.multiple_of(s_now * block, block)
    inverse = jnp.concatenate(
        [
            jnp.concatenate(
                [jnp.broadcast_to(r_ref[i, h], (HD, block // pieces)) for h in range(2)], 0
            )
            for i in range(pieces)
        ],
        1,
    ).T
    wide = pl.ds(pl.multiple_of(pair * WIDE, WIDE), WIDE)
    grad = (grads[pl.ds(row_start, block), wide].astype(F32) * inverse).astype(BF)
    grad_wide = grad.astype(F32)
    product = grad_wide * o_ref[:, wide].astype(F32)
    centered = []
    for h in range(2):
        other = (1 - h) * HD
        inside = lanes // HD == h
        row_dot = jnp.sum(jnp.where(inside, product, 0.0), -1, keepdims=True)
        high = row_dot.astype(BF).astype(F32)
        g_aug = jnp.where(
            inside,
            grad_wide,
            jnp.where(lanes == other, -high, jnp.where(lanes == other + 1, high - row_dot, 0.0)),
        ).astype(BF)
        centered.append(mm(v_aug[pair, h], g_aug, 1, 1))
    query_grads = []
    for h in range(2):
        cols_h = slice(h * HD, (h + 1) * HD)
        expon = jnp.concatenate([e_ref[i, h] for i in range(pieces)], 1)
        score_grad = (expon.astype(F32) * centered[h]).astype(BF)
        dvs[pair, h] += mm(expon, grad[:, cols_h], 1, 0)
        dks[pair, h] += mm(score_grad, q_ref[:, cols_h], 1, 0)
        query_grads.append(mm(k_t[pair, cols_h, :], score_grad, 1, 0))
    query_grad = jnp.concatenate(query_grads, 0).T.astype(BF)
    dq_ref[...] = query_grad
    dqs[pair, pl.ds(row_start, block), :WIDE] = query_grad

    @pl.when(s_now == 3)
    def _():
        for total, out, at in ((dks, dk_ref, WIDE), (dvs, dv_ref, 2 * WIDE)):
            joined = jnp.concatenate([total[pair, h] for h in range(2)], 1).astype(BF)
            out[:, wide] = joined
            dqs[pair, :, at : at + WIDE] = joined

    @pl.when(step == 5)
    def _():
        load_tokens.wait()
        projection_grads(tokens, dqs.at[0], p_low)
        advance((pair_sum, (3, 0, 1, 2), 0))

    @pl.when(step == 7)
    def _():
        advance((pair_sum, (3, 0, 1, 2), 2), (out_sum, 0, 3), (pair_sum, (3, 0, 1, 2), 3))
        small.finish(4)
        small_ref[...] = value[5]
        small_ref[6:7] = value[3, 6:7]
        wg_ref[...] = w_low[...]
        pg_ref[...] = p_low[...]
        gather.drain()
        save_down.wait()
        save_up.wait()


def projection_grads(tokens, joint, out_ref):
    tile = 256
    rows = tokens.shape[1]

    def body(t):
        cols = pl.ds(pl.multiple_of(t * tile, tile), tile)
        total = mm(tokens[0, :, cols], joint[pl.ds(0, rows)], 0, 0)
        for s in (1, 2, 3):
            total += mm(tokens[s, :, cols], joint[pl.ds(s * rows, rows)], 0, 0)
        out_ref[cols] = total.astype(BF)

    repeat(tokens.shape[2] // tile, body)


def attend_back(branch, out_weight, expon, inverse, q, k, v, attended, small, up, down, gathered):
    rows, width = branch.shape
    all_rows, cols = q.shape
    pairs = cols // WIDE
    pieces = HALVES

    def fixed(*shape):
        return pl.BlockSpec(shape, lambda i: (0,) * len(shape))

    def pair_at(i):
        return i // 2 % 2

    def rows_at(i):
        return i // 4 * 2 + i % 2

    anywhere = pl.BlockSpec(memory_space=pl.ANY)
    pair_rows = pl.BlockSpec((rows, WIDE), lambda i: (rows_at(i), pair_at(i)))
    pair_keys = pl.BlockSpec((all_rows, WIDE), lambda i: (0, pair_at(i)))
    return pl.pallas_call(
        attend_back_kernel,
        grid=(4 * pairs,),
        in_specs=[
            anywhere,
            fixed(cols, width),
            pl.BlockSpec((pieces, 2, all_rows, rows // pieces), lambda i: (rows_at(i), pair_at(i), 0, 0)),
            pl.BlockSpec((pieces, 2, 1, rows // pieces), lambda i: (rows_at(i), pair_at(i), 0, 0)),
            pair_rows,
            pair_keys,
            pair_keys,
            pl.BlockSpec((rows, cols), lambda i: (rows_at(i), 0)),
            fixed(*small.shape),
            anywhere,
            anywhere,
            anywhere,
        ],
        out_specs=[
            pair_rows,
            fixed(all_rows, cols),
            fixed(all_rows, cols),
            fixed(cols, width),
            fixed(width, 3 * WIDE),
            fixed(*small.shape),
            anywhere,
            anywhere,
        ],
        out_shape=[shaped(all_rows, cols)] * 3
        + [
            shaped(cols, width),
            shaped(width, 3 * WIDE),
            shaped(*small.shape, dtype=F32),
            shaped(*up.shape),
            shaped(*down.shape),
        ],
        scratch_shapes=[
            pltpu.VMEM((4, rows, width), BF),
            pltpu.VMEM((pairs, 2, all_rows, WIDE), BF),
            pltpu.VMEM((pairs, WIDE, all_rows), BF),
            pltpu.VMEM((pairs, 2, all_rows, HD), F32),
            pltpu.VMEM((pairs, 2, all_rows, HD), F32),
            pltpu.VMEM((pairs, all_rows, 3 * WIDE), BF),
            pltpu.VMEM((cols, width), F32),
            pltpu.VMEM((cols, width), BF),
            pltpu.VMEM((width, 3 * WIDE), BF),
            pltpu.VMEM((all_rows, cols), BF),
            pltpu.VMEM(up.shape, BF),
            pltpu.VMEM(down.shape, BF),
            pltpu.VMEM(gathered.shape, BF),
            pltpu.SemaphoreType.DMA((6 + JOBS,)),
            *transfer_sems(HALVES),
            spread_land(up.shape, MORE_X),
            *spread_sems(KINDS),
            *spread_sems(KINDS),
            spread_land((cols, width), "H"),
            *spread_sems("H"),
            spread_land((width, 3 * WIDE), KINDS),
            *spread_sems(KINDS),
            *hop_scratch(5, *small.shape),
        ],
        name="attend_back",
        compiler_params=comm_params(3),
    )(branch, out_weight, expon, inverse, q, k, v, attended, small, up, down, gathered)


def input_back_kernel(
    dq_ref, dk_ref, dv_ref, wq_ref, wk_ref, wv_ref, all_ref, r1_ref, wg_in, pg_in, up_in,
    x_ref, wg_ref, pg_ref, last_ref, bias_ref, up_out,
    out, land, mine, pending, send, recv, up, loads, up_send, up_recv, out_send, out_recv,
    pair_send, pair_recv, joint, w_full, p_full, last_full, last_low, last_land, last_send, last_recv,
    value, bias_land, bias_send, bias_recv,
):
    rows_here = r1_ref.shape[0]
    size = rows_here // CHUNKS
    last = dq_ref.shape[1] - WIDE
    up_sum = Spread(None, up, None, up_send, up_recv, MORE_X, 2, 3)
    out_sum = Spread(None, w_full, None, out_send, out_recv, "H", 2, 3)
    pair_sum = Spread(None, p_full, None, pair_send, pair_recv, MORE_X, 2, 3)
    last_sum = Spread(last_low, last_full, last_land, last_send, last_recv, KINDS)
    bias = Hops(value, bias_land, bias_send, bias_recv, [dp_peer(1), dp_peer(2), dp_peer(4)])
    reduce = Reduce(out, land, send, recv)
    save_up = pltpu.make_async_copy(up, up_out, loads.at[JOBS])
    load_up = [
        pltpu.make_async_copy(up_in.at[up_sum.own(job)], up.at[up_sum.own(job)], loads.at[job])
        for job in range(JOBS)
    ]
    for load in load_up:
        load.start()
    w_full[out_sum.own(0)] = wg_in[out_sum.own(0)]
    for job in range(JOBS):
        p_full[pair_sum.own(job)] = pg_in[pair_sum.own(job)]
    value[0, 0:1] = column_sum(dq_ref[...].astype(F32))
    value[0, 1:8] = jnp.broadcast_to(column_sum(dv_ref[...].astype(F32)), (7, dv_ref.shape[1]))
    greet_all()
    bias.start(0)
    for load in load_up:
        load.wait()
    advance((pair_sum, (3, 0, 1, 2), 3), (out_sum, 0, 3), (up_sum, (0, 1, 2, 3), 3))
    tail = pl.ds(last, WIDE)
    for at, grad in enumerate((dq_ref, dk_ref, dv_ref)):
        joint[:, at * WIDE : (at + 1) * WIDE] = grad[:, tail]
    projection_grads(all_ref, joint, last_low)
    advance((last_sum, (0, 1, 2, 3), 0))
    grads = ((dq_ref, wq_ref), (dk_ref, wk_ref), (dv_ref, wv_ref))

    def part_of(starts, count):
        total = None
        for grad, weight in grads:
            pieces = [grad[pl.ds(pl.multiple_of(at, size), count)] for at in starts]
            x = pieces[0] if len(pieces) == 1 else jnp.concatenate(pieces, 0)
            term = mm(x, weight[...], 1, 1)
            total = term if total is None else total + term
        return total

    def chunk_rows(j):
        return pl.ds(pl.multiple_of(j * size, size), size)

    def far(j):
        part = part_of((2 * rows_here + j * size, 3 * rows_here + j * size), size)
        pending[chunk_rows(j)] = part[:size]
        reduce.post(PAIR, j, part[size:])

        @pl.when(j > 0)
        def _():
            reduce.forward_pair(j - 1, pending[chunk_rows(j - 1)])

    repeat(CHUNKS, far)
    reduce.forward_pair(CHUNKS - 1, pending[chunk_rows(CHUNKS - 1)])
    bias.finish(0)
    bias.start(1)
    advance((pair_sum, (3, 0, 1, 2), 4), (last_sum, (0, 1, 2, 3), 1), (up_sum, (3, 0), 4))

    def near(i):
        part = part_of((rows_here + i * 2 * size,), 2 * size)
        reduce.post(NEAR, 2 * i, part[:size])
        reduce.post(NEAR, 2 * i + 1, part[size:])

    repeat(2, near)

    def own(i):
        mine[pl.ds(pl.multiple_of(i * 2 * size, 2 * size), 2 * size)] = part_of((i * 2 * size,), 2 * size)

    repeat(2, own)

    def finish(j):
        rows = chunk_rows(j)
        x_ref[rows] = (r1_ref[rows] + reduce.total(j, mine[rows])).astype(BF)

    advance((pair_sum, (3, 0, 1, 2), 5), (up_sum, (1, 2), 4))
    finish(0)
    bias.finish(1)
    bias.start(2)
    advance((last_sum, (0, 1, 2, 3), 2), (up_sum, (3, 0), 5), (out_sum, 0, 4))
    finish(1)
    advance((last_sum, (0, 1, 2, 3), 3), (up_sum, (1, 2), 5), (out_sum, 0, 5))
    finish(2)
    advance((last_sum, (0, 1, 2, 3), 4))
    finish(3)
    bias.finish(2)
    bias_ref[...] = value[3]
    advance((last_sum, (0, 1, 2, 3), 5), (up_sum, (0, 1, 2, 3), 6))
    save_up.start()
    advance((pair_sum, (3, 0, 1, 2), 6), (out_sum, 0, 6))
    wg_ref[...] = w_full[...]
    pg_ref[...] = p_full[...]
    advance((last_sum, (0, 1, 2, 3), 6))
    last_ref[...] = last_full[...]
    reduce.drain()
    save_up.wait()


def input_back(dq, dk, dv, wq, wk, wv, gathered, resid_grad, out_grad, pair_grad, up):
    rows, width = resid_grad.shape
    cols = dq.shape[1]
    return pl.pallas_call(
        input_back_kernel,
        in_specs=[WHOLE] * 10 + [pl.BlockSpec(memory_space=pl.ANY)],
        out_specs=[WHOLE] * 5 + [pl.BlockSpec(memory_space=pl.ANY)],
        out_shape=[
            shaped(rows, width),
            shaped(*out_grad.shape),
            shaped(*pair_grad.shape),
            shaped(*pair_grad.shape),
            shaped(8, cols, dtype=F32),
            shaped(*up.shape),
        ],
        scratch_shapes=[
            pltpu.VMEM((3, rows, width), BF),
            pltpu.VMEM((3, rows, width), BF),
            pltpu.VMEM((rows, width), F32),
            pltpu.VMEM((rows, width), F32),
            *transfer_sems(),
            pltpu.VMEM(up.shape, BF),
            pltpu.SemaphoreType.DMA((JOBS + 1,)),
            *spread_sems(KINDS),
            *spread_sems("H"),
            *spread_sems(KINDS),
            pltpu.VMEM((dq.shape[0], 3 * WIDE), BF),
            pltpu.VMEM(out_grad.shape, BF),
            *[pltpu.VMEM(pair_grad.shape, BF)] * 3,
            spread_land(pair_grad.shape, KINDS),
            *spread_sems(KINDS),
            *hop_scratch(3, 8, cols),
        ],
        name="input_back",
        compiler_params=comm_params(4),
    )(dq, dk, dv, wq, wk, wv, gathered, resid_grad, out_grad, pair_grad, up)


def widen_kernel(up_ref, down_ref, out_ref, pair_ref, last_ref, upw, downw, outw, qw, kw, vw):
    upw[...] = up_ref[...].astype(F32)
    downw[...] = down_ref[...].astype(F32)
    outw[...] = out_ref[...].astype(F32)
    for at, wide in enumerate((qw, kw, vw)):
        cols = slice(at * WIDE, (at + 1) * WIDE)
        wide[:, :WIDE] = pair_ref[:, cols].astype(F32)
        wide[:, WIDE:] = last_ref[:, cols].astype(F32)


def widen_grads(*grads):
    steps = 4
    shapes = [g.shape for g in grads[:3]] + [(grads[3].shape[0], 2 * WIDE)] * 3

    def tiles(shape):
        return pl.BlockSpec((shape[0] // steps, shape[1]), lambda i: (i, 0))

    return pl.pallas_call(
        widen_kernel,
        grid=(steps,),
        in_specs=[tiles(g.shape) for g in grads],
        out_specs=[tiles(shape) for shape in shapes],
        out_shape=[shaped(*shape, dtype=F32) for shape in shapes],
        name="widen_grads",
    )(*grads)


def per_device(
    tokens, lengths, query_weight, query_bias, key_weight, value_weight, value_bias, out_weight,
    out_bias, first_gain, first_shift, up_weight, up_bias, down_weight, down_bias, second_gain,
    second_shift, output_grad,
):
    pairs = query_weight.shape[1] // WIDE
    if (lax.axis_size("dp"), lax.axis_size("mp"), lengths.shape[1], pairs) != (8, 4, 1, 2):
        return per_device_general(
            tokens, lengths, query_weight, query_bias, key_weight, value_weight, value_bias,
            out_weight, out_bias, first_gain, first_shift, up_weight, up_bias, down_weight,
            down_bias, second_gain, second_shift, output_grad,
        )
    q, k, v, gathered, expon, attended, inverse, normed, inv_std, hidden = attend(
        lengths, tokens, query_weight, key_weight, value_weight, query_bias, value_bias, out_weight,
        out_bias, first_gain, first_shift,
    )
    layer_out, branch, resid_grad, up_grad, down_grad, small = feed_forward(
        hidden, normed, inv_std, output_grad, up_weight, up_bias, down_weight,
        first_gain, first_shift, down_bias, second_gain, second_shift,
    )
    dq, dk, dv, out_grad, pair_grad, small, up_grad, down_grad = attend_back(
        branch, out_weight, expon, inverse, q, k, v, attended, small, up_grad, down_grad, gathered
    )
    tokens_grad, out_grad, pair_grad, last_grad, bias_grads, up_grad = input_back(
        dq, dk, dv, query_weight, key_weight, value_weight, gathered, resid_grad, out_grad, pair_grad,
        up_grad,
    )

    up_grad, down_grad, out_grad, query_grad, key_grad, value_grad = widen_grads(
        up_grad, down_grad, out_grad, pair_grad, last_grad
    )
    return (
        layer_out,
        tokens_grad,
        query_grad,
        bias_grads[0],
        key_grad,
        value_grad,
        bias_grads[1],
        out_grad,
        small[5],
        small[3],
        small[4],
        up_grad,
        small[6],
        down_grad,
        small[2],
        small[0],
        small[1],
    )


def solution(mesh):
    placed = (
        P(("dp", "mp"), None),
        P("dp", None),
        P(None, "mp"),
        P("mp"),
        P(None, "mp"),
        P(None, "mp"),
        P("mp"),
        P("mp", None),
        P(),
        P(),
        P(),
        P(None, "mp"),
        P("mp"),
        P("mp", None),
        P(),
        P(),
        P(),
        P(("dp", "mp"), None),
    )
    return jax.shard_map(
        per_device,
        mesh=mesh,
        in_specs=placed,
        out_specs=(
            P(("dp", "mp"), None),
            P(("dp", "mp"), None),
            P(None, "mp"),
            P("mp"),
            P(None, "mp"),
            P(None, "mp"),
            P("mp"),
            P("mp", None),
            P(),
            P(),
            P(),
            P(None, "mp"),
            P("mp"),
            P("mp", None),
            P(),
            P(),
            P(),
        ),
        check_vma=False,
    )
```

```python
from functools import partial

import jax
import jax.numpy as jnp
from jax import lax
from jax.experimental import pallas as pl
from jax.experimental.pallas import tpu as pltpu
from jax.sharding import PartitionSpec as P

HD = 64


epsilon = 1e-12


def norm_forward(resid, gain, shift):
    center = resid - jnp.mean(resid, -1, keepdims=True)
    inv_std = lax.rsqrt(jnp.mean(center * center, -1, keepdims=True) + epsilon)
    normed = center * inv_std
    return (normed * gain + shift, normed, inv_std)


def norm_backward(grad, normed, inv_std, gain):
    scaled = grad * gain
    back = inv_std * (
        scaled
        - jnp.mean(scaled, -1, keepdims=True)
        - normed * jnp.mean(scaled * normed, -1, keepdims=True)
    )
    return (back, jnp.sum(grad * normed, 0), jnp.sum(grad, 0))


F32 = jnp.float32
BF = jnp.bfloat16
MASKED = -1000000000.0
WIDE = 2 * HD


def mm(a, b, ca, cb):
    return lax.dot_general(a, b, (((ca,), (cb,)), ((), ())), preferred_element_type=F32)


def forward_kernel(heads, len_ref, q_ref, k_ref, vt_ref, e_ref, o_ref, r_ref, v_aug, k_aug):
    seq, step = pl.program_id(0), pl.program_id(2)
    seq_len, block = k_ref.shape[0], q_ref.shape[0]

    @pl.when(step == 0)
    def _():
        rows = lax.broadcasted_iota(jnp.int32, (seq_len, WIDE), 0)
        lanes = lax.broadcasted_iota(jnp.int32, (seq_len, WIDE), 1)
        bias = jnp.where(rows < len_ref[seq], 0.0, MASKED)
        keys = k_ref[...].astype(F32)
        for h in range(heads):
            other = (1 - h) * HD
            k_aug[h] = jnp.where(
                lanes // HD == h, keys, jnp.where(lanes == other, bias, 0.0)
            ).astype(BF)
            v_aug[h, :HD] = vt_ref[h * HD : (h + 1) * HD, :]
            v_aug[h, HD:] = jnp.ones((16, seq_len), BF)

    query = q_ref[...].astype(F32) * HD**-0.5
    lanes = lax.broadcasted_iota(jnp.int32, (block, WIDE), 1)
    scores = []
    for h in range(heads):
        other = (1 - h) * HD
        q_aug = jnp.where(
            lanes // HD == h, query, jnp.where(lanes == other, 1.0, 0.0)
        ).astype(BF)
        scores.append(mm(k_aug[h], q_aug, 1, 1))
    outs = []
    for h in range(heads):
        top = jnp.max(scores[h], 0, keepdims=True)
        expon = jnp.exp(scores[h] - top).astype(BF)
        e_ref[h] = expon
        total = mm(v_aug[h], expon, 1, 0)
        inverse = 1.0 / total[HD : HD + 1]
        r_ref[h] = inverse
        outs.append(total[:HD] * inverse)
    if heads == 1:
        outs.append(jnp.zeros_like(outs[0]))
    o_ref[...] = jnp.concatenate(outs, 0).T.astype(BF)


def backward_kernel(
    heads, e_ref, r_ref, q_ref, k_ref, v_ref, o_ref, g_ref, dq_ref, dk_ref, dv_ref, v_aug, k_t, dks, dvs
):
    step, last = pl.program_id(2), pl.num_programs(2) - 1
    seq_len, block = k_ref.shape[0], q_ref.shape[0]

    @pl.when(step == 0)
    def _():
        lanes = lax.broadcasted_iota(jnp.int32, (seq_len, WIDE), 1)
        values = v_ref[...].astype(F32)
        for h in range(heads):
            other = (1 - h) * HD
            ones = jnp.where((lanes >= other) & (lanes < other + 2), 1.0, 0.0)
            v_aug[h] = jnp.where(lanes // HD == h, values, ones).astype(BF)
        k_t[...] = (k_ref[...].astype(F32) * HD**-0.5).T.astype(BF)
        dks[...] = jnp.zeros_like(dks)
        dvs[...] = jnp.zeros_like(dvs)

    lanes = lax.broadcasted_iota(jnp.int32, (block, WIDE), 1)
    inverse = jnp.concatenate(
        [jnp.broadcast_to(r_ref[h % heads], (HD, block)) for h in range(2)], 0
    ).T
    grad = (g_ref[...].astype(F32) * inverse).astype(BF)
    grad_wide = grad.astype(F32)
    scaled_query = (q_ref[...].astype(F32) * HD**-0.5).astype(BF)
    product = grad_wide * o_ref[...].astype(F32)
    centered = []
    for h in range(heads):
        other = (1 - h) * HD
        inside = lanes // HD == h
        row_dot = jnp.sum(jnp.where(inside, product, 0.0), -1, keepdims=True)
        high = row_dot.astype(BF).astype(F32)
        g_aug = jnp.where(
            inside,
            grad_wide,
            jnp.where(lanes == other, -high, jnp.where(lanes == other + 1, high - row_dot, 0.0)),
        ).astype(BF)
        centered.append(mm(v_aug[h], g_aug, 1, 1))
    query_grads = []
    for h in range(heads):
        cols = slice(h * HD, (h + 1) * HD)
        expon = e_ref[h]
        score_grad = (expon.astype(F32) * centered[h]).astype(BF)
        dvs[h] += mm(expon, grad[:, cols], 1, 0)
        dks[h] += mm(score_grad, scaled_query[:, cols], 1, 0)
        query_grads.append(mm(k_t[cols, :], score_grad, 1, 0))
    if heads == 1:
        query_grads.append(jnp.zeros_like(query_grads[0]))
    dq_ref[...] = jnp.concatenate(query_grads, 0).T.astype(BF)

    @pl.when(step == last)
    def _():
        for total, out in ((dks, dk_ref), (dvs, dv_ref)):
            halves = [total[h] for h in range(heads)]
            if heads == 1:
                halves.append(jnp.zeros_like(halves[0]))
            out[...] = jnp.concatenate(halves, 1).astype(BF)


def attention_shape(rows, cols, seqs):
    seq_len = rows // seqs
    block = min(512, seq_len)
    steps = seq_len // block
    pairs = max(1, cols // WIDE)
    heads = cols // HD // pairs
    row_spec = pl.BlockSpec((block, WIDE), lambda s, p, j, *_: (s * steps + j, p))
    key_spec = pl.BlockSpec((seq_len, WIDE), lambda s, p, j, *_: (s, p))
    e_spec = pl.BlockSpec((heads, seq_len, block), lambda s, p, j, *_: (p, s, j))
    r_spec = pl.BlockSpec((heads, 1, block), lambda s, p, j, *_: (p, 0, s * steps + j))
    return seq_len, heads, pairs, (seqs, pairs, steps), row_spec, key_spec, e_spec, r_spec


def widen(array):
    short = WIDE - array.shape[1]
    return array if short <= 0 else jnp.pad(array, ((0, 0), (0, short)))


def attention_forward(queries, keys, values, lengths):
    rows, cols = queries.shape
    seqs = lengths.shape[0]
    seq_len, heads, pairs, grid, row_spec, key_spec, e_spec, r_spec = attention_shape(rows, cols, seqs)
    wide_cols = pairs * WIDE
    expon, attended, inverse = pl.pallas_call(
        partial(forward_kernel, heads),
        grid_spec=pltpu.PrefetchScalarGridSpec(
            num_scalar_prefetch=1,
            grid=grid,
            in_specs=[
                row_spec,
                key_spec,
                pl.BlockSpec((WIDE, seq_len), lambda s, p, j, *_: (p, s)),
            ],
            out_specs=[e_spec, row_spec, r_spec],
            scratch_shapes=[
                pltpu.VMEM((heads, HD + 16, seq_len), BF),
                pltpu.VMEM((heads, seq_len, WIDE), BF),
            ],
        ),
        out_shape=[
            jax.ShapeDtypeStruct((heads * pairs, rows, seq_len), BF),
            jax.ShapeDtypeStruct((rows, wide_cols), BF),
            jax.ShapeDtypeStruct((heads * pairs, 1, rows), F32),
        ],
        name="attention_forward",
        compiler_params=pltpu.CompilerParams(vmem_limit_bytes=60 * 1024 * 1024),
    )(lengths, widen(queries), widen(keys), widen(values).T)
    return expon, attended[:, :cols], inverse


def attention_backward(expon, inverse, queries, keys, values, attended, grad, seqs):
    rows, cols = queries.shape
    seq_len, heads, pairs, grid, row_spec, key_spec, e_spec, r_spec = attention_shape(rows, cols, seqs)
    shape = jax.ShapeDtypeStruct((rows, pairs * WIDE), BF)
    outs = pl.pallas_call(
        partial(backward_kernel, heads),
        grid=grid,
        in_specs=[e_spec, r_spec, row_spec, key_spec, key_spec, row_spec, row_spec],
        out_specs=[row_spec, key_spec, key_spec],
        scratch_shapes=[
            pltpu.VMEM((heads, seq_len, WIDE), BF),
            pltpu.VMEM((WIDE, seq_len), BF),
            pltpu.VMEM((heads, seq_len, HD), F32),
            pltpu.VMEM((heads, seq_len, HD), F32),
        ],
        out_shape=[shape] * 3,
        name="attention_backward",
        compiler_params=pltpu.CompilerParams(vmem_limit_bytes=60 * 1024 * 1024),
    )(expon, inverse, *[widen(x) for x in (queries, keys, values, attended, grad)])
    return [x[:, :cols] for x in outs]


def contract_rows(left, right):
    return lax.dot_general(
        left, right, (((0,), (0,)), ((), ())), preferred_element_type=jnp.float32
    )


def contract_cols(left, right):
    return lax.dot_general(
        left, right, (((1,), (1,)), ((), ())), preferred_element_type=jnp.float32
    )


def split_projection(projected, width, q_bias, v_bias):
    query_part = (projected[:, :width] + q_bias).astype(jnp.bfloat16)
    key_part = projected[:, width : 2 * width].astype(jnp.bfloat16)
    value_part = (projected[:, 2 * width :] + v_bias).astype(jnp.bfloat16)
    return (query_part, key_part, value_part)


def per_device_general(
    tokens,
    lengths,
    query_weight,
    query_bias,
    key_weight,
    value_weight,
    value_bias,
    out_weight,
    out_bias,
    first_gain,
    first_shift,
    up_weight,
    up_bias,
    down_weight,
    down_bias,
    second_gain,
    second_shift,
    output_grad,
):
    local_rows = tokens.shape[0]
    head_cols = query_weight.shape[1]
    seq_count = lengths.shape[1]
    all_rows = local_rows * lax.axis_size("mp")
    gathered = lax.all_gather(tokens, "mp", axis=0, tiled=True)
    joint_weight = jnp.concatenate([query_weight, key_weight, value_weight], 1)
    projected = jnp.dot(gathered, joint_weight, preferred_element_type=jnp.float32)
    queries, key_rows, values = split_projection(projected, head_cols, query_bias, value_bias)
    expon, attended, inverse = attention_forward(queries, key_rows, values, lengths[0])
    branch_one = lax.psum_scatter(
        jnp.dot(
            lax.slice_in_dim(attended, 0, local_rows * lax.axis_size("mp"), axis=0),
            out_weight,
            preferred_element_type=jnp.float32,
        ).astype(jnp.bfloat16),
        "mp",
        scatter_dimension=0,
        tiled=True,
    ).astype(jnp.float32)
    hidden, normed_one, inv_one = norm_forward(
        tokens.astype(jnp.float32) + branch_one + out_bias, first_gain, first_shift
    )
    hidden_low = hidden.astype(jnp.bfloat16)
    hidden_all = lax.all_gather(hidden_low, "mp", axis=0, tiled=True)
    pre_act = jnp.dot(hidden_all, up_weight, preferred_element_type=jnp.float32) + up_bias
    act_low = jax.nn.gelu(pre_act, approximate=False).astype(jnp.bfloat16)
    branch_two = lax.psum_scatter(
        jnp.dot(
            lax.slice_in_dim(act_low, 0, local_rows * lax.axis_size("mp"), axis=0),
            down_weight,
            preferred_element_type=jnp.float32,
        ).astype(jnp.bfloat16),
        "mp",
        scatter_dimension=0,
        tiled=True,
    ).astype(jnp.float32)
    layer_out, normed_two, inv_two = norm_forward(
        hidden + branch_two + down_bias, second_gain, second_shift
    )
    resid_two_grad, second_gain_grad, second_shift_grad = norm_backward(
        output_grad.astype(jnp.float32), normed_two, inv_two, second_gain
    )
    down_bias_grad = jnp.sum(resid_two_grad, 0)
    branch_two_low = resid_two_grad.astype(jnp.bfloat16)
    row_piece = lax.all_gather(branch_two_low, "mp", axis=0, tiled=True)
    row_start = jnp.int32(0)
    weight_acc = jnp.zeros(down_weight.shape, jnp.float32)
    act_acc = jnp.zeros(act_low.shape, jnp.float32)
    act_rows = lax.dynamic_slice_in_dim(act_low, row_start, row_piece.shape[0], 0)
    weight_acc = weight_acc + contract_rows(act_rows, row_piece)
    act_acc = lax.dynamic_update_slice_in_dim(
        act_acc, contract_cols(row_piece, down_weight), row_start, 0
    )
    down_weight_grad = weight_acc
    unused_two, gelu_back = jax.vjp(partial(jax.nn.gelu, approximate=False), pre_act)
    pre_grad = gelu_back(act_acc)[0].astype(jnp.bfloat16)
    up_bias_grad = jnp.sum(pre_grad, 0, dtype=jnp.float32)
    up_weight_grad = contract_rows(hidden_all, pre_grad)
    hidden_back = lax.psum_scatter(
        contract_cols(
            lax.slice_in_dim(pre_grad, 0, local_rows * lax.axis_size("mp"), axis=0), up_weight
        ).astype(jnp.bfloat16),
        "mp",
        scatter_dimension=0,
        tiled=True,
    ).astype(jnp.float32)
    hidden_grad = resid_two_grad + hidden_back
    resid_one_grad, first_gain_grad, first_shift_grad = norm_backward(
        hidden_grad, normed_one, inv_one, first_gain
    )
    out_bias_grad = jnp.sum(resid_one_grad, 0)
    branch_one_low = resid_one_grad.astype(jnp.bfloat16)
    row_piece = lax.all_gather(branch_one_low, "mp", axis=0, tiled=True)
    row_start = jnp.int32(0)
    weight_acc = jnp.zeros(out_weight.shape, jnp.float32)
    attn_acc = jnp.zeros(attended.shape, jnp.float32)
    attn_rows = lax.dynamic_slice_in_dim(attended, row_start, row_piece.shape[0], 0)
    weight_acc = weight_acc + contract_rows(attn_rows, row_piece)
    attn_acc = lax.dynamic_update_slice_in_dim(
        attn_acc, contract_cols(row_piece, out_weight), row_start, 0
    )
    out_weight_grad = weight_acc
    attn_low = attn_acc.astype(jnp.bfloat16)
    query_flat, key_flat, value_flat = attention_backward(
        expon, inverse, queries, key_rows, values, attended, attn_low, seq_count
    )
    width_now = query_flat.shape[1]
    joint_grad = jnp.concatenate([query_flat, key_flat, value_flat], 1)
    query_bias_grad = jnp.sum(query_flat, 0, dtype=jnp.float32)
    value_bias_grad = jnp.sum(value_flat, 0, dtype=jnp.float32)
    joint_weight_grad = contract_rows(gathered, joint_grad)
    input_back = lax.psum_scatter(
        contract_cols(
            lax.slice_in_dim(joint_grad, 0, local_rows * lax.axis_size("mp"), axis=0), joint_weight
        ).astype(jnp.bfloat16),
        "mp",
        scatter_dimension=0,
        tiled=True,
    ).astype(jnp.float32)
    tokens_grad = (resid_one_grad + input_back).astype(jnp.bfloat16)
    query_weight_grad = joint_weight_grad[:, :width_now]
    key_weight_grad = joint_weight_grad[:, width_now : 2 * width_now]
    value_weight_grad = joint_weight_grad[:, 2 * width_now :]
    (
        query_weight_grad,
        query_bias_grad,
        key_weight_grad,
        value_weight_grad,
        value_bias_grad,
        out_weight_grad,
        up_weight_grad,
        up_bias_grad,
        down_weight_grad,
    ) = (
        lax.psum(query_weight_grad.astype(jnp.bfloat16), "dp").astype(jnp.float32),
        lax.psum(query_bias_grad.astype(jnp.bfloat16), "dp").astype(jnp.float32),
        lax.psum(key_weight_grad.astype(jnp.bfloat16), "dp").astype(jnp.float32),
        lax.psum(value_weight_grad.astype(jnp.bfloat16), "dp").astype(jnp.float32),
        lax.psum(value_bias_grad.astype(jnp.bfloat16), "dp").astype(jnp.float32),
        lax.psum(out_weight_grad.astype(jnp.bfloat16), "dp").astype(jnp.float32),
        lax.psum(up_weight_grad.astype(jnp.bfloat16), "dp").astype(jnp.float32),
        lax.psum(up_bias_grad.astype(jnp.bfloat16), "dp").astype(jnp.float32),
        lax.psum(down_weight_grad.astype(jnp.bfloat16), "dp").astype(jnp.float32),
    )
    (
        out_bias_grad,
        first_gain_grad,
        first_shift_grad,
        down_bias_grad,
        second_gain_grad,
        second_shift_grad,
    ) = lax.psum(
        (
            out_bias_grad,
            first_gain_grad,
            first_shift_grad,
            down_bias_grad,
            second_gain_grad,
            second_shift_grad,
        ),
        ("dp", "mp"),
    )
    return (
        layer_out.astype(jnp.bfloat16),
        tokens_grad,
        query_weight_grad,
        query_bias_grad,
        key_weight_grad,
        value_weight_grad,
        value_bias_grad,
        out_weight_grad,
        out_bias_grad,
        first_gain_grad,
        first_shift_grad,
        up_weight_grad,
        up_bias_grad,
        down_weight_grad,
        down_bias_grad,
        second_gain_grad,
        second_shift_grad,
    )


MESH = pl.DeviceIdType.MESH
VMEM_BYTES = 63 * 1024 * 1024
CHUNKS = 4
KINDS = "HBHB"
MORE_X = "HHHB"
JOBS = len(KINDS)


def flip(index, bit):
    low = index // bit % 2
    return index + bit * (1 - 2 * low)


def mp_peer(relation):
    dp, mp = lax.axis_index("dp"), lax.axis_index("mp")
    for bit in (1, 2):
        if relation // bit % 2:
            mp = flip(mp, bit)
    return (dp, mp)


def dp_peer(bit):
    return (flip(lax.axis_index("dp"), bit), lax.axis_index("mp"))


def greet(peers):
    barrier = pltpu.get_barrier_semaphore()
    for device in peers:
        pl.semaphore_signal(barrier, inc=1, device_id=device, device_id_type=MESH)
    pl.semaphore_wait(barrier, len(peers))


def remote(src, dst, send, recv, device):
    return pltpu.make_async_remote_copy(
        src_ref=src, dst_ref=dst, send_sem=send, recv_sem=recv, device_id=device, device_id_type=MESH
    )


def repeat(count, body):
    def step(i, carry):
        body(i)
        return carry

    lax.fori_loop(0, count, step, 0)


class Gather:
    def __init__(self, land, send, recv, chunks=CHUNKS):
        self.land, self.send, self.recv, self.chunks = land, send, recv, chunks
        self.size = land.shape[1] // chunks

    def copy(self, relation, j):
        rows = pl.ds(pl.multiple_of(j * self.size, self.size), self.size)
        return remote(
            self.land.at[2 if relation == 3 else 0, rows],
            self.land.at[relation, rows],
            self.send.at[relation - 1, j],
            self.recv.at[relation - 1, j],
            mp_peer(2 if relation == 2 else 1),
        )

    def start(self, j):
        self.copy(2, j).start()
        self.copy(1, j).start()

    def arrive(self, relation, j):
        self.copy(relation, j).wait_recv()
        if relation == 2:
            self.copy(3, j).start()

    def drain(self):
        def body(j):
            for relation in (1, 2, 3):
                self.copy(relation, j).wait_send()

        repeat(self.chunks, body)


PAIR, FAR, NEAR = 0, 1, 2


class Reduce:
    def __init__(self, out, land, send, recv, chunks=CHUNKS):
        self.out, self.land, self.send, self.recv, self.chunks = out, land, send, recv, chunks
        self.size = out.shape[1] // chunks

    def copy(self, kind, j):
        rows = pl.ds(j * self.size, self.size)
        return remote(
            self.out.at[kind, rows],
            self.land.at[kind, rows],
            self.send.at[kind, j],
            self.recv.at[kind, j],
            mp_peer(2 if kind == FAR else 1),
        )

    def post(self, kind, j, value):
        self.out[kind, pl.ds(j * self.size, self.size)] = value.astype(BF)
        self.copy(kind, j).start()

    def forward_pair(self, j, mine):
        self.copy(PAIR, j).wait_recv()
        rows = pl.ds(j * self.size, self.size)
        self.post(FAR, j, mine + self.land[PAIR, rows].astype(F32))

    def total(self, j, mine):
        self.copy(NEAR, j).wait_recv()
        self.copy(FAR, j).wait_recv()
        rows = pl.ds(j * self.size, self.size)
        return mine + self.land[NEAR, rows].astype(F32) + self.land[FAR, rows].astype(F32)

    def drain(self):
        def body(j):
            for kind in (PAIR, FAR, NEAR):
                self.copy(kind, j).wait_send()

        repeat(self.chunks, body)


ROUTES = {"H": "xlh", "B": "lxh"}


class Spread:
    def __init__(self, data, full, land, send, recv, kinds, first=0, last=3):
        self.data, self.full, self.land, self.send, self.recv = data, full, land, send, recv
        self.sums, self.hands = first < 2, last > 1
        self.kinds, self.jobs = kinds, len(kinds)
        self.count = (full if data is None else data).shape[0] // self.jobs

    def route(self, job):
        return ROUTES[self.kinds[job if isinstance(job, int) else 0]]

    def side(self, axis):
        dp = lax.axis_index("dp")
        return {"x": dp % 2, "z": dp // 2, "l": dp // 2 % 2, "h": dp // 4}[axis]

    def range_of(self, start, size):
        return pl.ds(pl.multiple_of(start, size), size)

    def place(self, job, level):
        start, size = job * self.count, self.count
        for axis in self.route(job)[:level]:
            size //= 4 if axis == "z" else 2
            start += self.side(axis) * size
        return start, size

    def landing(self, job, stage, k=1):
        at, size = 0, self.count
        for level in range(stage + 1):
            ways = 4 if self.route(job)[level] == "z" else 2
            size //= ways
            if level < stage:
                at += size * (ways - 1)
        return self.land.at[job, pl.ds(at + (k - 1) * size, size)]

    def copies(self, job, stage):
        dp, mp = lax.axis_index("dp"), lax.axis_index("mp")
        levels = len(self.route(job))
        back = stage >= levels
        level = 2 * levels - 1 - stage if back else stage
        start, size = self.place(job, level)
        axis = self.route(job)[level]
        here = self.side(axis)
        ways, step = (4, 2) if axis == "z" else (2, {"x": 1, "l": 2, "h": 4}[axis])
        found = []
        for k in range(1, ways):
            there = (here + k) % ways
            if back:
                src = dst = self.full.at[self.range_of(*self.place(job, level + 1))]
            else:
                src = self.data.at[self.range_of(start + there * (size // ways), size // ways)]
                dst = self.landing(job, level, k)
            at = (job, stage * 3 + k - 1)
            device = (dp + (there - here) * step, mp)
            found.append(remote(src, dst, self.send.at[at], self.recv.at[at], device))
        return found

    def own(self, job):
        return self.range_of(*self.place(job, len(self.route(job))))

    def stages(self, job):
        levels = len(self.route(job))
        return (0 if self.sums else levels), (2 * levels if self.hands else levels)

    def step(self, job, stage):
        first, end = self.stages(job)
        levels = len(self.route(job))
        if stage > first:
            arrived = self.copies(job, stage - 1)
            for done in arrived:
                done.wait_send()
                done.wait_recv()
            if stage <= levels:
                rows = self.range_of(*self.place(job, stage))
                total = self.data[rows].astype(F32)
                for k in range(len(arrived)):
                    total += self.landing(job, stage - 1, k + 1)[...].astype(F32)
                target = self.full if stage == levels and self.full is not None else self.data
                target[rows] = total.astype(BF)
        if stage < end:
            for copy in self.copies(job, stage):
                copy.start()


def advance(*moves):
    for total, jobs, stage in moves:
        for job in jobs if isinstance(jobs, tuple) else (jobs,):
            total.step(job, stage)


def spread_land(data, kinds):
    count = data[0] // len(kinds)
    return pltpu.VMEM((len(kinds), count - count // 8, data[1]), BF)


def spread_sems(kinds):
    return [pltpu.SemaphoreType.DMA((len(kinds), 18)), pltpu.SemaphoreType.DMA((len(kinds), 18))]


class Hops:
    def __init__(self, value, land, send, recv, peers):
        self.value, self.land, self.send, self.recv, self.peers = value, land, send, recv, peers

    def copy(self, i):
        return remote(
            self.value.at[i], self.land.at[i], self.send.at[i], self.recv.at[i], self.peers[i]
        )

    def start(self, i):
        self.copy(i).start()

    def finish(self, i):
        self.copy(i).wait_recv()
        self.value[i + 1] = self.value[i] + self.land[i]
        self.copy(i).wait_send()


def hop_scratch(count, *shape):
    return [
        pltpu.VMEM((count + 1, *shape), F32),
        pltpu.VMEM((count, *shape), F32),
        pltpu.SemaphoreType.DMA((count,)),
        pltpu.SemaphoreType.DMA((count,)),
    ]


def greet_all():
    dp, mp = lax.axis_index("dp"), lax.axis_index("mp")
    across = [((dp // 2 + k) % 4 * 2 + dp % 2, mp) for k in (1, 2, 3)]
    greet([mp_peer(1), mp_peer(2), dp_peer(1), *across])


def transfer_sems(chunks=CHUNKS):
    return [pltpu.SemaphoreType.DMA((3, chunks)), pltpu.SemaphoreType.DMA((3, chunks))]


def comm_params(collective_id):
    return pltpu.CompilerParams(
        collective_id=collective_id, has_side_effects=True, vmem_limit_bytes=VMEM_BYTES
    )


WHOLE = pl.BlockSpec(memory_space=pltpu.VMEM)


def shaped(*shape, dtype=None):
    return jax.ShapeDtypeStruct(shape, dtype or BF)


def as_row(ref):
    return ref[...].astype(F32)[None]


def column_sum(value):
    return jnp.sum(value, 0, keepdims=True)


def row_mean(value):
    return jnp.mean(value, -1, keepdims=True)


def project(x_ref, wq_ref, wk_ref, wv_ref, qb_ref, vb_ref, q_ref, k_ref, v_ref, vt_ref, land, send, recv, save):
    rows_here = land.shape[1]
    load = pltpu.make_async_copy(x_ref, land.at[0], save.at[0])
    load.start()
    load.wait()
    greet([mp_peer(1), mp_peer(2)])
    gather = Gather(land, send, recv)
    repeat(CHUNKS, gather.start)
    size = gather.size

    def emit(x, at):
        rows = pl.ds(pl.multiple_of(at, x.shape[0]), x.shape[0])
        q = (mm(x, wq_ref[...], 1, 0) + as_row(qb_ref)).astype(BF)
        q_ref[rows] = (q.astype(F32) * HD**-0.5).astype(BF)
        k_ref[rows] = mm(x, wk_ref[...], 1, 0).astype(BF)
        v = mm(x, wv_ref[...], 1, 0) + as_row(vb_ref)
        v_ref[rows] = v.astype(BF)
        vt_ref[:, rows] = v.T.astype(BF)

    def close(i):
        s, j = i // 2, i % 2 * 2

        @pl.when(i >= 2)
        def _():
            gather.arrive(1, j)
            gather.arrive(1, j + 1)

        emit(land[s, pl.ds(pl.multiple_of(j * size, 2 * size), 2 * size)], i * 2 * size)

    repeat(4, close)

    def far(j):
        gather.arrive(2, j)
        gather.arrive(3, j)

        def one(k):
            emit(land[2 + k, pl.ds(pl.multiple_of(j * size, size), size)], (2 + k) * rows_here + j * size)

        repeat(2, one)

    repeat(CHUNKS, far)
    gather.drain()


HALVES = 2


def forward_order(step):
    far = 2 * (3 - step % 2) + step // 2
    near = 2 * (1 - (step - 4) // 2) + step % 2
    return jnp.where(step < 4, far, near)


def attend_kernel(
    len_ref, x_ref, wq_ref, wk_ref, wv_ref, qb_ref, vb_ref, w_ref, ob_ref, gain_ref, shift_ref,
    q_out, k_out, v_out, all_out, e_ref, o_ref, r_ref, n_ref, i_ref, h_ref,
    tokens, q_ref, k_ref, v_ref, vt_ref, gather_send, gather_recv, save,
    k_aug, v_aug, out, land, mine, pending, send, recv,
):
    step = pl.program_id(0)
    seq_len, block = k_ref.shape[0], pending.shape[0]
    rows_here = tokens.shape[1]
    saves = [
        pltpu.make_async_copy(src, dst, save.at[1 + i])
        for i, (src, dst) in enumerate(
            ((q_ref, q_out), (k_ref, k_out), (v_ref, v_out), (tokens, all_out))
        )
    ]
    pairs = k_ref.shape[1] // WIDE
    reduce = Reduce(out, land, send, recv, HALVES)

    @pl.when(step == 0)
    def _():
        project(
            x_ref, wq_ref, wk_ref, wv_ref, qb_ref, vb_ref, q_ref, k_ref, v_ref, vt_ref,
            tokens, gather_send, gather_recv, save,
        )
        for each in saves:
            each.start()
        lanes = lax.broadcasted_iota(jnp.int32, (seq_len, WIDE), 1)
        rows = lax.broadcasted_iota(jnp.int32, (rows_here, WIDE), 0)
        bias = jnp.concatenate(
            [
                jnp.where(rows + mp_peer(s)[1] * rows_here < len_ref[0, 0], 0.0, MASKED)
                for s in range(4)
            ],
            0,
        )
        for p in range(pairs):
            keys = k_ref[:, p * WIDE : (p + 1) * WIDE].astype(F32)
            for h in range(2):
                other = (1 - h) * HD
                k_aug[2 * p + h] = jnp.where(
                    lanes // HD == h, keys, jnp.where(lanes == other, bias, 0.0)
                ).astype(BF)
                at = (2 * p + h) * HD
                v_aug[2 * p + h, :HD] = vt_ref[at : at + HD, :]
                v_aug[2 * p + h, HD:] = jnp.ones((16, seq_len), BF)

    lanes = lax.broadcasted_iota(jnp.int32, (block, WIDE), 1)
    q_rows = pl.ds(pl.multiple_of(forward_order(step) * block, block), block)
    outs = []
    for p in range(pairs):
        query = q_ref[q_rows, p * WIDE : (p + 1) * WIDE].astype(F32)
        scores = []
        for h in range(2):
            other = (1 - h) * HD
            q_aug = jnp.where(
                lanes // HD == h, query, jnp.where(lanes == other, 1.0, 0.0)
            ).astype(BF)
            scores.append(mm(k_aug[2 * p + h], q_aug, 1, 1))
        for h in range(2):
            top = jnp.max(scores[h], 0, keepdims=True)
            expon = jnp.exp(scores[h] - top).astype(BF)
            e_ref[0, 2 * p + h] = expon
            total = mm(v_aug[2 * p + h], expon, 1, 0)
            inverse = 1.0 / total[HD : HD + 1]
            r_ref[0, 2 * p + h] = inverse
            outs.append(total[:HD] * inverse)
    attended = jnp.concatenate(outs, 0).T.astype(BF)
    o_ref[...] = attended
    partial_rows = mm(attended, w_ref[...], 1, 0)

    for t in range(4 * HALVES):

        @pl.when(step == t)
        def _(t=t):
            if t < 4 and t % 2 == 0:
                reduce.post(PAIR, t // 2, partial_rows)
            elif t < 4:
                pending[...] = partial_rows
                reduce.forward_pair(t // 2, pending[...])
            elif t < 6:
                reduce.post(NEAR, t - 4, partial_rows)
            else:
                mine[pl.ds((t - 6) * block, block)] = partial_rows

    @pl.when(step == 4 * HALVES - 1)
    def _():
        for j in range(HALVES):
            rows = pl.ds(j * block, block)
            resid = tokens[0, rows].astype(F32) + reduce.total(j, mine[rows]) + as_row(ob_ref)
            center = resid - row_mean(resid)
            inv_std = lax.rsqrt(row_mean(center * center) + epsilon)
            normed = center * inv_std
            n_ref[rows] = normed
            i_ref[rows] = inv_std
            h_ref[rows] = (normed * as_row(gain_ref) + as_row(shift_ref)).astype(BF)
        reduce.drain()
        for each in saves:
            each.wait()


def attend(lengths, tokens, wq, wk, wv, q_bias, v_bias, out_weight, *vectors):
    rows, width = tokens.shape
    all_rows, cols = 4 * rows, wq.shape[1]
    block = rows // HALVES
    heads = cols // HD
    steps = all_rows // block

    def fixed(*shape):
        return pl.BlockSpec(shape, lambda i: (0,) * len(shape))

    anywhere = pl.BlockSpec(memory_space=pl.ANY)
    return pl.pallas_call(
        attend_kernel,
        grid=(steps,),
        in_specs=[
            pl.BlockSpec(memory_space=pltpu.SMEM),
            anywhere,
            *[fixed(width, cols)] * 3,
            *[fixed(cols)] * 2,
            fixed(cols, width),
            *[fixed(width)] * 3,
        ],
        out_specs=[
            *[anywhere] * 4,
            pl.BlockSpec((1, heads, all_rows, block), lambda i: (forward_order(i), 0, 0, 0)),
            pl.BlockSpec((block, cols), lambda i: (forward_order(i), 0)),
            pl.BlockSpec((1, heads, 1, block), lambda i: (forward_order(i), 0, 0, 0)),
            fixed(rows, width),
            fixed(rows, 1),
            fixed(rows, width),
        ],
        out_shape=[
            *[shaped(all_rows, cols)] * 3,
            shaped(4, rows, width),
            shaped(steps, heads, all_rows, block),
            shaped(all_rows, cols),
            shaped(steps, heads, 1, block, dtype=F32),
            shaped(rows, width, dtype=F32),
            shaped(rows, 1, dtype=F32),
            shaped(rows, width),
        ],
        scratch_shapes=[
            pltpu.VMEM((4, rows, width), BF),
            *[pltpu.VMEM((all_rows, cols), BF)] * 3,
            pltpu.VMEM((cols, all_rows), BF),
            *transfer_sems(),
            pltpu.SemaphoreType.DMA((5,)),
            pltpu.VMEM((heads, all_rows, WIDE), BF),
            pltpu.VMEM((heads, HD + 16, all_rows), BF),
            pltpu.VMEM((3, rows, width), BF),
            pltpu.VMEM((3, rows, width), BF),
            pltpu.VMEM((rows, width), F32),
            pltpu.VMEM((block, width), F32),
            *transfer_sems(HALVES),
        ],
        name="attend",
        compiler_params=comm_params(1),
    )(lengths, tokens, wq, wk, wv, q_bias, v_bias, out_weight, *vectors)


ROOT_HALF = 0.7071067811865476
ROOT_TAU = 0.3989422804014327


def feed_forward_kernel(
    h_ref, n_in, i_ref, g_in, up_in, ub_ref, down_in, *refs
):
    vectors, refs = refs[:5], refs[5:]
    (
        out_hbm, b1_ref, r1_ref, upg_hbm, downg_ref, small_ref,
        hidden, act, slope, branch, out1, land1, out2, land2, mine, pending, r2,
        gs1, gr1, gs2, gr2, rs1, rr1, rs2, rr2,
        down_land, down_send, down_recv, load, n_ref, g_ref, up_ref, down_ref, out_ref, upg_ref,
    ) = refs
    rows_here, width = h_ref.shape
    fetch = pltpu.make_async_copy(h_ref, hidden.at[0], load.at[0])
    fetch.start()
    fetches = [
        pltpu.make_async_copy(src, dst, load.at[1 + i])
        for i, (src, dst) in enumerate(
            ((up_in, up_ref), (down_in, down_ref), (n_in, n_ref), (g_in, g_ref))
        )
    ]
    save_out = pltpu.make_async_copy(out_ref, out_hbm, load.at[5])
    save_upg = pltpu.make_async_copy(upg_ref, upg_hbm, load.at[6])
    size = rows_here // CHUNKS
    first_gain, first_shift, down_bias, second_gain, second_shift = map(as_row, vectors)
    greet_all()
    down_sum = Spread(downg_ref, None, down_land, down_send, down_recv, KINDS, 0, 1)
    gather1, gather2 = Gather(hidden, gs1, gr1), Gather(branch, gs2, gr2)
    reduce1, reduce2 = Reduce(out1, land1, rs1, rr1), Reduce(out2, land2, rs2, rr2)
    fetch.wait()
    repeat(CHUNKS, gather1.start)
    for each in fetches:
        each.start()
    for each in fetches[:2]:
        each.wait()
    small_ref[...] = jnp.zeros_like(small_ref)

    def forward(x):
        pre = mm(x, up_ref[...], 1, 0) + as_row(ub_ref)
        cdf = 0.5 + 0.5 * lax.erf(pre * ROOT_HALF)
        active = (pre * cdf).astype(BF)
        steep = (cdf + pre * jnp.exp(-0.5 * pre * pre) * ROOT_TAU).astype(BF)
        return active, steep, mm(active, down_ref[...], 1, 0)

    def backward(grad, steep):
        pre_grad = (mm(grad, down_ref[...], 1, 1) * steep.astype(F32)).astype(BF)
        small_ref[6:7] += column_sum(pre_grad.astype(F32))
        return pre_grad, mm(pre_grad, up_ref[...], 1, 1)

    def chunk_rows(j):
        return pl.ds(pl.multiple_of(j * size, size), size)

    def double_rows(j):
        return pl.ds(pl.multiple_of(j * 2 * size, 2 * size), 2 * size)

    def halves(value):
        return value[:size], value[size:]

    def close_forward(i):
        s, half = i // 2, i % 2
        rows = double_rows(half)

        @pl.when(i >= 2)
        def _():
            gather1.arrive(1, 2 * half)
            gather1.arrive(1, 2 * half + 1)

        act[s, rows], slope[s, rows], part = forward(hidden[s, rows])

        @pl.when(i < 2)
        def _():
            mine[rows] = part

        @pl.when(i >= 2)
        def _():
            for k, piece in enumerate(halves(part)):
                reduce1.post(NEAR, 2 * half + k, piece)

    def far_forward(j):
        gather1.arrive(2, j)
        gather1.arrive(3, j)
        rows = chunk_rows(j)
        active, steep, part = forward(jnp.concatenate([hidden[2, rows], hidden[3, rows]], 0))
        for s in (2, 3):
            act[s, rows] = halves(active)[s - 2]
            slope[s, rows] = halves(steep)[s - 2]
        pending[rows] = part[:size]
        reduce1.post(PAIR, j, part[size:])

        @pl.when(j > 0)
        def _():
            reduce1.forward_pair(j - 1, pending[chunk_rows(j - 1)])

    repeat(4, close_forward)
    repeat(CHUNKS, far_forward)
    reduce1.forward_pair(CHUNKS - 1, pending[chunk_rows(CHUNKS - 1)])

    def second_norm(j):
        rows = chunk_rows(j)
        hidden = n_ref[rows] * first_gain + first_shift
        resid = hidden + reduce1.total(j, mine[rows]) + down_bias
        center = resid - row_mean(resid)
        inv_std = lax.rsqrt(row_mean(center * center) + epsilon)
        normed = center * inv_std
        out_ref[rows] = (normed * second_gain + second_shift).astype(BF)
        grad = g_ref[rows].astype(F32)
        product = grad * normed
        small_ref[0:1] += column_sum(product)
        small_ref[1:2] += column_sum(grad)
        scaled = grad * second_gain
        back = inv_std * (scaled - row_mean(scaled) - normed * row_mean(scaled * normed))
        small_ref[2:3] += column_sum(back)
        r2[rows] = back
        branch[0, rows] = back.astype(BF)
        gather2.start(j)

    for each in fetches[2:]:
        each.wait()
    repeat(CHUNKS, second_norm)
    save_out.start()

    def close_backward(i):
        s, half = i // 2, i % 2
        rows = double_rows(half)

        @pl.when(i >= 2)
        def _():
            gather2.arrive(1, 2 * half)
            gather2.arrive(1, 2 * half + 1)

        slope[s, rows], part = backward(branch[s, rows], slope[s, rows])

        @pl.when(i < 2)
        def _():
            mine[rows] = part

        @pl.when(i >= 2)
        def _():
            for k, piece in enumerate(halves(part)):
                reduce2.post(NEAR, 2 * half + k, piece)

    def far_backward(j):
        gather2.arrive(2, j)
        gather2.arrive(3, j)
        rows = chunk_rows(j)
        pre_grad, part = backward(
            jnp.concatenate([branch[2, rows], branch[3, rows]], 0),
            jnp.concatenate([slope[2, rows], slope[3, rows]], 0),
        )
        for s in (2, 3):
            slope[s, rows] = halves(pre_grad)[s - 2]
        pending[rows] = part[:size]
        reduce2.post(PAIR, j, part[size:])

        @pl.when(j > 0)
        def _():
            reduce2.forward_pair(j - 1, pending[chunk_rows(j - 1)])

    repeat(4, close_backward)
    repeat(CHUNKS, far_backward)
    reduce2.forward_pair(CHUNKS - 1, pending[chunk_rows(CHUNKS - 1)])

    tile = 256

    def down_grad(t):
        cols = pl.ds(pl.multiple_of(t * tile, tile), tile)
        total = mm(act[0, :, cols], branch[0], 0, 0)
        for s in (1, 2, 3):
            total += mm(act[s, :, cols], branch[s], 0, 0)
        downg_ref[cols] = total.astype(BF)

    def up_grad(t):
        cols = pl.ds(pl.multiple_of(t * tile, tile), tile)
        total = mm(hidden[0, :, cols], slope[0], 0, 0)
        for s in (1, 2, 3):
            total += mm(hidden[s, :, cols], slope[s], 0, 0)
        upg_ref[cols] = total.astype(BF)

    repeat(2, down_grad)
    advance((down_sum, (0, 1), 0))
    repeat(2, lambda t: down_grad(t + 2))
    advance((down_sum, (2, 3), 0))
    repeat(width // tile, up_grad)
    save_upg.start()

    def first_norm(j):
        rows = chunk_rows(j)
        normed = n_ref[rows]
        grad = r2[rows] + reduce2.total(j, mine[rows])
        small_ref[3:4] += column_sum(grad * normed)
        small_ref[4:5] += column_sum(grad)
        scaled = grad * first_gain
        back = i_ref[rows] * (scaled - row_mean(scaled) - normed * row_mean(scaled * normed))
        small_ref[5:6] += column_sum(back)
        r1_ref[rows] = back
        b1_ref[rows] = back.astype(BF)

    advance((down_sum, (0, 1), 1))
    first_norm(0)
    advance((down_sum, (2, 3), 1))
    first_norm(1)
    advance((down_sum, (0, 1), 2))
    first_norm(2)
    advance((down_sum, (2, 3), 2))
    first_norm(3)
    advance((down_sum, (0, 1, 2, 3), 3))
    for transfer in (gather1, gather2, reduce1, reduce2):
        transfer.drain()
    save_out.wait()
    save_upg.wait()


def feed_forward(hidden, normed, inv_std, output_grad, up, up_bias, down, *vectors):
    rows, width = hidden.shape
    units = up.shape[1]
    tall = (4, rows, units)
    anywhere = pl.BlockSpec(memory_space=pl.ANY)
    return pl.pallas_call(
        feed_forward_kernel,
        in_specs=[anywhere, anywhere, WHOLE, anywhere, anywhere, WHOLE, anywhere] + [WHOLE] * 5,
        out_specs=[anywhere, WHOLE, WHOLE, anywhere, WHOLE, WHOLE],
        out_shape=[
            shaped(rows, width),
            shaped(rows, width),
            shaped(rows, width, dtype=F32),
            shaped(width, units),
            shaped(units, width),
            shaped(8, width, dtype=F32),
        ],
        scratch_shapes=[
            pltpu.VMEM((4, rows, width), BF),
            pltpu.VMEM(tall, BF),
            pltpu.VMEM(tall, BF),
            pltpu.VMEM((4, rows, width), BF),
            *[pltpu.VMEM((3, rows, width), BF)] * 4,
            *[pltpu.VMEM((rows, width), F32)] * 3,
            *transfer_sems(),
            *transfer_sems(),
            *transfer_sems(),
            *transfer_sems(),
            spread_land((units, width), KINDS),
            *spread_sems(KINDS),
            pltpu.SemaphoreType.DMA((7,)),
            pltpu.VMEM((rows, width), F32),
            pltpu.VMEM((rows, width), BF),
            pltpu.VMEM((width, units), BF),
            pltpu.VMEM((units, width), BF),
            pltpu.VMEM((rows, width), BF),
            pltpu.VMEM((width, units), BF),
        ],
        name="feed_forward",
        compiler_params=comm_params(2),
    )(hidden, normed, inv_std, output_grad, up, up_bias, down, *vectors)


def attend_back_kernel(
    b_ref, w_ref, e_ref, r_ref, q_ref, k_ref, v_ref, o_ref, small_in, up_in, down_in, all_in,
    dq_ref, dk_ref, dv_ref, wg_ref, pg_ref, small_ref, up_out, down_out,
    land, v_aug, k_t, dks, dvs, dqs, w_total, w_low, p_low, grads, up, down, tokens, loads, send, recv,
    up_land, up_send, up_recv, down_send, down_recv, out_land, out_send, out_recv,
    pair_land, pair_send, pair_recv, value, small_land, small_send, small_recv,
):
    step = pl.program_id(0)
    pair, s_now = step // 2 % 2, step // 4 * 2 + step % 2
    seq_len, block = k_ref.shape[0], q_ref.shape[0]
    pieces = e_ref.shape[0]
    cols = w_ref.shape[0]
    width = w_ref.shape[1]
    half = block // 2
    gather = Gather(land, send, recv, HALVES)
    up_sum = Spread(up, None, up_land, up_send, up_recv, MORE_X, 0, 1)
    down_sum = Spread(None, down, None, down_send, down_recv, KINDS, 2, 3)
    out_sum = Spread(w_low, None, out_land, out_send, out_recv, "H", 0, 1)
    pair_sum = Spread(p_low, None, pair_land, pair_send, pair_recv, MORE_X, 0, 1)
    small = Hops(
        value, small_land, small_send, small_recv,
        [dp_peer(1), dp_peer(2), dp_peer(4), mp_peer(1), mp_peer(2)],
    )
    load_up = pltpu.make_async_copy(up_in, up, loads.at[0])
    load_down = [
        pltpu.make_async_copy(
            down_in.at[down_sum.own(job)], down.at[down_sum.own(job)], loads.at[5 + job]
        )
        for job in range(JOBS)
    ]
    load_tokens = pltpu.make_async_copy(all_in, tokens, loads.at[2])
    save_up = pltpu.make_async_copy(up, up_out, loads.at[3])
    save_down = pltpu.make_async_copy(down, down_out, loads.at[4])

    load_branch = pltpu.make_async_copy(b_ref, land.at[0], loads.at[5 + JOBS])

    @pl.when(step == 0)
    def _():
        load_branch.start()
        for load in load_down:
            load.start()
        load_up.start()
        load_tokens.start()
        value[0] = small_in[...]
        w_total[...] = jnp.zeros_like(w_total)
        greet_all()
        small.start(0)
        load_branch.wait()
        repeat(HALVES, gather.start)
        for load in load_down:
            load.wait()
        advance((down_sum, (0, 1, 2, 3), 3))
        load_up.wait()
        advance((up_sum, (3, 0, 1, 2), 0))

    @pl.when(step == 1)
    def _():
        repeat(HALVES, lambda j: gather.arrive(1, j))

    @pl.when(step == 2)
    def _():
        small.finish(0)
        small.start(1)
        advance((down_sum, (0, 1, 2, 3), 4), (up_sum, (3, 0), 1))

    @pl.when(step == 3)
    def _():
        advance((up_sum, (1, 2), 1), (down_sum, (0, 1), 5))

    @pl.when(step == 4)
    def _():
        small.finish(1)
        small.start(2)
        advance((up_sum, (3, 0), 2), (down_sum, (2, 3), 5))
        repeat(HALVES, lambda j: gather.arrive(2, j))

    @pl.when(step == 5)
    def _():
        repeat(HALVES, lambda j: gather.arrive(3, j))

    @pl.when(pair == 0)
    def _():
        branch = land[s_now]
        w_total[...] += mm(o_ref[...], branch, 0, 0)
        grads[pl.ds(pl.multiple_of(s_now * block, block), block)] = mm(
            branch, w_ref[...], 1, 1
        ).astype(BF)

    @pl.when(step == 5)
    def _():
        w_low[...] = w_total[...].astype(BF)
        advance((out_sum, 0, 0), (up_sum, (1, 2), 2))

    @pl.when(step == 6)
    def _():
        small.finish(2)
        small.start(3)
        advance((out_sum, 0, 1), (up_sum, (3, 0), 3), (down_sum, (0, 1), 6))

    @pl.when(step == 7)
    def _():
        small.finish(3)
        small.start(4)
        advance(
            (pair_sum, (3, 0, 1, 2), 1), (out_sum, 0, 2), (up_sum, (1, 2), 3), (down_sum, (2, 3), 6)
        )
        save_up.start()
        save_down.start()

    @pl.when(s_now == 0)
    def _():
        lanes = lax.broadcasted_iota(jnp.int32, (seq_len, WIDE), 1)
        values = v_ref[...].astype(F32)
        for h in range(2):
            other = (1 - h) * HD
            ones = jnp.where((lanes >= other) & (lanes < other + 2), 1.0, 0.0)
            v_aug[pair, h] = jnp.where(lanes // HD == h, values, ones).astype(BF)
        k_t[pair] = (k_ref[...].astype(F32) * HD**-0.5).T.astype(BF)
        dks[pair] = jnp.zeros(dks.shape[1:], F32)
        dvs[pair] = jnp.zeros(dvs.shape[1:], F32)

    lanes = lax.broadcasted_iota(jnp.int32, (block, WIDE), 1)
    row_start = pl.multiple_of(s_now * block, block)
    inverse = jnp.concatenate(
        [
            jnp.concatenate(
                [jnp.broadcast_to(r_ref[i, h], (HD, block // pieces)) for h in range(2)], 0
            )
            for i in range(pieces)
        ],
        1,
    ).T
    wide = pl.ds(pl.multiple_of(pair * WIDE, WIDE), WIDE)
    grad = (grads[pl.ds(row_start, block), wide].astype(F32) * inverse).astype(BF)
    grad_wide = grad.astype(F32)
    product = grad_wide * o_ref[:, wide].astype(F32)
    centered = []
    for h in range(2):
        other = (1 - h) * HD
        inside = lanes // HD == h
        row_dot = jnp.sum(jnp.where(inside, product, 0.0), -1, keepdims=True)
        high = row_dot.astype(BF).astype(F32)
        g_aug = jnp.where(
            inside,
            grad_wide,
            jnp.where(lanes == other, -high, jnp.where(lanes == other + 1, high - row_dot, 0.0)),
        ).astype(BF)
        centered.append(mm(v_aug[pair, h], g_aug, 1, 1))
    query_grads = []
    for h in range(2):
        cols_h = slice(h * HD, (h + 1) * HD)
        expon = jnp.concatenate([e_ref[i, h] for i in range(pieces)], 1)
        score_grad = (expon.astype(F32) * centered[h]).astype(BF)
        dvs[pair, h] += mm(expon, grad[:, cols_h], 1, 0)
        dks[pair, h] += mm(score_grad, q_ref[:, cols_h], 1, 0)
        query_grads.append(mm(k_t[pair, cols_h, :], score_grad, 1, 0))
    query_grad = jnp.concatenate(query_grads, 0).T.astype(BF)
    dq_ref[...] = query_grad
    dqs[pair, pl.ds(row_start, block), :WIDE] = query_grad

    @pl.when(s_now == 3)
    def _():
        for total, out, at in ((dks, dk_ref, WIDE), (dvs, dv_ref, 2 * WIDE)):
            joined = jnp.concatenate([total[pair, h] for h in range(2)], 1).astype(BF)
            out[:, wide] = joined
            dqs[pair, :, at : at + WIDE] = joined

    @pl.when(step == 5)
    def _():
        load_tokens.wait()
        projection_grads(tokens, dqs.at[0], p_low)
        advance((pair_sum, (3, 0, 1, 2), 0))

    @pl.when(step == 7)
    def _():
        advance((pair_sum, (3, 0, 1, 2), 2), (out_sum, 0, 3), (pair_sum, (3, 0, 1, 2), 3))
        small.finish(4)
        small_ref[...] = value[5]
        small_ref[6:7] = value[3, 6:7]
        wg_ref[...] = w_low[...]
        pg_ref[...] = p_low[...]
        gather.drain()
        save_down.wait()
        save_up.wait()


def projection_grads(tokens, joint, out_ref):
    tile = 256
    rows = tokens.shape[1]

    def body(t):
        cols = pl.ds(pl.multiple_of(t * tile, tile), tile)
        total = mm(tokens[0, :, cols], joint[pl.ds(0, rows)], 0, 0)
        for s in (1, 2, 3):
            total += mm(tokens[s, :, cols], joint[pl.ds(s * rows, rows)], 0, 0)
        out_ref[cols] = total.astype(BF)

    repeat(tokens.shape[2] // tile, body)


def attend_back(branch, out_weight, expon, inverse, q, k, v, attended, small, up, down, gathered):
    rows, width = branch.shape
    all_rows, cols = q.shape
    pairs = cols // WIDE
    pieces = HALVES

    def fixed(*shape):
        return pl.BlockSpec(shape, lambda i: (0,) * len(shape))

    def pair_at(i):
        return i // 2 % 2

    def rows_at(i):
        return i // 4 * 2 + i % 2

    anywhere = pl.BlockSpec(memory_space=pl.ANY)
    pair_rows = pl.BlockSpec((rows, WIDE), lambda i: (rows_at(i), pair_at(i)))
    pair_keys = pl.BlockSpec((all_rows, WIDE), lambda i: (0, pair_at(i)))
    return pl.pallas_call(
        attend_back_kernel,
        grid=(4 * pairs,),
        in_specs=[
            anywhere,
            fixed(cols, width),
            pl.BlockSpec((pieces, 2, all_rows, rows // pieces), lambda i: (rows_at(i), pair_at(i), 0, 0)),
            pl.BlockSpec((pieces, 2, 1, rows // pieces), lambda i: (rows_at(i), pair_at(i), 0, 0)),
            pair_rows,
            pair_keys,
            pair_keys,
            pl.BlockSpec((rows, cols), lambda i: (rows_at(i), 0)),
            fixed(*small.shape),
            anywhere,
            anywhere,
            anywhere,
        ],
        out_specs=[
            pair_rows,
            fixed(all_rows, cols),
            fixed(all_rows, cols),
            fixed(cols, width),
            fixed(width, 3 * WIDE),
            fixed(*small.shape),
            anywhere,
            anywhere,
        ],
        out_shape=[shaped(all_rows, cols)] * 3
        + [
            shaped(cols, width),
            shaped(width, 3 * WIDE),
            shaped(*small.shape, dtype=F32),
            shaped(*up.shape),
            shaped(*down.shape),
        ],
        scratch_shapes=[
            pltpu.VMEM((4, rows, width), BF),
            pltpu.VMEM((pairs, 2, all_rows, WIDE), BF),
            pltpu.VMEM((pairs, WIDE, all_rows), BF),
            pltpu.VMEM((pairs, 2, all_rows, HD), F32),
            pltpu.VMEM((pairs, 2, all_rows, HD), F32),
            pltpu.VMEM((pairs, all_rows, 3 * WIDE), BF),
            pltpu.VMEM((cols, width), F32),
            pltpu.VMEM((cols, width), BF),
            pltpu.VMEM((width, 3 * WIDE), BF),
            pltpu.VMEM((all_rows, cols), BF),
            pltpu.VMEM(up.shape, BF),
            pltpu.VMEM(down.shape, BF),
            pltpu.VMEM(gathered.shape, BF),
            pltpu.SemaphoreType.DMA((6 + JOBS,)),
            *transfer_sems(HALVES),
            spread_land(up.shape, MORE_X),
            *spread_sems(KINDS),
            *spread_sems(KINDS),
            spread_land((cols, width), "H"),
            *spread_sems("H"),
            spread_land((width, 3 * WIDE), KINDS),
            *spread_sems(KINDS),
            *hop_scratch(5, *small.shape),
        ],
        name="attend_back",
        compiler_params=comm_params(3),
    )(branch, out_weight, expon, inverse, q, k, v, attended, small, up, down, gathered)


def input_back_kernel(
    dq_ref, dk_ref, dv_ref, wq_ref, wk_ref, wv_ref, all_in, r1_in, wg_in, pg_in, up_in,
    x_ref, wg_ref, pg_ref, last_ref, bias_ref, up_out,
    out, land, mine, pending, send, recv, up, loads, up_send, up_recv, out_send, out_recv,
    pair_send, pair_recv, all_ref, r1_ref, joint, w_full, p_full, last_full, last_low, last_land, last_send, last_recv,
    value, bias_land, bias_send, bias_recv,
):
    rows_here = r1_ref.shape[0]
    size = rows_here // CHUNKS
    last = dq_ref.shape[1] - WIDE
    up_sum = Spread(None, up, None, up_send, up_recv, MORE_X, 2, 3)
    out_sum = Spread(None, w_full, None, out_send, out_recv, "H", 2, 3)
    pair_sum = Spread(None, p_full, None, pair_send, pair_recv, MORE_X, 2, 3)
    last_sum = Spread(last_low, last_full, last_land, last_send, last_recv, KINDS)
    bias = Hops(value, bias_land, bias_send, bias_recv, [dp_peer(1), dp_peer(2), dp_peer(4)])
    reduce = Reduce(out, land, send, recv)
    save_up = pltpu.make_async_copy(up, up_out, loads.at[JOBS])
    load_up = [
        pltpu.make_async_copy(up_in.at[up_sum.own(job)], up.at[up_sum.own(job)], loads.at[job])
        for job in range(JOBS)
    ]
    load_all = pltpu.make_async_copy(all_in, all_ref, loads.at[JOBS + 1])
    load_r1 = pltpu.make_async_copy(r1_in, r1_ref, loads.at[JOBS + 2])
    for load in load_up:
        load.start()
    load_all.start()
    load_r1.start()
    w_full[out_sum.own(0)] = wg_in[out_sum.own(0)]
    for job in range(JOBS):
        p_full[pair_sum.own(job)] = pg_in[pair_sum.own(job)]
    value[0, 0:1] = column_sum(dq_ref[...].astype(F32))
    value[0, 1:8] = jnp.broadcast_to(column_sum(dv_ref[...].astype(F32)), (7, dv_ref.shape[1]))
    greet_all()
    bias.start(0)
    for load in load_up:
        load.wait()
    advance((pair_sum, (3, 0, 1, 2), 3), (out_sum, 0, 3), (up_sum, (0, 1, 2, 3), 3))
    tail = pl.ds(last, WIDE)
    for at, grad in enumerate((dq_ref, dk_ref, dv_ref)):
        joint[:, at * WIDE : (at + 1) * WIDE] = grad[:, tail]
    load_all.wait()
    projection_grads(all_ref, joint, last_low)
    advance((last_sum, (0, 1, 2, 3), 0))
    grads = ((dq_ref, wq_ref), (dk_ref, wk_ref), (dv_ref, wv_ref))

    def part_of(starts, count):
        total = None
        for grad, weight in grads:
            pieces = [grad[pl.ds(pl.multiple_of(at, size), count)] for at in starts]
            x = pieces[0] if len(pieces) == 1 else jnp.concatenate(pieces, 0)
            term = mm(x, weight[...], 1, 1)
            total = term if total is None else total + term
        return total

    def chunk_rows(j):
        return pl.ds(pl.multiple_of(j * size, size), size)

    def far(j):
        part = part_of((2 * rows_here + j * size, 3 * rows_here + j * size), size)
        pending[chunk_rows(j)] = part[:size]
        reduce.post(PAIR, j, part[size:])

        @pl.when(j > 0)
        def _():
            reduce.forward_pair(j - 1, pending[chunk_rows(j - 1)])

    repeat(CHUNKS, far)
    reduce.forward_pair(CHUNKS - 1, pending[chunk_rows(CHUNKS - 1)])
    bias.finish(0)
    bias.start(1)
    advance((pair_sum, (3, 0, 1, 2), 4), (last_sum, (0, 1, 2, 3), 1), (up_sum, (3, 0), 4))

    def near(i):
        part = part_of((rows_here + i * 2 * size,), 2 * size)
        reduce.post(NEAR, 2 * i, part[:size])
        reduce.post(NEAR, 2 * i + 1, part[size:])

    repeat(2, near)

    def own(i):
        mine[pl.ds(pl.multiple_of(i * 2 * size, 2 * size), 2 * size)] = part_of((i * 2 * size,), 2 * size)

    repeat(2, own)

    def finish(j):
        rows = chunk_rows(j)
        x_ref[rows] = (r1_ref[rows] + reduce.total(j, mine[rows])).astype(BF)

    advance((pair_sum, (3, 0, 1, 2), 5), (up_sum, (1, 2), 4))
    load_r1.wait()
    finish(0)
    bias.finish(1)
    bias.start(2)
    advance((last_sum, (0, 1, 2, 3), 2), (up_sum, (3, 0), 5), (out_sum, 0, 4))
    finish(1)
    advance((last_sum, (0, 1, 2, 3), 3), (up_sum, (1, 2), 5), (out_sum, 0, 5))
    finish(2)
    advance((last_sum, (0, 1, 2, 3), 4))
    finish(3)
    bias.finish(2)
    bias_ref[...] = value[3]
    advance((last_sum, (0, 1, 2, 3), 5), (up_sum, (0, 1, 2, 3), 6))
    save_up.start()
    advance((pair_sum, (3, 0, 1, 2), 6), (out_sum, 0, 6))
    wg_ref[...] = w_full[...]
    pg_ref[...] = p_full[...]
    advance((last_sum, (0, 1, 2, 3), 6))
    last_ref[...] = last_full[...]
    reduce.drain()
    save_up.wait()


def input_back(dq, dk, dv, wq, wk, wv, gathered, resid_grad, out_grad, pair_grad, up):
    rows, width = resid_grad.shape
    cols = dq.shape[1]
    anywhere = pl.BlockSpec(memory_space=pl.ANY)
    return pl.pallas_call(
        input_back_kernel,
        in_specs=[WHOLE] * 6 + [anywhere] * 2 + [WHOLE] * 2 + [anywhere],
        out_specs=[WHOLE] * 5 + [pl.BlockSpec(memory_space=pl.ANY)],
        out_shape=[
            shaped(rows, width),
            shaped(*out_grad.shape),
            shaped(*pair_grad.shape),
            shaped(*pair_grad.shape),
            shaped(8, cols, dtype=F32),
            shaped(*up.shape),
        ],
        scratch_shapes=[
            pltpu.VMEM((3, rows, width), BF),
            pltpu.VMEM((3, rows, width), BF),
            pltpu.VMEM((rows, width), F32),
            pltpu.VMEM((rows, width), F32),
            *transfer_sems(),
            pltpu.VMEM(up.shape, BF),
            pltpu.SemaphoreType.DMA((JOBS + 3,)),
            *spread_sems(KINDS),
            *spread_sems("H"),
            *spread_sems(KINDS),
            pltpu.VMEM(gathered.shape, BF),
            pltpu.VMEM((rows, width), F32),
            pltpu.VMEM((dq.shape[0], 3 * WIDE), BF),
            pltpu.VMEM(out_grad.shape, BF),
            *[pltpu.VMEM(pair_grad.shape, BF)] * 3,
            spread_land(pair_grad.shape, KINDS),
            *spread_sems(KINDS),
            *hop_scratch(3, 8, cols),
        ],
        name="input_back",
        compiler_params=comm_params(4),
    )(dq, dk, dv, wq, wk, wv, gathered, resid_grad, out_grad, pair_grad, up)


def widen_kernel(up_ref, down_ref, out_ref, pair_ref, last_ref, upw, downw, outw, qw, kw, vw):
    upw[...] = up_ref[...].astype(F32)
    downw[...] = down_ref[...].astype(F32)
    outw[...] = out_ref[...].astype(F32)
    for at, wide in enumerate((qw, kw, vw)):
        cols = slice(at * WIDE, (at + 1) * WIDE)
        wide[:, :WIDE] = pair_ref[:, cols].astype(F32)
        wide[:, WIDE:] = last_ref[:, cols].astype(F32)


def widen_grads(*grads):
    steps = 4
    shapes = [g.shape for g in grads[:3]] + [(grads[3].shape[0], 2 * WIDE)] * 3

    def tiles(shape):
        return pl.BlockSpec((shape[0] // steps, shape[1]), lambda i: (i, 0))

    return pl.pallas_call(
        widen_kernel,
        grid=(steps,),
        in_specs=[tiles(g.shape) for g in grads],
        out_specs=[tiles(shape) for shape in shapes],
        out_shape=[shaped(*shape, dtype=F32) for shape in shapes],
        name="widen_grads",
    )(*grads)


def per_device(
    tokens, lengths, query_weight, query_bias, key_weight, value_weight, value_bias, out_weight,
    out_bias, first_gain, first_shift, up_weight, up_bias, down_weight, down_bias, second_gain,
    second_shift, output_grad,
):
    pairs = query_weight.shape[1] // WIDE
    if (lax.axis_size("dp"), lax.axis_size("mp"), lengths.shape[1], pairs) != (8, 4, 1, 2):
        return per_device_general(
            tokens, lengths, query_weight, query_bias, key_weight, value_weight, value_bias,
            out_weight, out_bias, first_gain, first_shift, up_weight, up_bias, down_weight,
            down_bias, second_gain, second_shift, output_grad,
        )
    q, k, v, gathered, expon, attended, inverse, normed, inv_std, hidden = attend(
        lengths, tokens, query_weight, key_weight, value_weight, query_bias, value_bias, out_weight,
        out_bias, first_gain, first_shift,
    )
    layer_out, branch, resid_grad, up_grad, down_grad, small = feed_forward(
        hidden, normed, inv_std, output_grad, up_weight, up_bias, down_weight,
        first_gain, first_shift, down_bias, second_gain, second_shift,
    )
    dq, dk, dv, out_grad, pair_grad, small, up_grad, down_grad = attend_back(
        branch, out_weight, expon, inverse, q, k, v, attended, small, up_grad, down_grad, gathered
    )
    tokens_grad, out_grad, pair_grad, last_grad, bias_grads, up_grad = input_back(
        dq, dk, dv, query_weight, key_weight, value_weight, gathered, resid_grad, out_grad, pair_grad,
        up_grad,
    )

    up_grad, down_grad, out_grad, query_grad, key_grad, value_grad = widen_grads(
        up_grad, down_grad, out_grad, pair_grad, last_grad
    )
    return (
        layer_out,
        tokens_grad,
        query_grad,
        bias_grads[0],
        key_grad,
        value_grad,
        bias_grads[1],
        out_grad,
        small[5],
        small[3],
        small[4],
        up_grad,
        small[6],
        down_grad,
        small[2],
        small[0],
        small[1],
    )


def solution(mesh):
    placed = (
        P(("dp", "mp"), None),
        P("dp", None),
        P(None, "mp"),
        P("mp"),
        P(None, "mp"),
        P(None, "mp"),
        P("mp"),
        P("mp", None),
        P(),
        P(),
        P(),
        P(None, "mp"),
        P("mp"),
        P("mp", None),
        P(),
        P(),
        P(),
        P(("dp", "mp"), None),
    )
    return jax.shard_map(
        per_device,
        mesh=mesh,
        in_specs=placed,
        out_specs=(
            P(("dp", "mp"), None),
            P(("dp", "mp"), None),
            P(None, "mp"),
            P("mp"),
            P(None, "mp"),
            P(None, "mp"),
            P("mp"),
            P("mp", None),
            P(),
            P(),
            P(),
            P(None, "mp"),
            P("mp"),
            P("mp", None),
            P(),
            P(),
            P(),
        ),
        check_vma=False,
    )
```
